32 devices in a mesh: shard: 4 (over y, x), replica: 8 (over z, core).
Axes of the slice: x: 2, y: 2, z: 4, core: 2. Of those that a mesh axis runs over, the one named last changes fastest.
Arguments:
- tokens: bfloat16 [32, 256, 768], P(('shard', 'replica')), may hold values from -6 to 6
- cotangent: bfloat16 [32, 256, 768], P(('shard', 'replica')), may hold values from -6 to 6
- segments: int32 [32, 256], P(('shard', 'replica')), may hold values from 0 to 3, never falling along the last dimension, each value on 1 to 128 neighbouring positions
- padding: int32 [32, 256], P(('shard', 'replica')), may hold values 0 or 1
- routes: int32 [32, 256, 2], P(('shard', 'replica')), may hold values from 0 to 5, as said below
- priority: int32 [32, 256], P(('shard', 'replica')), may hold values from 0 to 255, each once within a row
- attn_gain: bfloat16 [768], P('shard'), may hold values from 0.099609375 to 1.8984375
- query_weight: bfloat16 [768, 768], P('shard'), may hold values from -0.21875 to 0.21875
- key_weight: bfloat16 [768, 768], P('shard'), may hold values from -0.21875 to 0.21875
- value_weight: bfloat16 [768, 768], P('shard'), may hold values from -0.21875 to 0.21875
- output_weight: bfloat16 [768, 768], P('shard'), may hold values from -1.75 to 1.75
- ffn_gain: bfloat16 [768], P('shard'), may hold values from 0.099609375 to 1.8984375
- router_weight: bfloat16 [768, 6], P('shard'), may hold values from -0.4375 to 0.4375
- expert_gate: bfloat16 [6, 768, 2048], P(None, 'shard'), may hold values from -0.21875 to 0.21875
- expert_up: bfloat16 [6, 768, 2048], P(None, 'shard'), may hold values from -0.21875 to 0.21875
- expert_down: bfloat16 [6, 768, 2048], P(None, 'shard'), may hold values from -0.25 to 0.25
- shared_gate: bfloat16 [768, 2048], P('shard'), may hold values from -0.21875 to 0.21875
- shared_up: bfloat16 [768, 2048], P('shard'), may hold values from -0.21875 to 0.21875
- shared_down: bfloat16 [768, 2048], P('shard'), may hold values from -0.25 to 0.25
Outputs:
- output: bfloat16 [32, 256, 768], P(('shard', 'replica'))
- input_grad: bfloat16 [32, 256, 768], P(('shard', 'replica'))
- attn_gain_grad: float32 [768], P('shard')
- query_grad: float32 [768, 768], P('shard')
- key_grad: float32 [768, 768], P('shard')
- value_grad: float32 [768, 768], P('shard')
- output_weight_grad: float32 [768, 768], P('shard')
- ffn_gain_grad: float32 [768], P('shard')
- router_grad: float32 [768, 6], P('shard')
- expert_gate_grad: float32 [6, 768, 2048], P(None, 'shard')
- expert_up_grad: float32 [6, 768, 2048], P(None, 'shard')
- expert_down_grad: float32 [6, 768, 2048], P(None, 'shard')
- shared_gate_grad: float32 [768, 2048], P('shard')
- shared_up_grad: float32 [768, 2048], P('shard')
- shared_down_grad: float32 [768, 2048], P('shard')
The draws below stay inside these ranges and needn't reach their ends.
Inputs may be any that keep to these rules, and one draw needn't show every extreme that they name: `segments`: segment numbers never fall along a sequence. `routes`: the 2 experts named for one token differ. `priority`: each sequence's row is a permutation.
All inputs are finite; a program needn't handle non-finite values. No bound on the sum of `padding` on one device may be relied on, other than what follows from the above.
Results may differ from the reference program's by a relative error of at most 0.019.
The reference program's roundings to bfloat16 on the way count: a program that leaves them out, or rounds other values in their place, can miss the bound.
Values may be sent and summed in bfloat16 or wider, within the bound.
A program may use at most 384 MiB of HBM per device.

```python
import math
import jax
import jax.numpy as jnp
import numpy as np
from jax import lax

D = 768
NH = 12
HD = 64
H = 2048
HS = 2048
EXPERTS = 6
TOPK = 2
DOCS = 4
LEN = 256
CAP = 96
SEQS = 32


def draw_routes(key, part):
    busy = jax.random.randint(jax.random.fold_in(key, 11), (SEQS, 1), 0, EXPERTS)
    roll = jax.random.randint(jax.random.fold_in(key, 12), (SEQS, LEN), 0, 40)
    others = (busy + 1 + jax.random.randint(jax.random.fold_in(key, 13), (SEQS, LEN), 0, EXPERTS - 1)) % EXPERTS
    first = jnp.where(roll < 17, busy, others)
    second = (first + 1 + jax.random.randint(jax.random.fold_in(key, 14), (SEQS, LEN), 0, EXPERTS - 1)) % EXPERTS
    return jnp.stack([first, second], axis=-1).astype(jnp.int32)


def touch_ends(entries, rng, low, largest):
    spot = [jax.random.randint(jax.random.fold_in(rng, axis), (), 0, length) for axis, length in enumerate(entries.shape)]
    main_axis = entries.shape.index(max(entries.shape))
    neighbour = spot[:main_axis] + [(spot[main_axis] + 1) % entries.shape[main_axis]] + spot[main_axis + 1:]
    return entries.at[tuple(spot)].set(low).at[tuple(neighbour)].set(largest)


def spiked(entries, stream_key, source, target, parts, factor):
    owner, partner = [(jnp.arange(entries.shape[position]) // (entries.shape[position] // parts)).reshape([-1 if axis == position else 1 for axis in range(entries.ndim)]) for position in (source, target)]
    chosen = jax.random.permutation(stream_key, parts)[partner]
    strong = (owner == chosen) | (owner == (partner + parts // 2) % parts)
    return jnp.where(strong, factor * entries, entries)


def block_scale(stream_key, shape, cuts, least, high):
    gain = 1.0
    for position, parts in cuts:
        draws = jax.random.uniform(jax.random.fold_in(jax.random.fold_in(stream_key, 6), position), (parts,), jnp.float32, least / len(cuts), high / len(cuts))
        gain = gain * jnp.repeat(jnp.exp(draws), shape[position] // parts).reshape((-1,) + (1,) * (len(shape) - 1 - position))
    return gain


def profile(count, total, most, slope):
    weights = [(1 << 20) // math.isqrt(grade ** slope) + 1 for grade in range(2, count + 1)]
    surplus, counts = total - most - (count - 1), [1] * (count - 1)
    while surplus > 0:
        candidates = [i for i in range(count - 1) if counts[i] < most]
        whole, left = sum([weights[i] for i in candidates]), surplus
        for i in candidates:
            extra = min(most - counts[i], max(1, left * weights[i] // whole), surplus)
            counts[i] = counts[i] + extra
            surplus = surplus - extra
    return np.array([most] + counts)


def ragged_sizes(stream_key, amount, total, limit, slope):
    if amount == 2:
        one = jax.random.randint(stream_key, (), max(1, total - limit), min(limit, total - 1) + 1)
        return jnp.stack([one, total - one])
    lengths = jnp.asarray(profile(amount, total, limit, slope), jnp.int32)
    twos = (amount - 1) // 2
    donor, receiver = lengths[1:1 + 2 * twos:2], lengths[2:2 + 2 * twos:2]
    slack = jnp.minimum(donor - 1, limit - receiver)
    shifted = jax.random.randint(jax.random.fold_in(stream_key, 1), (twos,), 0, 1 << 20) % (slack + 1)
    lengths = lengths.at[1:1 + 2 * twos:2].set(donor - shifted).at[2:2 + 2 * twos:2].set(receiver + shifted)
    return lengths[jax.random.permutation(jax.random.fold_in(stream_key, 2), amount)]


def normal_values(own_key, extent, spread, limit, split=(), kind=jnp.bfloat16):
    factor_of = block_scale(own_key, extent, split, -0.22, 0.18) if split else 1.0
    entries = jax.random.normal(own_key, extent, jnp.float32) * spread * factor_of
    return jnp.minimum(jnp.maximum(entries, -limit), limit).astype(kind)


def noise_with(key, shape, scale, limit, pieces, heavy, kind=jnp.bfloat16):
    values = scale * jax.random.normal(key, shape, jnp.float32)
    if pieces:
        values = values * block_scale(key, shape, pieces, -0.22, 0.18)
    return jnp.clip(spiked(values, jax.random.fold_in(key, 3), *heavy), -limit, limit).astype(kind)


def setup_inputs(seed: int = 0) -> dict:
    arg_keys = jax.random.split(jax.random.key(seed), 20)
    tokens = normal_values(arg_keys[0], (SEQS, LEN, D), 1.0, 6.0, ((0, 32),))
    cotangent = noise_with(arg_keys[1], (SEQS, LEN, D), 1.0, 6.0, ((0, 32),), (0, 2, 32, 2.75))
    segments = jax.vmap(lambda own: jnp.searchsorted(jnp.cumsum(ragged_sizes(own, DOCS, LEN, LEN // 2, 0)), jnp.arange(LEN), side="right"))(jax.random.split(arg_keys[2], SEQS)).reshape((SEQS, LEN)).astype(jnp.int32)
    padding = touch_ends((jax.random.randint(arg_keys[3], (SEQS, LEN), 0, 8) < 7).astype(jnp.int32), jax.random.fold_in(arg_keys[3], 1), 0, 1)
    routes = draw_routes(jax.random.fold_in(arg_keys[19], 71), 0)
    priority = jax.vmap(lambda own: jax.random.permutation(own, LEN))(jax.random.split(arg_keys[5], SEQS)).reshape((SEQS, LEN)).astype(jnp.int32)
    attn_gain = jnp.clip(1.0 + 0.18 * jax.random.normal(arg_keys[6], (D,), jnp.float32), 0.099609375, 1.8984375).astype(jnp.bfloat16)
    query_weight = normal_values(arg_keys[7], (D, D), D ** -0.5, 0.21875, ((0, 4),))
    key_weight = normal_values(arg_keys[8], (D, D), D ** -0.5, 0.21875, ((0, 4),))
    value_weight = normal_values(arg_keys[9], (D, D), D ** -0.5, 0.21875, ((0, 4),))
    output_weight = normal_values(arg_keys[10], (D, D), (D // 64) ** -0.5, 1.75, ((0, 4),))
    ffn_gain = jnp.clip(1.0 + 0.18 * jax.random.normal(arg_keys[11], (D,), jnp.float32), 0.099609375, 1.8984375).astype(jnp.bfloat16)
    router_weight = normal_values(arg_keys[12], (D, EXPERTS), (D // 4) ** -0.5, 0.4375, ((0, 4),))
    expert_gate = normal_values(arg_keys[13], (EXPERTS, D, H), D ** -0.5, 0.21875, ((1, 4),))
    expert_up = normal_values(arg_keys[14], (EXPERTS, D, H), D ** -0.5, 0.21875, ((1, 4),))
    expert_down = normal_values(arg_keys[15], (EXPERTS, D, H), (H // 4) ** -0.5, 0.25, ((1, 4),))
    shared_gate = normal_values(arg_keys[16], (D, HS), D ** -0.5, 0.21875, ((0, 4),))
    shared_up = normal_values(arg_keys[17], (D, HS), D ** -0.5, 0.21875, ((0, 4),))
    shared_down = normal_values(arg_keys[18], (D, HS), (HS // 4) ** -0.5, 0.25, ((0, 4),))
    return dict(tokens=tokens, cotangent=cotangent, segments=segments, padding=padding, routes=routes, priority=priority, attn_gain=attn_gain, query_weight=query_weight, key_weight=key_weight, value_weight=value_weight, output_weight=output_weight, ffn_gain=ffn_gain, router_weight=router_weight, expert_gate=expert_gate, expert_up=expert_up, expert_down=expert_down, shared_gate=shared_gate, shared_up=shared_up, shared_down=shared_down)


highest = lax.Precision.HIGHEST
EPSILON = 1e-06
NEGATIVE = -1e+30

@jax.custom_vjp
def low(v):
    return lax.optimization_barrier(v.astype(jnp.bfloat16)).astype(jnp.float32)

@jax.custom_vjp
def low_back(v):
    return v

def low_keep(v):
    return (low(v), None)

def low_pass(kept, grad):
    return (grad,)

def back_keep(v):
    return (v, None)

def back_low(kept, grad):
    return (low(grad),)
low.defvjp(low_keep, low_pass)
low_back.defvjp(back_keep, back_low)

def rotate_half(values):
    half_size = values.shape[-1] // 2
    return jnp.concatenate([-values[..., half_size:], values[..., :half_size]], axis=-1)

def rotary_tables(length, head_dim):
    positions = jnp.arange(length, dtype=jnp.float32)
    frequency = jnp.exp(jnp.arange(head_dim // 2, dtype=jnp.float32) * (-2.0 * math.log(10000.0) / head_dim))
    angles = positions[:, None] * frequency[None, :]
    angles = jnp.concatenate([angles, angles], axis=1)
    return (jnp.cos(angles), jnp.sin(angles))

def apply_rotary(values, cosine, sine_table):
    return values * cosine[:, None, :] + rotate_half(values) * sine_table[:, None, :]

def attention_mask(segments, padding):
    places = jnp.arange(segments.shape[0])
    causal = places[None, :] <= places[:, None]
    shared_doc = segments[:, None] == segments[None, :]
    usable = (padding[None, :] == 1) | (places[None, :] == places[:, None])
    return causal & shared_doc & usable

def norm_factor(values):
    return lax.rsqrt(lax.optimization_barrier(jnp.mean(values * values, axis=-1, keepdims=True)) + EPSILON)

def pair_slots(routes, padding, priority):
    length = routes.shape[0]
    pair_expert = routes.T.reshape(-1)
    pair_live = jnp.tile(padding, TOPK) == 1
    pair_key = (jnp.arange(TOPK, dtype=jnp.int32)[:, None] * length + priority[None, :]).reshape(-1)
    earlier = (pair_key[None, :] < pair_key[:, None]) & (pair_expert[None, :] == pair_expert[:, None]) & pair_live[None, :]
    place = lax.optimization_barrier(jnp.sum(earlier.astype(jnp.int32), axis=1))
    kept = pair_live & (place < CAP)
    return (pair_expert, place, kept)

def layer(weights, inputs, segments, padding, routes, priority):
    attn_gain, query_weight, key_weight, value_weight, output_weight, ffn_gain, router_weight, expert_gate, expert_up, expert_down, shared_gate, shared_up, shared_down = weights
    length = inputs.shape[0]
    normed_one = low(inputs * norm_factor(inputs) * attn_gain)
    cosine, sine_table = rotary_tables(length, HD)
    query_pre = low_back(jnp.dot(normed_one, query_weight, precision=highest)).reshape(length, NH, HD)
    key_pre = low_back(jnp.dot(normed_one, key_weight, precision=highest)).reshape(length, NH, HD)
    values = low(low_back(jnp.dot(normed_one, value_weight, precision=highest))).reshape(length, NH, HD)
    queries = low(apply_rotary(query_pre, cosine, sine_table))
    keys_rot = low(apply_rotary(key_pre, cosine, sine_table))
    scores = low_back(jnp.einsum('qhd,khd->hqk', queries, keys_rot, precision=highest) * HD ** (-0.5))
    scores = jnp.where(attention_mask(segments, padding)[None], scores, NEGATIVE)
    probs = low(jax.nn.softmax(scores, axis=-1))
    attended = jnp.einsum('hqk,khd->qhd', probs, values, precision=highest).reshape(length, NH * HD)
    attended = low(low_back(attended))
    middle = inputs + low_back(jnp.dot(attended, output_weight, precision=highest))
    normed_two = low(middle * norm_factor(middle) * ffn_gain)
    router = jax.nn.softmax(jnp.dot(normed_two, router_weight, precision=highest), axis=-1)
    pair_expert, place, kept = pair_slots(routes, padding, priority)
    expert_range = jnp.arange(EXPERTS, dtype=jnp.int32)
    dispatch = ((expert_range[:, None, None] == pair_expert[None, None, :]) & (jnp.arange(CAP, dtype=jnp.int32)[:, None][None] == place[None, None, :]) & kept[None, None, :]).astype(jnp.float32)
    pair_inputs = jnp.tile(normed_two, (TOPK, 1))
    expert_in = jnp.einsum('ecp,pd->ecd', dispatch, pair_inputs, precision=highest)
    gate_act = low_back(jnp.einsum('ecd,edh->ech', expert_in, expert_gate, precision=highest))
    up_act = low_back(jnp.einsum('ecd,edh->ech', expert_in, expert_up, precision=highest))
    hidden = low(jax.nn.silu(gate_act) * up_act)
    expert_out = low(low_back(jnp.einsum('ech,edh->ecd', hidden, expert_down, precision=highest)))
    onehot = (pair_expert[:, None] == expert_range[None, :]).astype(jnp.float32)
    pair_gate = lax.optimization_barrier(jnp.sum(jnp.tile(router, (TOPK, 1)) * onehot, axis=1))
    pair_rows = jnp.einsum('ecp,ecd->pd', dispatch, expert_out, precision=highest)
    mixture = lax.optimization_barrier(jnp.sum((pair_gate[:, None] * pair_rows).reshape(TOPK, length, -1), axis=0))
    shared_g = low_back(jnp.dot(normed_two, shared_gate, precision=highest))
    shared_u = low_back(jnp.dot(normed_two, shared_up, precision=highest))
    shared_hidden = low(jax.nn.silu(shared_g) * shared_u)
    shared_out = low_back(jnp.dot(shared_hidden, shared_down.T, precision=highest))
    return middle + mixture + shared_out

def add_arrays(first, second):
    return first + second

def reference(tokens, cotangent, segments, padding, routes, priority, attn_gain, query_weight, key_weight, value_weight, output_weight, ffn_gain, router_weight, expert_gate, expert_up, expert_down, shared_gate, shared_up, shared_down):
    params = tuple((weight.astype(jnp.float32) for weight in (attn_gain, query_weight, key_weight, value_weight, output_weight, ffn_gain, router_weight, expert_gate, expert_up, expert_down, shared_gate, shared_up, shared_down)))
    zero_grads = tuple((jnp.zeros_like(weight) for weight in params))

    def one_sequence(carry, items):
        seq_tokens, seq_cot, seq_segments, seq_padding, seq_routes, seq_priority = items

        def forward(weights, inputs):
            return layer(weights, inputs, seq_segments, seq_padding, seq_routes, seq_priority)
        result, pullback = jax.vjp(forward, params, seq_tokens.astype(jnp.float32))
        weight_grads, seq_input_grad = pullback(seq_cot.astype(jnp.float32))
        carry = jax.tree.map(add_arrays, carry, weight_grads)
        return (carry, (result.astype(jnp.bfloat16), seq_input_grad.astype(jnp.bfloat16)))
    totals, (outputs, input_grads) = lax.scan(one_sequence, zero_grads, (tokens, cotangent, segments, padding, routes, priority))
    return (outputs, input_grads, totals[0], totals[1], totals[2], totals[3], totals[4], totals[5], totals[6], totals[7], totals[8], totals[9], totals[10], totals[11], totals[12])
```

```python
import math

import jax
import jax.numpy as jnp
from jax import lax
from jax.sharding import Mesh, PartitionSpec as P

NH = 12
HD = 64
EXPERTS = 6
TOPK = 2
CAP = 96
EPSILON = 1e-06
NEGATIVE = -1e30
GROUPS = ((0, 1), (2, 3), (4, 5))

highest = lax.Precision.HIGHEST
f32 = jnp.float32
bf16 = jnp.bfloat16


def dot(spec, first, second):
    return jnp.einsum(spec, first, second, preferred_element_type=f32)


def rotate_half(values):
    half_size = values.shape[-1] // 2
    return jnp.concatenate([-values[..., half_size:], values[..., :half_size]], axis=-1)


def rotate_back(values):
    half_size = values.shape[-1] // 2
    return jnp.concatenate([values[..., half_size:], -values[..., :half_size]], axis=-1)


def rotary_tables(length, head_dim):
    positions = jnp.arange(length, dtype=f32)
    frequency = jnp.exp(
        jnp.arange(head_dim // 2, dtype=f32) * (-2.0 * math.log(10000.0) / head_dim)
    )
    angles = positions[:, None] * frequency[None, :]
    angles = jnp.concatenate([angles, angles], axis=1)
    return (jnp.cos(angles), jnp.sin(angles))


def attention_mask(segments, padding):
    places = jnp.arange(segments.shape[0])
    causal = places[None, :] <= places[:, None]
    shared_doc = segments[:, None] == segments[None, :]
    usable = (padding[None, :] == 1) | (places[None, :] == places[:, None])
    return causal & shared_doc & usable


def norm_factor(values):
    return lax.rsqrt(jnp.mean(values * values, axis=-1, keepdims=True) + EPSILON)


def norm_back(values, factor, norm_gain, gradient):
    scaled = gradient * norm_gain
    gain_grad = jnp.sum(gradient * values * factor, axis=0)
    input_part = factor * scaled - values * factor**3 * jnp.mean(
        scaled * values, axis=-1, keepdims=True
    )
    return (input_part, gain_grad)


def silu_parts(gate_act):
    sigmoid = jax.nn.sigmoid(gate_act)
    return (gate_act * sigmoid, sigmoid * (1.0 + gate_act * (1.0 - sigmoid)))


def pair_slots(routes, padding, priority):
    length = routes.shape[0]
    pair_expert = routes.T.reshape(-1)
    pair_live = jnp.tile(padding, TOPK) == 1
    pair_key = (jnp.arange(TOPK, dtype=jnp.int32)[:, None] * length + priority[None, :]).reshape(-1)
    earlier = (
        (pair_key[None, :] < pair_key[:, None])
        & (pair_expert[None, :] == pair_expert[:, None])
        & pair_live[None, :]
    )
    place = jnp.sum(earlier.astype(jnp.int32), axis=1)
    kept = pair_live & (place < CAP)
    return (pair_expert, place, kept)


def swap(values, axis, mask, size):
    return lax.ppermute(values, axis, [(i, i ^ mask) for i in range(size)])


def pick_index(values, index, axis=0):
    return lax.dynamic_index_in_dim(values, index, axis, keepdims=False)


def make_shards(n, qn):
    bits = qn.bit_length() - 1

    def place_blocks(own, blocks):
        out = jnp.zeros((n,) + blocks[0].shape, blocks[0].dtype)
        for m in range(n):
            out = lax.dynamic_update_index_in_dim(out, blocks[m], own ^ m, 0)
        return out

    def join_bit(bit, own, other, axis):
        first = jnp.where(bit == 0, own, other)
        second = jnp.where(bit == 0, other, own)
        return jnp.concatenate([first, second], axis=axis)

    def shards(
        tokens,
        cotangent,
        segments,
        padding,
        routes,
        priority,
        attn_gain,
        query_weight,
        key_weight,
        value_weight,
        output_weight,
        ffn_gain,
        router_weight,
        expert_gate,
        expert_up,
        expert_down,
        shared_gate,
        shared_up,
        shared_down,
    ):
        s = lax.axis_index("shard")
        q = lax.axis_index("plane")
        c = lax.axis_index("core")
        length, d = tokens.shape[1], tokens.shape[2]
        rows = query_weight.shape[0]
        hidden = expert_gate.shape[2]
        hb = hidden // (2 * n)
        score_scale = HD ** (-0.5)

        small = jnp.concatenate(
            [attn_gain[:, None], ffn_gain[:, None], router_weight], axis=1
        )
        small = jnp.pad(small, ((0, 0), (0, 256 - small.shape[1])))
        wide = jnp.concatenate(
            [query_weight, key_weight, value_weight, output_weight, small], axis=1
        )
        half = wide.shape[1] // 2
        mine = lax.dynamic_slice_in_dim(wide, c * half, half, 1)
        blocks = [mine] + [swap(mine, "shard", m, n) for m in range(1, n)]
        mine = place_blocks(s, blocks).reshape(d, half)
        other = swap(mine, "core", 1, 2)
        wide = join_bit(c, mine, other, 1)
        wqkv, wo = wide[:, : 3 * d], wide[:, 3 * d : 4 * d]
        gain_one = wide[:, 4 * d].astype(f32)
        gain_two = wide[:, 4 * d + 1].astype(f32)
        wr = wide[:, 4 * d + 2 : 4 * d + 2 + EXPERTS]

        def block_for(m):
            start = ((s ^ m) * 2 + c) * hb
            cut = lambda w: lax.dynamic_slice_in_dim(w, start, hb, w.ndim - 1)
            return [
                jnp.concatenate([cut(e), cut(w)[None]], axis=0)
                for e, w in (
                    (expert_gate, shared_gate),
                    (expert_up, shared_up),
                    (expert_down, shared_down),
                )
            ]

        own_blocks = block_for(0)
        sent = [block_for(m) for m in range(1, n)]
        moe_w = []
        for k in range(3):
            got = [own_blocks[k]] + [swap(sent[m - 1][k], "shard", m, n) for m in range(1, n)]
            full = jnp.zeros((EXPERTS + 1, n, rows, hb), bf16)
            for m in range(n):
                full = lax.dynamic_update_index_in_dim(full, got[m], s ^ m, 1)
            moe_w.append(full.reshape(EXPERTS + 1, d, hb))

        def plane_gather(values):
            near = jnp.stack([values] + [swap(values, "shard", m, n) for m in range(1, n)])
            return jnp.concatenate([near, swap(near, "core", 1, 2)], axis=0)

        def plane_sum(partial):
            low = partial.astype(bf16)
            pair = (partial[:n] + swap(low[n:], "core", 1, 2).astype(f32)).astype(bf16)
            total = pair[0].astype(f32)
            for m in range(1, n):
                total = total + swap(pair[m], "shard", m, n).astype(f32)
            return total

        grads_b = plane_gather(cotangent[0])

        inputs = tokens[0].astype(f32)
        factor_one = norm_factor(inputs)
        normed_one = (inputs * factor_one * gain_one).astype(bf16)
        projected = jnp.dot(normed_one, wqkv, preferred_element_type=f32)
        cosine, sine = rotary_tables(length, HD)
        heads = projected.reshape(length, 3, NH, HD)
        cos_b, sin_b = cosine[:, None, :], sine[:, None, :]
        queries = (heads[:, 0] * cos_b + rotate_half(heads[:, 0]) * sin_b).astype(bf16)
        keys_rot = (heads[:, 1] * cos_b + rotate_half(heads[:, 1]) * sin_b).astype(bf16)
        values = heads[:, 2].astype(bf16)
        allowed = attention_mask(segments[0], padding[0])
        logits = dot("qhd,khd->hqk", queries, keys_rot) * score_scale
        logits = jnp.where(allowed[None], logits, NEGATIVE)
        maxima = jnp.max(logits, axis=-1, keepdims=True)
        exponent = jnp.exp(logits - maxima)
        soft = exponent / jnp.sum(exponent, axis=-1, keepdims=True)
        probs = soft.astype(bf16)
        attended = dot("hqk,khd->qhd", probs, values).reshape(length, d).astype(bf16)
        middle = inputs + jnp.dot(attended, wo, preferred_element_type=f32)
        factor_two = norm_factor(middle)
        normed_two = (middle * factor_two * gain_two).astype(bf16)
        router = jax.nn.softmax(
            jnp.dot(normed_two, wr, preferred_element_type=f32), axis=-1
        )

        pair_expert, place, kept = pair_slots(routes[0], padding[0], priority[0])
        slot_total = EXPERTS * CAP
        slot_index = jnp.where(kept, pair_expert * CAP + place, -1).reshape(TOPK, length)
        slots = jnp.arange(slot_total, dtype=jnp.int32)
        hit = (slots[None, :, None] == slot_index[:, None, :]).any(axis=0)
        onehot = hit.astype(bf16)
        token_of = jnp.max(
            jnp.where(hit, jnp.arange(length, dtype=jnp.int32)[None, :], -1), axis=1
        )
        slot_expert = jnp.repeat(jnp.arange(EXPERTS), CAP)
        gate_of = jnp.sum(
            jnp.where(hit, jnp.repeat(router.T, CAP, axis=0), 0.0), axis=1
        )

        tokens_b = plane_gather(normed_two)
        token_of_b = plane_gather(token_of)
        gate_of_b = plane_gather(gate_of)
        group = 2 * n
        onehot_b = (
            token_of_b[:, :, None] == jnp.arange(length, dtype=jnp.int32)[None, None, :]
        ).astype(bf16)
        onehot_b = onehot_b.reshape(group, EXPERTS, CAP, length)
        gate_b = gate_of_b.reshape(group, EXPERTS, CAP, 1)

        def reduce_and_return(stack):
            k = stack.shape[0]
            piece = rows // qn
            x = stack.reshape((k, n) + (2,) * bits + (piece, hb))
            for b in range(bits):
                axis = 2 + (bits - 1 - b)
                bit = (q >> b) & 1
                keep = pick_index(x, bit, axis)
                send = pick_index(x, 1 - bit, axis).astype(bf16)
                x = keep + swap(send, "plane", 1 << b, qn).astype(f32)
            x = x.astype(bf16)
            own = pick_index(x, s, 1)
            got = [own] + [swap(pick_index(x, s ^ m, 1), "shard", m, n) for m in range(1, n)]
            x = jnp.stack(got)
            x = x[None]
            for b in reversed(range(bits)):
                bit = (q >> b) & 1
                other = swap(x, "plane", 1 << b, qn)
                lead = x.shape[0]
                pair = jnp.stack(
                    [jnp.where(bit == 0, x, other), jnp.where(bit == 0, other, x)], axis=1
                )
                x = pair.reshape((2 * lead,) + x.shape[1:])
            other = swap(x, "core", 1, 2)
            x = jnp.stack(
                [jnp.where(c == 0, x, other), jnp.where(c == 0, other, x)]
            )
            out = jnp.zeros((n,) + (2, qn, k, piece, hb), bf16)
            for m in range(n):
                out = lax.dynamic_update_index_in_dim(out, x[:, :, m], s ^ m, 0)
            return out.transpose(3, 2, 4, 0, 1, 5).reshape(k, rows, hidden).astype(f32)

        w_gate, w_up, w_down = moe_w
        tokens_f = tokens_b.reshape(group * length, d)
        grads_f = grads_b.reshape(group * length, d)
        shared_g = jnp.dot(tokens_f, w_gate[EXPERTS], preferred_element_type=f32)
        shared_u = jnp.dot(tokens_f, w_up[EXPERTS], preferred_element_type=f32)
        value, slope = silu_parts(shared_g)
        shared_hidden = (value * shared_u).astype(bf16)
        shared_q = jnp.dot(grads_f, w_down[EXPERTS], preferred_element_type=f32)
        shared_gd = (shared_q * shared_u * slope).astype(bf16)
        shared_ud = (shared_q * value).astype(bf16)
        shared_grads = jnp.stack(
            [
                dot("ld,lh->dh", tokens_f, shared_gd),
                dot("ld,lh->dh", tokens_f, shared_ud),
                dot("ld,lh->dh", grads_f, shared_hidden),
            ]
        )
        out_partial = dot("lh,dh->ld", shared_hidden, w_down[EXPERTS])
        two_partial = dot("lh,dh->ld", shared_gd, w_gate[EXPERTS]) + dot(
            "lh,dh->ld", shared_ud, w_up[EXPERTS]
        )
        out_partial = out_partial.reshape(group, length, d)
        two_partial = two_partial.reshape(group, length, d)
        shared_done = reduce_and_return(shared_grads)

        pick_parts = []
        expert_done = []
        for part in GROUPS:
            lo, hi = part[0], part[-1] + 1
            hot = onehot_b[:, lo:hi]
            x_in = jnp.einsum("bect,btd->ebcd", hot, tokens_b, preferred_element_type=bf16)
            g_in = jnp.einsum("bect,btd->ebcd", hot, grads_b, preferred_element_type=bf16)
            gate_e = jnp.swapaxes(gate_b[:, lo:hi], 0, 1)
            wg, wu, wd = w_gate[lo:hi], w_up[lo:hi], w_down[lo:hi]
            gate_act = dot("ebcd,edh->ebch", x_in, wg)
            up_act = dot("ebcd,edh->ebch", x_in, wu)
            value, slope = silu_parts(gate_act)
            hid = (value * up_act).astype(bf16)
            e_out = dot("ebch,edh->ebcd", hid, wd)
            pick_parts.append(jnp.sum(e_out * g_in.astype(f32), axis=-1))
            slot_grad = (gate_e * g_in.astype(f32)).astype(bf16)
            hid_grad = dot("ebcd,edh->ebch", slot_grad, wd)
            gate_d = (hid_grad * up_act * slope).astype(bf16)
            up_d = (hid_grad * value).astype(bf16)
            in_grad = dot("ebch,edh->ebcd", gate_d, wg) + dot("ebch,edh->ebcd", up_d, wu)
            weighted = (gate_e * e_out).astype(bf16)
            out_partial = out_partial + dot("bect,ebcd->btd", hot, weighted)
            two_partial = two_partial + dot("bect,ebcd->btd", hot, in_grad.astype(bf16))
            stack = jnp.concatenate(
                [
                    dot("ebcd,ebch->edh", x_in, gate_d),
                    dot("ebcd,ebch->edh", x_in, up_d),
                    dot("ebcd,ebch->edh", slot_grad, hid),
                ]
            )
            expert_done.append(reduce_and_return(stack))

        two_grad = plane_sum(two_partial)
        picks = jnp.concatenate(pick_parts, axis=0)
        picks = jnp.swapaxes(picks, 0, 1).reshape(group, slot_total)
        picks = picks[:n] + swap(picks[n:], "core", 1, 2)
        pick_slot = picks[0]
        for m in range(1, n):
            pick_slot = pick_slot + swap(picks[m], "shard", m, n)
        mixed = plane_sum(out_partial)
        output = (middle + mixed).astype(bf16)

        upstream = cotangent[0].astype(f32)
        pick_grad = jnp.sum(
            jnp.where(hit, pick_slot[:, None], 0.0).reshape(EXPERTS, CAP, length), axis=1
        ).T
        logit_grad = router * (pick_grad - jnp.sum(router * pick_grad, axis=1, keepdims=True))
        two_grad = two_grad + jnp.dot(logit_grad, wr.astype(f32).T, precision=highest)
        router_grad = jnp.dot(normed_two.astype(f32).T, logit_grad, precision=highest)
        middle_part, ffn_gain_grad = norm_back(middle, factor_two, gain_two, two_grad)
        middle_grad = middle_part + upstream

        branch_grad = middle_grad.astype(bf16)
        output_weight_grad = dot("ld,le->de", attended, branch_grad)
        attended_grad = (
            dot("le,de->ld", branch_grad, wo).astype(bf16).reshape(length, NH, HD)
        )
        prob_grad = dot("qhd,khd->hqk", attended_grad, values)
        row_inner = jnp.sum(soft * prob_grad, axis=-1, keepdims=True)
        score_grad = (soft * (prob_grad - row_inner)).astype(bf16)
        query_parts = dot("hqk,khd->qhd", score_grad, keys_rot) * score_scale
        key_parts = dot("hqk,qhd->khd", score_grad, queries) * score_scale
        value_parts = dot("hqk,qhd->khd", probs, attended_grad)
        query_pre = query_parts * cos_b + rotate_back(query_parts * sin_b)
        key_pre = key_parts * cos_b + rotate_back(key_parts * sin_b)
        joint_grad = jnp.concatenate(
            [v.reshape(length, d) for v in (query_pre, key_pre, value_parts)], axis=1
        ).astype(bf16)
        one_grad = dot("lf,df->ld", joint_grad, wqkv)
        joint_weight_grad = dot("ld,lf->df", normed_one, joint_grad)
        input_part, attn_gain_grad = norm_back(inputs, factor_one, gain_one, one_grad)
        input_grad = (middle_grad + input_part).astype(bf16)

        small_grad = jnp.concatenate(
            [attn_gain_grad[:, None], ffn_gain_grad[:, None], router_grad], axis=1
        )
        small_grad = jnp.pad(small_grad, ((0, 0), (0, 256 - small_grad.shape[1])))
        total = jnp.concatenate([joint_weight_grad, output_weight_grad, small_grad], axis=1)
        keep = lax.dynamic_slice_in_dim(total, c * half, half, 1)
        send = lax.dynamic_slice_in_dim(total, (1 - c) * half, half, 1).astype(bf16)
        total = keep + swap(send, "core", 1, 2).astype(f32)
        total = total.reshape(n, rows, half)
        own = pick_index(total, s)
        low = total.astype(bf16)
        for m in range(1, n):
            own = own + swap(pick_index(low, s ^ m), "shard", m, n).astype(f32)
        x = own.reshape((2,) * bits + (rows // qn, half))
        for b in range(bits):
            axis = bits - 1 - b
            bit = (q >> b) & 1
            keep = pick_index(x, bit, axis)
            send = pick_index(x, 1 - bit, axis).astype(bf16)
            x = keep + swap(send, "plane", 1 << b, qn).astype(f32)
        x = x.astype(bf16)[None]
        for b in reversed(range(bits)):
            bit = (q >> b) & 1
            other = swap(x, "plane", 1 << b, qn)
            pair = jnp.stack(
                [jnp.where(bit == 0, x, other), jnp.where(bit == 0, other, x)], axis=1
            )
            x = pair.reshape((2 * x.shape[0],) + x.shape[1:])
        x = x.reshape(rows, half)
        x = join_bit(c, x, swap(x, "core", 1, 2), 1).astype(f32)
        stacks = [[], [], []]
        for part, done in zip(GROUPS, expert_done):
            for k in range(3):
                stacks[k].append(done[k * len(part) : (k + 1) * len(part)])
        expert_grads = [jnp.concatenate(parts, axis=0) for parts in stacks]
        return (
            output[None],
            input_grad[None],
            x[:, 4 * d],
            x[:, :d],
            x[:, d : 2 * d],
            x[:, 2 * d : 3 * d],
            x[:, 3 * d : 4 * d],
            x[:, 4 * d + 1],
            x[:, 4 * d + 2 : 4 * d + 2 + EXPERTS],
            expert_grads[0],
            expert_grads[1],
            expert_grads[2],
            shared_done[0],
            shared_done[1],
            shared_done[2],
        )

    return shards


def solution(mesh):
    n, replicas = mesh.shape["shard"], mesh.shape["replica"]
    fine = Mesh(mesh.devices.reshape(n, replicas // 2, 2), ("shard", "plane", "core"))
    every = ("shard", "plane", "core")
    in_specs = (
        P(every, None, None),
        P(every, None, None),
        P(every, None),
        P(every, None),
        P(every, None, None),
        P(every, None),
        P("shard"),
        P("shard", None),
        P("shard", None),
        P("shard", None),
        P("shard", None),
        P("shard"),
        P("shard", None),
        P(None, "shard", None),
        P(None, "shard", None),
        P(None, "shard", None),
        P("shard", None),
        P("shard", None),
        P("shard", None),
    )
    out_specs = (
        P(every, None, None),
        P(every, None, None),
        P("shard"),
        P("shard", None),
        P("shard", None),
        P("shard", None),
        P("shard", None),
        P("shard"),
        P("shard", None),
        P(None, "shard", None),
        P(None, "shard", None),
        P(None, "shard", None),
        P("shard", None),
        P("shard", None),
        P("shard", None),
    )
    return jax.shard_map(
        make_shards(n, replicas // 2),
        mesh=fine,
        in_specs=in_specs,
        out_specs=out_specs,
        check_vma=False,
    )
```

```python
import functools
import math

import jax
import jax.numpy as jnp
from jax import lax
from jax.experimental import pallas as pl
from jax.experimental.pallas import tpu as pltpu
from jax.sharding import Mesh, PartitionSpec as P

NH = 12
HD = 64
EXPERTS = 6
TOPK = 2
CAP = 96
EPSILON = 1e-06
NEGATIVE = -1e30
GROUPS = ((0, 1), (2, 3), (4, 5))
MOE_CALLS = ((0, 3), (3, 7))

highest = lax.Precision.HIGHEST
f32 = jnp.float32
bf16 = jnp.bfloat16


def dot(spec, first, second):
    return jnp.einsum(spec, first, second, preferred_element_type=f32)


def rotate_half(values):
    half_size = values.shape[-1] // 2
    return jnp.concatenate([-values[..., half_size:], values[..., :half_size]], axis=-1)


def rotate_back(values):
    half_size = values.shape[-1] // 2
    return jnp.concatenate([values[..., half_size:], -values[..., :half_size]], axis=-1)


def rotary_tables(length, head_dim):
    positions = jnp.arange(length, dtype=f32)
    frequency = jnp.exp(
        jnp.arange(head_dim // 2, dtype=f32) * (-2.0 * math.log(10000.0) / head_dim)
    )
    angles = positions[:, None] * frequency[None, :]
    angles = jnp.concatenate([angles, angles], axis=1)
    return (jnp.cos(angles), jnp.sin(angles))


def attention_mask(segments, padding):
    places = jnp.arange(segments.shape[0])
    causal = places[None, :] <= places[:, None]
    shared_doc = segments[:, None] == segments[None, :]
    usable = (padding[None, :] == 1) | (places[None, :] == places[:, None])
    return causal & shared_doc & usable


def norm_factor(values):
    return lax.rsqrt(jnp.mean(values * values, axis=-1, keepdims=True) + EPSILON)


def norm_back(values, factor, norm_gain, gradient):
    scaled = gradient * norm_gain
    gain_grad = jnp.sum(gradient * values * factor, axis=0)
    input_part = factor * scaled - values * factor**3 * jnp.mean(
        scaled * values, axis=-1, keepdims=True
    )
    return (input_part, gain_grad)


def silu_parts(gate_act):
    sigmoid = jax.nn.sigmoid(gate_act)
    return (gate_act * sigmoid, sigmoid * (1.0 + gate_act * (1.0 - sigmoid)))


def pair_slots(routes, padding, priority):
    length = routes.shape[0]
    pair_expert = routes.T.reshape(-1)
    pair_live = jnp.tile(padding, TOPK) == 1
    pair_key = (jnp.arange(TOPK, dtype=jnp.int32)[:, None] * length + priority[None, :]).reshape(-1)
    earlier = (
        (pair_key[None, :] < pair_key[:, None])
        & (pair_expert[None, :] == pair_expert[:, None])
        & pair_live[None, :]
    )
    place = jnp.sum(earlier.astype(jnp.int32), axis=1)
    kept = pair_live & (place < CAP)
    return (pair_expert, place, kept)


def swap(values, axis, mask, size):
    return lax.ppermute(values, axis, [(i, i ^ mask) for i in range(size)])


def pick_index(values, index, axis=0):
    return lax.dynamic_index_in_dim(values, index, axis, keepdims=False)


def mm(first, second, contract):
    return lax.dot_general(
        first, second, (contract, ((), ())), preferred_element_type=f32
    )


NN = ((1,), (0,))
NT = ((1,), (1,))
TN = ((0,), (0,))


def moe_kernel(
    lo,
    hi,
    n,
    qn,
    length,
    has_prev,
    where_ref,
    tok_ref,
    gate_ref,
    x_ref,
    g_ref,
    wg_ref,
    wu_ref,
    wd_ref,
    *rest,
):
    if has_prev:
        prev_y, prev_t, *rest = rest
    grads_ref, pick_ref, y_ref, t_ref, acc_y, acc_t, xs, gs, sg, dw = rest
    step = pl.program_id(0)
    expert = step + lo
    group = 2 * n
    d = x_ref.shape[1]
    hb = wg_ref.shape[2]
    piece = d // (n * qn)
    s, q = where_ref[0], where_ref[1]

    @pl.when(step == 0)
    def _():
        acc_y[...] = jnp.zeros_like(acc_y)
        acc_t[...] = jnp.zeros_like(acc_t)

    def branch(x, g, gs_rows, wg, wu, wd):
        gate_act = mm(x, wg, NN)
        up_act = mm(x, wu, NN)
        sigmoid = 1.0 / (1.0 + jnp.exp(-gate_act))
        value = gate_act * sigmoid
        slope = sigmoid * (1.0 + gate_act * (1.0 - sigmoid))
        hid = (value * up_act).astype(bf16)
        hid_grad = mm(gs_rows, wd, NN)
        gate_d = (hid_grad * up_act * slope).astype(bf16)
        up_d = (hid_grad * value).astype(bf16)
        return hid, gate_d, up_d

    if lo < EXPERTS:

        @pl.when(expert < EXPERTS)
        def _():
            lanes = lax.broadcasted_iota(jnp.int32, (CAP, length), 1)

            def gather(b, carry):
                slot = pl.ds(pl.multiple_of(b * CAP, 16), CAP)
                seq = pl.ds(pl.multiple_of(b * length, length), length)
                hot = (tok_ref[0, slot, :] == lanes).astype(bf16)
                xs[slot, :] = mm(hot, x_ref[seq, :], NN).astype(bf16)
                g_rows = mm(hot, g_ref[seq, :], NN)
                gs[slot, :] = g_rows.astype(bf16)
                sg[slot, :] = (g_rows * gate_ref[0, slot, :]).astype(bf16)
                return carry

            lax.fori_loop(0, group, gather, 0)
            wg, wu, wd = wg_ref[0], wu_ref[0], wd_ref[0]
            x, slot_grad = xs[...], sg[...]
            hid, gate_d, up_d = branch(x, None, slot_grad, wg, wu, wd)
            dw[0] = mm(x, gate_d, TN)
            dw[1] = mm(x, up_d, TN)
            dw[2] = mm(slot_grad, hid, TN)
            e_out = mm(hid, wd, NT)
            pick_ref[0] = jnp.sum(e_out * gs[...].astype(f32), axis=1, keepdims=True)
            gs[...] = (e_out * gate_ref[0]).astype(bf16)
            xs[...] = (mm(gate_d, wg, NT) + mm(up_d, wu, NT)).astype(bf16)

            def scatter(b, carry):
                slot = pl.ds(pl.multiple_of(b * CAP, 16), CAP)
                seq = pl.ds(pl.multiple_of(b * length, length), length)
                hot = (tok_ref[0, slot, :] == lanes).astype(bf16)
                acc_y[seq, :] += mm(hot, gs[slot, :], TN)
                acc_t[seq, :] += mm(hot, xs[slot, :], TN)
                return carry

            lax.fori_loop(0, group, scatter, 0)

    if hi > EXPERTS:

        @pl.when(expert == EXPERTS)
        def _():
            pick_ref[0] = jnp.zeros_like(pick_ref[0])
            dw[...] = jnp.zeros_like(dw)
            wg, wu, wd = wg_ref[0], wu_ref[0], wd_ref[0]

            def rows_step(i, carry):
                rows = pl.ds(pl.multiple_of(i * 2 * length, 2 * length), 2 * length)
                x, g = x_ref[rows, :], g_ref[rows, :]
                hid, gate_d, up_d = branch(x, None, g, wg, wu, wd)
                dw[0] += mm(x, gate_d, TN)
                dw[1] += mm(x, up_d, TN)
                dw[2] += mm(g, hid, TN)
                acc_y[rows, :] += mm(hid, wd, NT)
                acc_t[rows, :] += mm(gate_d, wg, NT) + mm(up_d, wu, NT)
                return carry

            lax.fori_loop(0, n, rows_step, 0)

    for j in range(qn):
        for m in range(n):
            start = pl.multiple_of(((s ^ m) * qn + (q ^ reverse_bits(j, qn))) * piece, 16)
            for k in range(3):
                grads_ref[0, j, m, k] = dw[k, pl.ds(start, piece), :].astype(bf16)

    @pl.when(step == hi - lo - 1)
    def _():
        if has_prev:
            y_ref[...] = (acc_y[...] + prev_y[...].astype(f32)).astype(bf16)
            t_ref[...] = (acc_t[...] + prev_t[...].astype(f32)).astype(bf16)
        else:
            y_ref[...] = acc_y[...].astype(bf16)
            t_ref[...] = acc_t[...].astype(bf16)


def moe_call(lo, hi, n, qn, length, where, tok, gate, x, g, weights, prev):
    d = x.shape[1]
    hb = weights[0].shape[2]
    rows = x.shape[0]
    slots = tok.shape[1]
    count = hi - lo
    piece = d // (n * qn)
    once = pl.Buffered(1)
    last = EXPERTS - 1
    per_expert = lambda e, *_: (jnp.minimum(e + lo, last), 0, 0)
    whole = pl.BlockSpec((rows, d), lambda e, *_: (0, 0), pipeline_mode=once)
    weight = pl.BlockSpec((1, d, hb), lambda e, *_: (e + lo, 0, 0))
    column = pl.BlockSpec((1, slots, 1), per_expert)
    in_specs = [column, column, whole, whole, weight, weight, weight]
    operands = [tok, gate, x, g, *weights]
    if prev is not None:
        in_specs += [whole, whole]
        operands += list(prev)
    return pl.pallas_call(
        functools.partial(moe_kernel, lo, hi, n, qn, length, prev is not None),
        grid_spec=pltpu.PrefetchScalarGridSpec(
            num_scalar_prefetch=1,
            grid=(count,),
            in_specs=in_specs,
            out_specs=[
                pl.BlockSpec((1, qn, n, 3, piece, hb), lambda e, *_: (e, 0, 0, 0, 0, 0)),
                pl.BlockSpec((1, slots, 1), lambda e, *_: (e, 0, 0)),
                whole,
                whole,
            ],
            scratch_shapes=[
                pltpu.VMEM((rows, d), f32),
                pltpu.VMEM((rows, d), f32),
                pltpu.VMEM((slots, d), bf16),
                pltpu.VMEM((slots, d), bf16),
                pltpu.VMEM((slots, d), bf16),
                pltpu.VMEM((3, d, hb), f32),
            ],
        ),
        out_shape=[
            jax.ShapeDtypeStruct((count, qn, n, 3, piece, hb), bf16),
            jax.ShapeDtypeStruct((count, slots, 1), f32),
            jax.ShapeDtypeStruct((rows, d), bf16),
            jax.ShapeDtypeStruct((rows, d), bf16),
        ],
        compiler_params=pltpu.CompilerParams(vmem_limit_bytes=62 << 20),
        cost_estimate=pl.CostEstimate(
            flops=18 * count * slots * d * hb, bytes_accessed=30 << 20, transcendentals=0
        ),
        name="moe_%d_%d" % (lo, hi),
    )(where, *operands)


def reverse_bits(j, size):
    bits = size.bit_length() - 1
    return sum(((j >> b) & 1) << (bits - 1 - b) for b in range(bits))


def assemble_kernel(n, qn, has_prev, where_ref, own_ref, far_ref, *rest):
    outs = rest[3:] if has_prev else rest
    s, q, c = where_ref[0], where_ref[1], where_ref[2]
    piece, hb = own_ref.shape[4], own_ref.shape[5]
    for side, ref in enumerate((own_ref, far_ref)):
        for j in range(qn):
            for m in range(n):
                row = pl.multiple_of((q ^ reverse_bits(j, qn)) * piece, 8)
                column = pl.multiple_of(((s ^ m) * 2 + (c ^ side)) * hb, 128)
                for k in range(3):
                    outs[k][0, pl.ds(row, piece), pl.ds(column, hb)] = ref[
                        0, j, m, k
                    ].astype(f32)


def assemble(n, qn, where, own, far, index, count, prev):
    piece, hb = own.shape[3], own.shape[4]
    rows, hidden = piece * qn, hb * 2 * n
    spec = pl.BlockSpec((1, qn, n, 3, piece, hb), lambda i, *_: (0, 0, 0, 0, 0, 0))
    in_specs = [spec, spec]
    operands = [own[None], far[None]]
    aliases = {}
    if prev is not None:
        in_specs += [pl.BlockSpec(memory_space=pl.ANY)] * 3
        operands += list(prev)
        aliases = {3: 0, 4: 1, 5: 2}
    return pl.pallas_call(
        functools.partial(assemble_kernel, n, qn, prev is not None),
        grid_spec=pltpu.PrefetchScalarGridSpec(
            num_scalar_prefetch=1,
            grid=(1,),
            in_specs=in_specs,
            out_specs=[pl.BlockSpec((1, rows, hidden), lambda i, *_: (index, 0, 0))] * 3,
        ),
        out_shape=[jax.ShapeDtypeStruct((count, rows, hidden), f32)] * 3,
        input_output_aliases=aliases,
        cost_estimate=pl.CostEstimate(
            flops=0, bytes_accessed=18 * rows * hidden, transcendentals=0
        ),
        name="assemble",
    )(where, *operands)


def make_shards(n, qn):
    bits = qn.bit_length() - 1

    def place_blocks(own, blocks):
        out = jnp.zeros((n,) + blocks[0].shape, blocks[0].dtype)
        for m in range(n):
            out = lax.dynamic_update_index_in_dim(out, blocks[m], own ^ m, 0)
        return out

    def join_bit(bit, own, other, axis):
        first = jnp.where(bit == 0, own, other)
        second = jnp.where(bit == 0, other, own)
        return jnp.concatenate([first, second], axis=axis)

    def shards(
        tokens,
        cotangent,
        segments,
        padding,
        routes,
        priority,
        attn_gain,
        query_weight,
        key_weight,
        value_weight,
        output_weight,
        ffn_gain,
        router_weight,
        expert_gate,
        expert_up,
        expert_down,
        shared_gate,
        shared_up,
        shared_down,
    ):
        s = lax.axis_index("shard")
        q = lax.axis_index("plane")
        c = lax.axis_index("core")
        length, d = tokens.shape[1], tokens.shape[2]
        rows = query_weight.shape[0]
        hidden = expert_gate.shape[2]
        hb = hidden // (2 * n)
        score_scale = HD ** (-0.5)

        small = jnp.concatenate(
            [attn_gain[:, None], ffn_gain[:, None], router_weight], axis=1
        )
        small = jnp.pad(small, ((0, 0), (0, 256 - small.shape[1])))
        wide = jnp.concatenate(
            [query_weight, key_weight, value_weight, output_weight, small], axis=1
        )
        half = wide.shape[1] // 2
        mine = lax.dynamic_slice_in_dim(wide, c * half, half, 1)
        blocks = [mine] + [swap(mine, "shard", m, n) for m in range(1, n)]
        mine = place_blocks(s, blocks).reshape(d, half)
        other = swap(mine, "core", 1, 2)
        wide = join_bit(c, mine, other, 1)
        wqkv, wo = wide[:, : 3 * d], wide[:, 3 * d : 4 * d]
        gain_one = wide[:, 4 * d].astype(f32)
        gain_two = wide[:, 4 * d + 1].astype(f32)
        wr = wide[:, 4 * d + 2 : 4 * d + 2 + EXPERTS]

        def block_for(m):
            start = ((s ^ m) * 2 + c) * hb
            cut = lambda w: lax.dynamic_slice_in_dim(w, start, hb, w.ndim - 1)
            return [
                jnp.concatenate([cut(e), cut(w)[None]], axis=0)
                for e, w in (
                    (expert_gate, shared_gate),
                    (expert_up, shared_up),
                    (expert_down, shared_down),
                )
            ]

        own_blocks = block_for(0)
        sent = [block_for(m) for m in range(1, n)]
        moe_w = []
        for k in range(3):
            got = [own_blocks[k]] + [swap(sent[m - 1][k], "shard", m, n) for m in range(1, n)]
            full = jnp.zeros((EXPERTS + 1, n, rows, hb), bf16)
            for m in range(n):
                full = lax.dynamic_update_index_in_dim(full, got[m], s ^ m, 1)
            moe_w.append(full.reshape(EXPERTS + 1, d, hb))

        def plane_gather(values):
            near = jnp.stack([values] + [swap(values, "shard", m, n) for m in range(1, n)])
            return jnp.concatenate([near, swap(near, "core", 1, 2)], axis=0)

        def plane_sum(partial):
            low = partial.astype(bf16)
            pair = (partial[:n] + swap(low[n:], "core", 1, 2).astype(f32)).astype(bf16)
            total = pair[0].astype(f32)
            for m in range(1, n):
                total = total + swap(pair[m], "shard", m, n).astype(f32)
            return total

        grads_b = plane_gather(cotangent[0])

        inputs = tokens[0].astype(f32)
        factor_one = norm_factor(inputs)
        normed_one = (inputs * factor_one * gain_one).astype(bf16)
        projected = jnp.dot(normed_one, wqkv, preferred_element_type=f32)
        cosine, sine = rotary_tables(length, HD)
        heads = projected.reshape(length, 3, NH, HD)
        cos_b, sin_b = cosine[:, None, :], sine[:, None, :]
        queries = (heads[:, 0] * cos_b + rotate_half(heads[:, 0]) * sin_b).astype(bf16)
        keys_rot = (heads[:, 1] * cos_b + rotate_half(heads[:, 1]) * sin_b).astype(bf16)
        values = heads[:, 2].astype(bf16)
        allowed = attention_mask(segments[0], padding[0])
        logits = dot("qhd,khd->hqk", queries, keys_rot) * score_scale
        logits = jnp.where(allowed[None], logits, NEGATIVE)
        maxima = jnp.max(logits, axis=-1, keepdims=True)
        exponent = jnp.exp(logits - maxima)
        soft = exponent / jnp.sum(exponent, axis=-1, keepdims=True)
        probs = soft.astype(bf16)
        attended = dot("hqk,khd->qhd", probs, values).reshape(length, d).astype(bf16)
        middle = inputs + jnp.dot(attended, wo, preferred_element_type=f32)
        factor_two = norm_factor(middle)
        normed_two = (middle * factor_two * gain_two).astype(bf16)
        router = jax.nn.softmax(
            jnp.dot(normed_two, wr, preferred_element_type=f32), axis=-1
        )

        pair_expert, place, kept = pair_slots(routes[0], padding[0], priority[0])
        slot_total = EXPERTS * CAP
        slot_index = jnp.where(kept, pair_expert * CAP + place, -1).reshape(TOPK, length)
        slots = jnp.arange(slot_total, dtype=jnp.int32)
        hit = (slots[None, :, None] == slot_index[:, None, :]).any(axis=0)
        onehot = hit.astype(bf16)
        token_of = jnp.max(
            jnp.where(hit, jnp.arange(length, dtype=jnp.int32)[None, :], -1), axis=1
        )
        slot_expert = jnp.repeat(jnp.arange(EXPERTS), CAP)
        gate_of = jnp.sum(
            jnp.where(hit, jnp.repeat(router.T, CAP, axis=0), 0.0), axis=1
        )

        tokens_b = plane_gather(normed_two)
        token_of_b = plane_gather(token_of)
        gate_of_b = plane_gather(gate_of)
        group = 2 * n
        onehot_b = (
            token_of_b[:, :, None] == jnp.arange(length, dtype=jnp.int32)[None, None, :]
        ).astype(bf16)
        onehot_b = onehot_b.reshape(group, EXPERTS, CAP, length)
        gate_b = gate_of_b.reshape(group, EXPERTS, CAP, 1)

        def reduce_and_return(stack):
            k = stack.shape[0]
            piece = rows // qn
            x = stack.reshape((k, n) + (2,) * bits + (piece, hb))
            for b in range(bits):
                axis = 2 + (bits - 1 - b)
                bit = (q >> b) & 1
                keep = pick_index(x, bit, axis)
                send = pick_index(x, 1 - bit, axis).astype(bf16)
                x = keep + swap(send, "plane", 1 << b, qn).astype(f32)
            x = x.astype(bf16)
            own = pick_index(x, s, 1)
            got = [own] + [swap(pick_index(x, s ^ m, 1), "shard", m, n) for m in range(1, n)]
            x = jnp.stack(got)
            x = x[None]
            for b in reversed(range(bits)):
                bit = (q >> b) & 1
                other = swap(x, "plane", 1 << b, qn)
                lead = x.shape[0]
                pair = jnp.stack(
                    [jnp.where(bit == 0, x, other), jnp.where(bit == 0, other, x)], axis=1
                )
                x = pair.reshape((2 * lead,) + x.shape[1:])
            other = swap(x, "core", 1, 2)
            x = jnp.stack(
                [jnp.where(c == 0, x, other), jnp.where(c == 0, other, x)]
            )
            out = jnp.zeros((n,) + (2, qn, k, piece, hb), bf16)
            for m in range(n):
                out = lax.dynamic_update_index_in_dim(out, x[:, :, m], s ^ m, 0)
            return out.transpose(3, 2, 4, 0, 1, 5).reshape(k, rows, hidden).astype(f32)

        def plain_moe():
            tokens_f = tokens_b.reshape(group * length, d)
            grads_f = grads_b.reshape(group * length, d)
            shared_g = jnp.dot(tokens_f, w_gate[EXPERTS], preferred_element_type=f32)
            shared_u = jnp.dot(tokens_f, w_up[EXPERTS], preferred_element_type=f32)
            value, slope = silu_parts(shared_g)
            shared_hidden = (value * shared_u).astype(bf16)
            shared_q = jnp.dot(grads_f, w_down[EXPERTS], preferred_element_type=f32)
            shared_gd = (shared_q * shared_u * slope).astype(bf16)
            shared_ud = (shared_q * value).astype(bf16)
            shared_grads = jnp.stack(
                [
                    dot("ld,lh->dh", tokens_f, shared_gd),
                    dot("ld,lh->dh", tokens_f, shared_ud),
                    dot("ld,lh->dh", grads_f, shared_hidden),
                ]
            )
            out_partial = dot("lh,dh->ld", shared_hidden, w_down[EXPERTS])
            two_partial = dot("lh,dh->ld", shared_gd, w_gate[EXPERTS]) + dot(
                "lh,dh->ld", shared_ud, w_up[EXPERTS]
            )
            out_partial = out_partial.reshape(group, length, d)
            two_partial = two_partial.reshape(group, length, d)
            shared_done = reduce_and_return(shared_grads)

            pick_parts = []
            expert_done = []
            for part in GROUPS:
                lo, hi = part[0], part[-1] + 1
                hot = onehot_b[:, lo:hi]
                x_in = jnp.einsum("bect,btd->ebcd", hot, tokens_b, preferred_element_type=bf16)
                g_in = jnp.einsum("bect,btd->ebcd", hot, grads_b, preferred_element_type=bf16)
                gate_e = jnp.swapaxes(gate_b[:, lo:hi], 0, 1)
                wg, wu, wd = w_gate[lo:hi], w_up[lo:hi], w_down[lo:hi]
                gate_act = dot("ebcd,edh->ebch", x_in, wg)
                up_act = dot("ebcd,edh->ebch", x_in, wu)
                value, slope = silu_parts(gate_act)
                hid = (value * up_act).astype(bf16)
                e_out = dot("ebch,edh->ebcd", hid, wd)
                pick_parts.append(jnp.sum(e_out * g_in.astype(f32), axis=-1))
                slot_grad = (gate_e * g_in.astype(f32)).astype(bf16)
                hid_grad = dot("ebcd,edh->ebch", slot_grad, wd)
                gate_d = (hid_grad * up_act * slope).astype(bf16)
                up_d = (hid_grad * value).astype(bf16)
                in_grad = dot("ebch,edh->ebcd", gate_d, wg) + dot("ebch,edh->ebcd", up_d, wu)
                weighted = (gate_e * e_out).astype(bf16)
                out_partial = out_partial + dot("bect,ebcd->btd", hot, weighted)
                two_partial = two_partial + dot("bect,ebcd->btd", hot, in_grad.astype(bf16))
                stack = jnp.concatenate(
                    [
                        dot("ebcd,ebch->edh", x_in, gate_d),
                        dot("ebcd,ebch->edh", x_in, up_d),
                        dot("ebcd,ebch->edh", slot_grad, hid),
                    ]
                )
                expert_done.append(reduce_and_return(stack))

            stacks = [[], [], []]
            for part, done in zip(GROUPS, expert_done):
                for k in range(3):
                    stacks[k].append(done[k * len(part) : (k + 1) * len(part)])
            return (
                jnp.concatenate(pick_parts, axis=0),
                plane_sum(two_partial),
                plane_sum(out_partial),
                [jnp.concatenate(parts, axis=0) for parts in stacks],
                shared_done,
            )

        def plane_sum_halves(near, far):
            pair = (near.astype(f32) + swap(far, "core", 1, 2).astype(f32)).astype(bf16)
            total = pair[0].astype(f32)
            for m in range(1, n):
                total = total + swap(pair[m], "shard", m, n).astype(f32)
            return total

        fast = rows // qn % 16 == 0 and hb % 128 == 0 and group <= 8
        w_gate, w_up, w_down = moe_w
        if fast:
            where = jnp.stack([s, q, c]).astype(jnp.int32)
            slots_all = group * CAP
            tok = jnp.swapaxes(token_of_b.reshape(group, EXPERTS, CAP), 0, 1)
            tok = tok.reshape(EXPERTS, slots_all, 1)
            gate_c = jnp.swapaxes(gate_of_b.reshape(group, EXPERTS, CAP), 0, 1)
            gate_c = gate_c.reshape(EXPERTS, slots_all, 1)
            x_all = tokens_b.reshape(group * length, d)
            g_all = grads_b.reshape(group * length, d)

            def reduce_chunk(x):
                for b in range(bits):
                    x = x.reshape((2, x.shape[0] // 2) + x.shape[1:])
                    got = swap(x[1], "plane", 1 << b, qn)
                    x = (x[0].astype(f32) + got.astype(f32)).astype(bf16)
                x = x[0]
                x = jnp.stack([x[0]] + [swap(x[m], "shard", m, n) for m in range(1, n)])[None]
                for b in reversed(range(bits)):
                    x = jnp.concatenate([x, swap(x, "plane", 1 << b, qn)], axis=0)
                return x, swap(x, "core", 1, 2)

            prev = None
            pick_list = []
            expert_prev = None
            for lo, hi in MOE_CALLS:
                grads, pick, *prev = moe_call(
                    lo, hi, n, qn, length, where, tok, gate_c, x_all, g_all, moe_w, prev
                )
                pick_list.append(pick[: min(hi, EXPERTS) - lo])
                for e in range(lo, hi):
                    own, far = reduce_chunk(grads[e - lo])
                    if e < EXPERTS:
                        expert_prev = assemble(
                            n, qn, where, own, far, e, EXPERTS, expert_prev
                        )
                    else:
                        shared_done = assemble(n, qn, where, own, far, 0, 1, None)
                        shared_done = [v[0] for v in shared_done]
            expert_grads = expert_prev
            two = prev[1].reshape(2, n, length, d)
            two_grad = plane_sum_halves(two[0], two[1])
            picks = jnp.concatenate(pick_list, axis=0).reshape(EXPERTS, group, CAP)
            out_part = prev[0].reshape(2, n, length, d)
            mixed = plane_sum_halves(out_part[0], out_part[1])
        else:
            picks, two_grad, mixed, expert_grads, shared_done = plain_moe()
        picks = jnp.swapaxes(picks, 0, 1).reshape(group, slot_total)
        picks = picks[:n] + swap(picks[n:], "core", 1, 2)
        pick_slot = picks[0]
        for m in range(1, n):
            pick_slot = pick_slot + swap(picks[m], "shard", m, n)
        output = (middle + mixed).astype(bf16)

        upstream = cotangent[0].astype(f32)
        pick_grad = jnp.sum(
            jnp.where(hit, pick_slot[:, None], 0.0).reshape(EXPERTS, CAP, length), axis=1
        ).T
        logit_grad = router * (pick_grad - jnp.sum(router * pick_grad, axis=1, keepdims=True))
        two_grad = two_grad + jnp.dot(logit_grad, wr.astype(f32).T, precision=highest)
        router_grad = jnp.dot(normed_two.astype(f32).T, logit_grad, precision=highest)
        middle_part, ffn_gain_grad = norm_back(middle, factor_two, gain_two, two_grad)
        middle_grad = middle_part + upstream

        branch_grad = middle_grad.astype(bf16)
        output_weight_grad = dot("ld,le->de", attended, branch_grad)
        attended_grad = (
            dot("le,de->ld", branch_grad, wo).astype(bf16).reshape(length, NH, HD)
        )
        prob_grad = dot("qhd,khd->hqk", attended_grad, values)
        row_inner = jnp.sum(soft * prob_grad, axis=-1, keepdims=True)
        score_grad = (soft * (prob_grad - row_inner)).astype(bf16)
        query_parts = dot("hqk,khd->qhd", score_grad, keys_rot) * score_scale
        key_parts = dot("hqk,qhd->khd", score_grad, queries) * score_scale
        value_parts = dot("hqk,qhd->khd", probs, attended_grad)
        query_pre = query_parts * cos_b + rotate_back(query_parts * sin_b)
        key_pre = key_parts * cos_b + rotate_back(key_parts * sin_b)
        joint_grad = jnp.concatenate(
            [v.reshape(length, d) for v in (query_pre, key_pre, value_parts)], axis=1
        ).astype(bf16)
        one_grad = dot("lf,df->ld", joint_grad, wqkv)
        joint_weight_grad = dot("ld,lf->df", normed_one, joint_grad)
        input_part, attn_gain_grad = norm_back(inputs, factor_one, gain_one, one_grad)
        input_grad = (middle_grad + input_part).astype(bf16)

        small_grad = jnp.concatenate(
            [attn_gain_grad[:, None], ffn_gain_grad[:, None], router_grad], axis=1
        )
        small_grad = jnp.pad(small_grad, ((0, 0), (0, 256 - small_grad.shape[1])))
        total = jnp.concatenate([joint_weight_grad, output_weight_grad, small_grad], axis=1)
        keep = lax.dynamic_slice_in_dim(total, c * half, half, 1)
        send = lax.dynamic_slice_in_dim(total, (1 - c) * half, half, 1).astype(bf16)
        total = keep + swap(send, "core", 1, 2).astype(f32)
        total = total.reshape(n, rows, half)
        own = pick_index(total, s)
        low = total.astype(bf16)
        for m in range(1, n):
            own = own + swap(pick_index(low, s ^ m), "shard", m, n).astype(f32)
        x = own.reshape((2,) * bits + (rows // qn, half))
        for b in range(bits):
            axis = bits - 1 - b
            bit = (q >> b) & 1
            keep = pick_index(x, bit, axis)
            send = pick_index(x, 1 - bit, axis).astype(bf16)
            x = keep + swap(send, "plane", 1 << b, qn).astype(f32)
        x = x.astype(bf16)[None]
        for b in reversed(range(bits)):
            bit = (q >> b) & 1
            other = swap(x, "plane", 1 << b, qn)
            pair = jnp.stack(
                [jnp.where(bit == 0, x, other), jnp.where(bit == 0, other, x)], axis=1
            )
            x = pair.reshape((2 * x.shape[0],) + x.shape[1:])
        x = x.reshape(rows, half)
        x = join_bit(c, x, swap(x, "core", 1, 2), 1).astype(f32)
        return (
            output[None],
            input_grad[None],
            x[:, 4 * d],
            x[:, :d],
            x[:, d : 2 * d],
            x[:, 2 * d : 3 * d],
            x[:, 3 * d : 4 * d],
            x[:, 4 * d + 1],
            x[:, 4 * d + 2 : 4 * d + 2 + EXPERTS],
            expert_grads[0],
            expert_grads[1],
            expert_grads[2],
            shared_done[0],
            shared_done[1],
            shared_done[2],
        )

    return shards


def solution(mesh):
    n, replicas = mesh.shape["shard"], mesh.shape["replica"]
    fine = Mesh(mesh.devices.reshape(n, replicas // 2, 2), ("shard", "plane", "core"))
    every = ("shard", "plane", "core")
    in_specs = (
        P(every, None, None),
        P(every, None, None),
        P(every, None),
        P(every, None),
        P(every, None, None),
        P(every, None),
        P("shard"),
        P("shard", None),
        P("shard", None),
        P("shard", None),
        P("shard", None),
        P("shard"),
        P("shard", None),
        P(None, "shard", None),
        P(None, "shard", None),
        P(None, "shard", None),
        P("shard", None),
        P("shard", None),
        P("shard", None),
    )
    out_specs = (
        P(every, None, None),
        P(every, None, None),
        P("shard"),
        P("shard", None),
        P("shard", None),
        P("shard", None),
        P("shard", None),
        P("shard"),
        P("shard", None),
        P(None, "shard", None),
        P(None, "shard", None),
        P(None, "shard", None),
        P("shard", None),
        P("shard", None),
        P("shard", None),
    )
    return jax.shard_map(
        make_shards(n, replicas // 2),
        mesh=fine,
        in_specs=in_specs,
        out_specs=out_specs,
        check_vma=False,
    )
```

```python
import functools
import math

import jax
import jax.numpy as jnp
from jax import lax
from jax.experimental import pallas as pl
from jax.experimental.pallas import tpu as pltpu
from jax.sharding import Mesh, PartitionSpec as P

NH = 12
HD = 64
EXPERTS = 6
TOPK = 2
CAP = 96
EPSILON = 1e-06
NEGATIVE = -1e30
GROUPS = ((0, 1), (2, 3), (4, 5))

highest = lax.Precision.HIGHEST
f32 = jnp.float32
bf16 = jnp.bfloat16


def dot(spec, first, second):
    return jnp.einsum(spec, first, second, preferred_element_type=f32)


def rotate_half(values):
    half_size = values.shape[-1] // 2
    return jnp.concatenate([-values[..., half_size:], values[..., :half_size]], axis=-1)


def rotate_back(values):
    half_size = values.shape[-1] // 2
    return jnp.concatenate([values[..., half_size:], -values[..., :half_size]], axis=-1)


def rotary_tables(length, head_dim):
    positions = jnp.arange(length, dtype=f32)
    frequency = jnp.exp(
        jnp.arange(head_dim // 2, dtype=f32) * (-2.0 * math.log(10000.0) / head_dim)
    )
    angles = positions[:, None] * frequency[None, :]
    angles = jnp.concatenate([angles, angles], axis=1)
    return (jnp.cos(angles), jnp.sin(angles))


def attention_mask(segments, padding):
    places = jnp.arange(segments.shape[0])
    causal = places[None, :] <= places[:, None]
    shared_doc = segments[:, None] == segments[None, :]
    usable = (padding[None, :] == 1) | (places[None, :] == places[:, None])
    return causal & shared_doc & usable


def norm_factor(values):
    return lax.rsqrt(jnp.mean(values * values, axis=-1, keepdims=True) + EPSILON)


def norm_back(values, factor, norm_gain, gradient):
    scaled = gradient * norm_gain
    gain_grad = jnp.sum(gradient * values * factor, axis=0)
    input_part = factor * scaled - values * factor**3 * jnp.mean(
        scaled * values, axis=-1, keepdims=True
    )
    return (input_part, gain_grad)


def silu_parts(gate_act):
    sigmoid = jax.nn.sigmoid(gate_act)
    return (gate_act * sigmoid, sigmoid * (1.0 + gate_act * (1.0 - sigmoid)))


def pair_slots(routes, padding, priority):
    length = routes.shape[0]
    pair_expert = routes.T.reshape(-1)
    pair_live = jnp.tile(padding, TOPK) == 1
    pair_key = (jnp.arange(TOPK, dtype=jnp.int32)[:, None] * length + priority[None, :]).reshape(-1)
    earlier = (
        (pair_key[None, :] < pair_key[:, None])
        & (pair_expert[None, :] == pair_expert[:, None])
        & pair_live[None, :]
    )
    place = jnp.sum(earlier.astype(jnp.int32), axis=1)
    kept = pair_live & (place < CAP)
    return (pair_expert, place, kept)


def swap(values, axis, mask, size):
    return lax.ppermute(values, axis, [(i, i ^ mask) for i in range(size)])


def pick_index(values, index, axis=0):
    return lax.dynamic_index_in_dim(values, index, axis, keepdims=False)


def mm(first, second, contract):
    return lax.dot_general(
        first, second, (contract, ((), ())), preferred_element_type=f32
    )


NN = ((1,), (0,))
NT = ((1,), (1,))
TN = ((0,), (0,))


def flip(value, mask, size):
    out = 0
    for b in range(size.bit_length() - 1):
        bit = (value // (1 << b)) % 2
        out = out + (1 << b) * ((1 - bit) if (mask >> b) & 1 else bit)
    return out


MESH = pl.DeviceIdType.MESH


def moe_kernel(
    n,
    qn,
    length,
    tok_ref,
    gate_ref,
    x_ref,
    g_ref,
    wg_ref,
    wu_ref,
    wd_ref,
    near_ref,
    far_ref,
    pick_ref,
    y_ref,
    t_ref,
    acc_y,
    acc_t,
    xs,
    gs,
    sg,
    dw,
    kept,
    sent,
    r1,
    r2,
    y_send,
    y_side,
    y_pair,
    y_in,
    send_sem,
    recv_sem,
    a2a_send,
    a2a_recv,
    local_sem,
    y_ssem,
    y_rsem,
):
    step = pl.program_id(0)
    total = EXPERTS + 1
    group = 2 * n
    d = x_ref.shape[1]
    piece = d // (n * qn)
    s, q, c = (lax.axis_index(a) for a in ("shard", "plane", "core"))
    near_q, far_q = flip(q, 1, qn), flip(q, 2, qn)
    other_c = 1 - c

    def remote(src, dst, stage, e, to):
        return pltpu.make_async_remote_copy(
            src,
            dst,
            send_sem.at[stage, e],
            recv_sem.at[stage, e],
            device_id=to,
            device_id_type=MESH,
        )

    def halve_near(e):
        return remote(sent.at[e], r1.at[e], 0, e, {"plane": near_q})

    def halve_far(e):
        return remote(kept.at[e, 1], r2.at[e], 1, e, {"plane": far_q})

    def across(e, m):
        return pltpu.make_async_remote_copy(
            kept.at[e, 0, m],
            near_ref.at[e, 0, m],
            a2a_send.at[m - 1, e],
            a2a_recv.at[m - 1, e],
            device_id={"shard": flip(s, m, n)},
            device_id_type=MESH,
        )

    def stay(e):
        return pltpu.make_async_copy(kept.at[e, 0, 0], near_ref.at[e, 0, 0], local_sem.at[e])

    def double_far(e):
        return remote(near_ref.at[e, 0], near_ref.at[e, 1], 2, e, {"plane": far_q})

    def double_near(e):
        return remote(
            near_ref.at[e, pl.ds(0, 2)], near_ref.at[e, pl.ds(2, 2)], 3, e, {"plane": near_q}
        )

    def side(e):
        return remote(near_ref.at[e], far_ref.at[e], 4, e, {"core": other_c})

    def y_side_copy():
        return pltpu.make_async_remote_copy(
            y_send,
            y_side,
            y_ssem.at[0],
            y_rsem.at[0],
            device_id={"core": other_c},
            device_id_type=MESH,
        )

    def y_across(m):
        return pltpu.make_async_remote_copy(
            y_pair.at[m - 1],
            y_in.at[m - 1],
            y_ssem.at[m],
            y_rsem.at[m],
            device_id={"shard": flip(s, m, n)},
            device_id_type=MESH,
        )

    @pl.when(step == 0)
    def _():
        barrier = pltpu.get_barrier_semaphore()
        peers = [{"plane": near_q}, {"plane": far_q}, {"core": other_c}]
        peers += [{"shard": flip(s, m, n)} for m in range(1, n)]
        for peer in peers:
            pl.semaphore_signal(barrier, 1, device_id=peer, device_id_type=MESH)
        pl.semaphore_wait(barrier, len(peers))
        acc_y[...] = jnp.zeros_like(acc_y)
        acc_t[...] = jnp.zeros_like(acc_t)

    def branch(x, gs_rows, wg, wu, wd):
        gate_act = mm(x, wg, NN)
        up_act = mm(x, wu, NN)
        sigmoid = 1.0 / (1.0 + jnp.exp(-gate_act))
        value = gate_act * sigmoid
        slope = sigmoid * (1.0 + gate_act * (1.0 - sigmoid))
        hid = (value * up_act).astype(bf16)
        hid_grad = mm(gs_rows, wd, NN)
        gate_d = (hid_grad * up_act * slope).astype(bf16)
        up_d = (hid_grad * value).astype(bf16)
        return hid, gate_d, up_d

    @pl.when(step < EXPERTS)
    def _():
        lanes = lax.broadcasted_iota(jnp.int32, (CAP, length), 1)

        def gather(b, carry):
            slot = pl.ds(pl.multiple_of(b * CAP, 16), CAP)
            seq = pl.ds(pl.multiple_of(b * length, length), length)
            hot = (tok_ref[0, slot, :] == lanes).astype(bf16)
            xs[slot, :] = mm(hot, x_ref[seq, :], NN).astype(bf16)
            g_rows = mm(hot, g_ref[seq, :], NN)
            gs[slot, :] = g_rows.astype(bf16)
            sg[slot, :] = (g_rows * gate_ref[0, slot, :]).astype(bf16)
            return carry

        lax.fori_loop(0, group, gather, 0)
        wg, wu, wd = wg_ref[0], wu_ref[0], wd_ref[0]
        x, slot_grad = xs[...], sg[...]
        hid, gate_d, up_d = branch(x, slot_grad, wg, wu, wd)
        dw[0] = mm(x, gate_d, TN)
        dw[1] = mm(x, up_d, TN)
        dw[2] = mm(slot_grad, hid, TN)
        e_out = mm(hid, wd, NT)
        pick_ref[0] = jnp.sum(e_out * gs[...].astype(f32), axis=1, keepdims=True)
        gs[...] = (e_out * gate_ref[0]).astype(bf16)
        xs[...] = (mm(gate_d, wg, NT) + mm(up_d, wu, NT)).astype(bf16)

        def scatter(b, carry):
            slot = pl.ds(pl.multiple_of(b * CAP, 16), CAP)
            seq = pl.ds(pl.multiple_of(b * length, length), length)
            hot = (tok_ref[0, slot, :] == lanes).astype(bf16)
            acc_y[seq, :] += mm(hot, gs[slot, :], TN)
            acc_t[seq, :] += mm(hot, xs[slot, :], TN)
            return carry

        lax.fori_loop(0, group, scatter, 0)

    @pl.when(step == EXPERTS)
    def _():
        dw[...] = jnp.zeros_like(dw)
        wg, wu, wd = wg_ref[0], wu_ref[0], wd_ref[0]

        def rows_step(i, carry):
            rows = pl.ds(pl.multiple_of(i * 2 * length, 2 * length), 2 * length)
            x, g = x_ref[rows, :], g_ref[rows, :]
            hid, gate_d, up_d = branch(x, g, wg, wu, wd)
            dw[0] += mm(x, gate_d, TN)
            dw[1] += mm(x, up_d, TN)
            dw[2] += mm(g, hid, TN)
            acc_y[rows, :] += mm(hid, wd, NT)
            acc_t[rows, :] += mm(gate_d, wg, NT) + mm(up_d, wu, NT)
            return carry

        lax.fori_loop(0, n, rows_step, 0)
        half = pl.ds(n * length, n * length)
        y_send[0] = acc_y[half, :].astype(bf16)
        y_send[1] = acc_t[half, :].astype(bf16)

    @pl.when(step < total)
    def _():
        for j in range(qn):
            into = kept if j < qn // 2 else sent
            for m in range(n):
                start = (flip(s, m, n) * qn + flip(q, reverse_bits(j, qn), qn)) * piece
                start = pl.multiple_of(start, 16)
                for k in range(3):
                    into[step, j % (qn // 2), m, k] = dw[k, pl.ds(start, piece), :].astype(bf16)
        halve_near(step).start()

    @pl.when(step == EXPERTS)
    def _():
        y_side_copy().start()

    def stage(delay, body):
        @pl.when((step >= delay) & (step < total + delay))
        def _():
            body(step - delay)

    def after_near(e):
        halve_near(e).wait()
        for j in (1, 0):
            for m in range(n):
                kept[e, j, m] = (
                    kept[e, j, m].astype(f32) + r1[e, j, m].astype(f32)
                ).astype(bf16)
        halve_far(e).start()

    def after_far(e):
        halve_far(e).wait()
        for m in range(n):
            kept[e, 0, m] = (kept[e, 0, m].astype(f32) + r2[e, m].astype(f32)).astype(bf16)
        for m in range(1, n):
            across(e, m).start()
        stay(e).start()

    def after_across(e):
        for m in range(1, n):
            across(e, m).wait()
        stay(e).wait()
        double_far(e).start()

    def after_double_far(e):
        double_far(e).wait()
        double_near(e).start()

    def after_double_near(e):
        double_near(e).wait()
        side(e).start()

    stage(1, after_near)
    stage(2, after_far)
    stage(3, after_across)
    stage(4, after_double_far)

    @pl.when(step == total)
    def _():
        y_side_copy().wait()
        rows = pl.ds(0, length)
        for k, acc in enumerate((acc_y, acc_t)):
            acc[rows, :] += y_side[k, rows, :].astype(f32)
            for m in range(1, n):
                seq = pl.ds(m * length, length)
                y_pair[m - 1, k] = (acc[seq, :] + y_side[k, seq, :].astype(f32)).astype(bf16)
        for m in range(1, n):
            y_across(m).start()

    @pl.when(step == total + 1)
    def _():
        for m in range(1, n):
            y_across(m).wait()
        rows = pl.ds(0, length)
        for k, (acc, out) in enumerate(((acc_y, y_ref), (acc_t, t_ref))):
            value = acc[rows, :]
            for m in range(1, n):
                value = value + y_in[m - 1, k].astype(f32)
            out[...] = value

    stage(5, after_double_near)
    stage(6, lambda e: side(e).wait())


def moe_call(n, qn, length, tok, gate, x, g, weights):
    d = x.shape[1]
    hb = weights[0].shape[2]
    rows = x.shape[0]
    slots = tok.shape[1]
    total = EXPERTS + 1
    piece = d // (n * qn)
    once = pl.Buffered(1)
    column = pl.BlockSpec((1, slots, 1), lambda t: (jnp.minimum(t, EXPERTS - 1), 0, 0))
    whole = pl.BlockSpec((rows, d), lambda t: (0, 0), pipeline_mode=once)
    weight = pl.BlockSpec((1, d, hb), lambda t: (jnp.minimum(t, EXPERTS), 0, 0))
    own = pl.BlockSpec((length, d), lambda t: (0, 0), pipeline_mode=once)
    anywhere = pl.BlockSpec(memory_space=pl.ANY)
    pieces = (total, qn, n, 3, piece, hb)
    dma = pltpu.SemaphoreType.DMA
    return pl.pallas_call(
        functools.partial(moe_kernel, n, qn, length),
        grid=(total + 6,),
        in_specs=[column, column, whole, whole, weight, weight, weight],
        out_specs=[anywhere, anywhere, column, own, own],
        scratch_shapes=[
            pltpu.VMEM((rows, d), f32),
            pltpu.VMEM((rows, d), f32),
            pltpu.VMEM((slots, d), bf16),
            pltpu.VMEM((slots, d), bf16),
            pltpu.VMEM((slots, d), bf16),
            pltpu.VMEM((3, d, hb), f32),
            pltpu.VMEM((total, qn // 2, n, 3, piece, hb), bf16),
            pltpu.VMEM((total, qn // 2, n, 3, piece, hb), bf16),
            pltpu.VMEM((total, qn // 2, n, 3, piece, hb), bf16),
            pltpu.VMEM((total, n, 3, piece, hb), bf16),
            pltpu.VMEM((2, n * length, d), bf16),
            pltpu.VMEM((2, n * length, d), bf16),
            pltpu.VMEM((n - 1, 2, length, d), bf16),
            pltpu.VMEM((n - 1, 2, length, d), bf16),
            dma((5, total)),
            dma((5, total)),
            dma((n - 1, total)),
            dma((n - 1, total)),
            dma((total,)),
            dma((n,)),
            dma((n,)),
        ],
        out_shape=[
            jax.ShapeDtypeStruct(pieces, bf16),
            jax.ShapeDtypeStruct(pieces, bf16),
            jax.ShapeDtypeStruct((EXPERTS, slots, 1), f32),
            jax.ShapeDtypeStruct((length, d), f32),
            jax.ShapeDtypeStruct((length, d), f32),
        ],
        compiler_params=pltpu.CompilerParams(
            vmem_limit_bytes=63 << 20, collective_id=0, has_side_effects=True
        ),
        cost_estimate=pl.CostEstimate(
            flops=18 * total * slots * d * hb, bytes_accessed=200 << 20, transcendentals=0
        ),
        name="moe",
    )(tok, gate, x, g, *weights)


def reverse_bits(j, size):
    bits = size.bit_length() - 1
    return sum(((j >> b) & 1) << (bits - 1 - b) for b in range(bits))


def assemble_kernel(n, qn, where_ref, own_ref, far_ref, *outs):
    s, q, c = where_ref[0], where_ref[1], where_ref[2]
    piece, hb = own_ref.shape[4], own_ref.shape[5]
    for side, ref in enumerate((own_ref, far_ref)):
        for j in range(qn):
            for m in range(n):
                row = pl.multiple_of((q ^ reverse_bits(j, qn)) * piece, 8)
                column = pl.multiple_of(((s ^ m) * 2 + (c ^ side)) * hb, 128)
                for k in range(3):
                    outs[k][0, pl.ds(row, piece), pl.ds(column, hb)] = ref[
                        0, j, m, k
                    ].astype(f32)


def assemble(n, qn, where, own, far, first, count):
    piece, hb = own.shape[4], own.shape[5]
    rows, hidden = piece * qn, hb * 2 * n
    spec = pl.BlockSpec((1, qn, n, 3, piece, hb), lambda i, *_: (i + first, 0, 0, 0, 0, 0))
    return pl.pallas_call(
        functools.partial(assemble_kernel, n, qn),
        grid_spec=pltpu.PrefetchScalarGridSpec(
            num_scalar_prefetch=1,
            grid=(count,),
            in_specs=[spec, spec],
            out_specs=[pl.BlockSpec((1, rows, hidden), lambda i, *_: (i, 0, 0))] * 3,
        ),
        out_shape=[jax.ShapeDtypeStruct((count, rows, hidden), f32)] * 3,
        cost_estimate=pl.CostEstimate(
            flops=0, bytes_accessed=18 * count * rows * hidden, transcendentals=0
        ),
        name="assemble",
    )(where, own, far)


def make_shards(n, qn):
    bits = qn.bit_length() - 1

    def place_blocks(own, blocks):
        out = jnp.zeros((n,) + blocks[0].shape, blocks[0].dtype)
        for m in range(n):
            out = lax.dynamic_update_index_in_dim(out, blocks[m], own ^ m, 0)
        return out

    def join_bit(bit, own, other, axis):
        first = jnp.where(bit == 0, own, other)
        second = jnp.where(bit == 0, other, own)
        return jnp.concatenate([first, second], axis=axis)

    def shards(
        tokens,
        cotangent,
        segments,
        padding,
        routes,
        priority,
        attn_gain,
        query_weight,
        key_weight,
        value_weight,
        output_weight,
        ffn_gain,
        router_weight,
        expert_gate,
        expert_up,
        expert_down,
        shared_gate,
        shared_up,
        shared_down,
    ):
        s = lax.axis_index("shard")
        q = lax.axis_index("plane")
        c = lax.axis_index("core")
        length, d = tokens.shape[1], tokens.shape[2]
        rows = query_weight.shape[0]
        hidden = expert_gate.shape[2]
        hb = hidden // (2 * n)
        score_scale = HD ** (-0.5)

        small = jnp.concatenate(
            [attn_gain[:, None], ffn_gain[:, None], router_weight], axis=1
        )
        small = jnp.pad(small, ((0, 0), (0, 256 - small.shape[1])))
        wide = jnp.concatenate(
            [query_weight, key_weight, value_weight, output_weight, small], axis=1
        )
        half = wide.shape[1] // 2
        mine = lax.dynamic_slice_in_dim(wide, c * half, half, 1)
        blocks = [mine] + [swap(mine, "shard", m, n) for m in range(1, n)]
        mine = place_blocks(s, blocks).reshape(d, half)
        other = swap(mine, "core", 1, 2)
        wide = join_bit(c, mine, other, 1)
        wqkv, wo = wide[:, : 3 * d], wide[:, 3 * d : 4 * d]
        gain_one = wide[:, 4 * d].astype(f32)
        gain_two = wide[:, 4 * d + 1].astype(f32)
        wr = wide[:, 4 * d + 2 : 4 * d + 2 + EXPERTS]

        def block_for(m):
            start = ((s ^ m) * 2 + c) * hb
            cut = lambda w: lax.dynamic_slice_in_dim(w, start, hb, w.ndim - 1)
            return [
                jnp.concatenate([cut(e), cut(w)[None]], axis=0)
                for e, w in (
                    (expert_gate, shared_gate),
                    (expert_up, shared_up),
                    (expert_down, shared_down),
                )
            ]

        own_blocks = block_for(0)
        sent = [block_for(m) for m in range(1, n)]
        moe_w = []
        for k in range(3):
            got = [own_blocks[k]] + [swap(sent[m - 1][k], "shard", m, n) for m in range(1, n)]
            full = jnp.zeros((EXPERTS + 1, n, rows, hb), bf16)
            for m in range(n):
                full = lax.dynamic_update_index_in_dim(full, got[m], s ^ m, 1)
            moe_w.append(full.reshape(EXPERTS + 1, d, hb))

        def plane_gather(values):
            near = jnp.stack([values] + [swap(values, "shard", m, n) for m in range(1, n)])
            return jnp.concatenate([near, swap(near, "core", 1, 2)], axis=0)

        def plane_sum(partial):
            low = partial.astype(bf16)
            pair = (partial[:n] + swap(low[n:], "core", 1, 2).astype(f32)).astype(bf16)
            total = pair[0].astype(f32)
            for m in range(1, n):
                total = total + swap(pair[m], "shard", m, n).astype(f32)
            return total

        grads_b = plane_gather(cotangent[0])

        inputs = tokens[0].astype(f32)
        factor_one = norm_factor(inputs)
        normed_one = (inputs * factor_one * gain_one).astype(bf16)
        projected = jnp.dot(normed_one, wqkv, preferred_element_type=f32)
        cosine, sine = rotary_tables(length, HD)
        heads = projected.reshape(length, 3, NH, HD)
        cos_b, sin_b = cosine[:, None, :], sine[:, None, :]
        queries = (heads[:, 0] * cos_b + rotate_half(heads[:, 0]) * sin_b).astype(bf16)
        keys_rot = (heads[:, 1] * cos_b + rotate_half(heads[:, 1]) * sin_b).astype(bf16)
        values = heads[:, 2].astype(bf16)
        allowed = attention_mask(segments[0], padding[0])
        logits = dot("qhd,khd->hqk", queries, keys_rot) * score_scale
        logits = jnp.where(allowed[None], logits, NEGATIVE)
        maxima = jnp.max(logits, axis=-1, keepdims=True)
        exponent = jnp.exp(logits - maxima)
        soft = exponent / jnp.sum(exponent, axis=-1, keepdims=True)
        probs = soft.astype(bf16)
        attended = dot("hqk,khd->qhd", probs, values).reshape(length, d).astype(bf16)
        middle = inputs + jnp.dot(attended, wo, preferred_element_type=f32)
        factor_two = norm_factor(middle)
        normed_two = (middle * factor_two * gain_two).astype(bf16)
        router = jax.nn.softmax(
            jnp.dot(normed_two, wr, preferred_element_type=f32), axis=-1
        )

        pair_expert, place, kept = pair_slots(routes[0], padding[0], priority[0])
        slot_total = EXPERTS * CAP
        slot_index = jnp.where(kept, pair_expert * CAP + place, -1).reshape(TOPK, length)
        slots = jnp.arange(slot_total, dtype=jnp.int32)
        hit = (slots[None, :, None] == slot_index[:, None, :]).any(axis=0)
        onehot = hit.astype(bf16)
        token_of = jnp.max(
            jnp.where(hit, jnp.arange(length, dtype=jnp.int32)[None, :], -1), axis=1
        )
        slot_expert = jnp.repeat(jnp.arange(EXPERTS), CAP)
        gate_of = jnp.sum(
            jnp.where(hit, jnp.repeat(router.T, CAP, axis=0), 0.0), axis=1
        )

        tokens_b = plane_gather(normed_two)
        token_of_b = plane_gather(token_of)
        gate_of_b = plane_gather(gate_of)
        group = 2 * n
        onehot_b = (
            token_of_b[:, :, None] == jnp.arange(length, dtype=jnp.int32)[None, None, :]
        ).astype(bf16)
        onehot_b = onehot_b.reshape(group, EXPERTS, CAP, length)
        gate_b = gate_of_b.reshape(group, EXPERTS, CAP, 1)

        def reduce_and_return(stack):
            k = stack.shape[0]
            piece = rows // qn
            x = stack.reshape((k, n) + (2,) * bits + (piece, hb))
            for b in range(bits):
                axis = 2 + (bits - 1 - b)
                bit = (q >> b) & 1
                keep = pick_index(x, bit, axis)
                send = pick_index(x, 1 - bit, axis).astype(bf16)
                x = keep + swap(send, "plane", 1 << b, qn).astype(f32)
            x = x.astype(bf16)
            own = pick_index(x, s, 1)
            got = [own] + [swap(pick_index(x, s ^ m, 1), "shard", m, n) for m in range(1, n)]
            x = jnp.stack(got)
            x = x[None]
            for b in reversed(range(bits)):
                bit = (q >> b) & 1
                other = swap(x, "plane", 1 << b, qn)
                lead = x.shape[0]
                pair = jnp.stack(
                    [jnp.where(bit == 0, x, other), jnp.where(bit == 0, other, x)], axis=1
                )
                x = pair.reshape((2 * lead,) + x.shape[1:])
            other = swap(x, "core", 1, 2)
            x = jnp.stack(
                [jnp.where(c == 0, x, other), jnp.where(c == 0, other, x)]
            )
            out = jnp.zeros((n,) + (2, qn, k, piece, hb), bf16)
            for m in range(n):
                out = lax.dynamic_update_index_in_dim(out, x[:, :, m], s ^ m, 0)
            return out.transpose(3, 2, 4, 0, 1, 5).reshape(k, rows, hidden).astype(f32)

        def plain_moe():
            tokens_f = tokens_b.reshape(group * length, d)
            grads_f = grads_b.reshape(group * length, d)
            shared_g = jnp.dot(tokens_f, w_gate[EXPERTS], preferred_element_type=f32)
            shared_u = jnp.dot(tokens_f, w_up[EXPERTS], preferred_element_type=f32)
            value, slope = silu_parts(shared_g)
            shared_hidden = (value * shared_u).astype(bf16)
            shared_q = jnp.dot(grads_f, w_down[EXPERTS], preferred_element_type=f32)
            shared_gd = (shared_q * shared_u * slope).astype(bf16)
            shared_ud = (shared_q * value).astype(bf16)
            shared_grads = jnp.stack(
                [
                    dot("ld,lh->dh", tokens_f, shared_gd),
                    dot("ld,lh->dh", tokens_f, shared_ud),
                    dot("ld,lh->dh", grads_f, shared_hidden),
                ]
            )
            out_partial = dot("lh,dh->ld", shared_hidden, w_down[EXPERTS])
            two_partial = dot("lh,dh->ld", shared_gd, w_gate[EXPERTS]) + dot(
                "lh,dh->ld", shared_ud, w_up[EXPERTS]
            )
            out_partial = out_partial.reshape(group, length, d)
            two_partial = two_partial.reshape(group, length, d)
            shared_done = reduce_and_return(shared_grads)

            pick_parts = []
            expert_done = []
            for part in GROUPS:
                lo, hi = part[0], part[-1] + 1
                hot = onehot_b[:, lo:hi]
                x_in = jnp.einsum("bect,btd->ebcd", hot, tokens_b, preferred_element_type=bf16)
                g_in = jnp.einsum("bect,btd->ebcd", hot, grads_b, preferred_element_type=bf16)
                gate_e = jnp.swapaxes(gate_b[:, lo:hi], 0, 1)
                wg, wu, wd = w_gate[lo:hi], w_up[lo:hi], w_down[lo:hi]
                gate_act = dot("ebcd,edh->ebch", x_in, wg)
                up_act = dot("ebcd,edh->ebch", x_in, wu)
                value, slope = silu_parts(gate_act)
                hid = (value * up_act).astype(bf16)
                e_out = dot("ebch,edh->ebcd", hid, wd)
                pick_parts.append(jnp.sum(e_out * g_in.astype(f32), axis=-1))
                slot_grad = (gate_e * g_in.astype(f32)).astype(bf16)
                hid_grad = dot("ebcd,edh->ebch", slot_grad, wd)
                gate_d = (hid_grad * up_act * slope).astype(bf16)
                up_d = (hid_grad * value).astype(bf16)
                in_grad = dot("ebch,edh->ebcd", gate_d, wg) + dot("ebch,edh->ebcd", up_d, wu)
                weighted = (gate_e * e_out).astype(bf16)
                out_partial = out_partial + dot("bect,ebcd->btd", hot, weighted)
                two_partial = two_partial + dot("bect,ebcd->btd", hot, in_grad.astype(bf16))
                stack = jnp.concatenate(
                    [
                        dot("ebcd,ebch->edh", x_in, gate_d),
                        dot("ebcd,ebch->edh", x_in, up_d),
                        dot("ebcd,ebch->edh", slot_grad, hid),
                    ]
                )
                expert_done.append(reduce_and_return(stack))

            stacks = [[], [], []]
            for part, done in zip(GROUPS, expert_done):
                for k in range(3):
                    stacks[k].append(done[k * len(part) : (k + 1) * len(part)])
            return (
                jnp.concatenate(pick_parts, axis=0),
                plane_sum(two_partial),
                plane_sum(out_partial),
                [jnp.concatenate(parts, axis=0) for parts in stacks],
                shared_done,
            )

        fast = rows // qn % 16 == 0 and hb % 128 == 0 and group <= 8 and qn == 4
        w_gate, w_up, w_down = moe_w
        if fast:
            where = jnp.stack([s, q, c]).astype(jnp.int32)
            slots_all = group * CAP
            tok = jnp.swapaxes(token_of_b.reshape(group, EXPERTS, CAP), 0, 1)
            tok = tok.reshape(EXPERTS, slots_all, 1)
            gate_c = jnp.swapaxes(gate_of_b.reshape(group, EXPERTS, CAP), 0, 1)
            gate_c = gate_c.reshape(EXPERTS, slots_all, 1)
            x_all = tokens_b.reshape(group * length, d)
            g_all = grads_b.reshape(group * length, d)

            near, far, picks, mixed, two_grad = moe_call(
                n, qn, length, tok, gate_c, x_all, g_all, moe_w
            )
            picks = picks.reshape(EXPERTS, group, CAP)
            expert_grads = assemble(n, qn, where, near, far, 0, EXPERTS)
            shared_done = [v[0] for v in assemble(n, qn, where, near, far, EXPERTS, 1)]
        else:
            picks, two_grad, mixed, expert_grads, shared_done = plain_moe()
        picks = jnp.swapaxes(picks, 0, 1).reshape(group, slot_total)
        picks = picks[:n] + swap(picks[n:], "core", 1, 2)
        pick_slot = picks[0]
        for m in range(1, n):
            pick_slot = pick_slot + swap(picks[m], "shard", m, n)
        output = (middle + mixed).astype(bf16)

        upstream = cotangent[0].astype(f32)
        pick_grad = jnp.sum(
            jnp.where(hit, pick_slot[:, None], 0.0).reshape(EXPERTS, CAP, length), axis=1
        ).T
        logit_grad = router * (pick_grad - jnp.sum(router * pick_grad, axis=1, keepdims=True))
        two_grad = two_grad + jnp.dot(logit_grad, wr.astype(f32).T, precision=highest)
        router_grad = jnp.dot(normed_two.astype(f32).T, logit_grad, precision=highest)
        middle_part, ffn_gain_grad = norm_back(middle, factor_two, gain_two, two_grad)
        middle_grad = middle_part + upstream

        branch_grad = middle_grad.astype(bf16)
        output_weight_grad = dot("ld,le->de", attended, branch_grad)
        attended_grad = (
            dot("le,de->ld", branch_grad, wo).astype(bf16).reshape(length, NH, HD)
        )
        prob_grad = dot("qhd,khd->hqk", attended_grad, values)
        row_inner = jnp.sum(soft * prob_grad, axis=-1, keepdims=True)
        score_grad = (soft * (prob_grad - row_inner)).astype(bf16)
        query_parts = dot("hqk,khd->qhd", score_grad, keys_rot) * score_scale
        key_parts = dot("hqk,qhd->khd", score_grad, queries) * score_scale
        value_parts = dot("hqk,qhd->khd", probs, attended_grad)
        query_pre = query_parts * cos_b + rotate_back(query_parts * sin_b)
        key_pre = key_parts * cos_b + rotate_back(key_parts * sin_b)
        joint_grad = jnp.concatenate(
            [v.reshape(length, d) for v in (query_pre, key_pre, value_parts)], axis=1
        ).astype(bf16)
        one_grad = dot("lf,df->ld", joint_grad, wqkv)
        joint_weight_grad = dot("ld,lf->df", normed_one, joint_grad)
        input_part, attn_gain_grad = norm_back(inputs, factor_one, gain_one, one_grad)
        input_grad = (middle_grad + input_part).astype(bf16)

        small_grad = jnp.concatenate(
            [attn_gain_grad[:, None], ffn_gain_grad[:, None], router_grad], axis=1
        )
        small_grad = jnp.pad(small_grad, ((0, 0), (0, 256 - small_grad.shape[1])))
        total = jnp.concatenate([joint_weight_grad, output_weight_grad, small_grad], axis=1)
        keep = lax.dynamic_slice_in_dim(total, c * half, half, 1)
        send = lax.dynamic_slice_in_dim(total, (1 - c) * half, half, 1).astype(bf16)
        total = keep + swap(send, "core", 1, 2).astype(f32)
        total = total.reshape(n, rows, half)
        own = pick_index(total, s)
        low = total.astype(bf16)
        for m in range(1, n):
            own = own + swap(pick_index(low, s ^ m), "shard", m, n).astype(f32)
        x = own.reshape((2,) * bits + (rows // qn, half))
        for b in range(bits):
            axis = bits - 1 - b
            bit = (q >> b) & 1
            keep = pick_index(x, bit, axis)
            send = pick_index(x, 1 - bit, axis).astype(bf16)
            x = keep + swap(send, "plane", 1 << b, qn).astype(f32)
        x = x.astype(bf16)[None]
        for b in reversed(range(bits)):
            bit = (q >> b) & 1
            other = swap(x, "plane", 1 << b, qn)
            pair = jnp.stack(
                [jnp.where(bit == 0, x, other), jnp.where(bit == 0, other, x)], axis=1
            )
            x = pair.reshape((2 * x.shape[0],) + x.shape[1:])
        x = x.reshape(rows, half)
        x = join_bit(c, x, swap(x, "core", 1, 2), 1).astype(f32)
        return (
            output[None],
            input_grad[None],
            x[:, 4 * d],
            x[:, :d],
            x[:, d : 2 * d],
            x[:, 2 * d : 3 * d],
            x[:, 3 * d : 4 * d],
            x[:, 4 * d + 1],
            x[:, 4 * d + 2 : 4 * d + 2 + EXPERTS],
            expert_grads[0],
            expert_grads[1],
            expert_grads[2],
            shared_done[0],
            shared_done[1],
            shared_done[2],
        )

    return shards


def solution(mesh):
    n, replicas = mesh.shape["shard"], mesh.shape["replica"]
    fine = Mesh(mesh.devices.reshape(n, replicas // 2, 2), ("shard", "plane", "core"))
    every = ("shard", "plane", "core")
    in_specs = (
        P(every, None, None),
        P(every, None, None),
        P(every, None),
        P(every, None),
        P(every, None, None),
        P(every, None),
        P("shard"),
        P("shard", None),
        P("shard", None),
        P("shard", None),
        P("shard", None),
        P("shard"),
        P("shard", None),
        P(None, "shard", None),
        P(None, "shard", None),
        P(None, "shard", None),
        P("shard", None),
        P("shard", None),
        P("shard", None),
    )
    out_specs = (
        P(every, None, None),
        P(every, None, None),
        P("shard"),
        P("shard", None),
        P("shard", None),
        P("shard", None),
        P("shard", None),
        P("shard"),
        P("shard", None),
        P(None, "shard", None),
        P(None, "shard", None),
        P(None, "shard", None),
        P("shard", None),
        P("shard", None),
        P("shard", None),
    )
    return jax.shard_map(
        make_shards(n, replicas // 2),
        mesh=fine,
        in_specs=in_specs,
        out_specs=out_specs,
        check_vma=False,
    )
```

```python
import functools
import math

import jax
import jax.numpy as jnp
from jax import lax
from jax.experimental import pallas as pl
from jax.experimental.pallas import tpu as pltpu
from jax.sharding import Mesh, PartitionSpec as P

NH = 12
HD = 64
EXPERTS = 6
TOPK = 2
CAP = 96
EPSILON = 1e-06
NEGATIVE = -1e30
GROUPS = ((0, 1), (2, 3), (4, 5))

highest = lax.Precision.HIGHEST
f32 = jnp.float32
bf16 = jnp.bfloat16


def dot(spec, first, second):
    return jnp.einsum(spec, first, second, preferred_element_type=f32)


def rotate_half(values):
    half_size = values.shape[-1] // 2
    return jnp.concatenate([-values[..., half_size:], values[..., :half_size]], axis=-1)


def rotate_back(values):
    half_size = values.shape[-1] // 2
    return jnp.concatenate([values[..., half_size:], -values[..., :half_size]], axis=-1)


def rotary_tables(length, head_dim):
    positions = jnp.arange(length, dtype=f32)
    frequency = jnp.exp(
        jnp.arange(head_dim // 2, dtype=f32) * (-2.0 * math.log(10000.0) / head_dim)
    )
    angles = positions[:, None] * frequency[None, :]
    angles = jnp.concatenate([angles, angles], axis=1)
    return (jnp.cos(angles), jnp.sin(angles))


def attention_mask(segments, padding):
    places = jnp.arange(segments.shape[0])
    causal = places[None, :] <= places[:, None]
    shared_doc = segments[:, None] == segments[None, :]
    usable = (padding[None, :] == 1) | (places[None, :] == places[:, None])
    return causal & shared_doc & usable


def norm_factor(values):
    return lax.rsqrt(jnp.mean(values * values, axis=-1, keepdims=True) + EPSILON)


def norm_back(values, factor, norm_gain, gradient):
    scaled = gradient * norm_gain
    gain_grad = jnp.sum(gradient * values * factor, axis=0)
    input_part = factor * scaled - values * factor**3 * jnp.mean(
        scaled * values, axis=-1, keepdims=True
    )
    return (input_part, gain_grad)


def silu_parts(gate_act):
    sigmoid = jax.nn.sigmoid(gate_act)
    return (gate_act * sigmoid, sigmoid * (1.0 + gate_act * (1.0 - sigmoid)))


def pair_slots(routes, padding, priority):
    length = routes.shape[0]
    pair_expert = routes.T.reshape(-1)
    pair_live = jnp.tile(padding, TOPK) == 1
    pair_key = (jnp.arange(TOPK, dtype=jnp.int32)[:, None] * length + priority[None, :]).reshape(-1)
    earlier = (
        (pair_key[None, :] < pair_key[:, None])
        & (pair_expert[None, :] == pair_expert[:, None])
        & pair_live[None, :]
    )
    place = jnp.sum(earlier.astype(jnp.int32), axis=1)
    kept = pair_live & (place < CAP)
    return (pair_expert, place, kept)


def swap(values, axis, mask, size):
    return lax.ppermute(values, axis, [(i, i ^ mask) for i in range(size)])


def pick_index(values, index, axis=0):
    return lax.dynamic_index_in_dim(values, index, axis, keepdims=False)


def mm(first, second, contract):
    return lax.dot_general(
        first, second, (contract, ((), ())), preferred_element_type=f32
    )


NN = ((1,), (0,))
NT = ((1,), (1,))
TN = ((0,), (0,))


def flip(value, mask, size):
    out = 0
    for b in range(size.bit_length() - 1):
        bit = (value // (1 << b)) % 2
        out = out + (1 << b) * ((1 - bit) if (mask >> b) & 1 else bit)
    return out


MESH = pl.DeviceIdType.MESH


def moe_kernel(
    n,
    qn,
    length,
    slot_ref,
    router_ref,
    x_ref,
    g_ref,
    wg_ref,
    wu_ref,
    wd_ref,
    near_ref,
    far_ref,
    pick_ref,
    y_ref,
    t_ref,
    acc_y,
    acc_t,
    xs,
    gs,
    sg,
    dw,
    kept,
    sent,
    r1,
    r2,
    y_send,
    y_side,
    y_pair,
    y_in,
    gate_s,
    pick_s,
    pick_acc,
    pick_side,
    pick_pair,
    pick_in,
    send_sem,
    recv_sem,
    a2a_send,
    a2a_recv,
    local_sem,
    y_ssem,
    y_rsem,
    p_ssem,
    p_rsem,
):
    step = pl.program_id(0)
    total = EXPERTS + 1
    group = 2 * n
    d = x_ref.shape[1]
    piece = d // (n * qn)
    s, q, c = (lax.axis_index(a) for a in ("shard", "plane", "core"))
    near_q, far_q = flip(q, 1, qn), flip(q, 2, qn)
    other_c = 1 - c

    def remote(src, dst, stage, e, to):
        return pltpu.make_async_remote_copy(
            src,
            dst,
            send_sem.at[stage, e],
            recv_sem.at[stage, e],
            device_id=to,
            device_id_type=MESH,
        )

    def halve_near(e):
        return remote(sent.at[e], r1.at[e], 0, e, {"plane": near_q})

    def halve_far(e):
        return remote(kept.at[e, 1], r2.at[e], 1, e, {"plane": far_q})

    def across(e, m):
        return pltpu.make_async_remote_copy(
            kept.at[e, 0, m],
            near_ref.at[e, 0, m],
            a2a_send.at[m - 1, e],
            a2a_recv.at[m - 1, e],
            device_id={"shard": flip(s, m, n)},
            device_id_type=MESH,
        )

    def stay(e):
        return pltpu.make_async_copy(kept.at[e, 0, 0], near_ref.at[e, 0, 0], local_sem.at[e])

    def double_far(e):
        return remote(near_ref.at[e, 0], near_ref.at[e, 1], 2, e, {"plane": far_q})

    def double_near(e):
        return remote(
            near_ref.at[e, pl.ds(0, 2)], near_ref.at[e, pl.ds(2, 2)], 3, e, {"plane": near_q}
        )

    def side(e):
        return remote(near_ref.at[e], far_ref.at[e], 4, e, {"core": other_c})

    def y_side_copy():
        return pltpu.make_async_remote_copy(
            y_send,
            y_side,
            y_ssem.at[0],
            y_rsem.at[0],
            device_id={"core": other_c},
            device_id_type=MESH,
        )

    def y_across(m):
        return pltpu.make_async_remote_copy(
            y_pair.at[m - 1],
            y_in.at[m - 1],
            y_ssem.at[m],
            y_rsem.at[m],
            device_id={"shard": flip(s, m, n)},
            device_id_type=MESH,
        )

    @pl.when(step == 0)
    def _():
        barrier = pltpu.get_barrier_semaphore()
        peers = [{"plane": near_q}, {"plane": far_q}, {"core": other_c}]
        peers += [{"shard": flip(s, m, n)} for m in range(1, n)]
        for peer in peers:
            pl.semaphore_signal(barrier, 1, device_id=peer, device_id_type=MESH)
        pl.semaphore_wait(barrier, len(peers))
        acc_y[...] = jnp.zeros_like(acc_y)
        acc_t[...] = jnp.zeros_like(acc_t)
        pick_acc[...] = jnp.zeros_like(pick_acc)

    def branch(x, gs_rows, wg, wu, wd):
        gate_act = mm(x, wg, NN)
        up_act = mm(x, wu, NN)
        sigmoid = 1.0 / (1.0 + jnp.exp(-gate_act))
        value = gate_act * sigmoid
        slope = sigmoid * (1.0 + gate_act * (1.0 - sigmoid))
        hid = (value * up_act).astype(bf16)
        hid_grad = mm(gs_rows, wd, NN)
        gate_d = (hid_grad * up_act * slope).astype(bf16)
        up_d = (hid_grad * value).astype(bf16)
        return hid, gate_d, up_d

    def pick_side_copy():
        return pltpu.make_async_remote_copy(
            pick_acc.at[pl.ds(n, n)],
            pick_side,
            p_ssem.at[0],
            p_rsem.at[0],
            device_id={"core": other_c},
            device_id_type=MESH,
        )

    def pick_across(m):
        return pltpu.make_async_remote_copy(
            pick_pair.at[m - 1],
            pick_in.at[m - 1],
            p_ssem.at[m],
            p_rsem.at[m],
            device_id={"shard": flip(s, m, n)},
            device_id_type=MESH,
        )

    @pl.when(step < EXPERTS)
    def _():
        ids = lax.broadcasted_iota(jnp.int32, (CAP, length), 0) + step * CAP

        def slots_of(b):
            first, second = slot_ref[b, 0:1, :], slot_ref[b, 1:2, :]
            return (first == ids) | (second == ids)

        def gather(b, carry):
            slot = pl.ds(pl.multiple_of(b * CAP, 16), CAP)
            seq = pl.ds(pl.multiple_of(b * length, length), length)
            hit = slots_of(b)
            hot = hit.astype(f32).astype(bf16)
            row = router_ref[b, pl.ds(step + 2, 1), :]
            gate = jnp.sum(jnp.where(hit, row, 0.0), axis=1, keepdims=True)
            gate_s[slot, :] = gate
            xs[slot, :] = mm(hot, x_ref[seq, :], NN).astype(bf16)
            g_rows = mm(hot, g_ref[seq, :], NN)
            gs[slot, :] = g_rows.astype(bf16)
            sg[slot, :] = (g_rows * gate).astype(bf16)
            return carry

        lax.fori_loop(0, group, gather, 0)
        wg, wu, wd = wg_ref[0], wu_ref[0], wd_ref[0]
        x, slot_grad = xs[...], sg[...]
        hid, gate_d, up_d = branch(x, slot_grad, wg, wu, wd)
        dw[0] = mm(x, gate_d, TN)
        dw[1] = mm(x, up_d, TN)
        dw[2] = mm(slot_grad, hid, TN)
        e_out = mm(hid, wd, NT)
        pick_s[...] = jnp.sum(e_out * gs[...].astype(f32), axis=1, keepdims=True)
        gs[...] = (e_out * gate_s[...]).astype(bf16)
        xs[...] = (mm(gate_d, wg, NT) + mm(up_d, wu, NT)).astype(bf16)

        def scatter(b, carry):
            slot = pl.ds(pl.multiple_of(b * CAP, 16), CAP)
            seq = pl.ds(pl.multiple_of(b * length, length), length)
            hit = slots_of(b)
            hot = hit.astype(f32).astype(bf16)
            pick_acc[b, pl.ds(step + 2, 1), :] = jnp.sum(
                jnp.where(hit, pick_s[slot, :], 0.0), axis=0, keepdims=True
            )
            acc_y[seq, :] += mm(hot, gs[slot, :], TN)
            acc_t[seq, :] += mm(hot, xs[slot, :], TN)
            return carry

        lax.fori_loop(0, group, scatter, 0)

    @pl.when(step == EXPERTS)
    def _():
        dw[...] = jnp.zeros_like(dw)
        wg, wu, wd = wg_ref[0], wu_ref[0], wd_ref[0]

        def rows_step(i, carry):
            rows = pl.ds(pl.multiple_of(i * 2 * length, 2 * length), 2 * length)
            x, g = x_ref[rows, :], g_ref[rows, :]
            hid, gate_d, up_d = branch(x, g, wg, wu, wd)
            dw[0] += mm(x, gate_d, TN)
            dw[1] += mm(x, up_d, TN)
            dw[2] += mm(g, hid, TN)
            acc_y[rows, :] += mm(hid, wd, NT)
            acc_t[rows, :] += mm(gate_d, wg, NT) + mm(up_d, wu, NT)
            return carry

        lax.fori_loop(0, n, rows_step, 0)
        half = pl.ds(n * length, n * length)
        y_send[0] = acc_y[half, :].astype(bf16)
        y_send[1] = acc_t[half, :].astype(bf16)

    @pl.when(step < total)
    def _():
        for j in range(qn):
            into = kept if j < qn // 2 else sent
            for m in range(n):
                start = (flip(s, m, n) * qn + flip(q, reverse_bits(j, qn), qn)) * piece
                start = pl.multiple_of(start, 16)
                for k in range(3):
                    into[step, j % (qn // 2), m, k] = dw[k, pl.ds(start, piece), :].astype(bf16)
        halve_near(step).start()

    @pl.when(step == EXPERTS)
    def _():
        y_side_copy().start()
        pick_side_copy().start()

    def stage(delay, body):
        @pl.when((step >= delay) & (step < total + delay))
        def _():
            body(step - delay)

    def after_near(e):
        halve_near(e).wait()
        for j in (1, 0):
            for m in range(n):
                kept[e, j, m] = (
                    kept[e, j, m].astype(f32) + r1[e, j, m].astype(f32)
                ).astype(bf16)
        halve_far(e).start()

    def after_far(e):
        halve_far(e).wait()
        for m in range(n):
            kept[e, 0, m] = (kept[e, 0, m].astype(f32) + r2[e, m].astype(f32)).astype(bf16)
        for m in range(1, n):
            across(e, m).start()
        stay(e).start()

    def after_across(e):
        for m in range(1, n):
            across(e, m).wait()
        stay(e).wait()
        double_far(e).start()

    def after_double_far(e):
        double_far(e).wait()
        double_near(e).start()

    def after_double_near(e):
        double_near(e).wait()
        side(e).start()

    stage(1, after_near)
    stage(2, after_far)
    stage(3, after_across)
    stage(4, after_double_far)

    @pl.when(step == total)
    def _():
        y_side_copy().wait()
        pick_side_copy().wait()
        pick_acc[pl.ds(0, n)] += pick_side[...]
        for m in range(1, n):
            pick_pair[m - 1] = pick_acc[m]
        rows = pl.ds(0, length)
        for k, acc in enumerate((acc_y, acc_t)):
            acc[rows, :] += y_side[k, rows, :].astype(f32)
            for m in range(1, n):
                seq = pl.ds(m * length, length)
                y_pair[m - 1, k] = (acc[seq, :] + y_side[k, seq, :].astype(f32)).astype(bf16)
        for m in range(1, n):
            y_across(m).start()
            pick_across(m).start()

    @pl.when(step == total + 1)
    def _():
        for m in range(1, n):
            y_across(m).wait()
            pick_across(m).wait()
        picks = pick_acc[0]
        for m in range(1, n):
            picks = picks + pick_in[m - 1]
        pick_ref[...] = picks
        rows = pl.ds(0, length)
        for k, (acc, out) in enumerate(((acc_y, y_ref), (acc_t, t_ref))):
            value = acc[rows, :]
            for m in range(1, n):
                value = value + y_in[m - 1, k].astype(f32)
            out[...] = value

    stage(5, after_double_near)
    stage(6, lambda e: side(e).wait())


def moe_call(n, qn, length, slot, router, x, g, weights):
    d = x.shape[1]
    hb = weights[0].shape[2]
    rows = x.shape[0]
    slots = 2 * n * CAP
    total = EXPERTS + 1
    piece = d // (n * qn)
    once = pl.Buffered(1)
    meta = pl.BlockSpec((2 * n, 8, length), lambda t: (0, 0, 0))
    rows8 = pl.BlockSpec((8, length), lambda t: (0, 0))
    whole = pl.BlockSpec((rows, d), lambda t: (0, 0), pipeline_mode=once)
    weight = pl.BlockSpec((1, d, hb), lambda t: (jnp.minimum(t, EXPERTS), 0, 0))
    own = pl.BlockSpec((length, d), lambda t: (0, 0), pipeline_mode=once)
    anywhere = pl.BlockSpec(memory_space=pl.ANY)
    pieces = (total, qn, n, 3, piece, hb)
    dma = pltpu.SemaphoreType.DMA
    return pl.pallas_call(
        functools.partial(moe_kernel, n, qn, length),
        grid=(total + 6,),
        in_specs=[meta, meta, whole, whole, weight, weight, weight],
        out_specs=[anywhere, anywhere, rows8, own, own],
        scratch_shapes=[
            pltpu.VMEM((rows, d), f32),
            pltpu.VMEM((rows, d), f32),
            pltpu.VMEM((slots, d), bf16),
            pltpu.VMEM((slots, d), bf16),
            pltpu.VMEM((slots, d), bf16),
            pltpu.VMEM((3, d, hb), f32),
            pltpu.VMEM((total, qn // 2, n, 3, piece, hb), bf16),
            pltpu.VMEM((total, qn // 2, n, 3, piece, hb), bf16),
            pltpu.VMEM((total, qn // 2, n, 3, piece, hb), bf16),
            pltpu.VMEM((total, n, 3, piece, hb), bf16),
            pltpu.VMEM((2, n * length, d), bf16),
            pltpu.VMEM((2, n * length, d), bf16),
            pltpu.VMEM((n - 1, 2, length, d), bf16),
            pltpu.VMEM((n - 1, 2, length, d), bf16),
            pltpu.VMEM((slots, 1), f32),
            pltpu.VMEM((slots, 1), f32),
            pltpu.VMEM((2 * n, 8, length), f32),
            pltpu.VMEM((n, 8, length), f32),
            pltpu.VMEM((n - 1, 8, length), f32),
            pltpu.VMEM((n - 1, 8, length), f32),
            dma((5, total)),
            dma((5, total)),
            dma((n - 1, total)),
            dma((n - 1, total)),
            dma((total,)),
            dma((n,)),
            dma((n,)),
            dma((n,)),
            dma((n,)),
        ],
        out_shape=[
            jax.ShapeDtypeStruct(pieces, bf16),
            jax.ShapeDtypeStruct(pieces, bf16),
            jax.ShapeDtypeStruct((8, length), f32),
            jax.ShapeDtypeStruct((length, d), f32),
            jax.ShapeDtypeStruct((length, d), f32),
        ],
        compiler_params=pltpu.CompilerParams(
            vmem_limit_bytes=63 << 20, collective_id=0, has_side_effects=True
        ),
        cost_estimate=pl.CostEstimate(
            flops=18 * total * slots * d * hb, bytes_accessed=200 << 20, transcendentals=0
        ),
        name="moe",
    )(slot, router, x, g, *weights)


def attention_forward(tokens, small, weight, allowed, cosine, sine, half_way, outs):
    q_ref, k_ref, v_ref, att_ref, one_ref, two_ref, mid_ref, soft_ref, router_ref = outs
    length, d = tokens.shape
    pair = 2 * HD
    small_rows = jnp.transpose(small[...].astype(f32))
    gain_one, gain_two = small_rows[0:1, :], small_rows[1:2, :]
    x = tokens[...].astype(f32)
    one = (x * lax.rsqrt(jnp.mean(x * x, axis=1, keepdims=True) + EPSILON) * gain_one).astype(bf16)
    one_ref[...] = one
    lane = lax.broadcasted_iota(jnp.int32, (length, pair), 1)
    lower = lane % HD < HD // 2
    cos, sin = cosine[...], sine[...]
    for i, ref in enumerate((q_ref, k_ref, v_ref)):
        for p in range(d // pair):
            cut = slice(p * pair, (p + 1) * pair)
            value = mm(one, weight(i)[:, cut], NN)
            if i < 2:
                up = pltpu.roll(value, pair - HD // 2, 1)
                down = pltpu.roll(value, HD // 2, 1)
                value = value * cos + jnp.where(lower, -up, down) * sin
            ref[:, cut] = value.astype(bf16)
    half_way()
    first = lane < HD

    def heads(p, carry):
        cut = pl.ds(pl.multiple_of(p * pair, pair), pair)
        queries, keys, values = q_ref[:, cut], k_ref[:, cut], v_ref[:, cut]
        parts = []
        for side in range(2):
            mine = first if side == 0 else jnp.logical_not(first)
            chosen = jnp.where(mine, queries.astype(f32), 0.0).astype(bf16)
            scores = mm(chosen, keys, NT) * HD ** (-0.5)
            scores = jnp.where(allowed[...] > 0.0, scores, NEGATIVE)
            exponent = jnp.exp(scores - jnp.max(scores, axis=1, keepdims=True))
            soft = exponent / jnp.sum(exponent, axis=1, keepdims=True)
            soft_ref[2 * p + side] = soft
            parts.append(mm(soft.astype(bf16), values, NN))
        att_ref[:, cut] = jnp.where(first, parts[0], parts[1]).astype(bf16)
        return carry

    lax.fori_loop(0, d // pair, heads, 0)
    middle = x + mm(att_ref[...], weight(3)[...], NN)
    mid_ref[...] = middle
    two = middle * lax.rsqrt(jnp.mean(middle * middle, axis=1, keepdims=True) + EPSILON) * gain_two
    two = two.astype(bf16)
    two_ref[...] = two
    logits = mm(two, small[...], NN)
    column = lax.broadcasted_iota(jnp.int32, logits.shape, 1)
    valid = (column >= 2) & (column < 2 + EXPERTS)
    logits = jnp.where(valid, logits, NEGATIVE)
    exponent = jnp.exp(logits - jnp.max(logits, axis=1, keepdims=True))
    exponent = jnp.where(valid, exponent, 0.0)
    router = exponent / jnp.sum(exponent, axis=1, keepdims=True)
    router_ref[...] = router
    return router


def front_kernel(
    n,
    qn,
    tokens,
    cot,
    cot_hbm,
    small_own,
    attn_own,
    slot_own,
    allowed,
    cosine,
    sine,
    eg,
    eu,
    ed,
    sg,
    su,
    sd,
    x_all,
    g_all,
    slot_all,
    router_all,
    w_gate,
    w_up,
    w_down,
    attn_all,
    small_all,
    q_ref,
    k_ref,
    v_ref,
    att_ref,
    one_ref,
    two_ref,
    mid_ref,
    soft_ref,
    router_ref,
    wide,
    small,
    full,
    two_buf,
    rt_buf,
    a_send,
    a_recv,
    s_send,
    s_recv,
    w_send,
    w_recv,
    z_send,
    z_recv,
    t_send,
    t_recv,
    side_send,
    side_recv,
    local_sem,
):
    s, q, c = (lax.axis_index(a) for a in ("shard", "plane", "core"))
    rows = small_own.shape[0]
    d = tokens.shape[1]
    hb = full.shape[3]
    part = rows // 2
    parity = q % 2
    near_q, other_c = flip(q, 1, qn), 1 - c
    shards_to = [None] + [flip(s, m, n) for m in range(1, n)]

    def send(src, dst, ssem, rsem, to):
        return pltpu.make_async_remote_copy(
            src, dst, ssem, rsem, device_id=to, device_id_type=MESH
        )

    barrier = pltpu.get_barrier_semaphore()
    peers = [{"plane": near_q}, {"core": other_c}]
    peers += [{"shard": shards_to[m]} for m in range(1, n)]
    for peer in peers:
        pl.semaphore_signal(barrier, 1, device_id=peer, device_id_type=MESH)
    pl.semaphore_wait(barrier, len(peers))

    mine = pl.ds(2 * c, 2)
    my_rows = pl.ds(pl.multiple_of(s * rows, 16), rows)
    attn = [
        send(
            attn_own.at[mine],
            wide.at[mine, my_rows],
            a_send.at[m - 1],
            a_recv.at[m - 1],
            {"shard": shards_to[m]},
        )
        for m in range(1, n)
    ]
    smalls = [
        send(
            small_own, small.at[my_rows], s_send.at[m - 1], s_recv.at[m - 1], {"shard": shards_to[m]}
        )
        for m in range(1, n)
    ]
    for copy in smalls + attn:
        copy.start()
    keep_attn = pltpu.make_async_copy(attn_own.at[mine], wide.at[mine, my_rows], local_sem.at[0])
    keep_small = pltpu.make_async_copy(small_own, small.at[my_rows], local_sem.at[1])
    keep_attn.start()
    keep_small.start()

    half_rows = pl.ds(pl.multiple_of(parity * part, 16), part)
    half_at = pl.ds(pl.multiple_of(s * rows + parity * part, 16), part)
    experts = pl.ds(0, EXPERTS)

    def columns(m):
        owner = s if m == 0 else shards_to[m]
        return pl.ds(pl.multiple_of((owner * 2 + c) * hb, 128), hb)

    def weight_sends(k):
        big, one = ((eg, sg), (eu, su), (ed, sd))[k]
        copies = []
        for m in range(1, n):
            copies.append(
                send(
                    big.at[:, half_rows, columns(m)],
                    full.at[k, experts, half_at],
                    w_send.at[k, m - 1, 0],
                    w_recv.at[k, m - 1, 0],
                    {"shard": shards_to[m]},
                )
            )
            copies.append(
                send(
                    one.at[half_rows, columns(m)],
                    full.at[k, EXPERTS, half_at],
                    w_send.at[k, m - 1, 1],
                    w_recv.at[k, m - 1, 1],
                    {"shard": shards_to[m]},
                )
            )
        return copies

    def pair_sends(k):
        copies = []
        for m in range(1, n):
            at = pl.ds(pl.multiple_of(shards_to[m] * rows + parity * part, 16), part)
            copies.append(
                send(
                    full.at[k, :, at],
                    full.at[k, :, at],
                    z_send.at[k, m - 1],
                    z_recv.at[k, m - 1],
                    {"plane": near_q},
                )
            )
        return copies

    keep_weights = []
    for k, (big, one) in enumerate(((eg, sg), (eu, su), (ed, sd))):
        keep_weights.append(
            pltpu.make_async_copy(
                big.at[:, :, columns(0)], full.at[k, experts, my_rows], local_sem.at[2 + 2 * k]
            )
        )
        keep_weights.append(
            pltpu.make_async_copy(
                one.at[:, columns(0)], full.at[k, EXPERTS, my_rows], local_sem.at[3 + 2 * k]
            )
        )
    for copy in keep_weights:
        copy.start()
    weights = [weight_sends(k) for k in range(3)]
    for k in range(3):
        for copy in weights[k]:
            copy.start()

    def token_sends(i, src, dst):
        return [
            send(src, dst.at[m], t_send.at[i, m - 1], t_recv.at[i, m - 1], {"shard": shards_to[m]})
            for m in range(1, n)
        ]

    def side_send_of(i, ref):
        return send(
            ref.at[pl.ds(0, n)],
            ref.at[pl.ds(n, n)],
            side_send.at[i],
            side_recv.at[i],
            {"core": other_c},
        )

    g_copies = token_sends(0, cot_hbm, g_all)
    slot_copies = token_sends(1, slot_own, slot_all)
    for copy in slot_copies + g_copies:
        copy.start()
    keep_g = pltpu.make_async_copy(cot, g_all.at[0], local_sem.at[8])
    keep_slot = pltpu.make_async_copy(slot_own, slot_all.at[0], local_sem.at[9])
    keep_g.start()
    keep_slot.start()

    keep_attn.wait()
    for copy in attn:
        copy.wait()
    attn_side = send(wide.at[mine], wide.at[mine], side_send.at[0], side_recv.at[0], {"core": other_c})
    attn_side.start()
    keep_small.wait()
    for copy in smalls:
        copy.wait()
    attn_side.wait()
    save_attn = pltpu.make_async_copy(wide, attn_all, local_sem.at[10])
    save_small = pltpu.make_async_copy(small, small_all, local_sem.at[11])
    save_attn.start()
    save_small.start()

    pairs = [pair_sends(k) for k in range(3)]

    def half_way():
        for copy in weights[0]:
            copy.wait()
        for copy in pairs[0]:
            copy.start()

    outs = (q_ref, k_ref, v_ref, att_ref, one_ref, two_buf, mid_ref, soft_ref, router_ref)
    router = attention_forward(
        tokens, small, lambda i: wide.at[i], allowed, cosine, sine, half_way, outs
    )
    rt_buf[...] = jnp.transpose(router)[0:8, :]
    two_ref[...] = two_buf[...]
    x_copies = token_sends(2, two_buf, x_all)
    rt_copies = token_sends(3, rt_buf, router_all)
    for copy in x_copies + rt_copies:
        copy.start()
    keep_x = pltpu.make_async_copy(two_buf, x_all.at[0], local_sem.at[12])
    keep_rt = pltpu.make_async_copy(rt_buf, router_all.at[0], local_sem.at[13])
    keep_x.start()
    keep_rt.start()
    for k in (1, 2):
        for copy in weights[k]:
            copy.wait()
        for copy in pairs[k]:
            copy.start()
    keep_g.wait()
    keep_slot.wait()
    for copy in slot_copies + g_copies:
        copy.wait()
    g_side, slot_side = side_send_of(1, g_all), side_send_of(2, slot_all)
    g_side.start()
    slot_side.start()
    keep_x.wait()
    keep_rt.wait()
    for copy in x_copies + rt_copies:
        copy.wait()
    x_side, rt_side = side_send_of(3, x_all), side_send_of(4, router_all)
    x_side.start()
    rt_side.start()
    for copy in keep_weights:
        copy.wait()
    saves = []
    for k, out in enumerate((w_gate, w_up, w_down)):
        for copy in pairs[k]:
            copy.wait()
        save = pltpu.make_async_copy(full.at[k], out, local_sem.at[14 + k])
        save.start()
        saves.append(save)
    for copy in (g_side, slot_side, x_side, rt_side, save_attn, save_small, *saves):
        copy.wait()


def front_call(n, qn, operands):
    tokens, _, _, small, attn, slot = operands[:6]
    eg = operands[9]
    length, d = tokens.shape
    rows = small.shape[0]
    hidden = eg.shape[2]
    hb = hidden // (2 * n)
    group = 2 * n
    anywhere = pl.BlockSpec(memory_space=pl.ANY)
    vmem = pl.BlockSpec(memory_space=pltpu.VMEM)
    dma = pltpu.SemaphoreType.DMA
    shape = jax.ShapeDtypeStruct
    wide_out = [shape((length, d), bf16)] * 6
    return pl.pallas_call(
        functools.partial(front_kernel, n, qn),
        in_specs=[vmem, vmem] + [anywhere] * 4 + [vmem] * 3 + [anywhere] * 6,
        out_specs=[anywhere] * 9 + [vmem] * 9,
        out_shape=[
            shape((group, length, d), bf16),
            shape((group, length, d), bf16),
            shape((group, 8, length), jnp.int32),
            shape((group, 8, length), f32),
            shape((EXPERTS + 1, d, hb), bf16),
            shape((EXPERTS + 1, d, hb), bf16),
            shape((EXPERTS + 1, d, hb), bf16),
            shape((4, d, d), bf16),
            shape((d, 128), bf16),
            *wide_out,
            shape((length, d), f32),
            shape((NH, length, length), f32),
            shape((length, 128), f32),
        ],
        scratch_shapes=[
            pltpu.VMEM((4, d, d), bf16),
            pltpu.VMEM((d, 128), bf16),
            pltpu.VMEM((3, EXPERTS + 1, d, hb), bf16),
            pltpu.VMEM((length, d), bf16),
            pltpu.VMEM((8, length), f32),
            dma((n - 1,)),
            dma((n - 1,)),
            dma((n - 1,)),
            dma((n - 1,)),
            dma((3, n - 1, 2)),
            dma((3, n - 1, 2)),
            dma((3, n - 1)),
            dma((3, n - 1)),
            dma((4, n - 1)),
            dma((4, n - 1)),
            dma((5,)),
            dma((5,)),
            dma((17,)),
        ],
        compiler_params=pltpu.CompilerParams(
            vmem_limit_bytes=56 << 20, collective_id=1, has_side_effects=True
        ),
        cost_estimate=pl.CostEstimate(
            flops=4 * 10**9, bytes_accessed=40 << 20, transcendentals=0
        ),
        name="front",
    )(*operands)


def reverse_bits(j, size):
    bits = size.bit_length() - 1
    return sum(((j >> b) & 1) << (bits - 1 - b) for b in range(bits))


def assemble_kernel(n, qn, where_ref, own_ref, far_ref, *outs):
    s, q, c = where_ref[0], where_ref[1], where_ref[2]
    piece, hb = own_ref.shape[4], own_ref.shape[5]
    for side, ref in enumerate((own_ref, far_ref)):
        for j in range(qn):
            for m in range(n):
                row = pl.multiple_of((q ^ reverse_bits(j, qn)) * piece, 8)
                column = pl.multiple_of(((s ^ m) * 2 + (c ^ side)) * hb, 128)
                for k in range(3):
                    outs[k][0, pl.ds(row, piece), pl.ds(column, hb)] = ref[
                        0, j, m, k
                    ].astype(f32)


def assemble(n, qn, where, own, far, first, count):
    piece, hb = own.shape[4], own.shape[5]
    rows, hidden = piece * qn, hb * 2 * n
    spec = pl.BlockSpec((1, qn, n, 3, piece, hb), lambda i, *_: (i + first, 0, 0, 0, 0, 0))
    return pl.pallas_call(
        functools.partial(assemble_kernel, n, qn),
        grid_spec=pltpu.PrefetchScalarGridSpec(
            num_scalar_prefetch=1,
            grid=(count,),
            in_specs=[spec, spec],
            out_specs=[pl.BlockSpec((1, rows, hidden), lambda i, *_: (i, 0, 0))] * 3,
        ),
        out_shape=[jax.ShapeDtypeStruct((count, rows, hidden), f32)] * 3,
        cost_estimate=pl.CostEstimate(
            flops=0, bytes_accessed=18 * count * rows * hidden, transcendentals=0
        ),
        name="assemble",
    )(where, own, far)


def make_plain(n, qn):
    bits = qn.bit_length() - 1

    def place_blocks(own, blocks):
        out = jnp.zeros((n,) + blocks[0].shape, blocks[0].dtype)
        for m in range(n):
            out = lax.dynamic_update_index_in_dim(out, blocks[m], own ^ m, 0)
        return out

    def join_bit(bit, own, other, axis):
        first = jnp.where(bit == 0, own, other)
        second = jnp.where(bit == 0, other, own)
        return jnp.concatenate([first, second], axis=axis)

    def shards(
        tokens,
        cotangent,
        segments,
        padding,
        routes,
        priority,
        attn_gain,
        query_weight,
        key_weight,
        value_weight,
        output_weight,
        ffn_gain,
        router_weight,
        expert_gate,
        expert_up,
        expert_down,
        shared_gate,
        shared_up,
        shared_down,
    ):
        s = lax.axis_index("shard")
        q = lax.axis_index("plane")
        c = lax.axis_index("core")
        length, d = tokens.shape[1], tokens.shape[2]
        rows = query_weight.shape[0]
        hidden = expert_gate.shape[2]
        hb = hidden // (2 * n)
        score_scale = HD ** (-0.5)

        small = jnp.concatenate(
            [attn_gain[:, None], ffn_gain[:, None], router_weight], axis=1
        )
        small = jnp.pad(small, ((0, 0), (0, 256 - small.shape[1])))
        wide = jnp.concatenate(
            [query_weight, key_weight, value_weight, output_weight, small], axis=1
        )
        half = wide.shape[1] // 2
        mine = lax.dynamic_slice_in_dim(wide, c * half, half, 1)
        blocks = [mine] + [swap(mine, "shard", m, n) for m in range(1, n)]
        mine = place_blocks(s, blocks).reshape(d, half)
        other = swap(mine, "core", 1, 2)
        wide = join_bit(c, mine, other, 1)
        wqkv, wo = wide[:, : 3 * d], wide[:, 3 * d : 4 * d]
        gain_one = wide[:, 4 * d].astype(f32)
        gain_two = wide[:, 4 * d + 1].astype(f32)
        wr = wide[:, 4 * d + 2 : 4 * d + 2 + EXPERTS]

        def block_for(m):
            start = ((s ^ m) * 2 + c) * hb
            cut = lambda w: lax.dynamic_slice_in_dim(w, start, hb, w.ndim - 1)
            return [
                jnp.concatenate([cut(e), cut(w)[None]], axis=0)
                for e, w in (
                    (expert_gate, shared_gate),
                    (expert_up, shared_up),
                    (expert_down, shared_down),
                )
            ]

        own_blocks = block_for(0)
        sent = [block_for(m) for m in range(1, n)]
        moe_w = []
        for k in range(3):
            got = [own_blocks[k]] + [swap(sent[m - 1][k], "shard", m, n) for m in range(1, n)]
            full = jnp.zeros((EXPERTS + 1, n, rows, hb), bf16)
            for m in range(n):
                full = lax.dynamic_update_index_in_dim(full, got[m], s ^ m, 1)
            moe_w.append(full.reshape(EXPERTS + 1, d, hb))

        def plane_gather(values):
            near = jnp.stack([values] + [swap(values, "shard", m, n) for m in range(1, n)])
            return jnp.concatenate([near, swap(near, "core", 1, 2)], axis=0)

        def plane_sum(partial):
            low = partial.astype(bf16)
            pair = (partial[:n] + swap(low[n:], "core", 1, 2).astype(f32)).astype(bf16)
            total = pair[0].astype(f32)
            for m in range(1, n):
                total = total + swap(pair[m], "shard", m, n).astype(f32)
            return total

        grads_b = plane_gather(cotangent[0])

        inputs = tokens[0].astype(f32)
        factor_one = norm_factor(inputs)
        normed_one = (inputs * factor_one * gain_one).astype(bf16)
        projected = jnp.dot(normed_one, wqkv, preferred_element_type=f32)
        cosine, sine = rotary_tables(length, HD)
        heads = projected.reshape(length, 3, NH, HD)
        cos_b, sin_b = cosine[:, None, :], sine[:, None, :]
        queries = (heads[:, 0] * cos_b + rotate_half(heads[:, 0]) * sin_b).astype(bf16)
        keys_rot = (heads[:, 1] * cos_b + rotate_half(heads[:, 1]) * sin_b).astype(bf16)
        values = heads[:, 2].astype(bf16)
        allowed = attention_mask(segments[0], padding[0])
        logits = dot("qhd,khd->hqk", queries, keys_rot) * score_scale
        logits = jnp.where(allowed[None], logits, NEGATIVE)
        maxima = jnp.max(logits, axis=-1, keepdims=True)
        exponent = jnp.exp(logits - maxima)
        soft = exponent / jnp.sum(exponent, axis=-1, keepdims=True)
        probs = soft.astype(bf16)
        attended = dot("hqk,khd->qhd", probs, values).reshape(length, d).astype(bf16)
        middle = inputs + jnp.dot(attended, wo, preferred_element_type=f32)
        factor_two = norm_factor(middle)
        normed_two = (middle * factor_two * gain_two).astype(bf16)
        router = jax.nn.softmax(
            jnp.dot(normed_two, wr, preferred_element_type=f32), axis=-1
        )

        pair_expert, place, kept = pair_slots(routes[0], padding[0], priority[0])
        slot_total = EXPERTS * CAP
        slot_index = jnp.where(kept, pair_expert * CAP + place, -1).reshape(TOPK, length)
        slots = jnp.arange(slot_total, dtype=jnp.int32)
        hit = (slots[None, :, None] == slot_index[:, None, :]).any(axis=0)
        onehot = hit.astype(bf16)
        token_of = jnp.max(
            jnp.where(hit, jnp.arange(length, dtype=jnp.int32)[None, :], -1), axis=1
        )
        slot_expert = jnp.repeat(jnp.arange(EXPERTS), CAP)
        gate_of = jnp.sum(
            jnp.where(hit, jnp.repeat(router.T, CAP, axis=0), 0.0), axis=1
        )

        tokens_b = plane_gather(normed_two)
        token_of_b = plane_gather(token_of)
        gate_of_b = plane_gather(gate_of)
        group = 2 * n
        onehot_b = (
            token_of_b[:, :, None] == jnp.arange(length, dtype=jnp.int32)[None, None, :]
        ).astype(bf16)
        onehot_b = onehot_b.reshape(group, EXPERTS, CAP, length)
        gate_b = gate_of_b.reshape(group, EXPERTS, CAP, 1)

        def reduce_and_return(stack):
            k = stack.shape[0]
            piece = rows // qn
            x = stack.reshape((k, n) + (2,) * bits + (piece, hb))
            for b in range(bits):
                axis = 2 + (bits - 1 - b)
                bit = (q >> b) & 1
                keep = pick_index(x, bit, axis)
                send = pick_index(x, 1 - bit, axis).astype(bf16)
                x = keep + swap(send, "plane", 1 << b, qn).astype(f32)
            x = x.astype(bf16)
            own = pick_index(x, s, 1)
            got = [own] + [swap(pick_index(x, s ^ m, 1), "shard", m, n) for m in range(1, n)]
            x = jnp.stack(got)
            x = x[None]
            for b in reversed(range(bits)):
                bit = (q >> b) & 1
                other = swap(x, "plane", 1 << b, qn)
                lead = x.shape[0]
                pair = jnp.stack(
                    [jnp.where(bit == 0, x, other), jnp.where(bit == 0, other, x)], axis=1
                )
                x = pair.reshape((2 * lead,) + x.shape[1:])
            other = swap(x, "core", 1, 2)
            x = jnp.stack(
                [jnp.where(c == 0, x, other), jnp.where(c == 0, other, x)]
            )
            out = jnp.zeros((n,) + (2, qn, k, piece, hb), bf16)
            for m in range(n):
                out = lax.dynamic_update_index_in_dim(out, x[:, :, m], s ^ m, 0)
            return out.transpose(3, 2, 4, 0, 1, 5).reshape(k, rows, hidden).astype(f32)

        w_gate, w_up, w_down = moe_w
        tokens_f = tokens_b.reshape(group * length, d)
        grads_f = grads_b.reshape(group * length, d)
        shared_g = jnp.dot(tokens_f, w_gate[EXPERTS], preferred_element_type=f32)
        shared_u = jnp.dot(tokens_f, w_up[EXPERTS], preferred_element_type=f32)
        value, slope = silu_parts(shared_g)
        shared_hidden = (value * shared_u).astype(bf16)
        shared_q = jnp.dot(grads_f, w_down[EXPERTS], preferred_element_type=f32)
        shared_gd = (shared_q * shared_u * slope).astype(bf16)
        shared_ud = (shared_q * value).astype(bf16)
        shared_grads = jnp.stack(
            [
                dot("ld,lh->dh", tokens_f, shared_gd),
                dot("ld,lh->dh", tokens_f, shared_ud),
                dot("ld,lh->dh", grads_f, shared_hidden),
            ]
        )
        out_partial = dot("lh,dh->ld", shared_hidden, w_down[EXPERTS])
        two_partial = dot("lh,dh->ld", shared_gd, w_gate[EXPERTS]) + dot(
            "lh,dh->ld", shared_ud, w_up[EXPERTS]
        )
        out_partial = out_partial.reshape(group, length, d)
        two_partial = two_partial.reshape(group, length, d)
        shared_done = reduce_and_return(shared_grads)

        pick_parts = []
        expert_done = []
        for part in GROUPS:
            lo, hi = part[0], part[-1] + 1
            hot = onehot_b[:, lo:hi]
            x_in = jnp.einsum("bect,btd->ebcd", hot, tokens_b, preferred_element_type=bf16)
            g_in = jnp.einsum("bect,btd->ebcd", hot, grads_b, preferred_element_type=bf16)
            gate_e = jnp.swapaxes(gate_b[:, lo:hi], 0, 1)
            wg, wu, wd = w_gate[lo:hi], w_up[lo:hi], w_down[lo:hi]
            gate_act = dot("ebcd,edh->ebch", x_in, wg)
            up_act = dot("ebcd,edh->ebch", x_in, wu)
            value, slope = silu_parts(gate_act)
            hid = (value * up_act).astype(bf16)
            e_out = dot("ebch,edh->ebcd", hid, wd)
            pick_parts.append(jnp.sum(e_out * g_in.astype(f32), axis=-1))
            slot_grad = (gate_e * g_in.astype(f32)).astype(bf16)
            hid_grad = dot("ebcd,edh->ebch", slot_grad, wd)
            gate_d = (hid_grad * up_act * slope).astype(bf16)
            up_d = (hid_grad * value).astype(bf16)
            in_grad = dot("ebch,edh->ebcd", gate_d, wg) + dot("ebch,edh->ebcd", up_d, wu)
            weighted = (gate_e * e_out).astype(bf16)
            out_partial = out_partial + dot("bect,ebcd->btd", hot, weighted)
            two_partial = two_partial + dot("bect,ebcd->btd", hot, in_grad.astype(bf16))
            stack = jnp.concatenate(
                [
                    dot("ebcd,ebch->edh", x_in, gate_d),
                    dot("ebcd,ebch->edh", x_in, up_d),
                    dot("ebcd,ebch->edh", slot_grad, hid),
                ]
            )
            expert_done.append(reduce_and_return(stack))

        two_grad = plane_sum(two_partial)
        picks = jnp.concatenate(pick_parts, axis=0)
        picks = jnp.swapaxes(picks, 0, 1).reshape(group, slot_total)
        picks = picks[:n] + swap(picks[n:], "core", 1, 2)
        pick_slot = picks[0]
        for m in range(1, n):
            pick_slot = pick_slot + swap(picks[m], "shard", m, n)
        mixed = plane_sum(out_partial)
        output = (middle + mixed).astype(bf16)

        upstream = cotangent[0].astype(f32)
        pick_grad = jnp.sum(
            jnp.where(hit, pick_slot[:, None], 0.0).reshape(EXPERTS, CAP, length), axis=1
        ).T
        logit_grad = router * (pick_grad - jnp.sum(router * pick_grad, axis=1, keepdims=True))
        two_grad = two_grad + jnp.dot(logit_grad, wr.astype(f32).T, precision=highest)
        router_grad = jnp.dot(normed_two.astype(f32).T, logit_grad, precision=highest)
        middle_part, ffn_gain_grad = norm_back(middle, factor_two, gain_two, two_grad)
        middle_grad = middle_part + upstream

        branch_grad = middle_grad.astype(bf16)
        output_weight_grad = dot("ld,le->de", attended, branch_grad)
        attended_grad = (
            dot("le,de->ld", branch_grad, wo).astype(bf16).reshape(length, NH, HD)
        )
        prob_grad = dot("qhd,khd->hqk", attended_grad, values)
        row_inner = jnp.sum(soft * prob_grad, axis=-1, keepdims=True)
        score_grad = (soft * (prob_grad - row_inner)).astype(bf16)
        query_parts = dot("hqk,khd->qhd", score_grad, keys_rot) * score_scale
        key_parts = dot("hqk,qhd->khd", score_grad, queries) * score_scale
        value_parts = dot("hqk,qhd->khd", probs, attended_grad)
        query_pre = query_parts * cos_b + rotate_back(query_parts * sin_b)
        key_pre = key_parts * cos_b + rotate_back(key_parts * sin_b)
        joint_grad = jnp.concatenate(
            [v.reshape(length, d) for v in (query_pre, key_pre, value_parts)], axis=1
        ).astype(bf16)
        one_grad = dot("lf,df->ld", joint_grad, wqkv)
        joint_weight_grad = dot("ld,lf->df", normed_one, joint_grad)
        input_part, attn_gain_grad = norm_back(inputs, factor_one, gain_one, one_grad)
        input_grad = (middle_grad + input_part).astype(bf16)

        small_grad = jnp.concatenate(
            [attn_gain_grad[:, None], ffn_gain_grad[:, None], router_grad], axis=1
        )
        small_grad = jnp.pad(small_grad, ((0, 0), (0, 256 - small_grad.shape[1])))
        total = jnp.concatenate([joint_weight_grad, output_weight_grad, small_grad], axis=1)
        keep = lax.dynamic_slice_in_dim(total, c * half, half, 1)
        send = lax.dynamic_slice_in_dim(total, (1 - c) * half, half, 1).astype(bf16)
        total = keep + swap(send, "core", 1, 2).astype(f32)
        total = total.reshape(n, rows, half)
        own = pick_index(total, s)
        low = total.astype(bf16)
        for m in range(1, n):
            own = own + swap(pick_index(low, s ^ m), "shard", m, n).astype(f32)
        x = own.reshape((2,) * bits + (rows // qn, half))
        for b in range(bits):
            axis = bits - 1 - b
            bit = (q >> b) & 1
            keep = pick_index(x, bit, axis)
            send = pick_index(x, 1 - bit, axis).astype(bf16)
            x = keep + swap(send, "plane", 1 << b, qn).astype(f32)
        x = x.astype(bf16)[None]
        for b in reversed(range(bits)):
            bit = (q >> b) & 1
            other = swap(x, "plane", 1 << b, qn)
            pair = jnp.stack(
                [jnp.where(bit == 0, x, other), jnp.where(bit == 0, other, x)], axis=1
            )
            x = pair.reshape((2 * x.shape[0],) + x.shape[1:])
        x = x.reshape(rows, half)
        x = join_bit(c, x, swap(x, "core", 1, 2), 1).astype(f32)
        stacks = [[], [], []]
        for part, done in zip(GROUPS, expert_done):
            for k in range(3):
                stacks[k].append(done[k * len(part) : (k + 1) * len(part)])
        expert_grads = [jnp.concatenate(parts, axis=0) for parts in stacks]
        return (
            output[None],
            input_grad[None],
            x[:, 4 * d],
            x[:, :d],
            x[:, d : 2 * d],
            x[:, 2 * d : 3 * d],
            x[:, 3 * d : 4 * d],
            x[:, 4 * d + 1],
            x[:, 4 * d + 2 : 4 * d + 2 + EXPERTS],
            expert_grads[0],
            expert_grads[1],
            expert_grads[2],
            shared_done[0],
            shared_done[1],
            shared_done[2],
        )

    return shards


def make_fast(n, qn):
    bits = qn.bit_length() - 1

    def shards(
        tokens,
        cotangent,
        segments,
        padding,
        routes,
        priority,
        attn_gain,
        query_weight,
        key_weight,
        value_weight,
        output_weight,
        ffn_gain,
        router_weight,
        expert_gate,
        expert_up,
        expert_down,
        shared_gate,
        shared_up,
        shared_down,
    ):
        s = lax.axis_index("shard")
        q = lax.axis_index("plane")
        c = lax.axis_index("core")
        length, d = tokens.shape[1], tokens.shape[2]
        rows = query_weight.shape[0]
        group = 2 * n
        score_scale = HD ** (-0.5)
        where = jnp.stack([s, q, c]).astype(jnp.int32)

        pair_expert, place, kept = pair_slots(routes[0], padding[0], priority[0])
        slot_index = jnp.where(kept, pair_expert * CAP + place, -1).reshape(TOPK, length)
        slot = jnp.pad(slot_index, ((0, 8 - TOPK), (0, 0)), constant_values=-1)
        allowed = attention_mask(segments[0], padding[0])
        cosine, sine = rotary_tables(length, HD)
        cos_b, sin_b = cosine[:, None, :], sine[:, None, :]
        small = jnp.concatenate([attn_gain[:, None], ffn_gain[:, None], router_weight], axis=1)
        small = jnp.pad(small, ((0, 0), (0, 128 - small.shape[1])))
        attn = jnp.stack([query_weight, key_weight, value_weight, output_weight])

        (
            x_all,
            g_all,
            slot_all,
            router_all,
            w_gate,
            w_up,
            w_down,
            wide,
            small_all,
            queries,
            keys_rot,
            values,
            attended,
            normed_one,
            normed_two,
            middle,
            soft,
            router_wide,
        ) = front_call(
            n,
            qn,
            (
                tokens[0],
                cotangent[0],
                cotangent[0],
                small,
                attn,
                slot,
                allowed.astype(f32),
                jnp.concatenate([cosine, cosine], axis=1),
                jnp.concatenate([sine, sine], axis=1),
                expert_gate,
                expert_up,
                expert_down,
                shared_gate,
                shared_up,
                shared_down,
            ),
        )
        near, far, picks, mixed, two_grad = moe_call(
            n,
            qn,
            length,
            slot_all,
            router_all,
            x_all.reshape(group * length, d),
            g_all.reshape(group * length, d),
            (w_gate, w_up, w_down),
        )
        expert_grads = assemble(n, qn, where, near, far, 0, EXPERTS)
        shared_done = [v[0] for v in assemble(n, qn, where, near, far, EXPERTS, 1)]
        output = (middle + mixed).astype(bf16)

        gain_one = small_all[:, 0].astype(f32)
        gain_two = small_all[:, 1].astype(f32)
        wr = small_all[:, 2 : 2 + EXPERTS]
        router = router_wide[:, 2 : 2 + EXPERTS]
        inputs = tokens[0].astype(f32)
        factor_one = norm_factor(inputs)
        factor_two = norm_factor(middle)
        upstream = cotangent[0].astype(f32)
        pick_grad = picks[2 : 2 + EXPERTS].T
        logit_grad = router * (pick_grad - jnp.sum(router * pick_grad, axis=1, keepdims=True))
        two_grad = two_grad + jnp.dot(logit_grad, wr.astype(f32).T, precision=highest)
        router_grad = jnp.dot(normed_two.astype(f32).T, logit_grad, precision=highest)
        middle_part, ffn_gain_grad = norm_back(middle, factor_two, gain_two, two_grad)
        middle_grad = middle_part + upstream

        branch_grad = middle_grad.astype(bf16)
        output_weight_grad = dot("ld,le->de", attended, branch_grad)
        attended_grad = dot("le,de->ld", branch_grad, wide[3]).astype(bf16)
        heads = lambda v: v.reshape(length, NH, HD)
        attended_grad = heads(attended_grad)
        probs = soft.astype(bf16)
        prob_grad = dot("qhd,khd->hqk", attended_grad, heads(values))
        row_inner = jnp.sum(soft * prob_grad, axis=-1, keepdims=True)
        score_grad = (soft * (prob_grad - row_inner)).astype(bf16)
        query_parts = dot("hqk,khd->qhd", score_grad, heads(keys_rot)) * score_scale
        key_parts = dot("hqk,qhd->khd", score_grad, heads(queries)) * score_scale
        value_parts = dot("hqk,qhd->khd", probs, attended_grad)
        query_pre = query_parts * cos_b + rotate_back(query_parts * sin_b)
        key_pre = key_parts * cos_b + rotate_back(key_parts * sin_b)
        pre = [v.reshape(length, d).astype(bf16) for v in (query_pre, key_pre, value_parts)]
        one_grad = sum(dot("lf,df->ld", pre[i], wide[i]) for i in range(3))
        weight_grads = [dot("ld,lf->df", normed_one, v) for v in pre]
        input_part, attn_gain_grad = norm_back(inputs, factor_one, gain_one, one_grad)
        input_grad = (middle_grad + input_part).astype(bf16)

        small_grad = jnp.concatenate(
            [attn_gain_grad[:, None], ffn_gain_grad[:, None], router_grad], axis=1
        )
        small_grad = jnp.pad(small_grad, ((0, 0), (0, 256 - small_grad.shape[1])))
        total = jnp.concatenate([*weight_grads, output_weight_grad, small_grad], axis=1)
        half = total.shape[1] // 2
        keep = lax.dynamic_slice_in_dim(total, c * half, half, 1)
        send = lax.dynamic_slice_in_dim(total, (1 - c) * half, half, 1).astype(bf16)
        total = keep + swap(send, "core", 1, 2).astype(f32)
        total = total.reshape(n, rows, half)
        own = pick_index(total, s)
        low = total.astype(bf16)
        for m in range(1, n):
            own = own + swap(pick_index(low, s ^ m), "shard", m, n).astype(f32)
        x = own.reshape((2,) * bits + (rows // qn, half))
        for b in range(bits):
            axis = bits - 1 - b
            bit = (q >> b) & 1
            keep = pick_index(x, bit, axis)
            send = pick_index(x, 1 - bit, axis).astype(bf16)
            x = keep + swap(send, "plane", 1 << b, qn).astype(f32)
        x = x.astype(bf16)[None]
        for b in reversed(range(bits)):
            bit = (q >> b) & 1
            other = swap(x, "plane", 1 << b, qn)
            pair = jnp.stack(
                [jnp.where(bit == 0, x, other), jnp.where(bit == 0, other, x)], axis=1
            )
            x = pair.reshape((2 * x.shape[0],) + x.shape[1:])
        x = x.reshape(rows, half)
        other = swap(x, "core", 1, 2)
        x = jnp.concatenate(
            [jnp.where(c == 0, x, other), jnp.where(c == 0, other, x)], axis=1
        ).astype(f32)
        return (
            output[None],
            input_grad[None],
            x[:, 4 * d],
            x[:, :d],
            x[:, d : 2 * d],
            x[:, 2 * d : 3 * d],
            x[:, 3 * d : 4 * d],
            x[:, 4 * d + 1],
            x[:, 4 * d + 2 : 4 * d + 2 + EXPERTS],
            expert_grads[0],
            expert_grads[1],
            expert_grads[2],
            shared_done[0],
            shared_done[1],
            shared_done[2],
        )

    return shards


def make_shards(n, qn):
    plain, fast = make_plain(n, qn), make_fast(n, qn)

    def shards(*arguments):
        d, hidden = arguments[0].shape[2], arguments[13].shape[2]
        fits = n == 4 and qn == 4 and d % (16 * n * qn) == 0 and hidden % (256 * n) == 0
        return (fast if fits else plain)(*arguments)

    return shards


def solution(mesh):
    n, replicas = mesh.shape["shard"], mesh.shape["replica"]
    fine = Mesh(mesh.devices.reshape(n, replicas // 2, 2), ("shard", "plane", "core"))
    every = ("shard", "plane", "core")
    in_specs = (
        P(every, None, None),
        P(every, None, None),
        P(every, None),
        P(every, None),
        P(every, None, None),
        P(every, None),
        P("shard"),
        P("shard", None),
        P("shard", None),
        P("shard", None),
        P("shard", None),
        P("shard"),
        P("shard", None),
        P(None, "shard", None),
        P(None, "shard", None),
        P(None, "shard", None),
        P("shard", None),
        P("shard", None),
        P("shard", None),
    )
    out_specs = (
        P(every, None, None),
        P(every, None, None),
        P("shard"),
        P("shard", None),
        P("shard", None),
        P("shard", None),
        P("shard", None),
        P("shard"),
        P("shard", None),
        P(None, "shard", None),
        P(None, "shard", None),
        P(None, "shard", None),
        P("shard", None),
        P("shard", None),
        P("shard", None),
    )
    return jax.shard_map(
        make_shards(n, replicas // 2),
        mesh=fine,
        in_specs=in_specs,
        out_specs=out_specs,
        check_vma=False,
    )
```

```python
import functools
import math

import jax
import jax.numpy as jnp
from jax import lax
from jax.experimental import pallas as pl
from jax.experimental.pallas import tpu as pltpu
from jax.sharding import Mesh, PartitionSpec as P

NH = 12
HD = 64
EXPERTS = 6
TOPK = 2
CAP = 96
EPSILON = 1e-06
NEGATIVE = -1e30
GROUPS = ((0, 1), (2, 3), (4, 5))

highest = lax.Precision.HIGHEST
f32 = jnp.float32
bf16 = jnp.bfloat16


def dot(spec, first, second):
    return jnp.einsum(spec, first, second, preferred_element_type=f32)


def rotate_half(values):
    half_size = values.shape[-1] // 2
    return jnp.concatenate([-values[..., half_size:], values[..., :half_size]], axis=-1)


def rotate_back(values):
    half_size = values.shape[-1] // 2
    return jnp.concatenate([values[..., half_size:], -values[..., :half_size]], axis=-1)


def rotary_tables(length, head_dim):
    positions = jnp.arange(length, dtype=f32)
    frequency = jnp.exp(
        jnp.arange(head_dim // 2, dtype=f32) * (-2.0 * math.log(10000.0) / head_dim)
    )
    angles = positions[:, None] * frequency[None, :]
    angles = jnp.concatenate([angles, angles], axis=1)
    return (jnp.cos(angles), jnp.sin(angles))


def attention_mask(segments, padding):
    places = jnp.arange(segments.shape[0])
    causal = places[None, :] <= places[:, None]
    shared_doc = segments[:, None] == segments[None, :]
    usable = (padding[None, :] == 1) | (places[None, :] == places[:, None])
    return causal & shared_doc & usable


def norm_factor(values):
    return lax.rsqrt(jnp.mean(values * values, axis=-1, keepdims=True) + EPSILON)


def norm_back(values, factor, norm_gain, gradient):
    scaled = gradient * norm_gain
    gain_grad = jnp.sum(gradient * values * factor, axis=0)
    input_part = factor * scaled - values * factor**3 * jnp.mean(
        scaled * values, axis=-1, keepdims=True
    )
    return (input_part, gain_grad)


def silu_parts(gate_act):
    sigmoid = jax.nn.sigmoid(gate_act)
    return (gate_act * sigmoid, sigmoid * (1.0 + gate_act * (1.0 - sigmoid)))


def pair_slots(routes, padding, priority):
    length = routes.shape[0]
    pair_expert = routes.T.reshape(-1)
    pair_live = jnp.tile(padding, TOPK) == 1
    pair_key = (jnp.arange(TOPK, dtype=jnp.int32)[:, None] * length + priority[None, :]).reshape(-1)
    earlier = (
        (pair_key[None, :] < pair_key[:, None])
        & (pair_expert[None, :] == pair_expert[:, None])
        & pair_live[None, :]
    )
    place = jnp.sum(earlier.astype(jnp.int32), axis=1)
    kept = pair_live & (place < CAP)
    return (pair_expert, place, kept)


def swap(values, axis, mask, size):
    return lax.ppermute(values, axis, [(i, i ^ mask) for i in range(size)])


def pick_index(values, index, axis=0):
    return lax.dynamic_index_in_dim(values, index, axis, keepdims=False)


def mm(first, second, contract):
    return lax.dot_general(
        first, second, (contract, ((), ())), preferred_element_type=f32
    )


NN = ((1,), (0,))
NT = ((1,), (1,))
TN = ((0,), (0,))


def flip(value, mask, size):
    out = 0
    for b in range(size.bit_length() - 1):
        bit = (value // (1 << b)) % 2
        out = out + (1 << b) * ((1 - bit) if (mask >> b) & 1 else bit)
    return out


MESH = pl.DeviceIdType.MESH


def moe_kernel(
    n,
    length,
    slot_ref,
    router_ref,
    x_hbm,
    g_hbm,
    wg_ref,
    wu_ref,
    wd_ref,
    soft_hbm,
    mid_hbm,
    wide_hbm,
    q_hbm,
    k_hbm,
    v_hbm,
    att_hbm,
    one_hbm,
    tok_hbm,
    probs_ref,
    small_ref,
    cos_ref,
    sin_ref,
    near_ref,
    far_ref,
    near_z,
    far_z,
    out_ref,
    in_grad_ref,
    xg,
    acc_y,
    acc_t,
    work,
    dw,
    own,
    land,
    swap_in,
    y_side,
    y_in,
    gate_s,
    pick_s,
    pick_acc,
    pick_side,
    pick_pair,
    pick_in,
    branch_s,
    ag_s,
    small_acc,
    z_own,
    z_land,
    z_swap,
    ch_send,
    ch_recv,
    x_send,
    x_recv,
    stay_sem,
    z_send,
    z_recv,
    zx_send,
    zx_recv,
    y_send_sem,
    y_recv_sem,
    p_send,
    p_recv,
    load_sem,
    free_side,
    free_in,
    gains_s,
    gains_side,
    gains_in,
):
    t = pl.program_id(0)
    group = 2 * n
    d = xg.shape[1]
    hb = dw.shape[2]
    part = d // (2 * n)
    chunks = 3 * (EXPERTS + 1)
    plane_rows = group * length
    s, q, c = (lax.axis_index(a) for a in ("shard", "plane", "core"))
    middle = (q == 1) | (q == 2)
    ends = (q == 0) | (q == 3)
    keep_h, give_h = (q + 1) % 2, q % 2
    other_mid = 3 - q
    mid_of = 1 + q // 3
    end_of = (q // 2) * 3
    other_c = 1 - c
    shard_of = [None] + [flip(s, m, n) for m in range(1, n)]

    def remote(src, dst, ssem, rsem, to):
        return pltpu.make_async_remote_copy(
            src, dst, ssem, rsem, device_id=to, device_id_type=MESH
        )

    def chunk(kind, src, dst, u, to):
        return remote(src, dst, ch_send.at[kind, u], ch_recv.at[kind, u], to)

    def to_mid(u):
        return chunk(0, own.at[u], land.at[u], u, {"plane": mid_of})

    def from_end(u):
        return chunk(0, own.at[u], land.at[u], u, {"plane": end_of})

    def swap_sums(u):
        return chunk(1, own.at[u, give_h], swap_in.at[u], u, {"plane": other_mid})

    def swap_done(u):
        return chunk(2, near_ref.at[u, keep_h], near_ref.at[u, keep_h], u, {"plane": other_mid})

    def swap_done_in(u):
        return chunk(2, near_ref.at[u, give_h], near_ref.at[u, give_h], u, {"plane": other_mid})

    def to_end(u, first):
        half = keep_h if first else give_h
        return chunk(
            3 if first else 4, near_ref.at[u, half], near_ref.at[u, half], u, {"plane": end_of}
        )

    def from_mid(u, first):
        half = (q // 3) if first else 1 - q // 3
        return chunk(
            3 if first else 4, near_ref.at[u, half], near_ref.at[u, half], u, {"plane": mid_of}
        )

    def across(u, m):
        return remote(
            own.at[u, keep_h, m],
            near_ref.at[u, keep_h, m],
            x_send.at[m - 1, u],
            x_recv.at[m - 1, u],
            {"shard": shard_of[m]},
        )

    def stay(u):
        return pltpu.make_async_copy(
            own.at[u, keep_h, 0], near_ref.at[u, keep_h, 0], stay_sem.at[u]
        )

    def side(u):
        return chunk(5, near_ref.at[u], far_ref.at[u], u, {"core": other_c})

    far_rows = pl.ds(0, plane_rows)

    def y_side_copy():
        return remote(
            work.at[far_rows], y_side, y_send_sem.at[0, 0], y_recv_sem.at[0, 0], {"core": other_c}
        )

    def y_across(k, m):
        at = pl.ds((k * n + m) * length, length)
        return remote(
            y_side.at[at],
            y_in.at[m - 1, k],
            y_send_sem.at[1 + k, m - 1],
            y_recv_sem.at[1 + k, m - 1],
            {"shard": shard_of[m]},
        )

    def pick_side_copy():
        return remote(
            pick_acc.at[pl.ds(n, n)], pick_side, p_send.at[0], p_recv.at[0], {"core": other_c}
        )

    def pick_across(m):
        return remote(
            pick_pair.at[m - 1],
            pick_in.at[m - 1],
            p_send.at[m],
            p_recv.at[m],
            {"shard": shard_of[m]},
        )

    def load(i, src, dst):
        return pltpu.make_async_copy(src, dst, load_sem.at[i])

    def tokens_in():
        return [
            load(0, x_hbm, xg.at[pl.ds(0, plane_rows)]),
            load(1, g_hbm, xg.at[pl.ds(plane_rows, plane_rows)]),
        ]

    def back_rows(i):
        return pl.ds(i * length, length)

    two_w = [length, length + d, plane_rows + length, plane_rows + length + d]

    def saved_in():
        copies = [
            load(2, soft_hbm, acc_y.at[pl.ds(n * length, n * length)]),
            load(3, mid_hbm, acc_t.at[pl.ds(n * length, length)]),
        ]
        for i in range(4):
            copies.append(load(4 + i, wide_hbm.at[i], xg.at[pl.ds(two_w[i], d)]))
        for i, ref in enumerate((q_hbm, k_hbm, v_hbm, att_hbm, one_hbm, tok_hbm)):
            copies.append(load(8 + i, ref, work.at[back_rows(i)]))
        return copies

    @pl.when(t == 0)
    def _():
        for copy in tokens_in():
            copy.start()
        barrier = pltpu.get_barrier_semaphore()
        peers = [{"core": other_c}] + [{"shard": shard_of[m]} for m in range(1, n)]
        for peer in peers:
            pl.semaphore_signal(barrier, 1, device_id=peer, device_id_type=MESH)

        @pl.when(middle)
        def _():
            for peer in ({"plane": other_mid}, {"plane": end_of}):
                pl.semaphore_signal(barrier, 1, device_id=peer, device_id_type=MESH)
            pl.semaphore_wait(barrier, len(peers) + 2)

        @pl.when(ends)
        def _():
            pl.semaphore_signal(
                barrier, 1, device_id={"plane": mid_of}, device_id_type=MESH
            )
            pl.semaphore_wait(barrier, len(peers) + 1)

        acc_y[...] = jnp.zeros_like(acc_y)
        acc_t[...] = jnp.zeros_like(acc_t)
        pick_acc[...] = jnp.zeros_like(pick_acc)
        for copy in tokens_in():
            copy.wait()

    def branch(x, gs_rows, wg, wu, wd):
        gate_act = mm(x, wg, NN)
        up_act = mm(x, wu, NN)
        sigmoid = 1.0 / (1.0 + jnp.exp(-gate_act))
        value = gate_act * sigmoid
        slope = sigmoid * (1.0 + gate_act * (1.0 - sigmoid))
        hid = (value * up_act).astype(bf16)
        hid_grad = mm(gs_rows, wd, NN)
        gate_d = (hid_grad * up_act * slope).astype(bf16)
        up_d = (hid_grad * value).astype(bf16)
        return hid, gate_d, up_d

    slots = group * CAP
    xs_at, gs_at, sg_at = 0, slots, 2 * slots

    @pl.when(t < EXPERTS)
    def _():
        ids = lax.broadcasted_iota(jnp.int32, (CAP, length), 0) + t * CAP

        def slots_of(b):
            first, second = slot_ref[b, 0:1, :], slot_ref[b, 1:2, :]
            return (first == ids) | (second == ids)

        for b in range(group):
            slot = pl.ds(b * CAP, CAP)
            hit = slots_of(b)
            hot = hit.astype(f32).astype(bf16)
            row = router_ref[b, pl.ds(t + 2, 1), :]
            gate = jnp.sum(jnp.where(hit, row, 0.0), axis=1, keepdims=True)
            gate_s[slot, :] = gate
            x_rows = mm(hot, xg[pl.ds(b * length, length), :], NN)
            work[pl.ds(xs_at + b * CAP, CAP), :] = x_rows.astype(bf16)
            g_rows = mm(hot, xg[pl.ds(plane_rows + b * length, length), :], NN)
            work[pl.ds(gs_at + b * CAP, CAP), :] = g_rows.astype(bf16)
            work[pl.ds(sg_at + b * CAP, CAP), :] = (g_rows * gate).astype(bf16)
        wg, wu, wd = wg_ref[0], wu_ref[0], wd_ref[0]
        x, slot_grad = work[pl.ds(xs_at, slots), :], work[pl.ds(sg_at, slots), :]
        hid, gate_d, up_d = branch(x, slot_grad, wg, wu, wd)
        dw[0] = mm(x, gate_d, TN)
        dw[1] = mm(x, up_d, TN)
        dw[2] = mm(slot_grad, hid, TN)
        e_out = mm(hid, wd, NT)
        g_rows = work[pl.ds(gs_at, slots), :].astype(f32)
        pick_s[...] = jnp.sum(e_out * g_rows, axis=1, keepdims=True)
        work[pl.ds(gs_at, slots), :] = (e_out * gate_s[...]).astype(bf16)
        work[pl.ds(xs_at, slots), :] = (mm(gate_d, wg, NT) + mm(up_d, wu, NT)).astype(bf16)
        for b in range(group):
            slot = pl.ds(b * CAP, CAP)
            seq = pl.ds(b * length, length)
            hit = slots_of(b)
            hot = hit.astype(f32).astype(bf16)
            pick_acc[b, pl.ds(t + 2, 1), :] = jnp.sum(
                jnp.where(hit, pick_s[slot, :], 0.0), axis=0, keepdims=True
            )
            acc_y[seq, :] += mm(hot, work[pl.ds(gs_at + b * CAP, CAP), :], TN)
            acc_t[seq, :] += mm(hot, work[pl.ds(xs_at + b * CAP, CAP), :], TN)

    @pl.when(t == EXPERTS)
    def _():
        dw[...] = jnp.zeros_like(dw)
        wg, wu, wd = wg_ref[0], wu_ref[0], wd_ref[0]

        def rows_step(i, carry):
            at = pl.multiple_of(i * 2 * length, 2 * length)
            rows = pl.ds(at, 2 * length)
            x, g = xg[rows, :], xg[pl.ds(plane_rows + at, 2 * length), :]
            hid, gate_d, up_d = branch(x, g, wg, wu, wd)
            dw[0] += mm(x, gate_d, TN)
            dw[1] += mm(x, up_d, TN)
            dw[2] += mm(g, hid, TN)
            acc_y[rows, :] += mm(hid, wd, NT)
            acc_t[rows, :] += mm(gate_d, wg, NT) + mm(up_d, wu, NT)
            return carry

        lax.fori_loop(0, n, rows_step, 0)
        half = pl.ds(n * length, n * length)
        work[pl.ds(0, n * length), :] = acc_y[half, :].astype(bf16)
        work[pl.ds(n * length, n * length), :] = acc_t[half, :].astype(bf16)

    def spread(k, unit):
        for h in range(2):
            for m in range(n):
                owner = s if m == 0 else shard_of[m]
                start = pl.multiple_of((owner * 2 + h) * part, 16)
                own[unit, h, m] = dw[k, pl.ds(start, part), :].astype(bf16)

    @pl.when(t <= EXPERTS)
    def _():
        for k in range(3):
            spread(k, 3 * t + k)

        @pl.when(ends)
        def _():
            for k in range(3):
                to_mid(3 * t + k).start()

    @pl.when(t == EXPERTS)
    def _():
        y_side_copy().start()
        pick_side_copy().start()

    def stage(delay, where, body):
        @pl.when((t >= delay) & (t < chunks + delay) & where)
        def _():
            body(t - delay)

    def add_halves(u):
        from_end(u).wait_recv()
        for h in range(2):
            for m in range(n):
                own[u, h, m] = (own[u, h, m].astype(f32) + land[u, h, m].astype(f32)).astype(bf16)
        swap_sums(u).start()

    def add_swapped(u):
        swap_sums(u).wait()
        for m in range(n):
            own[u, keep_h, m] = (
                own[u, keep_h, m].astype(f32) + swap_in[u, m].astype(f32)
            ).astype(bf16)
        for m in range(1, n):
            across(u, m).start()
        stay(u).start()

    def send_done(u):
        for m in range(1, n):
            across(u, m).wait()
        stay(u).wait()
        swap_done(u).start()
        to_end(u, True).start()

    def send_second(u):
        swap_done_in(u).wait_recv()
        to_end(u, False).start()
        side(u).start()

    def end_side(u):
        to_mid(u).wait_send()
        from_mid(u, True).wait_recv()
        from_mid(u, False).wait_recv()
        side(u).start()

    def middle_last(u):
        swap_done(u).wait_send()
        to_end(u, True).wait_send()
        to_end(u, False).wait_send()
        side(u).wait()

    mine_rows = pl.ds(0, length)
    mid_rows = pl.ds(n * length, length)
    grad_rows = pl.ds((n + 1) * length, length)

    @pl.when(t == EXPERTS + 5)
    def _():
        total = acc_y[mine_rows, :]
        for m in range(1, n):
            y_across(0, m).wait()
            total = total + y_in[m - 1, 0].astype(f32)
        out_ref[...] = (acc_t[mid_rows, :] + total).astype(bf16)
        pl.semaphore_signal(free_side, 1, device_id={"core": other_c}, device_id_type=MESH)
        for m in range(1, n):
            pl.semaphore_signal(free_in, 1, device_id={"shard": shard_of[m]}, device_id_type=MESH)

    stage(1, middle, add_halves)
    stage(2, middle, add_swapped)
    stage(3, middle, send_done)
    stage(4, middle, send_second)
    stage(5, ends, end_side)
    stage(6, middle, middle_last)
    stage(6, ends, lambda u: side(u).wait())

    @pl.when(t == EXPERTS + 1)
    def _():
        y_side_copy().wait()
        pick_side_copy().wait()
        for copy in saved_in():
            copy.start()
        pick_acc[pl.ds(0, n)] += pick_side[...]
        for m in range(1, n):
            pick_pair[m - 1] = pick_acc[m]
        for k, acc in ((1, acc_t), (0, acc_y)):
            for m in range(n):
                seq, at = pl.ds(m * length, length), pl.ds((k * n + m) * length, length)
                total = acc[seq, :] + y_side[at, :].astype(f32)
                if m == 0:
                    acc[seq, :] = total
                else:
                    y_side[at, :] = total.astype(bf16)
            for m in range(1, n):
                y_across(k, m).start()
                if k:
                    pick_across(m).start()

    pre_at = 6 * length
    exact = lax.Precision.HIGHEST

    @pl.when(t == EXPERTS + 3)
    def _():
        for m in range(1, n):
            y_across(1, m).wait()
            pick_across(m).wait()
        for copy in saved_in():
            copy.wait()
        two = acc_t[mine_rows, :]
        picks = pick_acc[0]
        for m in range(1, n):
            two = two + y_in[m - 1, 1].astype(f32)
            picks = picks + pick_in[m - 1]
        picks = jnp.concatenate([picks, jnp.zeros((120, length), f32)], axis=0)
        picks = jnp.transpose(picks)
        router = probs_ref[...]
        logit_grad = router * (picks - jnp.sum(router * picks, axis=1, keepdims=True))
        small = small_ref[...].astype(f32)
        gain_two = jnp.transpose(small)[1:2, :]
        two = two + lax.dot_general(
            logit_grad, small, (NT, ((), ())), precision=exact, preferred_element_type=f32
        )
        router_grad = lax.dot_general(
            logit_grad,
            xg[mine_rows, :].astype(f32),
            (TN, ((), ())),
            precision=exact,
            preferred_element_type=f32,
        )
        mid = acc_t[mid_rows, :]
        factor = lax.rsqrt(jnp.mean(mid * mid, axis=1, keepdims=True) + EPSILON)
        gain_grad = jnp.sum(two * mid * factor, axis=0, keepdims=True)
        row = lax.broadcasted_iota(jnp.int32, router_grad.shape, 0)
        small_acc[...] = jnp.where(row == 1, gain_grad, router_grad)
        scaled = two * gain_two
        grad = (
            xg[pl.ds(plane_rows, length), :].astype(f32)
            + factor * scaled
            - mid * (factor * factor * factor) * jnp.mean(scaled * mid, axis=1, keepdims=True)
        )
        acc_t[grad_rows, :] = grad
        branch_s[...] = grad.astype(bf16)
        ag_s[...] = mm(branch_s[...], xg[pl.ds(two_w[3], d), :], NT).astype(bf16)

    pair = 2 * HD

    @pl.when((t >= EXPERTS + 4) & (t < EXPERTS + 7))
    def _():
        lane = lax.broadcasted_iota(jnp.int32, (length, pair), 1)
        first = lane < HD
        lower = lane % HD < HD // 2
        cos, sin = cos_ref[...], sin_ref[...]

        def turn_back(w):
            y = w * sin
            up = pltpu.roll(y, pair - HD // 2, 1)
            down = pltpu.roll(y, HD // 2, 1)
            return w * cos + jnp.where(lower, up, -down)

        def heads(i, carry):
            p = 2 * (t - EXPERTS - 4) + i
            cut = pl.ds(pl.multiple_of(p * pair, pair), pair)
            queries, keys, values = (work[back_rows(j), cut] for j in range(3))
            grads = ag_s[:, cut]
            parts = []
            for one_side in range(2):
                h = 2 * p + one_side
                rows = pl.ds(pl.multiple_of(n * length + (h // 3) * length, length), length)
                columns = pl.ds(pl.multiple_of((h % 3) * length, length), length)
                soft = acc_y[rows, columns]
                mine = first if one_side == 0 else jnp.logical_not(first)
                chosen = jnp.where(mine, grads.astype(f32), 0.0).astype(bf16)
                prob_grad = mm(chosen, values, NT)
                inner = jnp.sum(soft * prob_grad, axis=1, keepdims=True)
                score_grad = (soft * (prob_grad - inner)).astype(bf16)
                parts.append(
                    (
                        mm(score_grad, keys, NN) * HD ** (-0.5),
                        mm(score_grad, queries, TN) * HD ** (-0.5),
                        mm(soft.astype(bf16), grads, TN),
                    )
                )
            joined = [jnp.where(first, parts[0][j], parts[1][j]) for j in range(3)]
            joined = [turn_back(joined[0]), turn_back(joined[1]), joined[2]]
            for j in range(3):
                work[pl.ds(pre_at + j * length, length), cut] = joined[j].astype(bf16)
            return carry

        lax.fori_loop(0, 2, heads, 0)

    two_d = 2 * d
    give_rows = pl.ds(pl.multiple_of((1 - c) * two_d, 16), two_d)

    def attn_side():
        return [
            remote(
                xg.at[give_rows],
                y_side.at[pl.ds(0, two_d)],
                z_send.at[5],
                z_recv.at[5],
                {"core": other_c},
            ),
            remote(gains_s, gains_side, z_send.at[7], z_recv.at[7], {"core": other_c}),
        ]

    def attn_across(m):
        copies = []
        at = pl.multiple_of(shard_of[m] * 2 * part, 16)
        for i in range(2):
            copies.append(
                remote(
                    xg.at[pl.ds(pl.multiple_of(c * two_d + i * d + at, 16), 2 * part)],
                    y_in.at[m - 1, i, pl.ds(0, 2 * part)],
                    zx_send.at[m - 1, i],
                    zx_recv.at[m - 1, i],
                    {"shard": shard_of[m]},
                )
            )
        copies.append(
            remote(
                gains_s.at[pl.ds(at, 2 * part)],
                gains_in.at[m - 1],
                zx_send.at[m - 1, 2],
                zx_recv.at[m - 1, 2],
                {"shard": shard_of[m]},
            )
        )
        return copies

    @pl.when(t == EXPERTS + 7)
    def _():
        pre = [work[pl.ds(pre_at + j * length, length), :] for j in range(3)]
        one_grad = mm(pre[0], xg[pl.ds(two_w[0], d), :], NT)
        for j in (1, 2):
            one_grad = one_grad + mm(pre[j], xg[pl.ds(two_w[j], d), :], NT)
        x = work[back_rows(5), :].astype(f32)
        gain_one = jnp.transpose(small_ref[...].astype(f32))[0:1, :]
        factor = lax.rsqrt(jnp.mean(x * x, axis=1, keepdims=True) + EPSILON)
        gain_grad = jnp.sum(one_grad * x * factor, axis=0, keepdims=True)
        scaled = one_grad * gain_one
        in_grad_ref[...] = (
            acc_t[grad_rows, :]
            + factor * scaled
            - x * (factor * factor * factor) * jnp.mean(scaled * x, axis=1, keepdims=True)
        ).astype(bf16)
        gains = small_acc[...]
        row = lax.broadcasted_iota(jnp.int32, gains.shape, 0)
        gains_s[...] = jnp.transpose(jnp.where(row == 0, gain_grad, gains)).astype(bf16)
        for i in range(4):
            lhs = work[back_rows(4 if i < 3 else 3), :]
            for k in range(3):
                cut = slice(k * hb, (k + 1) * hb)
                rhs = work[pl.ds(pre_at + i * length, length), cut] if i < 3 else branch_s[:, cut]
                xg[pl.ds(i * d, d), cut] = mm(lhs, rhs, TN).astype(bf16)
        pl.semaphore_wait(free_side, 1)
        for copy in attn_side():
            copy.start()

    @pl.when(t == EXPERTS + 8)
    def _():
        for copy in attn_side():
            copy.wait()
        for i in range(8):
            rows = pl.ds(pl.multiple_of(c * two_d + i * (d // 4), 16), d // 4)
            other = y_side[pl.ds(i * (d // 4), d // 4), :]
            xg[rows, :] = (xg[rows, :].astype(f32) + other.astype(f32)).astype(bf16)
        gains_s[...] = (gains_s[...].astype(f32) + gains_side[...].astype(f32)).astype(bf16)
        pl.semaphore_wait(free_in, n - 1)
        for m in range(1, n):
            for copy in attn_across(m):
                copy.start()

    def z_copy(i, src, dst, to):
        return remote(src, dst, z_send.at[i], z_recv.at[i], to)

    def z_to_mid():
        return z_copy(0, z_own, z_land, {"plane": mid_of})

    def z_from_end():
        return z_copy(0, z_own, z_land, {"plane": end_of})

    def z_swap_sums():
        return z_copy(1, z_own.at[give_h], z_swap, {"plane": other_mid})

    def z_swap_done():
        return z_copy(2, z_own.at[keep_h], near_z.at[keep_h], {"plane": other_mid})

    def z_swap_done_in():
        return z_copy(2, z_own.at[give_h], near_z.at[give_h], {"plane": other_mid})

    def z_to_end(first):
        if first:
            return z_copy(3, z_own.at[keep_h], near_z.at[keep_h], {"plane": end_of})
        return z_copy(4, near_z.at[give_h], near_z.at[give_h], {"plane": end_of})

    def z_from_mid(first):
        half = (q // 3) if first else 1 - q // 3
        return z_copy(3 if first else 4, near_z.at[half], near_z.at[half], {"plane": mid_of})

    def z_stay():
        return pltpu.make_async_copy(z_own.at[keep_h], near_z.at[keep_h], load_sem.at[14])

    def z_side():
        return z_copy(6, near_z, far_z, {"core": other_c})

    @pl.when(t == Z_STEPS[0])
    def _():
        for m in range(1, n):
            for copy in attn_across(m):
                copy.wait()
        for h in range(2):
            at = pl.multiple_of(s * 2 * part + h * part, 16)
            for i in range(2):
                total = xg[pl.ds(pl.multiple_of(c * two_d + i * d + at, 16), part), :].astype(f32)
                for m in range(1, n):
                    total = total + y_in[m - 1, i, pl.ds(h * part, part), :].astype(f32)
                z_own[h, pl.ds(i * part, part), :] = total.astype(bf16)
            total = gains_s[pl.ds(at, part), :].astype(f32)
            for m in range(1, n):
                total = total + gains_in[m - 1, pl.ds(h * part, part), :].astype(f32)
            total = total.astype(bf16)
            for r in range(part // 16):
                z_own[h, 2 * part : 2 * part + 16, r * 128 : (r + 1) * 128] = total[
                    r * 16 : (r + 1) * 16, :
                ]

        @pl.when(ends)
        def _():
            z_to_mid().start()

    @pl.when((t == Z_STEPS[1]) & middle)
    def _():
        z_from_end().wait_recv()
        for h in range(2):
            z_own[h] = (z_own[h].astype(f32) + z_land[h].astype(f32)).astype(bf16)
        z_swap_sums().start()

    @pl.when((t == Z_STEPS[2]) & middle)
    def _():
        z_swap_sums().wait()
        z_own[keep_h] = (z_own[keep_h].astype(f32) + z_swap[...].astype(f32)).astype(bf16)
        z_stay().start()
        z_swap_done().start()
        z_to_end(True).start()

    @pl.when((t == Z_STEPS[3]) & middle)
    def _():
        z_swap_done_in().wait_recv()
        z_stay().wait()
        z_to_end(False).start()
        z_side().start()

    @pl.when((t == Z_STEPS[4]) & ends)
    def _():
        z_to_mid().wait_send()
        z_from_mid(True).wait_recv()
        z_from_mid(False).wait_recv()
        z_side().start()

    @pl.when(t == Z_STEPS[5])
    def _():
        z_side().wait()

        @pl.when(middle)
        def _():
            z_swap_done().wait_send()
            z_to_end(True).wait_send()
            z_to_end(False).wait_send()


Z_STEPS = (18, 23, 24, 25, 26, 27)


def moe_call(n, length, slot, router, x, g, weights, saved, extra):
    d = x.shape[1]
    hb = weights[0].shape[2]
    rows = x.shape[0]
    slots = 2 * n * CAP
    chunks = 3 * (EXPERTS + 1)
    part = d // (2 * n)
    steps = max(chunks + 7, Z_STEPS[5] + 1)
    once = pl.Buffered(1)

    def whole(shape):
        return pl.BlockSpec(shape, lambda t: (0,) * len(shape), pipeline_mode=once)

    weight = pl.BlockSpec((1, d, hb), lambda t: (jnp.minimum(t, EXPERTS), 0, 0))
    anywhere = pl.BlockSpec(memory_space=pl.ANY)
    dma = pltpu.SemaphoreType.DMA
    shape = jax.ShapeDtypeStruct
    pieces = (chunks, 2, n, part, hb)
    z_pieces = (2, 2 * part + 16, d)
    return pl.pallas_call(
        functools.partial(moe_kernel, n, length),
        grid=(steps,),
        in_specs=[whole(slot.shape), whole(router.shape), anywhere, anywhere]
        + [weight] * 3
        + [anywhere] * len(saved)
        + [whole(v.shape) for v in extra],
        out_specs=[anywhere] * 4 + [whole((length, d))] * 2,
        out_shape=[
            shape(pieces, bf16),
            shape(pieces, bf16),
            shape(z_pieces, bf16),
            shape(z_pieces, bf16),
            shape((length, d), bf16),
            shape((length, d), bf16),
        ],
        scratch_shapes=[
            pltpu.VMEM((2 * rows, d), bf16),
            pltpu.VMEM((rows, d), f32),
            pltpu.VMEM((rows, d), f32),
            pltpu.VMEM((max(3 * slots, rows, 9 * length), d), bf16),
            pltpu.VMEM((3, d, hb), f32),
            pltpu.VMEM(pieces, bf16),
            pltpu.VMEM(pieces, bf16),
            pltpu.VMEM((chunks, n, part, hb), bf16),
            pltpu.VMEM((rows, d), bf16),
            pltpu.VMEM((n - 1, 2, length, d), bf16),
            pltpu.VMEM((slots, 1), f32),
            pltpu.VMEM((slots, 1), f32),
            pltpu.VMEM((2 * n, 8, length), f32),
            pltpu.VMEM((n, 8, length), f32),
            pltpu.VMEM((n - 1, 8, length), f32),
            pltpu.VMEM((n - 1, 8, length), f32),
            pltpu.VMEM((length, d), bf16),
            pltpu.VMEM((length, d), bf16),
            pltpu.VMEM((128, d), f32),
            pltpu.VMEM(z_pieces, bf16),
            pltpu.VMEM(z_pieces, bf16),
            pltpu.VMEM(z_pieces[1:], bf16),
            dma((6, chunks)),
            dma((6, chunks)),
            dma((n - 1, chunks)),
            dma((n - 1, chunks)),
            dma((chunks,)),
            dma((8,)),
            dma((8,)),
            dma((n - 1, 3)),
            dma((n - 1, 3)),
            dma((3, n - 1)),
            dma((3, n - 1)),
            dma((n,)),
            dma((n,)),
            dma((15,)),
            pltpu.SemaphoreType.REGULAR,
            pltpu.SemaphoreType.REGULAR,
            pltpu.VMEM((d, 128), bf16),
            pltpu.VMEM((d, 128), bf16),
            pltpu.VMEM((n - 1, 2 * part, 128), bf16),
        ],
        compiler_params=pltpu.CompilerParams(
            vmem_limit_bytes=67043328, collective_id=0, has_side_effects=True
        ),
        cost_estimate=pl.CostEstimate(
            flops=30 * 10**9, bytes_accessed=200 << 20, transcendentals=0
        ),
        name="moe",
    )(slot, router, x, g, *weights, *saved, *extra)


def attention_forward(tokens, small, weight, allowed, cosine, sine, half_way, outs):
    q_ref, k_ref, v_ref, att_ref, one_ref, two_ref, mid_ref, soft_ref, router_ref = outs
    length, d = tokens.shape
    pair = 2 * HD
    small_rows = jnp.transpose(small[...].astype(f32))
    gain_one, gain_two = small_rows[0:1, :], small_rows[1:2, :]
    x = tokens[...].astype(f32)
    one = (x * lax.rsqrt(jnp.mean(x * x, axis=1, keepdims=True) + EPSILON) * gain_one).astype(bf16)
    one_ref[...] = one
    lane = lax.broadcasted_iota(jnp.int32, (length, pair), 1)
    lower = lane % HD < HD // 2
    cos, sin = cosine[...], sine[...]
    for i, ref in enumerate((q_ref, k_ref, v_ref)):
        for p in range(d // pair):
            cut = slice(p * pair, (p + 1) * pair)
            value = mm(one, weight(i)[:, cut], NN)
            if i < 2:
                up = pltpu.roll(value, pair - HD // 2, 1)
                down = pltpu.roll(value, HD // 2, 1)
                value = value * cos + jnp.where(lower, -up, down) * sin
            ref[:, cut] = value.astype(bf16)
    half_way()
    first = lane < HD

    def heads(p, carry):
        cut = pl.ds(pl.multiple_of(p * pair, pair), pair)
        queries, keys, values = q_ref[:, cut], k_ref[:, cut], v_ref[:, cut]
        parts = []
        for side in range(2):
            mine = first if side == 0 else jnp.logical_not(first)
            chosen = jnp.where(mine, queries.astype(f32), 0.0).astype(bf16)
            scores = mm(chosen, keys, NT) * HD ** (-0.5)
            scores = jnp.where(allowed[...] > 0.0, scores, NEGATIVE)
            exponent = jnp.exp(scores - jnp.max(scores, axis=1, keepdims=True))
            soft = exponent / jnp.sum(exponent, axis=1, keepdims=True)
            h = 2 * p + side
            at = pl.ds(pl.multiple_of((h // 3) * length, length), length)
            soft_ref[at, pl.ds(pl.multiple_of((h % 3) * length, length), length)] = soft
            parts.append(mm(soft.astype(bf16), values, NN))
        att_ref[:, cut] = jnp.where(first, parts[0], parts[1]).astype(bf16)
        return carry

    lax.fori_loop(0, d // pair, heads, 0)
    middle = x + mm(att_ref[...], weight(3)[...], NN)
    mid_ref[...] = middle
    two = middle * lax.rsqrt(jnp.mean(middle * middle, axis=1, keepdims=True) + EPSILON) * gain_two
    two = two.astype(bf16)
    two_ref[...] = two
    logits = mm(two, small[...], NN)
    column = lax.broadcasted_iota(jnp.int32, logits.shape, 1)
    valid = (column >= 2) & (column < 2 + EXPERTS)
    logits = jnp.where(valid, logits, NEGATIVE)
    exponent = jnp.exp(logits - jnp.max(logits, axis=1, keepdims=True))
    exponent = jnp.where(valid, exponent, 0.0)
    router = exponent / jnp.sum(exponent, axis=1, keepdims=True)
    router_ref[...] = router
    return router


def front_kernel(
    n,
    qn,
    tokens,
    cot,
    cot_hbm,
    small_own,
    attn_own,
    slot_own,
    allowed,
    cosine,
    sine,
    eg,
    eu,
    ed,
    sg,
    su,
    sd,
    x_all,
    g_all,
    slot_all,
    router_all,
    w_gate,
    w_up,
    w_down,
    attn_all,
    small_all,
    q_ref,
    k_ref,
    v_ref,
    att_ref,
    one_ref,
    two_ref,
    mid_ref,
    soft_ref,
    router_ref,
    wide,
    small,
    full,
    two_buf,
    rt_buf,
    a_send,
    a_recv,
    s_send,
    s_recv,
    w_send,
    w_recv,
    z_send,
    z_recv,
    t_send,
    t_recv,
    side_send,
    side_recv,
    local_sem,
):
    s, q, c = (lax.axis_index(a) for a in ("shard", "plane", "core"))
    rows = small_own.shape[0]
    d = tokens.shape[1]
    hb = full.shape[3]
    part = rows // 2
    parity = q % 2
    near_q, other_c = flip(q, 1, qn), 1 - c
    shards_to = [None] + [flip(s, m, n) for m in range(1, n)]

    def send(src, dst, ssem, rsem, to):
        return pltpu.make_async_remote_copy(
            src, dst, ssem, rsem, device_id=to, device_id_type=MESH
        )

    barrier = pltpu.get_barrier_semaphore()
    peers = [{"plane": near_q}, {"core": other_c}]
    peers += [{"shard": shards_to[m]} for m in range(1, n)]
    for peer in peers:
        pl.semaphore_signal(barrier, 1, device_id=peer, device_id_type=MESH)
    pl.semaphore_wait(barrier, len(peers))

    mine = pl.ds(2 * c, 2)
    my_rows = pl.ds(pl.multiple_of(s * rows, 16), rows)
    attn = [
        send(
            attn_own.at[mine],
            wide.at[mine, my_rows],
            a_send.at[m - 1],
            a_recv.at[m - 1],
            {"shard": shards_to[m]},
        )
        for m in range(1, n)
    ]
    smalls = [
        send(
            small_own, small.at[my_rows], s_send.at[m - 1], s_recv.at[m - 1], {"shard": shards_to[m]}
        )
        for m in range(1, n)
    ]
    for copy in smalls + attn:
        copy.start()
    keep_attn = pltpu.make_async_copy(attn_own.at[mine], wide.at[mine, my_rows], local_sem.at[0])
    keep_small = pltpu.make_async_copy(small_own, small.at[my_rows], local_sem.at[1])
    keep_attn.start()
    keep_small.start()

    half_rows = pl.ds(pl.multiple_of(parity * part, 16), part)
    half_at = pl.ds(pl.multiple_of(s * rows + parity * part, 16), part)
    experts = pl.ds(0, EXPERTS)

    def columns(m):
        owner = s if m == 0 else shards_to[m]
        return pl.ds(pl.multiple_of((owner * 2 + c) * hb, 128), hb)

    def weight_sends(k):
        big, one = ((eg, sg), (eu, su), (ed, sd))[k]
        copies = []
        for m in range(1, n):
            copies.append(
                send(
                    big.at[:, half_rows, columns(m)],
                    full.at[k, experts, half_at],
                    w_send.at[k, m - 1, 0],
                    w_recv.at[k, m - 1, 0],
                    {"shard": shards_to[m]},
                )
            )
            copies.append(
                send(
                    one.at[half_rows, columns(m)],
                    full.at[k, EXPERTS, half_at],
                    w_send.at[k, m - 1, 1],
                    w_recv.at[k, m - 1, 1],
                    {"shard": shards_to[m]},
                )
            )
        return copies

    def pair_sends(k):
        copies = []
        for m in range(1, n):
            at = pl.ds(pl.multiple_of(shards_to[m] * rows + parity * part, 16), part)
            copies.append(
                send(
                    full.at[k, :, at],
                    full.at[k, :, at],
                    z_send.at[k, m - 1],
                    z_recv.at[k, m - 1],
                    {"plane": near_q},
                )
            )
        return copies

    keep_weights = []
    for k, (big, one) in enumerate(((eg, sg), (eu, su), (ed, sd))):
        keep_weights.append(
            pltpu.make_async_copy(
                big.at[:, :, columns(0)], full.at[k, experts, my_rows], local_sem.at[2 + 2 * k]
            )
        )
        keep_weights.append(
            pltpu.make_async_copy(
                one.at[:, columns(0)], full.at[k, EXPERTS, my_rows], local_sem.at[3 + 2 * k]
            )
        )
    for copy in keep_weights:
        copy.start()
    weights = [weight_sends(k) for k in range(3)]
    for k in range(3):
        for copy in weights[k]:
            copy.start()

    def token_sends(i, src, dst):
        return [
            send(src, dst.at[m], t_send.at[i, m - 1], t_recv.at[i, m - 1], {"shard": shards_to[m]})
            for m in range(1, n)
        ]

    def side_send_of(i, ref):
        return send(
            ref.at[pl.ds(0, n)],
            ref.at[pl.ds(n, n)],
            side_send.at[i],
            side_recv.at[i],
            {"core": other_c},
        )

    g_copies = token_sends(0, cot_hbm, g_all)
    slot_copies = token_sends(1, slot_own, slot_all)
    for copy in slot_copies + g_copies:
        copy.start()
    keep_g = pltpu.make_async_copy(cot, g_all.at[0], local_sem.at[8])
    keep_slot = pltpu.make_async_copy(slot_own, slot_all.at[0], local_sem.at[9])
    keep_g.start()
    keep_slot.start()

    keep_attn.wait()
    for copy in attn:
        copy.wait()
    attn_side = send(wide.at[mine], wide.at[mine], side_send.at[0], side_recv.at[0], {"core": other_c})
    attn_side.start()
    keep_small.wait()
    for copy in smalls:
        copy.wait()
    attn_side.wait()
    save_attn = pltpu.make_async_copy(wide, attn_all, local_sem.at[10])
    save_small = pltpu.make_async_copy(small, small_all, local_sem.at[11])
    save_attn.start()
    save_small.start()

    pairs = [pair_sends(k) for k in range(3)]

    def half_way():
        for copy in weights[0]:
            copy.wait()
        for copy in pairs[0]:
            copy.start()

    outs = (q_ref, k_ref, v_ref, att_ref, one_ref, two_buf, mid_ref, soft_ref, router_ref)
    router = attention_forward(
        tokens, small, lambda i: wide.at[i], allowed, cosine, sine, half_way, outs
    )
    rt_buf[...] = jnp.transpose(router)[0:8, :]
    two_ref[...] = two_buf[...]
    x_copies = token_sends(2, two_buf, x_all)
    rt_copies = token_sends(3, rt_buf, router_all)
    for copy in x_copies + rt_copies:
        copy.start()
    keep_x = pltpu.make_async_copy(two_buf, x_all.at[0], local_sem.at[12])
    keep_rt = pltpu.make_async_copy(rt_buf, router_all.at[0], local_sem.at[13])
    keep_x.start()
    keep_rt.start()
    for k in (1, 2):
        for copy in weights[k]:
            copy.wait()
        for copy in pairs[k]:
            copy.start()
    keep_g.wait()
    keep_slot.wait()
    for copy in slot_copies + g_copies:
        copy.wait()
    g_side, slot_side = side_send_of(1, g_all), side_send_of(2, slot_all)
    g_side.start()
    slot_side.start()
    keep_x.wait()
    keep_rt.wait()
    for copy in x_copies + rt_copies:
        copy.wait()
    x_side, rt_side = side_send_of(3, x_all), side_send_of(4, router_all)
    x_side.start()
    rt_side.start()
    for copy in keep_weights:
        copy.wait()
    saves = []
    for k, out in enumerate((w_gate, w_up, w_down)):
        for copy in pairs[k]:
            copy.wait()
        save = pltpu.make_async_copy(full.at[k], out, local_sem.at[14 + k])
        save.start()
        saves.append(save)
    for copy in (g_side, slot_side, x_side, rt_side, save_attn, save_small, *saves):
        copy.wait()


def front_call(n, qn, operands):
    tokens, _, _, small, attn, slot = operands[:6]
    eg = operands[9]
    length, d = tokens.shape
    rows = small.shape[0]
    hidden = eg.shape[2]
    hb = hidden // (2 * n)
    group = 2 * n
    anywhere = pl.BlockSpec(memory_space=pl.ANY)
    vmem = pl.BlockSpec(memory_space=pltpu.VMEM)
    dma = pltpu.SemaphoreType.DMA
    shape = jax.ShapeDtypeStruct
    wide_out = [shape((length, d), bf16)] * 6
    return pl.pallas_call(
        functools.partial(front_kernel, n, qn),
        in_specs=[vmem, vmem] + [anywhere] * 4 + [vmem] * 3 + [anywhere] * 6,
        out_specs=[anywhere] * 9 + [vmem] * 9,
        out_shape=[
            shape((group, length, d), bf16),
            shape((group, length, d), bf16),
            shape((group, 8, length), jnp.int32),
            shape((group, 8, length), f32),
            shape((EXPERTS + 1, d, hb), bf16),
            shape((EXPERTS + 1, d, hb), bf16),
            shape((EXPERTS + 1, d, hb), bf16),
            shape((4, d, d), bf16),
            shape((d, 128), bf16),
            *wide_out,
            shape((length, d), f32),
            shape((NH // 3 * length, 3 * length), f32),
            shape((length, 128), f32),
        ],
        scratch_shapes=[
            pltpu.VMEM((4, d, d), bf16),
            pltpu.VMEM((d, 128), bf16),
            pltpu.VMEM((3, EXPERTS + 1, d, hb), bf16),
            pltpu.VMEM((length, d), bf16),
            pltpu.VMEM((8, length), f32),
            dma((n - 1,)),
            dma((n - 1,)),
            dma((n - 1,)),
            dma((n - 1,)),
            dma((3, n - 1, 2)),
            dma((3, n - 1, 2)),
            dma((3, n - 1)),
            dma((3, n - 1)),
            dma((4, n - 1)),
            dma((4, n - 1)),
            dma((5,)),
            dma((5,)),
            dma((17,)),
        ],
        compiler_params=pltpu.CompilerParams(
            vmem_limit_bytes=56 << 20, collective_id=1, has_side_effects=True
        ),
        cost_estimate=pl.CostEstimate(
            flops=4 * 10**9, bytes_accessed=40 << 20, transcendentals=0
        ),
        name="front",
    )(*operands)


def assemble_kernel(n, where_ref, own_ref, far_ref, *outs):
    s, c = where_ref[0], where_ref[1]
    part, hb = own_ref.shape[3], own_ref.shape[4]
    for side, ref in enumerate((own_ref, far_ref)):
        for m in range(n):
            column = pl.multiple_of(((s ^ m) * 2 + (c ^ side)) * hb, 128)
            for k in range(3):
                for h in range(2):
                    outs[k][0, h * part : (h + 1) * part, pl.ds(column, hb)] = ref[
                        k, h, m
                    ].astype(f32)


def assemble(n, where, own, far, first, count):
    part, hb = own.shape[3], own.shape[4]
    rows, hidden = part * 2, hb * 2 * n
    spec = pl.BlockSpec((3, 2, n, part, hb), lambda i, *_: (i + first, 0, 0, 0, 0))
    return pl.pallas_call(
        functools.partial(assemble_kernel, n),
        grid_spec=pltpu.PrefetchScalarGridSpec(
            num_scalar_prefetch=1,
            grid=(count,),
            in_specs=[spec, spec],
            out_specs=[pl.BlockSpec((1, rows, hidden), lambda i, *_: (i, 0, 0))] * 3,
        ),
        out_shape=[jax.ShapeDtypeStruct((count, rows, hidden), f32)] * 3,
        cost_estimate=pl.CostEstimate(
            flops=0, bytes_accessed=18 * count * rows * hidden, transcendentals=0
        ),
        name="assemble",
    )(where, own, far)


def make_plain(n, qn):
    bits = qn.bit_length() - 1

    def place_blocks(own, blocks):
        out = jnp.zeros((n,) + blocks[0].shape, blocks[0].dtype)
        for m in range(n):
            out = lax.dynamic_update_index_in_dim(out, blocks[m], own ^ m, 0)
        return out

    def join_bit(bit, own, other, axis):
        first = jnp.where(bit == 0, own, other)
        second = jnp.where(bit == 0, other, own)
        return jnp.concatenate([first, second], axis=axis)

    def shards(
        tokens,
        cotangent,
        segments,
        padding,
        routes,
        priority,
        attn_gain,
        query_weight,
        key_weight,
        value_weight,
        output_weight,
        ffn_gain,
        router_weight,
        expert_gate,
        expert_up,
        expert_down,
        shared_gate,
        shared_up,
        shared_down,
    ):
        s = lax.axis_index("shard")
        q = lax.axis_index("plane")
        c = lax.axis_index("core")
        length, d = tokens.shape[1], tokens.shape[2]
        rows = query_weight.shape[0]
        hidden = expert_gate.shape[2]
        hb = hidden // (2 * n)
        score_scale = HD ** (-0.5)

        small = jnp.concatenate(
            [attn_gain[:, None], ffn_gain[:, None], router_weight], axis=1
        )
        small = jnp.pad(small, ((0, 0), (0, 256 - small.shape[1])))
        wide = jnp.concatenate(
            [query_weight, key_weight, value_weight, output_weight, small], axis=1
        )
        half = wide.shape[1] // 2
        mine = lax.dynamic_slice_in_dim(wide, c * half, half, 1)
        blocks = [mine] + [swap(mine, "shard", m, n) for m in range(1, n)]
        mine = place_blocks(s, blocks).reshape(d, half)
        other = swap(mine, "core", 1, 2)
        wide = join_bit(c, mine, other, 1)
        wqkv, wo = wide[:, : 3 * d], wide[:, 3 * d : 4 * d]
        gain_one = wide[:, 4 * d].astype(f32)
        gain_two = wide[:, 4 * d + 1].astype(f32)
        wr = wide[:, 4 * d + 2 : 4 * d + 2 + EXPERTS]

        def block_for(m):
            start = ((s ^ m) * 2 + c) * hb
            cut = lambda w: lax.dynamic_slice_in_dim(w, start, hb, w.ndim - 1)
            return [
                jnp.concatenate([cut(e), cut(w)[None]], axis=0)
                for e, w in (
                    (expert_gate, shared_gate),
                    (expert_up, shared_up),
                    (expert_down, shared_down),
                )
            ]

        own_blocks = block_for(0)
        sent = [block_for(m) for m in range(1, n)]
        moe_w = []
        for k in range(3):
            got = [own_blocks[k]] + [swap(sent[m - 1][k], "shard", m, n) for m in range(1, n)]
            full = jnp.zeros((EXPERTS + 1, n, rows, hb), bf16)
            for m in range(n):
                full = lax.dynamic_update_index_in_dim(full, got[m], s ^ m, 1)
            moe_w.append(full.reshape(EXPERTS + 1, d, hb))

        def plane_gather(values):
            near = jnp.stack([values] + [swap(values, "shard", m, n) for m in range(1, n)])
            return jnp.concatenate([near, swap(near, "core", 1, 2)], axis=0)

        def plane_sum(partial):
            low = partial.astype(bf16)
            pair = (partial[:n] + swap(low[n:], "core", 1, 2).astype(f32)).astype(bf16)
            total = pair[0].astype(f32)
            for m in range(1, n):
                total = total + swap(pair[m], "shard", m, n).astype(f32)
            return total

        grads_b = plane_gather(cotangent[0])

        inputs = tokens[0].astype(f32)
        factor_one = norm_factor(inputs)
        normed_one = (inputs * factor_one * gain_one).astype(bf16)
        projected = jnp.dot(normed_one, wqkv, preferred_element_type=f32)
        cosine, sine = rotary_tables(length, HD)
        heads = projected.reshape(length, 3, NH, HD)
        cos_b, sin_b = cosine[:, None, :], sine[:, None, :]
        queries = (heads[:, 0] * cos_b + rotate_half(heads[:, 0]) * sin_b).astype(bf16)
        keys_rot = (heads[:, 1] * cos_b + rotate_half(heads[:, 1]) * sin_b).astype(bf16)
        values = heads[:, 2].astype(bf16)
        allowed = attention_mask(segments[0], padding[0])
        logits = dot("qhd,khd->hqk", queries, keys_rot) * score_scale
        logits = jnp.where(allowed[None], logits, NEGATIVE)
        maxima = jnp.max(logits, axis=-1, keepdims=True)
        exponent = jnp.exp(logits - maxima)
        soft = exponent / jnp.sum(exponent, axis=-1, keepdims=True)
        probs = soft.astype(bf16)
        attended = dot("hqk,khd->qhd", probs, values).reshape(length, d).astype(bf16)
        middle = inputs + jnp.dot(attended, wo, preferred_element_type=f32)
        factor_two = norm_factor(middle)
        normed_two = (middle * factor_two * gain_two).astype(bf16)
        router = jax.nn.softmax(
            jnp.dot(normed_two, wr, preferred_element_type=f32), axis=-1
        )

        pair_expert, place, kept = pair_slots(routes[0], padding[0], priority[0])
        slot_total = EXPERTS * CAP
        slot_index = jnp.where(kept, pair_expert * CAP + place, -1).reshape(TOPK, length)
        slots = jnp.arange(slot_total, dtype=jnp.int32)
        hit = (slots[None, :, None] == slot_index[:, None, :]).any(axis=0)
        onehot = hit.astype(bf16)
        token_of = jnp.max(
            jnp.where(hit, jnp.arange(length, dtype=jnp.int32)[None, :], -1), axis=1
        )
        slot_expert = jnp.repeat(jnp.arange(EXPERTS), CAP)
        gate_of = jnp.sum(
            jnp.where(hit, jnp.repeat(router.T, CAP, axis=0), 0.0), axis=1
        )

        tokens_b = plane_gather(normed_two)
        token_of_b = plane_gather(token_of)
        gate_of_b = plane_gather(gate_of)
        group = 2 * n
        onehot_b = (
            token_of_b[:, :, None] == jnp.arange(length, dtype=jnp.int32)[None, None, :]
        ).astype(bf16)
        onehot_b = onehot_b.reshape(group, EXPERTS, CAP, length)
        gate_b = gate_of_b.reshape(group, EXPERTS, CAP, 1)

        def reduce_and_return(stack):
            k = stack.shape[0]
            piece = rows // qn
            x = stack.reshape((k, n) + (2,) * bits + (piece, hb))
            for b in range(bits):
                axis = 2 + (bits - 1 - b)
                bit = (q >> b) & 1
                keep = pick_index(x, bit, axis)
                send = pick_index(x, 1 - bit, axis).astype(bf16)
                x = keep + swap(send, "plane", 1 << b, qn).astype(f32)
            x = x.astype(bf16)
            own = pick_index(x, s, 1)
            got = [own] + [swap(pick_index(x, s ^ m, 1), "shard", m, n) for m in range(1, n)]
            x = jnp.stack(got)
            x = x[None]
            for b in reversed(range(bits)):
                bit = (q >> b) & 1
                other = swap(x, "plane", 1 << b, qn)
                lead = x.shape[0]
                pair = jnp.stack(
                    [jnp.where(bit == 0, x, other), jnp.where(bit == 0, other, x)], axis=1
                )
                x = pair.reshape((2 * lead,) + x.shape[1:])
            other = swap(x, "core", 1, 2)
            x = jnp.stack(
                [jnp.where(c == 0, x, other), jnp.where(c == 0, other, x)]
            )
            out = jnp.zeros((n,) + (2, qn, k, piece, hb), bf16)
            for m in range(n):
                out = lax.dynamic_update_index_in_dim(out, x[:, :, m], s ^ m, 0)
            return out.transpose(3, 2, 4, 0, 1, 5).reshape(k, rows, hidden).astype(f32)

        w_gate, w_up, w_down = moe_w
        tokens_f = tokens_b.reshape(group * length, d)
        grads_f = grads_b.reshape(group * length, d)
        shared_g = jnp.dot(tokens_f, w_gate[EXPERTS], preferred_element_type=f32)
        shared_u = jnp.dot(tokens_f, w_up[EXPERTS], preferred_element_type=f32)
        value, slope = silu_parts(shared_g)
        shared_hidden = (value * shared_u).astype(bf16)
        shared_q = jnp.dot(grads_f, w_down[EXPERTS], preferred_element_type=f32)
        shared_gd = (shared_q * shared_u * slope).astype(bf16)
        shared_ud = (shared_q * value).astype(bf16)
        shared_grads = jnp.stack(
            [
                dot("ld,lh->dh", tokens_f, shared_gd),
                dot("ld,lh->dh", tokens_f, shared_ud),
                dot("ld,lh->dh", grads_f, shared_hidden),
            ]
        )
        out_partial = dot("lh,dh->ld", shared_hidden, w_down[EXPERTS])
        two_partial = dot("lh,dh->ld", shared_gd, w_gate[EXPERTS]) + dot(
            "lh,dh->ld", shared_ud, w_up[EXPERTS]
        )
        out_partial = out_partial.reshape(group, length, d)
        two_partial = two_partial.reshape(group, length, d)
        shared_done = reduce_and_return(shared_grads)

        pick_parts = []
        expert_done = []
        for part in GROUPS:
            lo, hi = part[0], part[-1] + 1
            hot = onehot_b[:, lo:hi]
            x_in = jnp.einsum("bect,btd->ebcd", hot, tokens_b, preferred_element_type=bf16)
            g_in = jnp.einsum("bect,btd->ebcd", hot, grads_b, preferred_element_type=bf16)
            gate_e = jnp.swapaxes(gate_b[:, lo:hi], 0, 1)
            wg, wu, wd = w_gate[lo:hi], w_up[lo:hi], w_down[lo:hi]
            gate_act = dot("ebcd,edh->ebch", x_in, wg)
            up_act = dot("ebcd,edh->ebch", x_in, wu)
            value, slope = silu_parts(gate_act)
            hid = (value * up_act).astype(bf16)
            e_out = dot("ebch,edh->ebcd", hid, wd)
            pick_parts.append(jnp.sum(e_out * g_in.astype(f32), axis=-1))
            slot_grad = (gate_e * g_in.astype(f32)).astype(bf16)
            hid_grad = dot("ebcd,edh->ebch", slot_grad, wd)
            gate_d = (hid_grad * up_act * slope).astype(bf16)
            up_d = (hid_grad * value).astype(bf16)
            in_grad = dot("ebch,edh->ebcd", gate_d, wg) + dot("ebch,edh->ebcd", up_d, wu)
            weighted = (gate_e * e_out).astype(bf16)
            out_partial = out_partial + dot("bect,ebcd->btd", hot, weighted)
            two_partial = two_partial + dot("bect,ebcd->btd", hot, in_grad.astype(bf16))
            stack = jnp.concatenate(
                [
                    dot("ebcd,ebch->edh", x_in, gate_d),
                    dot("ebcd,ebch->edh", x_in, up_d),
                    dot("ebcd,ebch->edh", slot_grad, hid),
                ]
            )
            expert_done.append(reduce_and_return(stack))

        two_grad = plane_sum(two_partial)
        picks = jnp.concatenate(pick_parts, axis=0)
        picks = jnp.swapaxes(picks, 0, 1).reshape(group, slot_total)
        picks = picks[:n] + swap(picks[n:], "core", 1, 2)
        pick_slot = picks[0]
        for m in range(1, n):
            pick_slot = pick_slot + swap(picks[m], "shard", m, n)
        mixed = plane_sum(out_partial)
        output = (middle + mixed).astype(bf16)

        upstream = cotangent[0].astype(f32)
        pick_grad = jnp.sum(
            jnp.where(hit, pick_slot[:, None], 0.0).reshape(EXPERTS, CAP, length), axis=1
        ).T
        logit_grad = router * (pick_grad - jnp.sum(router * pick_grad, axis=1, keepdims=True))
        two_grad = two_grad + jnp.dot(logit_grad, wr.astype(f32).T, precision=highest)
        router_grad = jnp.dot(normed_two.astype(f32).T, logit_grad, precision=highest)
        middle_part, ffn_gain_grad = norm_back(middle, factor_two, gain_two, two_grad)
        middle_grad = middle_part + upstream

        branch_grad = middle_grad.astype(bf16)
        output_weight_grad = dot("ld,le->de", attended, branch_grad)
        attended_grad = (
            dot("le,de->ld", branch_grad, wo).astype(bf16).reshape(length, NH, HD)
        )
        prob_grad = dot("qhd,khd->hqk", attended_grad, values)
        row_inner = jnp.sum(soft * prob_grad, axis=-1, keepdims=True)
        score_grad = (soft * (prob_grad - row_inner)).astype(bf16)
        query_parts = dot("hqk,khd->qhd", score_grad, keys_rot) * score_scale
        key_parts = dot("hqk,qhd->khd", score_grad, queries) * score_scale
        value_parts = dot("hqk,qhd->khd", probs, attended_grad)
        query_pre = query_parts * cos_b + rotate_back(query_parts * sin_b)
        key_pre = key_parts * cos_b + rotate_back(key_parts * sin_b)
        joint_grad = jnp.concatenate(
            [v.reshape(length, d) for v in (query_pre, key_pre, value_parts)], axis=1
        ).astype(bf16)
        one_grad = dot("lf,df->ld", joint_grad, wqkv)
        joint_weight_grad = dot("ld,lf->df", normed_one, joint_grad)
        input_part, attn_gain_grad = norm_back(inputs, factor_one, gain_one, one_grad)
        input_grad = (middle_grad + input_part).astype(bf16)

        small_grad = jnp.concatenate(
            [attn_gain_grad[:, None], ffn_gain_grad[:, None], router_grad], axis=1
        )
        small_grad = jnp.pad(small_grad, ((0, 0), (0, 256 - small_grad.shape[1])))
        total = jnp.concatenate([joint_weight_grad, output_weight_grad, small_grad], axis=1)
        keep = lax.dynamic_slice_in_dim(total, c * half, half, 1)
        send = lax.dynamic_slice_in_dim(total, (1 - c) * half, half, 1).astype(bf16)
        total = keep + swap(send, "core", 1, 2).astype(f32)
        total = total.reshape(n, rows, half)
        own = pick_index(total, s)
        low = total.astype(bf16)
        for m in range(1, n):
            own = own + swap(pick_index(low, s ^ m), "shard", m, n).astype(f32)
        x = own.reshape((2,) * bits + (rows // qn, half))
        for b in range(bits):
            axis = bits - 1 - b
            bit = (q >> b) & 1
            keep = pick_index(x, bit, axis)
            send = pick_index(x, 1 - bit, axis).astype(bf16)
            x = keep + swap(send, "plane", 1 << b, qn).astype(f32)
        x = x.astype(bf16)[None]
        for b in reversed(range(bits)):
            bit = (q >> b) & 1
            other = swap(x, "plane", 1 << b, qn)
            pair = jnp.stack(
                [jnp.where(bit == 0, x, other), jnp.where(bit == 0, other, x)], axis=1
            )
            x = pair.reshape((2 * x.shape[0],) + x.shape[1:])
        x = x.reshape(rows, half)
        x = join_bit(c, x, swap(x, "core", 1, 2), 1).astype(f32)
        stacks = [[], [], []]
        for part, done in zip(GROUPS, expert_done):
            for k in range(3):
                stacks[k].append(done[k * len(part) : (k + 1) * len(part)])
        expert_grads = [jnp.concatenate(parts, axis=0) for parts in stacks]
        return (
            output[None],
            input_grad[None],
            x[:, 4 * d],
            x[:, :d],
            x[:, d : 2 * d],
            x[:, 2 * d : 3 * d],
            x[:, 3 * d : 4 * d],
            x[:, 4 * d + 1],
            x[:, 4 * d + 2 : 4 * d + 2 + EXPERTS],
            expert_grads[0],
            expert_grads[1],
            expert_grads[2],
            shared_done[0],
            shared_done[1],
            shared_done[2],
        )

    return shards


def make_fast(n, qn):
    def shards(
        tokens,
        cotangent,
        segments,
        padding,
        routes,
        priority,
        attn_gain,
        query_weight,
        key_weight,
        value_weight,
        output_weight,
        ffn_gain,
        router_weight,
        expert_gate,
        expert_up,
        expert_down,
        shared_gate,
        shared_up,
        shared_down,
    ):
        s = lax.axis_index("shard")
        c = lax.axis_index("core")
        length, d = tokens.shape[1], tokens.shape[2]
        rows = query_weight.shape[0]
        group = 2 * n
        where = jnp.stack([s, c]).astype(jnp.int32)

        pair_expert, place, kept = pair_slots(routes[0], padding[0], priority[0])
        slot_index = jnp.where(kept, pair_expert * CAP + place, -1).reshape(TOPK, length)
        slot = jnp.pad(slot_index, ((0, 8 - TOPK), (0, 0)), constant_values=-1)
        allowed = attention_mask(segments[0], padding[0])
        cosine, sine = rotary_tables(length, HD)
        cos_pair = jnp.concatenate([cosine, cosine], axis=1)
        sin_pair = jnp.concatenate([sine, sine], axis=1)
        small = jnp.concatenate([attn_gain[:, None], ffn_gain[:, None], router_weight], axis=1)
        small = jnp.pad(small, ((0, 0), (0, 128 - small.shape[1])))
        attn = jnp.stack([query_weight, key_weight, value_weight, output_weight])

        (
            x_all,
            g_all,
            slot_all,
            router_all,
            w_gate,
            w_up,
            w_down,
            wide,
            small_all,
            queries,
            keys_rot,
            values,
            attended,
            normed_one,
            normed_two,
            middle,
            soft,
            router_wide,
        ) = front_call(
            n,
            qn,
            (
                tokens[0],
                cotangent[0],
                cotangent[0],
                small,
                attn,
                slot,
                allowed.astype(f32),
                cos_pair,
                sin_pair,
                expert_gate,
                expert_up,
                expert_down,
                shared_gate,
                shared_up,
                shared_down,
            ),
        )
        near, far, near_z, far_z, output, input_grad = moe_call(
            n,
            length,
            slot_all,
            router_all,
            x_all.reshape(group * length, d),
            g_all.reshape(group * length, d),
            (w_gate, w_up, w_down),
            (
                soft,
                middle,
                wide,
                queries,
                keys_rot,
                values,
                attended,
                normed_one,
                tokens[0],
            ),
            (router_wide, small_all, cos_pair, sin_pair),
        )
        expert_grads = assemble(n, where, near, far, 0, EXPERTS)
        shared_done = [v[0] for v in assemble(n, where, near, far, EXPERTS, 1)]
        low = jnp.where(c == 0, near_z, far_z)
        high = jnp.where(c == 0, far_z, near_z)
        part = rows // 2

        def matrix(v, i):
            return v[:, i * part : (i + 1) * part].reshape(rows, d)

        tail = low[:, 2 * part :].reshape(2, 16, part // 16, 128)
        tail = jnp.swapaxes(tail, 1, 2).reshape(rows, 128)
        x = jnp.concatenate(
            [matrix(low, 0), matrix(low, 1), matrix(high, 0), matrix(high, 1), tail], axis=1
        ).astype(f32)
        return (
            output[None],
            input_grad[None],
            x[:, 4 * d],
            x[:, :d],
            x[:, d : 2 * d],
            x[:, 2 * d : 3 * d],
            x[:, 3 * d : 4 * d],
            x[:, 4 * d + 1],
            x[:, 4 * d + 2 : 4 * d + 2 + EXPERTS],
            expert_grads[0],
            expert_grads[1],
            expert_grads[2],
            shared_done[0],
            shared_done[1],
            shared_done[2],
        )

    return shards


def make_shards(n, qn):
    plain, fast = make_plain(n, qn), make_fast(n, qn)

    def shards(*arguments):
        d, hidden = arguments[0].shape[2], arguments[13].shape[2]
        fits = n == 4 and qn == 4 and d == 768 and hidden == 2048 and arguments[0].shape[1] == 256
        return (fast if fits else plain)(*arguments)

    return shards


def solution(mesh):
    n, replicas = mesh.shape["shard"], mesh.shape["replica"]
    fine = Mesh(mesh.devices.reshape(n, replicas // 2, 2), ("shard", "plane", "core"))
    every = ("shard", "plane", "core")
    in_specs = (
        P(every, None, None),
        P(every, None, None),
        P(every, None),
        P(every, None),
        P(every, None, None),
        P(every, None),
        P("shard"),
        P("shard", None),
        P("shard", None),
        P("shard", None),
        P("shard", None),
        P("shard"),
        P("shard", None),
        P(None, "shard", None),
        P(None, "shard", None),
        P(None, "shard", None),
        P("shard", None),
        P("shard", None),
        P("shard", None),
    )
    out_specs = (
        P(every, None, None),
        P(every, None, None),
        P("shard"),
        P("shard", None),
        P("shard", None),
        P("shard", None),
        P("shard", None),
        P("shard"),
        P("shard", None),
        P(None, "shard", None),
        P(None, "shard", None),
        P(None, "shard", None),
        P("shard", None),
        P("shard", None),
        P("shard", None),
    )
    return jax.shard_map(
        make_shards(n, replicas // 2),
        mesh=fine,
        in_specs=in_specs,
        out_specs=out_specs,
        check_vma=False,
    )
```

```python
import functools
import math

import jax
import jax.numpy as jnp
from jax import lax
from jax.experimental import pallas as pl
from jax.experimental.pallas import tpu as pltpu
from jax.sharding import Mesh, PartitionSpec as P

NH = 12
HD = 64
EXPERTS = 6
TOPK = 2
CAP = 96
EPSILON = 1e-06
NEGATIVE = -1e30
GROUPS = ((0, 1), (2, 3), (4, 5))

highest = lax.Precision.HIGHEST
f32 = jnp.float32
bf16 = jnp.bfloat16


def dot(spec, first, second):
    return jnp.einsum(spec, first, second, preferred_element_type=f32)


def rotate_half(values):
    half_size = values.shape[-1] // 2
    return jnp.concatenate([-values[..., half_size:], values[..., :half_size]], axis=-1)


def rotate_back(values):
    half_size = values.shape[-1] // 2
    return jnp.concatenate([values[..., half_size:], -values[..., :half_size]], axis=-1)


def rotary_tables(length, head_dim):
    positions = jnp.arange(length, dtype=f32)
    frequency = jnp.exp(
        jnp.arange(head_dim // 2, dtype=f32) * (-2.0 * math.log(10000.0) / head_dim)
    )
    angles = positions[:, None] * frequency[None, :]
    angles = jnp.concatenate([angles, angles], axis=1)
    return (jnp.cos(angles), jnp.sin(angles))


def attention_mask(segments, padding):
    places = jnp.arange(segments.shape[0])
    causal = places[None, :] <= places[:, None]
    shared_doc = segments[:, None] == segments[None, :]
    usable = (padding[None, :] == 1) | (places[None, :] == places[:, None])
    return causal & shared_doc & usable


def norm_factor(values):
    return lax.rsqrt(jnp.mean(values * values, axis=-1, keepdims=True) + EPSILON)


def norm_back(values, factor, norm_gain, gradient):
    scaled = gradient * norm_gain
    gain_grad = jnp.sum(gradient * values * factor, axis=0)
    input_part = factor * scaled - values * factor**3 * jnp.mean(
        scaled * values, axis=-1, keepdims=True
    )
    return (input_part, gain_grad)


def silu_parts(gate_act):
    sigmoid = jax.nn.sigmoid(gate_act)
    return (gate_act * sigmoid, sigmoid * (1.0 + gate_act * (1.0 - sigmoid)))


def pair_slots(routes, padding, priority):
    length = routes.shape[0]
    pair_expert = routes.T.reshape(-1)
    pair_live = jnp.tile(padding, TOPK) == 1
    pair_key = (jnp.arange(TOPK, dtype=jnp.int32)[:, None] * length + priority[None, :]).reshape(-1)
    earlier = (
        (pair_key[None, :] < pair_key[:, None])
        & (pair_expert[None, :] == pair_expert[:, None])
        & pair_live[None, :]
    )
    place = jnp.sum(earlier.astype(jnp.int32), axis=1)
    kept = pair_live & (place < CAP)
    return (pair_expert, place, kept)


def swap(values, axis, mask, size):
    return lax.ppermute(values, axis, [(i, i ^ mask) for i in range(size)])


def pick_index(values, index, axis=0):
    return lax.dynamic_index_in_dim(values, index, axis, keepdims=False)


def mm(first, second, contract):
    return lax.dot_general(
        first, second, (contract, ((), ())), preferred_element_type=f32
    )


NN = ((1,), (0,))
NT = ((1,), (1,))
TN = ((0,), (0,))


def flip(value, mask, size):
    out = 0
    for b in range(size.bit_length() - 1):
        bit = (value // (1 << b)) % 2
        out = out + (1 << b) * ((1 - bit) if (mask >> b) & 1 else bit)
    return out


MESH = pl.DeviceIdType.MESH


def layer_kernel(
    n,
    tokens,
    allowed,
    cos_ref,
    sin_ref,
    tok_hbm,
    cot_hbm,
    small_own,
    attn_own,
    slot_own,
    eg,
    eu,
    ed,
    sg,
    su,
    sd,
    near_ref,
    far_ref,
    near_z,
    far_z,
    wide_hbm,
    work_hbm,
    soft_hbm,
    mid_hbm,
    w_land,
    out_ref,
    in_grad_ref,
    xg,
    acc_y,
    acc_t,
    work,
    dw,
    own,
    land,
    swap_in,
    y_side,
    y_in,
    wbuf,
    slot_ref,
    router_ref,
    probs_ref,
    small_ref,
    gate_s,
    pick_s,
    pick_acc,
    pick_side,
    pick_pair,
    pick_in,
    branch_s,
    ag_s,
    small_acc,
    z_own,
    z_swap,
    ch_send,
    ch_recv,
    x_send,
    x_recv,
    stay_sem,
    z_send,
    z_recv,
    zx_send,
    zx_recv,
    y_send_sem,
    y_recv_sem,
    p_send,
    p_recv,
    load_sem,
    free_side,
    free_in,
    gains_s,
    gains_side,
    gains_in,
    a_send,
    a_recv,
    w_send,
    w_recv,
    w_load,
    t_send,
    t_recv,
    side_send,
    side_recv,
):
    t = pl.program_id(0) - 1
    group = 2 * n
    length, d = tokens.shape
    hb = dw.shape[2]
    part = d // (2 * n)
    half = n * part
    chunks = 3 * (EXPERTS + 1)
    plane_rows = group * length
    s, q, c = (lax.axis_index(a) for a in ("shard", "plane", "core"))
    middle = (q == 1) | (q == 2)
    ends = (q == 0) | (q == 3)
    keep_h, give_h = (q + 1) % 2, q % 2
    other_mid = 3 - q
    mid_of = 1 + q // 3
    end_of = (q // 2) * 3
    other_c = 1 - c
    shard_of = [None] + [flip(s, m, n) for m in range(1, n)]

    def at_chunk(u, row=0, count=d):
        start = pl.multiple_of((u // 3) * d + row, 16)
        return pl.ds(start, count), pl.ds(pl.multiple_of((u % 3) * hb, 128), hb)

    def half_rows(h):
        return pl.ds(pl.multiple_of(h * half, 16), half)

    def remote(src, dst, ssem, rsem, to):
        return pltpu.make_async_remote_copy(
            src, dst, ssem, rsem, device_id=to, device_id_type=MESH
        )

    def chunk(kind, src, dst, u, to):
        return remote(src, dst, ch_send.at[kind, u], ch_recv.at[kind, u], to)

    def to_mid(u):
        return chunk(0, own.at[at_chunk(u)], land.at[u], u, {"plane": mid_of})

    def from_end(u):
        return chunk(0, own.at[at_chunk(u)], land.at[u], u, {"plane": end_of})

    def swap_sums(u):
        src = own.at[at_chunk(u, give_h * half, half)]
        return chunk(1, src, swap_in.at[u], u, {"plane": other_mid})

    def swap_done(u):
        ref = near_ref.at[u, half_rows(keep_h)]
        return chunk(2, ref, ref, u, {"plane": other_mid})

    def swap_done_in(u):
        ref = near_ref.at[u, half_rows(give_h)]
        return chunk(2, ref, ref, u, {"plane": other_mid})

    def to_end(u, first):
        ref = near_ref.at[u, half_rows(keep_h if first else give_h)]
        return chunk(3 if first else 4, ref, ref, u, {"plane": end_of})

    def from_mid(u, first):
        ref = near_ref.at[u, half_rows((q // 3) if first else 1 - q // 3)]
        return chunk(3 if first else 4, ref, ref, u, {"plane": mid_of})

    def across(u, m):
        return remote(
            own.at[at_chunk(u, keep_h * half + m * part, part)],
            near_ref.at[u, pl.ds(pl.multiple_of(keep_h * half + m * part, 16), part)],
            x_send.at[m - 1, u],
            x_recv.at[m - 1, u],
            {"shard": shard_of[m]},
        )

    def stay(u):
        return pltpu.make_async_copy(
            own.at[at_chunk(u, keep_h * half, part)],
            near_ref.at[u, pl.ds(pl.multiple_of(keep_h * half, 16), part)],
            stay_sem.at[u],
        )

    def side(u):
        return chunk(5, near_ref.at[u], far_ref.at[u], u, {"core": other_c})

    far_rows = pl.ds(0, plane_rows)

    def y_side_copy():
        return remote(
            work.at[far_rows], y_side, y_send_sem.at[0, 0], y_recv_sem.at[0, 0], {"core": other_c}
        )

    def y_across(k, m):
        at = pl.ds((k * n + m) * length, length)
        return remote(
            y_side.at[at],
            y_in.at[m - 1, k],
            y_send_sem.at[1 + k, m - 1],
            y_recv_sem.at[1 + k, m - 1],
            {"shard": shard_of[m]},
        )

    def pick_side_copy():
        return remote(
            pick_acc.at[pl.ds(n, n)], pick_side, p_send.at[0], p_recv.at[0], {"core": other_c}
        )

    def pick_across(m):
        return remote(
            pick_pair.at[m - 1],
            pick_in.at[m - 1],
            p_send.at[m],
            p_recv.at[m],
            {"shard": shard_of[m]},
        )

    def load(i, src, dst):
        return pltpu.make_async_copy(src, dst, load_sem.at[i])

    def back_rows(i):
        return pl.ds(i * length, length)

    two_w = [length, length + d, plane_rows + length, plane_rows + length + d]

    saved_rows = pl.ds(0, 5 * length)
    soft_rows = pl.ds(n * length, n * length)
    mid_rows = pl.ds(n * length, length)

    def saved_out():
        return [
            load(2, acc_y.at[soft_rows], soft_hbm),
            load(3, acc_t.at[mid_rows], mid_hbm),
            load(4, own.at[pl.ds(0, 4 * d)], wide_hbm),
            load(5, work.at[saved_rows], work_hbm),
        ]

    def saved_in():
        copies = [
            load(6, soft_hbm, acc_y.at[soft_rows]),
            load(7, mid_hbm, acc_t.at[mid_rows]),
            load(8, work_hbm, work.at[saved_rows]),
            load(9, tok_hbm, work.at[back_rows(5)]),
        ]
        for i in range(4):
            copies.append(load(10 + i, wide_hbm.at[pl.ds(i * d, d)], xg.at[pl.ds(two_w[i], d)]))
        return copies

    def columns(m):
        owner = s if m == 0 else shard_of[m]
        return pl.ds(pl.multiple_of((owner * 2 + c) * hb, 128), hb)

    def weight_ref(e, k, m, shared):
        big, one = ((eg, sg), (eu, su), (ed, sd))[k]
        return one.at[:, columns(m)] if shared else big.at[e, :, columns(m)]

    def weight_sends(e, shared):
        return [
            remote(
                weight_ref(e, k, m, shared),
                w_land.at[e, k, m - 1],
                w_send.at[e, 3 * k + m - 1],
                w_recv.at[e, 3 * k + m - 1],
                {"shard": shard_of[m]},
            )
            for k in range(3)
            for m in range(1, n)
        ]

    def weight_loads(e, shared):
        copies = []
        for k in range(3):
            for m in range(n):
                owner = s if m == 0 else shard_of[m]
                src = weight_ref(e, k, 0, shared) if m == 0 else w_land.at[e, k, m - 1]
                dst = wbuf.at[
                    e % 2, k, pl.ds(pl.multiple_of(owner * 2 * part, 16), 2 * part)
                ]
                copies.append(pltpu.make_async_copy(src, dst, w_load.at[e % 2, n * k + m]))
        return copies

    def for_expert(e, body):
        @pl.when(e < EXPERTS)
        def _():
            body(e, False)

        @pl.when(e == EXPERTS)
        def _():
            body(e, True)

    def fetch_weights(e, shared):
        for copy in weight_sends(e, shared):
            copy.wait()
        for copy in weight_loads(e, shared):
            copy.start()

    def finish_weights(e, shared):
        for copy in weight_loads(e, shared):
            copy.wait()

    @pl.when(t < 0)
    def _():
        barrier = pltpu.get_barrier_semaphore()
        peers = [{"core": other_c}] + [{"shard": shard_of[m]} for m in range(1, n)]
        for peer in peers:
            pl.semaphore_signal(barrier, 1, device_id=peer, device_id_type=MESH)

        @pl.when(middle)
        def _():
            for peer in ({"plane": other_mid}, {"plane": end_of}):
                pl.semaphore_signal(barrier, 1, device_id=peer, device_id_type=MESH)
            pl.semaphore_wait(barrier, len(peers) + 2)

        @pl.when(ends)
        def _():
            pl.semaphore_signal(barrier, 1, device_id={"plane": mid_of}, device_id_type=MESH)
            pl.semaphore_wait(barrier, len(peers) + 1)

        my_rows = pl.multiple_of(s * 2 * part, 16)

        def wide_at(i, row, count):
            return own.at[pl.ds(pl.multiple_of((2 * c + i) * d + row, 16), count)]

        attn = [
            remote(
                attn_own.at[2 * c + i],
                wide_at(i, my_rows, 2 * part),
                a_send.at[i, m - 1],
                a_recv.at[i, m - 1],
                {"shard": shard_of[m]},
            )
            for i in range(2)
            for m in range(1, n)
        ]
        smalls = [
            remote(
                small_own,
                small_ref.at[pl.ds(my_rows, 2 * part)],
                a_send.at[2, m - 1],
                a_recv.at[2, m - 1],
                {"shard": shard_of[m]},
            )
            for m in range(1, n)
        ]
        stay_here = [
            load(i, attn_own.at[2 * c + i], wide_at(i, my_rows, 2 * part)) for i in range(2)
        ]
        stay_here += [
            load(14, small_own, small_ref.at[pl.ds(my_rows, 2 * part)]),
            load(15, cot_hbm, xg.at[pl.ds(plane_rows, length)]),
            load(16, slot_own, slot_ref.at[0]),
        ]
        for copy in smalls + attn + stay_here:
            copy.start()

        def spread_out(i, src, place):
            return [
                remote(
                    src, place(m), t_send.at[i, m - 1], t_recv.at[i, m - 1], {"shard": shard_of[m]}
                )
                for m in range(1, n)
            ]

        def to_core(i, src, dst):
            return remote(src, dst, side_send.at[i], side_recv.at[i], {"core": other_c})

        def rows_to_core(i, base):
            return to_core(
                i, xg.at[pl.ds(base, n * length)], xg.at[pl.ds(base + n * length, n * length)]
            )

        g_copies = spread_out(
            0, cot_hbm, lambda m: xg.at[pl.ds(plane_rows + m * length, length)]
        )
        slot_copies = spread_out(1, slot_own, lambda m: slot_ref.at[m])
        for copy in slot_copies + g_copies + weight_sends(0, False):
            copy.start()
        for copy in stay_here:
            copy.wait()
        for copy in attn:
            copy.wait()
        pair_rows = own.at[pl.ds(pl.multiple_of(c * 2 * d, 16), 2 * d)]
        attn_side_copy = to_core(0, pair_rows, pair_rows)
        attn_side_copy.start()
        for copy in smalls:
            copy.wait()
        attn_side_copy.wait()
        work_part = lambda i: work.at[pl.ds(i * length, length)]
        outs = tuple(work_part(i) for i in range(5)) + (
            xg.at[pl.ds(0, length)],
            acc_t.at[mid_rows],
            acc_y.at[soft_rows],
            probs_ref,
        )
        router = attention_forward(
            tokens,
            small_ref,
            lambda i: own.at[pl.ds(i * d, d)],
            allowed,
            cos_ref,
            sin_ref,
            outs,
        )
        router_ref[0] = jnp.transpose(router)[0:8, :]
        for copy in saved_out():
            copy.start()
        x_copies = spread_out(
            2, xg.at[pl.ds(0, length)], lambda m: xg.at[pl.ds(m * length, length)]
        )
        rt_copies = spread_out(3, router_ref.at[0], lambda m: router_ref.at[m])
        for copy in x_copies + rt_copies:
            copy.start()

        def send_weights(e, carry):
            for copy in weight_sends(e, False):
                copy.start()
            return carry

        lax.fori_loop(1, EXPERTS, send_weights, 0)
        for copy in weight_sends(EXPERTS, True):
            copy.start()
        for copy in slot_copies + g_copies:
            copy.wait()
        g_side = rows_to_core(1, plane_rows)
        slot_side = to_core(2, slot_ref.at[pl.ds(0, n)], slot_ref.at[pl.ds(n, n)])
        g_side.start()
        slot_side.start()
        for copy in saved_out():
            copy.wait()
        acc_y[...] = jnp.zeros_like(acc_y)
        acc_t[...] = jnp.zeros_like(acc_t)
        pick_acc[...] = jnp.zeros_like(pick_acc)
        fetch_weights(0, False)
        for copy in x_copies + rt_copies:
            copy.wait()
        x_side = rows_to_core(3, 0)
        rt_side = to_core(4, router_ref.at[pl.ds(0, n)], router_ref.at[pl.ds(n, n)])
        x_side.start()
        rt_side.start()
        for copy in (g_side, slot_side, x_side, rt_side):
            copy.wait()

    def branch(x, gs_rows, wg, wu, wd):
        gate_act = mm(x, wg, NN)
        up_act = mm(x, wu, NN)
        sigmoid = 1.0 / (1.0 + jnp.exp(-gate_act))
        value = gate_act * sigmoid
        slope = sigmoid * (1.0 + gate_act * (1.0 - sigmoid))
        hid = (value * up_act).astype(bf16)
        hid_grad = mm(gs_rows, wd, NN)
        gate_d = (hid_grad * up_act * slope).astype(bf16)
        up_d = (hid_grad * value).astype(bf16)
        return hid, gate_d, up_d

    slots = group * CAP
    xs_at, gs_at, sg_at = 0, slots, 2 * slots

    @pl.when((t >= 0) & (t <= EXPERTS))
    def _():
        for_expert(t, finish_weights)

    @pl.when((t >= 0) & (t < EXPERTS))
    def _():
        ids = lax.broadcasted_iota(jnp.int32, (CAP, length), 0) + t * CAP

        def slots_of(b):
            first, second = slot_ref[b, 0:1, :], slot_ref[b, 1:2, :]
            return (first == ids) | (second == ids)

        for b in range(group):
            slot = pl.ds(b * CAP, CAP)
            hit = slots_of(b)
            hot = hit.astype(f32).astype(bf16)
            row = router_ref[b, pl.ds(t + 2, 1), :]
            gate = jnp.sum(jnp.where(hit, row, 0.0), axis=1, keepdims=True)
            gate_s[slot, :] = gate
            x_rows = mm(hot, xg[pl.ds(b * length, length), :], NN)
            work[pl.ds(xs_at + b * CAP, CAP), :] = x_rows.astype(bf16)
            g_rows = mm(hot, xg[pl.ds(plane_rows + b * length, length), :], NN)
            work[pl.ds(gs_at + b * CAP, CAP), :] = g_rows.astype(bf16)
            work[pl.ds(sg_at + b * CAP, CAP), :] = (g_rows * gate).astype(bf16)
        wg, wu, wd = wbuf[t % 2, 0], wbuf[t % 2, 1], wbuf[t % 2, 2]
        x, slot_grad = work[pl.ds(xs_at, slots), :], work[pl.ds(sg_at, slots), :]
        hid, gate_d, up_d = branch(x, slot_grad, wg, wu, wd)
        dw[0] = mm(x, gate_d, TN)
        dw[1] = mm(x, up_d, TN)
        dw[2] = mm(slot_grad, hid, TN)
        e_out = mm(hid, wd, NT)
        g_rows = work[pl.ds(gs_at, slots), :].astype(f32)
        pick_s[...] = jnp.sum(e_out * g_rows, axis=1, keepdims=True)
        work[pl.ds(gs_at, slots), :] = (e_out * gate_s[...]).astype(bf16)
        work[pl.ds(xs_at, slots), :] = (mm(gate_d, wg, NT) + mm(up_d, wu, NT)).astype(bf16)
        for b in range(group):
            slot = pl.ds(b * CAP, CAP)
            seq = pl.ds(b * length, length)
            hit = slots_of(b)
            hot = hit.astype(f32).astype(bf16)
            pick_acc[b, pl.ds(t + 2, 1), :] = jnp.sum(
                jnp.where(hit, pick_s[slot, :], 0.0), axis=0, keepdims=True
            )
            acc_y[seq, :] += mm(hot, work[pl.ds(gs_at + b * CAP, CAP), :], TN)
            acc_t[seq, :] += mm(hot, work[pl.ds(xs_at + b * CAP, CAP), :], TN)

    @pl.when(t == EXPERTS)
    def _():
        dw[...] = jnp.zeros_like(dw)
        wg, wu, wd = wbuf[t % 2, 0], wbuf[t % 2, 1], wbuf[t % 2, 2]

        def rows_step(i, carry):
            at = pl.multiple_of(i * 2 * length, 2 * length)
            rows = pl.ds(at, 2 * length)
            x, g = xg[rows, :], xg[pl.ds(plane_rows + at, 2 * length), :]
            hid, gate_d, up_d = branch(x, g, wg, wu, wd)
            dw[0] += mm(x, gate_d, TN)
            dw[1] += mm(x, up_d, TN)
            dw[2] += mm(g, hid, TN)
            acc_y[rows, :] += mm(hid, wd, NT)
            acc_t[rows, :] += mm(gate_d, wg, NT) + mm(up_d, wu, NT)
            return carry

        lax.fori_loop(0, n, rows_step, 0)
        work[pl.ds(0, n * length), :] = acc_y[soft_rows, :].astype(bf16)
        work[pl.ds(n * length, n * length), :] = acc_t[soft_rows, :].astype(bf16)

    @pl.when((t >= 0) & (t <= EXPERTS))
    def _():
        for k in range(3):
            for h in range(2):
                for m in range(n):
                    owner = s if m == 0 else shard_of[m]
                    start = pl.multiple_of((owner * 2 + h) * part, 16)
                    row = pl.multiple_of(t * d + (h * n + m) * part, 16)
                    own[pl.ds(row, part), k * hb : (k + 1) * hb] = dw[
                        k, pl.ds(start, part), :
                    ].astype(bf16)

        @pl.when(ends)
        def _():
            for k in range(3):
                to_mid(3 * t + k).start()

    @pl.when(t == EXPERTS)
    def _():
        y_side_copy().start()
        pick_side_copy().start()

    def stage(delay, where, body):
        @pl.when((t >= delay) & (t < chunks + delay) & where)
        def _():
            body(t - delay)

    def add_halves(u):
        from_end(u).wait_recv()
        for i in range(2 * n):
            rows, columns_at = at_chunk(u, i * part, part)
            own[rows, columns_at] = (
                own[rows, columns_at].astype(f32)
                + land[u, pl.ds(i * part, part), :].astype(f32)
            ).astype(bf16)
        swap_sums(u).start()

    def add_swapped(u):
        swap_sums(u).wait()
        for m in range(n):
            rows, columns_at = at_chunk(u, keep_h * half + m * part, part)
            own[rows, columns_at] = (
                own[rows, columns_at].astype(f32)
                + swap_in[u, pl.ds(m * part, part), :].astype(f32)
            ).astype(bf16)
        for m in range(1, n):
            across(u, m).start()
        stay(u).start()

    def send_done(u):
        for m in range(1, n):
            across(u, m).wait()
        stay(u).wait()
        swap_done(u).start()
        to_end(u, True).start()

    def send_second(u):
        swap_done_in(u).wait_recv()
        to_end(u, False).start()
        side(u).start()

    def end_side(u):
        to_mid(u).wait_send()
        from_mid(u, True).wait_recv()
        from_mid(u, False).wait_recv()
        side(u).start()

    def middle_last(u):
        swap_done(u).wait_send()
        to_end(u, True).wait_send()
        to_end(u, False).wait_send()
        side(u).wait()

    mine_rows = pl.ds(0, length)
    grad_rows = pl.ds((n + 1) * length, length)

    def out_copy():
        return load(14, xg.at[mine_rows], out_ref)

    def in_grad_copy():
        return load(15, work.at[back_rows(5)], in_grad_ref)

    @pl.when(t == EXPERTS + 5)
    def _():
        total = acc_y[mine_rows, :]
        for m in range(1, n):
            y_across(0, m).wait()
            total = total + y_in[m - 1, 0].astype(f32)
        xg[mine_rows, :] = (acc_t[mid_rows, :] + total).astype(bf16)
        out_copy().start()
        pl.semaphore_signal(free_side, 1, device_id={"core": other_c}, device_id_type=MESH)
        for m in range(1, n):
            pl.semaphore_signal(free_in, 1, device_id={"shard": shard_of[m]}, device_id_type=MESH)

    stage(1, middle, add_halves)
    stage(2, middle, add_swapped)
    stage(3, middle, send_done)
    stage(4, middle, send_second)
    stage(5, ends, end_side)
    stage(6, middle, middle_last)
    stage(6, ends, lambda u: side(u).wait())

    @pl.when((t >= 0) & (t < EXPERTS))
    def _():
        for_expert(t + 1, fetch_weights)

    @pl.when(t == EXPERTS + 1)
    def _():
        y_side_copy().wait()
        pick_side_copy().wait()
        for copy in saved_in():
            copy.start()
        pick_acc[pl.ds(0, n)] += pick_side[...]
        for m in range(1, n):
            pick_pair[m - 1] = pick_acc[m]
        for k, acc in ((1, acc_t), (0, acc_y)):
            for m in range(n):
                seq, at = pl.ds(m * length, length), pl.ds((k * n + m) * length, length)
                total = acc[seq, :] + y_side[at, :].astype(f32)
                if m == 0:
                    acc[seq, :] = total
                else:
                    y_side[at, :] = total.astype(bf16)
            for m in range(1, n):
                y_across(k, m).start()
                if k:
                    pick_across(m).start()

    pre_at = 6 * length
    exact = lax.Precision.HIGHEST

    @pl.when(t == EXPERTS + 3)
    def _():
        for m in range(1, n):
            y_across(1, m).wait()
            pick_across(m).wait()
        for copy in saved_in():
            copy.wait()
        two = acc_t[mine_rows, :]
        picks = pick_acc[0]
        for m in range(1, n):
            two = two + y_in[m - 1, 1].astype(f32)
            picks = picks + pick_in[m - 1]
        picks = jnp.concatenate([picks, jnp.zeros((120, length), f32)], axis=0)
        picks = jnp.transpose(picks)
        router = probs_ref[...]
        logit_grad = router * (picks - jnp.sum(router * picks, axis=1, keepdims=True))
        small = small_ref[...].astype(f32)
        gain_two = jnp.transpose(small)[1:2, :]
        two = two + lax.dot_general(
            logit_grad, small, (NT, ((), ())), precision=exact, preferred_element_type=f32
        )
        router_grad = lax.dot_general(
            logit_grad,
            xg[mine_rows, :].astype(f32),
            (TN, ((), ())),
            precision=exact,
            preferred_element_type=f32,
        )
        mid = acc_t[mid_rows, :]
        factor = lax.rsqrt(jnp.mean(mid * mid, axis=1, keepdims=True) + EPSILON)
        gain_grad = jnp.sum(two * mid * factor, axis=0, keepdims=True)
        row = lax.broadcasted_iota(jnp.int32, router_grad.shape, 0)
        small_acc[...] = jnp.where(row == 1, gain_grad, router_grad)
        scaled = two * gain_two
        grad = (
            xg[pl.ds(plane_rows, length), :].astype(f32)
            + factor * scaled
            - mid * (factor * factor * factor) * jnp.mean(scaled * mid, axis=1, keepdims=True)
        )
        acc_t[grad_rows, :] = grad
        branch_s[...] = grad.astype(bf16)
        ag_s[...] = mm(branch_s[...], xg[pl.ds(two_w[3], d), :], NT).astype(bf16)

    pair = 2 * HD

    @pl.when((t >= EXPERTS + 4) & (t < EXPERTS + 7))
    def _():
        lane = lax.broadcasted_iota(jnp.int32, (length, pair), 1)
        first = lane < HD
        lower = lane % HD < HD // 2
        cos, sin = cos_ref[...], sin_ref[...]

        def turn_back(w):
            y = w * sin
            up = pltpu.roll(y, pair - HD // 2, 1)
            down = pltpu.roll(y, HD // 2, 1)
            return w * cos + jnp.where(lower, up, -down)

        def heads(i, carry):
            p = 2 * (t - EXPERTS - 4) + i
            cut = pl.ds(pl.multiple_of(p * pair, pair), pair)
            queries, keys, values = (work[back_rows(j), cut] for j in range(3))
            grads = ag_s[:, cut]
            parts = []
            for one_side in range(2):
                h = 2 * p + one_side
                rows = pl.ds(pl.multiple_of(n * length + (h // 3) * length, length), length)
                columns = pl.ds(pl.multiple_of((h % 3) * length, length), length)
                soft = acc_y[rows, columns]
                mine = first if one_side == 0 else jnp.logical_not(first)
                chosen = jnp.where(mine, grads.astype(f32), 0.0).astype(bf16)
                prob_grad = mm(chosen, values, NT)
                inner = jnp.sum(soft * prob_grad, axis=1, keepdims=True)
                score_grad = (soft * (prob_grad - inner)).astype(bf16)
                parts.append(
                    (
                        mm(score_grad, keys, NN) * HD ** (-0.5),
                        mm(score_grad, queries, TN) * HD ** (-0.5),
                        mm(soft.astype(bf16), grads, TN),
                    )
                )
            joined = [jnp.where(first, parts[0][j], parts[1][j]) for j in range(3)]
            joined = [turn_back(joined[0]), turn_back(joined[1]), joined[2]]
            for j in range(3):
                work[pl.ds(pre_at + j * length, length), cut] = joined[j].astype(bf16)
            return carry

        lax.fori_loop(0, 2, heads, 0)

    two_d = 2 * d
    give_rows = pl.ds(pl.multiple_of((1 - c) * two_d, 16), two_d)

    def attn_side():
        return [
            remote(
                xg.at[give_rows],
                y_side.at[pl.ds(0, two_d)],
                z_send.at[5],
                z_recv.at[5],
                {"core": other_c},
            ),
            remote(gains_s, gains_side, z_send.at[7], z_recv.at[7], {"core": other_c}),
        ]

    def attn_across(m):
        copies = []
        at = pl.multiple_of(shard_of[m] * 2 * part, 16)
        for i in range(2):
            copies.append(
                remote(
                    xg.at[pl.ds(pl.multiple_of(c * two_d + i * d + at, 16), 2 * part)],
                    y_in.at[m - 1, i, pl.ds(0, 2 * part)],
                    zx_send.at[m - 1, i],
                    zx_recv.at[m - 1, i],
                    {"shard": shard_of[m]},
                )
            )
        copies.append(
            remote(
                gains_s.at[pl.ds(at, 2 * part)],
                gains_in.at[m - 1],
                zx_send.at[m - 1, 2],
                zx_recv.at[m - 1, 2],
                {"shard": shard_of[m]},
            )
        )
        return copies

    @pl.when(t == EXPERTS + 7)
    def _():
        pre = [work[pl.ds(pre_at + j * length, length), :] for j in range(3)]
        one_grad = mm(pre[0], xg[pl.ds(two_w[0], d), :], NT)
        for j in (1, 2):
            one_grad = one_grad + mm(pre[j], xg[pl.ds(two_w[j], d), :], NT)
        x = work[back_rows(5), :].astype(f32)
        gain_one = jnp.transpose(small_ref[...].astype(f32))[0:1, :]
        factor = lax.rsqrt(jnp.mean(x * x, axis=1, keepdims=True) + EPSILON)
        gain_grad = jnp.sum(one_grad * x * factor, axis=0, keepdims=True)
        scaled = one_grad * gain_one
        work[back_rows(5), :] = (
            acc_t[grad_rows, :]
            + factor * scaled
            - x * (factor * factor * factor) * jnp.mean(scaled * x, axis=1, keepdims=True)
        ).astype(bf16)
        in_grad_copy().start()
        out_copy().wait()
        gains = small_acc[...]
        row = lax.broadcasted_iota(jnp.int32, gains.shape, 0)
        gains_s[...] = jnp.transpose(jnp.where(row == 0, gain_grad, gains)).astype(bf16)
        for i in range(4):
            lhs = work[back_rows(4 if i < 3 else 3), :]
            for k in range(3):
                cut = slice(k * hb, (k + 1) * hb)
                rhs = work[pl.ds(pre_at + i * length, length), cut] if i < 3 else branch_s[:, cut]
                xg[pl.ds(i * d, d), cut] = mm(lhs, rhs, TN).astype(bf16)
        pl.semaphore_wait(free_side, 1)
        for copy in attn_side():
            copy.start()

    @pl.when(t == EXPERTS + 8)
    def _():
        in_grad_copy().wait()
        for copy in attn_side():
            copy.wait()
        for i in range(8):
            rows = pl.ds(pl.multiple_of(c * two_d + i * (d // 4), 16), d // 4)
            other = y_side[pl.ds(i * (d // 4), d // 4), :]
            xg[rows, :] = (xg[rows, :].astype(f32) + other.astype(f32)).astype(bf16)
        gains_s[...] = (gains_s[...].astype(f32) + gains_side[...].astype(f32)).astype(bf16)
        pl.semaphore_wait(free_in, n - 1)
        for m in range(1, n):
            for copy in attn_across(m):
                copy.start()

    def z_copy(i, src, dst, to):
        return remote(src, dst, z_send.at[i], z_recv.at[i], to)

    z_rows = 2 * part + 16
    z_land = y_side.at[pl.ds(two_d, 2 * z_rows)]

    def z_half(h):
        return pl.ds(pl.multiple_of(h * z_rows, 16), z_rows)

    def z_to_mid():
        return z_copy(0, z_own, z_land, {"plane": mid_of})

    def z_from_end():
        return z_copy(0, z_own, z_land, {"plane": end_of})

    def z_swap_sums():
        return z_copy(1, z_own.at[z_half(give_h)], z_swap, {"plane": other_mid})

    def z_swap_done():
        at = z_half(keep_h)
        return z_copy(2, z_own.at[at], near_z.at[at], {"plane": other_mid})

    def z_swap_done_in():
        at = z_half(give_h)
        return z_copy(2, z_own.at[at], near_z.at[at], {"plane": other_mid})

    def z_to_end(first):
        at = z_half(keep_h if first else give_h)
        source = z_own if first else near_z
        return z_copy(3 if first else 4, source.at[at], near_z.at[at], {"plane": end_of})

    def z_from_mid(first):
        at = z_half((q // 3) if first else 1 - q // 3)
        return z_copy(3 if first else 4, near_z.at[at], near_z.at[at], {"plane": mid_of})

    def z_stay():
        at = z_half(keep_h)
        return pltpu.make_async_copy(z_own.at[at], near_z.at[at], load_sem.at[17])

    def z_side():
        return z_copy(6, near_z, far_z, {"core": other_c})

    @pl.when(t == Z_STEPS[0])
    def _():
        for m in range(1, n):
            for copy in attn_across(m):
                copy.wait()
        for h in range(2):
            at = pl.multiple_of(s * 2 * part + h * part, 16)
            for i in range(2):
                total = xg[pl.ds(pl.multiple_of(c * two_d + i * d + at, 16), part), :].astype(f32)
                for m in range(1, n):
                    total = total + y_in[m - 1, i, pl.ds(h * part, part), :].astype(f32)
                z_own[pl.ds(h * z_rows + i * part, part), :] = total.astype(bf16)
            total = gains_s[pl.ds(at, part), :].astype(f32)
            for m in range(1, n):
                total = total + gains_in[m - 1, pl.ds(h * part, part), :].astype(f32)
            total = total.astype(bf16)
            for r in range(part // 16):
                z_own[pl.ds(h * z_rows + 2 * part, 16), r * 128 : (r + 1) * 128] = total[
                    r * 16 : (r + 1) * 16, :
                ]

        @pl.when(ends)
        def _():
            z_to_mid().start()

    @pl.when((t == Z_STEPS[1]) & middle)
    def _():
        z_from_end().wait_recv()
        for h in range(2):
            at = pl.ds(h * z_rows, z_rows)
            other = y_side[pl.ds(two_d + h * z_rows, z_rows), :]
            z_own[at, :] = (z_own[at, :].astype(f32) + other.astype(f32)).astype(bf16)
        z_swap_sums().start()

    @pl.when((t == Z_STEPS[2]) & middle)
    def _():
        z_swap_sums().wait()
        at = z_half(keep_h)
        z_own[at, :] = (z_own[at, :].astype(f32) + z_swap[...].astype(f32)).astype(bf16)
        z_stay().start()
        z_swap_done().start()
        z_to_end(True).start()

    @pl.when((t == Z_STEPS[3]) & middle)
    def _():
        z_swap_done_in().wait_recv()
        z_stay().wait()
        z_to_end(False).start()
        z_side().start()

    @pl.when((t == Z_STEPS[4]) & ends)
    def _():
        z_to_mid().wait_send()
        z_from_mid(True).wait_recv()
        z_from_mid(False).wait_recv()
        z_side().start()

    @pl.when(t == Z_STEPS[5])
    def _():
        z_side().wait()

        @pl.when(middle)
        def _():
            z_swap_done().wait_send()
            z_to_end(True).wait_send()
            z_to_end(False).wait_send()


Z_STEPS = (18, 23, 24, 25, 26, 27)


def layer_call(n, operands):
    tokens, eg = operands[0], operands[9]
    length, d = tokens.shape
    hb = eg.shape[2] // (2 * n)
    rows = 2 * n * length
    slots = 2 * n * CAP
    chunks = 3 * (EXPERTS + 1)
    part = d // (2 * n)
    steps = 1 + max(chunks + 7, Z_STEPS[5] + 1)
    vmem = lambda v: pl.BlockSpec(v.shape, lambda t: (0, 0), pipeline_mode=pl.Buffered(1))
    anywhere = pl.BlockSpec(memory_space=pl.ANY)
    dma = pltpu.SemaphoreType.DMA
    shape = jax.ShapeDtypeStruct
    z_pieces = (2 * (2 * part + 16), d)
    return pl.pallas_call(
        functools.partial(layer_kernel, n),
        grid=(steps,),
        in_specs=[vmem(v) for v in operands[:4]] + [anywhere] * (len(operands) - 4),
        out_specs=[anywhere] * 11,
        out_shape=[
            shape((chunks, d, hb), bf16),
            shape((chunks, d, hb), bf16),
            shape(z_pieces, bf16),
            shape(z_pieces, bf16),
            shape((4 * d, d), bf16),
            shape((5 * length, d), bf16),
            shape((n * length, d), f32),
            shape((length, d), f32),
            shape((EXPERTS + 1, 3, n - 1, 2 * part, hb), bf16),
            shape((length, d), bf16),
            shape((length, d), bf16),
        ],
        scratch_shapes=[
            pltpu.VMEM((2 * rows, d), bf16),
            pltpu.VMEM((rows, d), f32),
            pltpu.VMEM((rows, d), f32),
            pltpu.VMEM((max(3 * slots, rows, 9 * length), d), bf16),
            pltpu.VMEM((3, d, hb), f32),
            pltpu.VMEM(((EXPERTS + 1) * d, 3 * hb), bf16),
            pltpu.VMEM((chunks, d, hb), bf16),
            pltpu.VMEM((chunks, d // 2, hb), bf16),
            pltpu.VMEM((rows, d), bf16),
            pltpu.VMEM((n - 1, 2, length, d), bf16),
            pltpu.VMEM((2, 3, d, hb), bf16),
            pltpu.VMEM((2 * n, 8, length), jnp.int32),
            pltpu.VMEM((2 * n, 8, length), f32),
            pltpu.VMEM((length, 128), f32),
            pltpu.VMEM((d, 128), bf16),
            pltpu.VMEM((slots, 1), f32),
            pltpu.VMEM((slots, 1), f32),
            pltpu.VMEM((2 * n, 8, length), f32),
            pltpu.VMEM((n, 8, length), f32),
            pltpu.VMEM((n - 1, 8, length), f32),
            pltpu.VMEM((n - 1, 8, length), f32),
            pltpu.VMEM((length, d), bf16),
            pltpu.VMEM((length, d), bf16),
            pltpu.VMEM((128, d), f32),
            pltpu.VMEM(z_pieces, bf16),
            pltpu.VMEM((2 * part + 16, d), bf16),
            dma((6, chunks)),
            dma((6, chunks)),
            dma((n - 1, chunks)),
            dma((n - 1, chunks)),
            dma((chunks,)),
            dma((8,)),
            dma((8,)),
            dma((n - 1, 3)),
            dma((n - 1, 3)),
            dma((3, n - 1)),
            dma((3, n - 1)),
            dma((n,)),
            dma((n,)),
            dma((18,)),
            pltpu.SemaphoreType.REGULAR,
            pltpu.SemaphoreType.REGULAR,
            pltpu.VMEM((d, 128), bf16),
            pltpu.VMEM((d, 128), bf16),
            pltpu.VMEM((n - 1, 2 * part, 128), bf16),
            dma((3, n - 1)),
            dma((3, n - 1)),
            dma((EXPERTS + 1, 3 * (n - 1))),
            dma((EXPERTS + 1, 3 * (n - 1))),
            dma((2, 3 * n)),
            dma((4, n - 1)),
            dma((4, n - 1)),
            dma((5,)),
            dma((5,)),
        ],
        compiler_params=pltpu.CompilerParams(
            vmem_limit_bytes=67043328, collective_id=0, has_side_effects=True
        ),
        cost_estimate=pl.CostEstimate(
            flops=30 * 10**9, bytes_accessed=200 << 20, transcendentals=0
        ),
        name="layer",
    )(*operands)


def attention_forward(tokens, small, weight, allowed, cosine, sine, outs):
    q_ref, k_ref, v_ref, att_ref, one_ref, two_ref, mid_ref, soft_ref, router_ref = outs
    length, d = tokens.shape
    pair = 2 * HD
    small_rows = jnp.transpose(small[...].astype(f32))
    gain_one, gain_two = small_rows[0:1, :], small_rows[1:2, :]
    x = tokens[...].astype(f32)
    one = (x * lax.rsqrt(jnp.mean(x * x, axis=1, keepdims=True) + EPSILON) * gain_one).astype(bf16)
    one_ref[...] = one
    lane = lax.broadcasted_iota(jnp.int32, (length, pair), 1)
    lower = lane % HD < HD // 2
    cos, sin = cosine[...], sine[...]
    for i, ref in enumerate((q_ref, k_ref, v_ref)):
        for p in range(d // pair):
            cut = slice(p * pair, (p + 1) * pair)
            value = mm(one, weight(i)[:, cut], NN)
            if i < 2:
                up = pltpu.roll(value, pair - HD // 2, 1)
                down = pltpu.roll(value, HD // 2, 1)
                value = value * cos + jnp.where(lower, -up, down) * sin
            ref[:, cut] = value.astype(bf16)
    first = lane < HD

    def heads(p, carry):
        cut = pl.ds(pl.multiple_of(p * pair, pair), pair)
        queries, keys, values = q_ref[:, cut], k_ref[:, cut], v_ref[:, cut]
        parts = []
        for side in range(2):
            mine = first if side == 0 else jnp.logical_not(first)
            chosen = jnp.where(mine, queries.astype(f32), 0.0).astype(bf16)
            scores = mm(chosen, keys, NT) * HD ** (-0.5)
            scores = jnp.where(allowed[...] > 0.0, scores, NEGATIVE)
            exponent = jnp.exp(scores - jnp.max(scores, axis=1, keepdims=True))
            soft = exponent / jnp.sum(exponent, axis=1, keepdims=True)
            h = 2 * p + side
            at = pl.ds(pl.multiple_of((h // 3) * length, length), length)
            soft_ref[at, pl.ds(pl.multiple_of((h % 3) * length, length), length)] = soft
            parts.append(mm(soft.astype(bf16), values, NN))
        att_ref[:, cut] = jnp.where(first, parts[0], parts[1]).astype(bf16)
        return carry

    lax.fori_loop(0, d // pair, heads, 0)
    middle = x + mm(att_ref[...], weight(3)[...], NN)
    mid_ref[...] = middle
    two = middle * lax.rsqrt(jnp.mean(middle * middle, axis=1, keepdims=True) + EPSILON) * gain_two
    two = two.astype(bf16)
    two_ref[...] = two
    logits = mm(two, small[...], NN)
    column = lax.broadcasted_iota(jnp.int32, logits.shape, 1)
    valid = (column >= 2) & (column < 2 + EXPERTS)
    logits = jnp.where(valid, logits, NEGATIVE)
    exponent = jnp.exp(logits - jnp.max(logits, axis=1, keepdims=True))
    exponent = jnp.where(valid, exponent, 0.0)
    router = exponent / jnp.sum(exponent, axis=1, keepdims=True)
    router_ref[...] = router
    return router


def finish_kernel(n, where_ref, own_ref, far_ref, own_z, far_z, *outs):
    step = pl.program_id(0)
    s, c = where_ref[0], where_ref[1]
    part = own_ref.shape[1] // (2 * n)
    hb = own_ref.shape[2]
    z_rows = own_z.shape[0] // 2

    def write(targets):
        for side, ref in enumerate((own_ref, far_ref)):
            for m in range(n):
                column = pl.multiple_of(((s ^ m) * 2 + (c ^ side)) * hb, 128)
                for k in range(3):
                    for h in range(2):
                        row = (h * n + m) * part
                        targets[k][0, h * part : (h + 1) * part, pl.ds(column, hb)] = ref[
                            k, row : row + part, :
                        ].astype(f32)

    @pl.when(step < EXPERTS)
    def _():
        write(outs[:3])

    @pl.when(step == EXPERTS)
    def _():
        write(outs[3:6])

    @pl.when(step == 0)
    def _():
        tail = outs[10]
        for h in range(2):
            at = slice(h * z_rows, (h + 1) * z_rows)
            mine, other = own_z[at, :].astype(f32), far_z[at, :].astype(f32)
            low = jnp.where(c == 0, mine, other)
            high = jnp.where(c == 0, other, mine)
            for i, out in enumerate(outs[6:10]):
                source = (low if i < 2 else high)[(i % 2) * part : (i % 2 + 1) * part, :]
                out[h * part : (h + 1) * part, :] = source
            for r in range(part // 16):
                row = h * part + r * 16
                tail[row : row + 16, :] = low[2 * part : 2 * part + 16, r * 128 : (r + 1) * 128]


def finish(n, where, own, far, own_z, far_z):
    hb, d = own.shape[2], own.shape[1]
    rows, hidden = d // n, hb * 2 * n
    spec = pl.BlockSpec((3, d, hb), lambda i, *_: (i, 0, 0))
    z_spec = pl.BlockSpec(own_z.shape, lambda i, *_: (0, 0))
    expert = pl.BlockSpec((1, rows, hidden), lambda i, *_: (jnp.minimum(i, EXPERTS - 1), 0, 0))
    shared = pl.BlockSpec((1, rows, hidden), lambda i, *_: (0, 0, 0))
    square = pl.BlockSpec((rows, d), lambda i, *_: (0, 0))
    tail = pl.BlockSpec((rows, 128), lambda i, *_: (0, 0))
    shape = jax.ShapeDtypeStruct
    return pl.pallas_call(
        functools.partial(finish_kernel, n),
        grid_spec=pltpu.PrefetchScalarGridSpec(
            num_scalar_prefetch=1,
            grid=(EXPERTS + 1,),
            in_specs=[spec, spec, z_spec, z_spec],
            out_specs=[expert] * 3 + [shared] * 3 + [square] * 4 + [tail],
        ),
        out_shape=[shape((EXPERTS, rows, hidden), f32)] * 3
        + [shape((1, rows, hidden), f32)] * 3
        + [shape((rows, d), f32)] * 4
        + [shape((rows, 128), f32)],
        cost_estimate=pl.CostEstimate(
            flops=0, bytes_accessed=130 * rows * hidden, transcendentals=0
        ),
        compiler_params=pltpu.CompilerParams(vmem_limit_bytes=56 << 20),
        name="finish",
    )(where, own, far, own_z, far_z)


def make_plain(n, qn):
    bits = qn.bit_length() - 1

    def place_blocks(own, blocks):
        out = jnp.zeros((n,) + blocks[0].shape, blocks[0].dtype)
        for m in range(n):
            out = lax.dynamic_update_index_in_dim(out, blocks[m], own ^ m, 0)
        return out

    def join_bit(bit, own, other, axis):
        first = jnp.where(bit == 0, own, other)
        second = jnp.where(bit == 0, other, own)
        return jnp.concatenate([first, second], axis=axis)

    def shards(
        tokens,
        cotangent,
        segments,
        padding,
        routes,
        priority,
        attn_gain,
        query_weight,
        key_weight,
        value_weight,
        output_weight,
        ffn_gain,
        router_weight,
        expert_gate,
        expert_up,
        expert_down,
        shared_gate,
        shared_up,
        shared_down,
    ):
        s = lax.axis_index("shard")
        q = lax.axis_index("plane")
        c = lax.axis_index("core")
        length, d = tokens.shape[1], tokens.shape[2]
        rows = query_weight.shape[0]
        hidden = expert_gate.shape[2]
        hb = hidden // (2 * n)
        score_scale = HD ** (-0.5)

        small = jnp.concatenate(
            [attn_gain[:, None], ffn_gain[:, None], router_weight], axis=1
        )
        small = jnp.pad(small, ((0, 0), (0, 256 - small.shape[1])))
        wide = jnp.concatenate(
            [query_weight, key_weight, value_weight, output_weight, small], axis=1
        )
        half = wide.shape[1] // 2
        mine = lax.dynamic_slice_in_dim(wide, c * half, half, 1)
        blocks = [mine] + [swap(mine, "shard", m, n) for m in range(1, n)]
        mine = place_blocks(s, blocks).reshape(d, half)
        other = swap(mine, "core", 1, 2)
        wide = join_bit(c, mine, other, 1)
        wqkv, wo = wide[:, : 3 * d], wide[:, 3 * d : 4 * d]
        gain_one = wide[:, 4 * d].astype(f32)
        gain_two = wide[:, 4 * d + 1].astype(f32)
        wr = wide[:, 4 * d + 2 : 4 * d + 2 + EXPERTS]

        def block_for(m):
            start = ((s ^ m) * 2 + c) * hb
            cut = lambda w: lax.dynamic_slice_in_dim(w, start, hb, w.ndim - 1)
            return [
                jnp.concatenate([cut(e), cut(w)[None]], axis=0)
                for e, w in (
                    (expert_gate, shared_gate),
                    (expert_up, shared_up),
                    (expert_down, shared_down),
                )
            ]

        own_blocks = block_for(0)
        sent = [block_for(m) for m in range(1, n)]
        moe_w = []
        for k in range(3):
            got = [own_blocks[k]] + [swap(sent[m - 1][k], "shard", m, n) for m in range(1, n)]
            full = jnp.zeros((EXPERTS + 1, n, rows, hb), bf16)
            for m in range(n):
                full = lax.dynamic_update_index_in_dim(full, got[m], s ^ m, 1)
            moe_w.append(full.reshape(EXPERTS + 1, d, hb))

        def plane_gather(values):
            near = jnp.stack([values] + [swap(values, "shard", m, n) for m in range(1, n)])
            return jnp.concatenate([near, swap(near, "core", 1, 2)], axis=0)

        def plane_sum(partial):
            low = partial.astype(bf16)
            pair = (partial[:n] + swap(low[n:], "core", 1, 2).astype(f32)).astype(bf16)
            total = pair[0].astype(f32)
            for m in range(1, n):
                total = total + swap(pair[m], "shard", m, n).astype(f32)
            return total

        grads_b = plane_gather(cotangent[0])

        inputs = tokens[0].astype(f32)
        factor_one = norm_factor(inputs)
        normed_one = (inputs * factor_one * gain_one).astype(bf16)
        projected = jnp.dot(normed_one, wqkv, preferred_element_type=f32)
        cosine, sine = rotary_tables(length, HD)
        heads = projected.reshape(length, 3, NH, HD)
        cos_b, sin_b = cosine[:, None, :], sine[:, None, :]
        queries = (heads[:, 0] * cos_b + rotate_half(heads[:, 0]) * sin_b).astype(bf16)
        keys_rot = (heads[:, 1] * cos_b + rotate_half(heads[:, 1]) * sin_b).astype(bf16)
        values = heads[:, 2].astype(bf16)
        allowed = attention_mask(segments[0], padding[0])
        logits = dot("qhd,khd->hqk", queries, keys_rot) * score_scale
        logits = jnp.where(allowed[None], logits, NEGATIVE)
        maxima = jnp.max(logits, axis=-1, keepdims=True)
        exponent = jnp.exp(logits - maxima)
        soft = exponent / jnp.sum(exponent, axis=-1, keepdims=True)
        probs = soft.astype(bf16)
        attended = dot("hqk,khd->qhd", probs, values).reshape(length, d).astype(bf16)
        middle = inputs + jnp.dot(attended, wo, preferred_element_type=f32)
        factor_two = norm_factor(middle)
        normed_two = (middle * factor_two * gain_two).astype(bf16)
        router = jax.nn.softmax(
            jnp.dot(normed_two, wr, preferred_element_type=f32), axis=-1
        )

        pair_expert, place, kept = pair_slots(routes[0], padding[0], priority[0])
        slot_total = EXPERTS * CAP
        slot_index = jnp.where(kept, pair_expert * CAP + place, -1).reshape(TOPK, length)
        slots = jnp.arange(slot_total, dtype=jnp.int32)
        hit = (slots[None, :, None] == slot_index[:, None, :]).any(axis=0)
        onehot = hit.astype(bf16)
        token_of = jnp.max(
            jnp.where(hit, jnp.arange(length, dtype=jnp.int32)[None, :], -1), axis=1
        )
        slot_expert = jnp.repeat(jnp.arange(EXPERTS), CAP)
        gate_of = jnp.sum(
            jnp.where(hit, jnp.repeat(router.T, CAP, axis=0), 0.0), axis=1
        )

        tokens_b = plane_gather(normed_two)
        token_of_b = plane_gather(token_of)
        gate_of_b = plane_gather(gate_of)
        group = 2 * n
        onehot_b = (
            token_of_b[:, :, None] == jnp.arange(length, dtype=jnp.int32)[None, None, :]
        ).astype(bf16)
        onehot_b = onehot_b.reshape(group, EXPERTS, CAP, length)
        gate_b = gate_of_b.reshape(group, EXPERTS, CAP, 1)

        def reduce_and_return(stack):
            k = stack.shape[0]
            piece = rows // qn
            x = stack.reshape((k, n) + (2,) * bits + (piece, hb))
            for b in range(bits):
                axis = 2 + (bits - 1 - b)
                bit = (q >> b) & 1
                keep = pick_index(x, bit, axis)
                send = pick_index(x, 1 - bit, axis).astype(bf16)
                x = keep + swap(send, "plane", 1 << b, qn).astype(f32)
            x = x.astype(bf16)
            own = pick_index(x, s, 1)
            got = [own] + [swap(pick_index(x, s ^ m, 1), "shard", m, n) for m in range(1, n)]
            x = jnp.stack(got)
            x = x[None]
            for b in reversed(range(bits)):
                bit = (q >> b) & 1
                other = swap(x, "plane", 1 << b, qn)
                lead = x.shape[0]
                pair = jnp.stack(
                    [jnp.where(bit == 0, x, other), jnp.where(bit == 0, other, x)], axis=1
                )
                x = pair.reshape((2 * lead,) + x.shape[1:])
            other = swap(x, "core", 1, 2)
            x = jnp.stack(
                [jnp.where(c == 0, x, other), jnp.where(c == 0, other, x)]
            )
            out = jnp.zeros((n,) + (2, qn, k, piece, hb), bf16)
            for m in range(n):
                out = lax.dynamic_update_index_in_dim(out, x[:, :, m], s ^ m, 0)
            return out.transpose(3, 2, 4, 0, 1, 5).reshape(k, rows, hidden).astype(f32)

        w_gate, w_up, w_down = moe_w
        tokens_f = tokens_b.reshape(group * length, d)
        grads_f = grads_b.reshape(group * length, d)
        shared_g = jnp.dot(tokens_f, w_gate[EXPERTS], preferred_element_type=f32)
        shared_u = jnp.dot(tokens_f, w_up[EXPERTS], preferred_element_type=f32)
        value, slope = silu_parts(shared_g)
        shared_hidden = (value * shared_u).astype(bf16)
        shared_q = jnp.dot(grads_f, w_down[EXPERTS], preferred_element_type=f32)
        shared_gd = (shared_q * shared_u * slope).astype(bf16)
        shared_ud = (shared_q * value).astype(bf16)
        shared_grads = jnp.stack(
            [
                dot("ld,lh->dh", tokens_f, shared_gd),
                dot("ld,lh->dh", tokens_f, shared_ud),
                dot("ld,lh->dh", grads_f, shared_hidden),
            ]
        )
        out_partial = dot("lh,dh->ld", shared_hidden, w_down[EXPERTS])
        two_partial = dot("lh,dh->ld", shared_gd, w_gate[EXPERTS]) + dot(
            "lh,dh->ld", shared_ud, w_up[EXPERTS]
        )
        out_partial = out_partial.reshape(group, length, d)
        two_partial = two_partial.reshape(group, length, d)
        shared_done = reduce_and_return(shared_grads)

        pick_parts = []
        expert_done = []
        for part in GROUPS:
            lo, hi = part[0], part[-1] + 1
            hot = onehot_b[:, lo:hi]
            x_in = jnp.einsum("bect,btd->ebcd", hot, tokens_b, preferred_element_type=bf16)
            g_in = jnp.einsum("bect,btd->ebcd", hot, grads_b, preferred_element_type=bf16)
            gate_e = jnp.swapaxes(gate_b[:, lo:hi], 0, 1)
            wg, wu, wd = w_gate[lo:hi], w_up[lo:hi], w_down[lo:hi]
            gate_act = dot("ebcd,edh->ebch", x_in, wg)
            up_act = dot("ebcd,edh->ebch", x_in, wu)
            value, slope = silu_parts(gate_act)
            hid = (value * up_act).astype(bf16)
            e_out = dot("ebch,edh->ebcd", hid, wd)
            pick_parts.append(jnp.sum(e_out * g_in.astype(f32), axis=-1))
            slot_grad = (gate_e * g_in.astype(f32)).astype(bf16)
            hid_grad = dot("ebcd,edh->ebch", slot_grad, wd)
            gate_d = (hid_grad * up_act * slope).astype(bf16)
            up_d = (hid_grad * value).astype(bf16)
            in_grad = dot("ebch,edh->ebcd", gate_d, wg) + dot("ebch,edh->ebcd", up_d, wu)
            weighted = (gate_e * e_out).astype(bf16)
            out_partial = out_partial + dot("bect,ebcd->btd", hot, weighted)
            two_partial = two_partial + dot("bect,ebcd->btd", hot, in_grad.astype(bf16))
            stack = jnp.concatenate(
                [
                    dot("ebcd,ebch->edh", x_in, gate_d),
                    dot("ebcd,ebch->edh", x_in, up_d),
                    dot("ebcd,ebch->edh", slot_grad, hid),
                ]
            )
            expert_done.append(reduce_and_return(stack))

        two_grad = plane_sum(two_partial)
        picks = jnp.concatenate(pick_parts, axis=0)
        picks = jnp.swapaxes(picks, 0, 1).reshape(group, slot_total)
        picks = picks[:n] + swap(picks[n:], "core", 1, 2)
        pick_slot = picks[0]
        for m in range(1, n):
            pick_slot = pick_slot + swap(picks[m], "shard", m, n)
        mixed = plane_sum(out_partial)
        output = (middle + mixed).astype(bf16)

        upstream = cotangent[0].astype(f32)
        pick_grad = jnp.sum(
            jnp.where(hit, pick_slot[:, None], 0.0).reshape(EXPERTS, CAP, length), axis=1
        ).T
        logit_grad = router * (pick_grad - jnp.sum(router * pick_grad, axis=1, keepdims=True))
        two_grad = two_grad + jnp.dot(logit_grad, wr.astype(f32).T, precision=highest)
        router_grad = jnp.dot(normed_two.astype(f32).T, logit_grad, precision=highest)
        middle_part, ffn_gain_grad = norm_back(middle, factor_two, gain_two, two_grad)
        middle_grad = middle_part + upstream

        branch_grad = middle_grad.astype(bf16)
        output_weight_grad = dot("ld,le->de", attended, branch_grad)
        attended_grad = (
            dot("le,de->ld", branch_grad, wo).astype(bf16).reshape(length, NH, HD)
        )
        prob_grad = dot("qhd,khd->hqk", attended_grad, values)
        row_inner = jnp.sum(soft * prob_grad, axis=-1, keepdims=True)
        score_grad = (soft * (prob_grad - row_inner)).astype(bf16)
        query_parts = dot("hqk,khd->qhd", score_grad, keys_rot) * score_scale
        key_parts = dot("hqk,qhd->khd", score_grad, queries) * score_scale
        value_parts = dot("hqk,qhd->khd", probs, attended_grad)
        query_pre = query_parts * cos_b + rotate_back(query_parts * sin_b)
        key_pre = key_parts * cos_b + rotate_back(key_parts * sin_b)
        joint_grad = jnp.concatenate(
            [v.reshape(length, d) for v in (query_pre, key_pre, value_parts)], axis=1
        ).astype(bf16)
        one_grad = dot("lf,df->ld", joint_grad, wqkv)
        joint_weight_grad = dot("ld,lf->df", normed_one, joint_grad)
        input_part, attn_gain_grad = norm_back(inputs, factor_one, gain_one, one_grad)
        input_grad = (middle_grad + input_part).astype(bf16)

        small_grad = jnp.concatenate(
            [attn_gain_grad[:, None], ffn_gain_grad[:, None], router_grad], axis=1
        )
        small_grad = jnp.pad(small_grad, ((0, 0), (0, 256 - small_grad.shape[1])))
        total = jnp.concatenate([joint_weight_grad, output_weight_grad, small_grad], axis=1)
        keep = lax.dynamic_slice_in_dim(total, c * half, half, 1)
        send = lax.dynamic_slice_in_dim(total, (1 - c) * half, half, 1).astype(bf16)
        total = keep + swap(send, "core", 1, 2).astype(f32)
        total = total.reshape(n, rows, half)
        own = pick_index(total, s)
        low = total.astype(bf16)
        for m in range(1, n):
            own = own + swap(pick_index(low, s ^ m), "shard", m, n).astype(f32)
        x = own.reshape((2,) * bits + (rows // qn, half))
        for b in range(bits):
            axis = bits - 1 - b
            bit = (q >> b) & 1
            keep = pick_index(x, bit, axis)
            send = pick_index(x, 1 - bit, axis).astype(bf16)
            x = keep + swap(send, "plane", 1 << b, qn).astype(f32)
        x = x.astype(bf16)[None]
        for b in reversed(range(bits)):
            bit = (q >> b) & 1
            other = swap(x, "plane", 1 << b, qn)
            pair = jnp.stack(
                [jnp.where(bit == 0, x, other), jnp.where(bit == 0, other, x)], axis=1
            )
            x = pair.reshape((2 * x.shape[0],) + x.shape[1:])
        x = x.reshape(rows, half)
        x = join_bit(c, x, swap(x, "core", 1, 2), 1).astype(f32)
        stacks = [[], [], []]
        for part, done in zip(GROUPS, expert_done):
            for k in range(3):
                stacks[k].append(done[k * len(part) : (k + 1) * len(part)])
        expert_grads = [jnp.concatenate(parts, axis=0) for parts in stacks]
        return (
            output[None],
            input_grad[None],
            x[:, 4 * d],
            x[:, :d],
            x[:, d : 2 * d],
            x[:, 2 * d : 3 * d],
            x[:, 3 * d : 4 * d],
            x[:, 4 * d + 1],
            x[:, 4 * d + 2 : 4 * d + 2 + EXPERTS],
            expert_grads[0],
            expert_grads[1],
            expert_grads[2],
            shared_done[0],
            shared_done[1],
            shared_done[2],
        )

    return shards


def make_fast(n, qn):
    def shards(
        tokens,
        cotangent,
        segments,
        padding,
        routes,
        priority,
        attn_gain,
        query_weight,
        key_weight,
        value_weight,
        output_weight,
        ffn_gain,
        router_weight,
        expert_gate,
        expert_up,
        expert_down,
        shared_gate,
        shared_up,
        shared_down,
    ):
        s = lax.axis_index("shard")
        c = lax.axis_index("core")
        length, d = tokens.shape[1], tokens.shape[2]
        where = jnp.stack([s, c]).astype(jnp.int32)

        pair_expert, place, kept = pair_slots(routes[0], padding[0], priority[0])
        slot_index = jnp.where(kept, pair_expert * CAP + place, -1).reshape(TOPK, length)
        slot = jnp.pad(slot_index, ((0, 8 - TOPK), (0, 0)), constant_values=-1)
        allowed = attention_mask(segments[0], padding[0])
        cosine, sine = rotary_tables(length, HD)
        cos_pair = jnp.concatenate([cosine, cosine], axis=1)
        sin_pair = jnp.concatenate([sine, sine], axis=1)
        small = jnp.concatenate([attn_gain[:, None], ffn_gain[:, None], router_weight], axis=1)
        small = jnp.pad(small, ((0, 0), (0, 128 - small.shape[1])))
        attn = jnp.stack([query_weight, key_weight, value_weight, output_weight])

        near, far, near_z, far_z, *_, output, input_grad = layer_call(
            n,
            (
                tokens[0],
                allowed.astype(f32),
                cos_pair,
                sin_pair,
                tokens[0],
                cotangent[0],
                small,
                attn,
                slot,
                expert_gate,
                expert_up,
                expert_down,
                shared_gate,
                shared_up,
                shared_down,
            ),
        )
        done = finish(n, where, near, far, near_z, far_z)
        tail = done[10]
        return (
            output[None],
            input_grad[None],
            tail[:, 0],
            *done[6:10],
            tail[:, 1],
            tail[:, 2 : 2 + EXPERTS],
            *done[:3],
            *(v[0] for v in done[3:6]),
        )

    return shards


def make_shards(n, qn):
    plain, fast = make_plain(n, qn), make_fast(n, qn)

    def shards(*arguments):
        d, hidden = arguments[0].shape[2], arguments[13].shape[2]
        fits = n == 4 and qn == 4 and d == 768 and hidden == 2048 and arguments[0].shape[1] == 256
        return (fast if fits else plain)(*arguments)

    return shards


def solution(mesh):
    n, replicas = mesh.shape["shard"], mesh.shape["replica"]
    fine = Mesh(mesh.devices.reshape(n, replicas // 2, 2), ("shard", "plane", "core"))
    every = ("shard", "plane", "core")
    in_specs = (
        P(every, None, None),
        P(every, None, None),
        P(every, None),
        P(every, None),
        P(every, None, None),
        P(every, None),
        P("shard"),
        P("shard", None),
        P("shard", None),
        P("shard", None),
        P("shard", None),
        P("shard"),
        P("shard", None),
        P(None, "shard", None),
        P(None, "shard", None),
        P(None, "shard", None),
        P("shard", None),
        P("shard", None),
        P("shard", None),
    )
    out_specs = (
        P(every, None, None),
        P(every, None, None),
        P("shard"),
        P("shard", None),
        P("shard", None),
        P("shard", None),
        P("shard", None),
        P("shard"),
        P("shard", None),
        P(None, "shard", None),
        P(None, "shard", None),
        P(None, "shard", None),
        P("shard", None),
        P("shard", None),
        P("shard", None),
    )
    return jax.shard_map(
        make_shards(n, replicas // 2),
        mesh=fine,
        in_specs=in_specs,
        out_specs=out_specs,
        check_vma=False,
    )
```

```python
import functools
import math

import jax
import jax.numpy as jnp
from jax import lax
from jax.experimental import pallas as pl
from jax.experimental.pallas import tpu as pltpu
from jax.sharding import Mesh, PartitionSpec as P

NH = 12
HD = 64
EXPERTS = 6
TOPK = 2
CAP = 96
EPSILON = 1e-06
NEGATIVE = -1e30
GROUPS = ((0, 1), (2, 3), (4, 5))

highest = lax.Precision.HIGHEST
f32 = jnp.float32
bf16 = jnp.bfloat16


def dot(spec, first, second):
    return jnp.einsum(spec, first, second, preferred_element_type=f32)


def rotate_half(values):
    half_size = values.shape[-1] // 2
    return jnp.concatenate([-values[..., half_size:], values[..., :half_size]], axis=-1)


def rotate_back(values):
    half_size = values.shape[-1] // 2
    return jnp.concatenate([values[..., half_size:], -values[..., :half_size]], axis=-1)


def rotary_tables(length, head_dim):
    positions = jnp.arange(length, dtype=f32)
    frequency = jnp.exp(
        jnp.arange(head_dim // 2, dtype=f32) * (-2.0 * math.log(10000.0) / head_dim)
    )
    angles = positions[:, None] * frequency[None, :]
    angles = jnp.concatenate([angles, angles], axis=1)
    return (jnp.cos(angles), jnp.sin(angles))


def attention_mask(segments, padding):
    places = jnp.arange(segments.shape[0])
    causal = places[None, :] <= places[:, None]
    shared_doc = segments[:, None] == segments[None, :]
    usable = (padding[None, :] == 1) | (places[None, :] == places[:, None])
    return causal & shared_doc & usable


def norm_factor(values):
    return lax.rsqrt(jnp.mean(values * values, axis=-1, keepdims=True) + EPSILON)


def norm_back(values, factor, norm_gain, gradient):
    scaled = gradient * norm_gain
    gain_grad = jnp.sum(gradient * values * factor, axis=0)
    input_part = factor * scaled - values * factor**3 * jnp.mean(
        scaled * values, axis=-1, keepdims=True
    )
    return (input_part, gain_grad)


def silu_parts(gate_act):
    sigmoid = jax.nn.sigmoid(gate_act)
    return (gate_act * sigmoid, sigmoid * (1.0 + gate_act * (1.0 - sigmoid)))


def pair_slots(routes, padding, priority):
    length = routes.shape[0]
    pair_expert = routes.T.reshape(-1)
    pair_live = jnp.tile(padding, TOPK) == 1
    pair_key = (jnp.arange(TOPK, dtype=jnp.int32)[:, None] * length + priority[None, :]).reshape(-1)
    earlier = (
        (pair_key[None, :] < pair_key[:, None])
        & (pair_expert[None, :] == pair_expert[:, None])
        & pair_live[None, :]
    )
    place = jnp.sum(earlier.astype(jnp.int32), axis=1)
    kept = pair_live & (place < CAP)
    return (pair_expert, place, kept)


def swap(values, axis, mask, size):
    return lax.ppermute(values, axis, [(i, i ^ mask) for i in range(size)])


def pick_index(values, index, axis=0):
    return lax.dynamic_index_in_dim(values, index, axis, keepdims=False)


def mm(first, second, contract):
    return lax.dot_general(
        first, second, (contract, ((), ())), preferred_element_type=f32
    )


NN = ((1,), (0,))
NT = ((1,), (1,))
TN = ((0,), (0,))


def flip(value, mask, size):
    out = 0
    for b in range(size.bit_length() - 1):
        bit = (value // (1 << b)) % 2
        out = out + (1 << b) * ((1 - bit) if (mask >> b) & 1 else bit)
    return out


MESH = pl.DeviceIdType.MESH


def layer_kernel(
    n,
    tokens,
    allowed,
    cos_ref,
    sin_ref,
    tok_hbm,
    cot_hbm,
    small_own,
    attn_own,
    slot_own,
    eg,
    eu,
    ed,
    sg,
    su,
    sd,
    near_ref,
    far_ref,
    near_z,
    far_z,
    wide_hbm,
    work_hbm,
    soft_hbm,
    mid_hbm,
    w_land,
    out_ref,
    in_grad_ref,
    xg,
    acc_y,
    acc_t,
    work,
    dw,
    own,
    land,
    swap_in,
    y_side,
    y_in,
    wbuf,
    slot_ref,
    router_ref,
    probs_ref,
    small_ref,
    gate_s,
    pick_s,
    pick_acc,
    pick_side,
    pick_pair,
    pick_in,
    branch_s,
    ag_s,
    small_acc,
    z_own,
    z_swap,
    ch_send,
    ch_recv,
    x_send,
    x_recv,
    stay_sem,
    z_send,
    z_recv,
    zx_send,
    zx_recv,
    y_send_sem,
    y_recv_sem,
    p_send,
    p_recv,
    load_sem,
    free_side,
    free_in,
    gains_s,
    gains_side,
    gains_in,
    a_send,
    a_recv,
    w_send,
    w_recv,
    w_load,
    t_send,
    t_recv,
    side_send,
    side_recv,
):
    t = pl.program_id(0) - 1
    group = 2 * n
    length, d = tokens.shape
    hb = dw.shape[2]
    part = d // (2 * n)
    half = n * part
    chunks = 3 * (EXPERTS + 1)
    plane_rows = group * length
    s, q, c = (lax.axis_index(a) for a in ("shard", "plane", "core"))
    middle = (q == 1) | (q == 2)
    ends = (q == 0) | (q == 3)
    keep_h, give_h = (q + 1) % 2, q % 2
    other_mid = 3 - q
    mid_of = 1 + q // 3
    end_of = (q // 2) * 3
    other_c = 1 - c
    shard_of = [None] + [flip(s, m, n) for m in range(1, n)]

    def at_chunk(u, row=0, count=d):
        start = pl.multiple_of((u // 3) * d + row, 16)
        return pl.ds(start, count), pl.ds(pl.multiple_of((u % 3) * hb, 128), hb)

    def half_rows(h):
        return pl.ds(pl.multiple_of(h * half, 16), half)

    def remote(src, dst, ssem, rsem, to):
        return pltpu.make_async_remote_copy(
            src, dst, ssem, rsem, device_id=to, device_id_type=MESH
        )

    def chunk(kind, src, dst, u, to):
        return remote(src, dst, ch_send.at[kind, u], ch_recv.at[kind, u], to)

    def to_mid(u):
        return chunk(0, own.at[at_chunk(u)], land.at[u], u, {"plane": mid_of})

    def from_end(u):
        return chunk(0, own.at[at_chunk(u)], land.at[u], u, {"plane": end_of})

    def swap_sums(u):
        src = own.at[at_chunk(u, give_h * half, half)]
        return chunk(1, src, swap_in.at[u], u, {"plane": other_mid})

    def swap_done(u):
        ref = near_ref.at[u, half_rows(keep_h)]
        return chunk(2, ref, ref, u, {"plane": other_mid})

    def swap_done_in(u):
        ref = near_ref.at[u, half_rows(give_h)]
        return chunk(2, ref, ref, u, {"plane": other_mid})

    def to_end(u, first):
        ref = near_ref.at[u, half_rows(keep_h if first else give_h)]
        return chunk(3 if first else 4, ref, ref, u, {"plane": end_of})

    def from_mid(u, first):
        ref = near_ref.at[u, half_rows((q // 3) if first else 1 - q // 3)]
        return chunk(3 if first else 4, ref, ref, u, {"plane": mid_of})

    def across(u, m):
        return remote(
            own.at[at_chunk(u, keep_h * half + m * part, part)],
            near_ref.at[u, pl.ds(pl.multiple_of(keep_h * half + m * part, 16), part)],
            x_send.at[m - 1, u],
            x_recv.at[m - 1, u],
            {"shard": shard_of[m]},
        )

    def stay(u):
        return pltpu.make_async_copy(
            own.at[at_chunk(u, keep_h * half, part)],
            near_ref.at[u, pl.ds(pl.multiple_of(keep_h * half, 16), part)],
            stay_sem.at[u],
        )

    def side(u):
        return chunk(5, near_ref.at[u], far_ref.at[u], u, {"core": other_c})

    far_rows = pl.ds(0, plane_rows)

    def y_side_copy():
        return remote(
            work.at[far_rows], y_side, y_send_sem.at[0, 0], y_recv_sem.at[0, 0], {"core": other_c}
        )

    def y_across(k, m):
        at = pl.ds((k * n + m) * length, length)
        return remote(
            y_side.at[at],
            y_in.at[m - 1, k],
            y_send_sem.at[1 + k, m - 1],
            y_recv_sem.at[1 + k, m - 1],
            {"shard": shard_of[m]},
        )

    def pick_side_copy():
        return remote(
            pick_acc.at[pl.ds(n, n)], pick_side, p_send.at[0], p_recv.at[0], {"core": other_c}
        )

    def pick_across(m):
        return remote(
            pick_pair.at[m - 1],
            pick_in.at[m - 1],
            p_send.at[m],
            p_recv.at[m],
            {"shard": shard_of[m]},
        )

    def load(i, src, dst):
        return pltpu.make_async_copy(src, dst, load_sem.at[i])

    def back_rows(i):
        return pl.ds(i * length, length)

    two_w = [length, length + d, plane_rows + length, plane_rows + length + d]

    saved_rows = pl.ds(0, 5 * length)
    soft_rows = pl.ds(n * length, n * length)
    mid_rows = pl.ds(n * length, length)

    def saved_out():
        return [
            load(2, acc_y.at[soft_rows], soft_hbm),
            load(3, acc_t.at[mid_rows], mid_hbm),
            load(4, own.at[pl.ds(0, 4 * d)], wide_hbm),
            load(5, work.at[saved_rows], work_hbm),
        ]

    def saved_in():
        copies = [
            load(6, soft_hbm, acc_y.at[soft_rows]),
            load(7, mid_hbm, acc_t.at[mid_rows]),
            load(8, work_hbm, work.at[saved_rows]),
            load(9, tok_hbm, work.at[back_rows(5)]),
        ]
        for i in range(4):
            copies.append(load(10 + i, wide_hbm.at[pl.ds(i * d, d)], xg.at[pl.ds(two_w[i], d)]))
        return copies

    def columns(m):
        owner = s if m == 0 else shard_of[m]
        return pl.ds(pl.multiple_of((owner * 2 + c) * hb, 128), hb)

    def weight_ref(e, k, m, shared):
        big, one = ((eg, sg), (eu, su), (ed, sd))[k]
        return one.at[:, columns(m)] if shared else big.at[e, :, columns(m)]

    def weight_sends(e, shared):
        return [
            remote(
                weight_ref(e, k, m, shared),
                w_land.at[e, k, m - 1],
                w_send.at[e, 3 * k + m - 1],
                w_recv.at[e, 3 * k + m - 1],
                {"shard": shard_of[m]},
            )
            for k in range(3)
            for m in range(1, n)
        ]

    def weight_loads(e, shared):
        copies = []
        for k in range(3):
            for m in range(n):
                owner = s if m == 0 else shard_of[m]
                src = weight_ref(e, k, 0, shared) if m == 0 else w_land.at[e, k, m - 1]
                dst = wbuf.at[
                    e % 2, k, pl.ds(pl.multiple_of(owner * 2 * part, 16), 2 * part)
                ]
                copies.append(pltpu.make_async_copy(src, dst, w_load.at[e % 2, n * k + m]))
        return copies

    def for_expert(e, body):
        @pl.when(e < EXPERTS)
        def _():
            body(e, False)

        @pl.when(e == EXPERTS)
        def _():
            body(e, True)

    def fetch_weights(e, shared):
        for copy in weight_sends(e, shared):
            copy.wait()
        for copy in weight_loads(e, shared):
            copy.start()

    def start_weights(e, shared):
        for copy in weight_sends(e, shared):
            copy.start()

    def finish_weights(e, shared):
        for copy in weight_loads(e, shared):
            copy.wait()

    @pl.when(t < 0)
    def _():
        barrier = pltpu.get_barrier_semaphore()
        peers = [{"core": other_c}] + [{"shard": shard_of[m]} for m in range(1, n)]
        for peer in peers:
            pl.semaphore_signal(barrier, 1, device_id=peer, device_id_type=MESH)

        @pl.when(middle)
        def _():
            for peer in ({"plane": other_mid}, {"plane": end_of}):
                pl.semaphore_signal(barrier, 1, device_id=peer, device_id_type=MESH)
            pl.semaphore_wait(barrier, len(peers) + 2)

        @pl.when(ends)
        def _():
            pl.semaphore_signal(barrier, 1, device_id={"plane": mid_of}, device_id_type=MESH)
            pl.semaphore_wait(barrier, len(peers) + 1)

        my_rows = pl.multiple_of(s * 2 * part, 16)

        def wide_at(i, row, count):
            return own.at[pl.ds(pl.multiple_of((2 * c + i) * d + row, 16), count)]

        attn = [
            remote(
                attn_own.at[2 * c + i],
                wide_at(i, my_rows, 2 * part),
                a_send.at[i, m - 1],
                a_recv.at[i, m - 1],
                {"shard": shard_of[m]},
            )
            for i in range(2)
            for m in range(1, n)
        ]
        smalls = [
            remote(
                small_own,
                small_ref.at[pl.ds(my_rows, 2 * part)],
                a_send.at[2, m - 1],
                a_recv.at[2, m - 1],
                {"shard": shard_of[m]},
            )
            for m in range(1, n)
        ]
        stay_here = [
            load(i, attn_own.at[2 * c + i], wide_at(i, my_rows, 2 * part)) for i in range(2)
        ]
        stay_here += [
            load(14, small_own, small_ref.at[pl.ds(my_rows, 2 * part)]),
            load(15, cot_hbm, xg.at[pl.ds(plane_rows, length)]),
            load(16, slot_own, slot_ref.at[0]),
        ]
        for copy in smalls + attn + stay_here:
            copy.start()

        def spread_out(i, src, place):
            return [
                remote(
                    src, place(m), t_send.at[i, m - 1], t_recv.at[i, m - 1], {"shard": shard_of[m]}
                )
                for m in range(1, n)
            ]

        def to_core(i, src, dst):
            return remote(src, dst, side_send.at[i], side_recv.at[i], {"core": other_c})

        def rows_to_core(i, base):
            return to_core(
                i, xg.at[pl.ds(base, n * length)], xg.at[pl.ds(base + n * length, n * length)]
            )

        g_copies = spread_out(
            0, cot_hbm, lambda m: xg.at[pl.ds(plane_rows + m * length, length)]
        )
        slot_copies = spread_out(1, slot_own, lambda m: slot_ref.at[m])
        for copy in slot_copies + g_copies:
            copy.start()
        for e in range(EARLY):
            start_weights(e, False)
        for copy in stay_here:
            copy.wait()
        for copy in attn:
            copy.wait()
        pair_rows = own.at[pl.ds(pl.multiple_of(c * 2 * d, 16), 2 * d)]
        attn_side_copy = to_core(0, pair_rows, pair_rows)
        attn_side_copy.start()
        for copy in smalls:
            copy.wait()
        attn_side_copy.wait()
        work_part = lambda i: work.at[pl.ds(i * length, length)]
        outs = tuple(work_part(i) for i in range(5)) + (
            xg.at[pl.ds(0, length)],
            acc_t.at[mid_rows],
            acc_y.at[soft_rows],
            probs_ref,
        )
        router = attention_forward(
            tokens,
            small_ref,
            lambda i: own.at[pl.ds(i * d, d)],
            allowed,
            cos_ref,
            sin_ref,
            outs,
        )
        router_ref[0] = jnp.transpose(router)[0:8, :]
        for copy in saved_out():
            copy.start()
        x_copies = spread_out(
            2, xg.at[pl.ds(0, length)], lambda m: xg.at[pl.ds(m * length, length)]
        )
        rt_copies = spread_out(3, router_ref.at[0], lambda m: router_ref.at[m])
        for copy in x_copies + rt_copies:
            copy.start()

        for e in range(EARLY, AHEAD):
            start_weights(e, False)
        for copy in slot_copies + g_copies:
            copy.wait()
        g_side = rows_to_core(1, plane_rows)
        slot_side = to_core(2, slot_ref.at[pl.ds(0, n)], slot_ref.at[pl.ds(n, n)])
        g_side.start()
        slot_side.start()
        for copy in saved_out():
            copy.wait()
        acc_y[...] = jnp.zeros_like(acc_y)
        acc_t[...] = jnp.zeros_like(acc_t)
        pick_acc[...] = jnp.zeros_like(pick_acc)
        fetch_weights(0, False)
        for copy in x_copies + rt_copies:
            copy.wait()
        x_side = rows_to_core(3, 0)
        rt_side = to_core(4, router_ref.at[pl.ds(0, n)], router_ref.at[pl.ds(n, n)])
        x_side.start()
        rt_side.start()
        for copy in (g_side, slot_side, x_side, rt_side):
            copy.wait()

    def branch(x, gs_rows, wg, wu, wd):
        gate_act = mm(x, wg, NN)
        up_act = mm(x, wu, NN)
        sigmoid = 1.0 / (1.0 + jnp.exp(-gate_act))
        value = gate_act * sigmoid
        slope = sigmoid * (1.0 + gate_act * (1.0 - sigmoid))
        hid = (value * up_act).astype(bf16)
        hid_grad = mm(gs_rows, wd, NN)
        gate_d = (hid_grad * up_act * slope).astype(bf16)
        up_d = (hid_grad * value).astype(bf16)
        return hid, gate_d, up_d

    slots = group * CAP
    xs_at, gs_at, sg_at = 0, slots, 2 * slots

    @pl.when((t >= 0) & (t <= EXPERTS))
    def _():
        for_expert(t + AHEAD, start_weights)
        for_expert(t, finish_weights)

    @pl.when((t >= 0) & (t < EXPERTS))
    def _():
        ids = lax.broadcasted_iota(jnp.int32, (CAP, length), 0) + t * CAP

        def slots_of(b):
            first, second = slot_ref[b, 0:1, :], slot_ref[b, 1:2, :]
            return (first == ids) | (second == ids)

        for b in range(group):
            slot = pl.ds(b * CAP, CAP)
            hit = slots_of(b)
            hot = hit.astype(f32).astype(bf16)
            row = router_ref[b, pl.ds(t + 2, 1), :]
            gate = jnp.sum(jnp.where(hit, row, 0.0), axis=1, keepdims=True)
            gate_s[slot, :] = gate
            x_rows = mm(hot, xg[pl.ds(b * length, length), :], NN)
            work[pl.ds(xs_at + b * CAP, CAP), :] = x_rows.astype(bf16)
            g_rows = mm(hot, xg[pl.ds(plane_rows + b * length, length), :], NN)
            work[pl.ds(gs_at + b * CAP, CAP), :] = g_rows.astype(bf16)
            work[pl.ds(sg_at + b * CAP, CAP), :] = (g_rows * gate).astype(bf16)
        wg, wu, wd = wbuf[t % 2, 0], wbuf[t % 2, 1], wbuf[t % 2, 2]
        x, slot_grad = work[pl.ds(xs_at, slots), :], work[pl.ds(sg_at, slots), :]
        hid, gate_d, up_d = branch(x, slot_grad, wg, wu, wd)
        dw[0] = mm(x, gate_d, TN)
        dw[1] = mm(x, up_d, TN)
        dw[2] = mm(slot_grad, hid, TN)
        e_out = mm(hid, wd, NT)
        g_rows = work[pl.ds(gs_at, slots), :].astype(f32)
        pick_s[...] = jnp.sum(e_out * g_rows, axis=1, keepdims=True)
        work[pl.ds(gs_at, slots), :] = (e_out * gate_s[...]).astype(bf16)
        work[pl.ds(xs_at, slots), :] = (mm(gate_d, wg, NT) + mm(up_d, wu, NT)).astype(bf16)
        for b in range(group):
            slot = pl.ds(b * CAP, CAP)
            seq = pl.ds(b * length, length)
            hit = slots_of(b)
            hot = hit.astype(f32).astype(bf16)
            pick_acc[b, pl.ds(t + 2, 1), :] = jnp.sum(
                jnp.where(hit, pick_s[slot, :], 0.0), axis=0, keepdims=True
            )
            acc_y[seq, :] += mm(hot, work[pl.ds(gs_at + b * CAP, CAP), :], TN)
            acc_t[seq, :] += mm(hot, work[pl.ds(xs_at + b * CAP, CAP), :], TN)

    @pl.when(t == EXPERTS)
    def _():
        dw[...] = jnp.zeros_like(dw)
        wg, wu, wd = wbuf[t % 2, 0], wbuf[t % 2, 1], wbuf[t % 2, 2]

        def rows_step(i, carry):
            at = pl.multiple_of(i * 2 * length, 2 * length)
            rows = pl.ds(at, 2 * length)
            x, g = xg[rows, :], xg[pl.ds(plane_rows + at, 2 * length), :]
            hid, gate_d, up_d = branch(x, g, wg, wu, wd)
            dw[0] += mm(x, gate_d, TN)
            dw[1] += mm(x, up_d, TN)
            dw[2] += mm(g, hid, TN)
            acc_y[rows, :] += mm(hid, wd, NT)
            acc_t[rows, :] += mm(gate_d, wg, NT) + mm(up_d, wu, NT)
            return carry

        lax.fori_loop(0, n, rows_step, 0)
        work[pl.ds(0, n * length), :] = acc_y[soft_rows, :].astype(bf16)
        work[pl.ds(n * length, n * length), :] = acc_t[soft_rows, :].astype(bf16)

    @pl.when((t >= 0) & (t <= EXPERTS))
    def _():
        for k in range(3):
            for h in range(2):
                for m in range(n):
                    owner = s if m == 0 else shard_of[m]
                    start = pl.multiple_of((owner * 2 + h) * part, 16)
                    row = pl.multiple_of(t * d + (h * n + m) * part, 16)
                    own[pl.ds(row, part), k * hb : (k + 1) * hb] = dw[
                        k, pl.ds(start, part), :
                    ].astype(bf16)

        @pl.when(ends)
        def _():
            for k in range(3):
                to_mid(3 * t + k).start()

    @pl.when(t == EXPERTS)
    def _():
        y_side_copy().start()
        pick_side_copy().start()

    def add_halves(u):
        from_end(u).wait_recv()
        for i in range(2 * n):
            rows, columns_at = at_chunk(u, i * part, part)
            own[rows, columns_at] = (
                own[rows, columns_at].astype(f32)
                + land[u, pl.ds(i * part, part), :].astype(f32)
            ).astype(bf16)
        swap_sums(u).start()

    def add_swapped(u):
        swap_sums(u).wait()
        for m in range(n):
            rows, columns_at = at_chunk(u, keep_h * half + m * part, part)
            own[rows, columns_at] = (
                own[rows, columns_at].astype(f32)
                + swap_in[u, pl.ds(m * part, part), :].astype(f32)
            ).astype(bf16)
        for m in range(1, n):
            across(u, m).start()
        stay(u).start()

    def send_done(u):
        for m in range(1, n):
            across(u, m).wait()
        stay(u).wait()
        swap_done(u).start()
        to_end(u, True).start()

    def send_second(u):
        swap_done_in(u).wait_recv()
        to_end(u, False).start()
        side(u).start()

    def end_side(u):
        to_mid(u).wait_send()
        from_mid(u, True).wait_recv()
        from_mid(u, False).wait_recv()
        side(u).start()

    def middle_last(u):
        swap_done(u).wait_send()
        to_end(u, True).wait_send()
        to_end(u, False).wait_send()
        side(u).wait()

    mine_rows = pl.ds(0, length)
    grad_rows = pl.ds((n + 1) * length, length)

    def out_copy():
        return load(14, xg.at[mine_rows], out_ref)

    def in_grad_copy():
        return load(15, work.at[back_rows(5)], in_grad_ref)

    @pl.when(t == Y_STEPS[2])
    def _():
        total = acc_y[mine_rows, :]
        for m in range(1, n):
            y_across(0, m).wait()
            total = total + y_in[m - 1, 0].astype(f32)
        xg[mine_rows, :] = (acc_t[mid_rows, :] + total).astype(bf16)
        out_copy().start()
        pl.semaphore_signal(free_side, 1, device_id={"core": other_c}, device_id_type=MESH)
        for m in range(1, n):
            pl.semaphore_signal(free_in, 1, device_id={"shard": shard_of[m]}, device_id_type=MESH)

    stages = (
        (middle, add_halves),
        (middle, add_swapped),
        (middle, send_done),
        (middle, send_second),
        (ends, end_side),
        (middle, middle_last),
        (ends, lambda u: side(u).wait()),
    )

    def chunk_step(i, carry):
        v = t + jnp.minimum(t, DOUBLE) + i
        live = (i == 0) | (t < DOUBLE)
        for k in STAGE_ORDER:
            where, body = stages[k]
            u = v - STAGE_DELAY[k]

            @pl.when(live & (u >= 0) & (u < chunks) & where)
            def _():
                body(u)

        return carry

    lax.fori_loop(0, 2, chunk_step, 0)

    @pl.when((t >= 0) & (t < EXPERTS))
    def _():
        for_expert(t + 1, fetch_weights)

    @pl.when(t == Y_STEPS[0])
    def _():
        y_side_copy().wait()
        pick_side_copy().wait()
        for copy in saved_in():
            copy.start()
        pick_acc[pl.ds(0, n)] += pick_side[...]
        for m in range(1, n):
            pick_pair[m - 1] = pick_acc[m]
        for k, acc in ((1, acc_t), (0, acc_y)):
            for m in range(n):
                seq, at = pl.ds(m * length, length), pl.ds((k * n + m) * length, length)
                total = acc[seq, :] + y_side[at, :].astype(f32)
                if m == 0:
                    acc[seq, :] = total
                else:
                    y_side[at, :] = total.astype(bf16)
            for m in range(1, n):
                y_across(k, m).start()
                if k:
                    pick_across(m).start()

    pre_at = 6 * length
    exact = lax.Precision.HIGHEST

    @pl.when(t == Y_STEPS[1])
    def _():
        for m in range(1, n):
            y_across(1, m).wait()
            pick_across(m).wait()
        for copy in saved_in():
            copy.wait()
        two = acc_t[mine_rows, :]
        picks = pick_acc[0]
        for m in range(1, n):
            two = two + y_in[m - 1, 1].astype(f32)
            picks = picks + pick_in[m - 1]
        picks = jnp.concatenate([picks, jnp.zeros((120, length), f32)], axis=0)
        picks = jnp.transpose(picks)
        router = probs_ref[...]
        logit_grad = router * (picks - jnp.sum(router * picks, axis=1, keepdims=True))
        small = small_ref[...].astype(f32)
        gain_two = jnp.transpose(small)[1:2, :]
        two = two + lax.dot_general(
            logit_grad, small, (NT, ((), ())), precision=exact, preferred_element_type=f32
        )
        router_grad = lax.dot_general(
            logit_grad,
            xg[mine_rows, :].astype(f32),
            (TN, ((), ())),
            precision=exact,
            preferred_element_type=f32,
        )
        mid = acc_t[mid_rows, :]
        factor = lax.rsqrt(jnp.mean(mid * mid, axis=1, keepdims=True) + EPSILON)
        gain_grad = jnp.sum(two * mid * factor, axis=0, keepdims=True)
        row = lax.broadcasted_iota(jnp.int32, router_grad.shape, 0)
        small_acc[...] = jnp.where(row == 1, gain_grad, router_grad)
        scaled = two * gain_two
        grad = (
            xg[pl.ds(plane_rows, length), :].astype(f32)
            + factor * scaled
            - mid * (factor * factor * factor) * jnp.mean(scaled * mid, axis=1, keepdims=True)
        )
        acc_t[grad_rows, :] = grad
        branch_s[...] = grad.astype(bf16)
        ag_s[...] = mm(branch_s[...], xg[pl.ds(two_w[3], d), :], NT).astype(bf16)

    pair = 2 * HD

    @pl.when((t >= HEAD_STEP) & (t < HEAD_STEP + 3))
    def _():
        lane = lax.broadcasted_iota(jnp.int32, (length, pair), 1)
        first = lane < HD
        lower = lane % HD < HD // 2
        cos, sin = cos_ref[...], sin_ref[...]

        def turn_back(w):
            y = w * sin
            up = pltpu.roll(y, pair - HD // 2, 1)
            down = pltpu.roll(y, HD // 2, 1)
            return w * cos + jnp.where(lower, up, -down)

        def heads(i, carry):
            p = 2 * (t - HEAD_STEP) + i
            cut = pl.ds(pl.multiple_of(p * pair, pair), pair)
            queries, keys, values = (work[back_rows(j), cut] for j in range(3))
            grads = ag_s[:, cut]
            parts = []
            for one_side in range(2):
                h = 2 * p + one_side
                rows = pl.ds(pl.multiple_of(n * length + (h // 3) * length, length), length)
                columns = pl.ds(pl.multiple_of((h % 3) * length, length), length)
                soft = acc_y[rows, columns]
                mine = first if one_side == 0 else jnp.logical_not(first)
                chosen = jnp.where(mine, grads.astype(f32), 0.0).astype(bf16)
                prob_grad = mm(chosen, values, NT)
                inner = jnp.sum(soft * prob_grad, axis=1, keepdims=True)
                score_grad = (soft * (prob_grad - inner)).astype(bf16)
                parts.append(
                    (
                        mm(score_grad, keys, NN) * HD ** (-0.5),
                        mm(score_grad, queries, TN) * HD ** (-0.5),
                        mm(soft.astype(bf16), grads, TN),
                    )
                )
            joined = [jnp.where(first, parts[0][j], parts[1][j]) for j in range(3)]
            joined = [turn_back(joined[0]), turn_back(joined[1]), joined[2]]
            for j in range(3):
                work[pl.ds(pre_at + j * length, length), cut] = joined[j].astype(bf16)
            return carry

        lax.fori_loop(0, 2, heads, 0)

    two_d = 2 * d
    give_rows = pl.ds(pl.multiple_of((1 - c) * two_d, 16), two_d)

    def attn_side():
        return [
            remote(
                xg.at[give_rows],
                y_side.at[pl.ds(0, two_d)],
                z_send.at[5],
                z_recv.at[5],
                {"core": other_c},
            ),
            remote(gains_s, gains_side, z_send.at[7], z_recv.at[7], {"core": other_c}),
        ]

    def attn_across(m):
        copies = []
        at = pl.multiple_of(shard_of[m] * 2 * part, 16)
        for i in range(2):
            copies.append(
                remote(
                    xg.at[pl.ds(pl.multiple_of(c * two_d + i * d + at, 16), 2 * part)],
                    y_in.at[m - 1, i, pl.ds(0, 2 * part)],
                    zx_send.at[m - 1, i],
                    zx_recv.at[m - 1, i],
                    {"shard": shard_of[m]},
                )
            )
        copies.append(
            remote(
                gains_s.at[pl.ds(at, 2 * part)],
                gains_in.at[m - 1],
                zx_send.at[m - 1, 2],
                zx_recv.at[m - 1, 2],
                {"shard": shard_of[m]},
            )
        )
        return copies

    @pl.when(t == HEAD_STEP + 3)
    def _():
        pre = [work[pl.ds(pre_at + j * length, length), :] for j in range(3)]
        one_grad = mm(pre[0], xg[pl.ds(two_w[0], d), :], NT)
        for j in (1, 2):
            one_grad = one_grad + mm(pre[j], xg[pl.ds(two_w[j], d), :], NT)
        x = work[back_rows(5), :].astype(f32)
        gain_one = jnp.transpose(small_ref[...].astype(f32))[0:1, :]
        factor = lax.rsqrt(jnp.mean(x * x, axis=1, keepdims=True) + EPSILON)
        gain_grad = jnp.sum(one_grad * x * factor, axis=0, keepdims=True)
        scaled = one_grad * gain_one
        work[back_rows(5), :] = (
            acc_t[grad_rows, :]
            + factor * scaled
            - x * (factor * factor * factor) * jnp.mean(scaled * x, axis=1, keepdims=True)
        ).astype(bf16)
        in_grad_copy().start()
        out_copy().wait()
        gains = small_acc[...]
        row = lax.broadcasted_iota(jnp.int32, gains.shape, 0)
        gains_s[...] = jnp.transpose(jnp.where(row == 0, gain_grad, gains)).astype(bf16)
        for i in range(4):
            lhs = work[back_rows(4 if i < 3 else 3), :]
            for k in range(3):
                cut = slice(k * hb, (k + 1) * hb)
                rhs = work[pl.ds(pre_at + i * length, length), cut] if i < 3 else branch_s[:, cut]
                xg[pl.ds(i * d, d), cut] = mm(lhs, rhs, TN).astype(bf16)
        pl.semaphore_wait(free_side, 1)
        for copy in attn_side():
            copy.start()

    @pl.when(t == HEAD_STEP + 4)
    def _():
        in_grad_copy().wait()
        for copy in attn_side():
            copy.wait()
        for i in range(8):
            rows = pl.ds(pl.multiple_of(c * two_d + i * (d // 4), 16), d // 4)
            other = y_side[pl.ds(i * (d // 4), d // 4), :]
            xg[rows, :] = (xg[rows, :].astype(f32) + other.astype(f32)).astype(bf16)
        gains_s[...] = (gains_s[...].astype(f32) + gains_side[...].astype(f32)).astype(bf16)
        pl.semaphore_wait(free_in, n - 1)
        for m in range(1, n):
            for copy in attn_across(m):
                copy.start()

    def z_copy(i, src, dst, to):
        return remote(src, dst, z_send.at[i], z_recv.at[i], to)

    z_rows = 2 * part + 16
    z_land = y_side.at[pl.ds(two_d, 2 * z_rows)]

    def z_half(h):
        return pl.ds(pl.multiple_of(h * z_rows, 16), z_rows)

    def z_to_mid():
        return z_copy(0, z_own, z_land, {"plane": mid_of})

    def z_from_end():
        return z_copy(0, z_own, z_land, {"plane": end_of})

    def z_swap_sums():
        return z_copy(1, z_own.at[z_half(give_h)], z_swap, {"plane": other_mid})

    def z_swap_done():
        at = z_half(keep_h)
        return z_copy(2, z_own.at[at], near_z.at[at], {"plane": other_mid})

    def z_swap_done_in():
        at = z_half(give_h)
        return z_copy(2, z_own.at[at], near_z.at[at], {"plane": other_mid})

    def z_to_end(first):
        at = z_half(keep_h if first else give_h)
        source = z_own if first else near_z
        return z_copy(3 if first else 4, source.at[at], near_z.at[at], {"plane": end_of})

    def z_from_mid(first):
        at = z_half((q // 3) if first else 1 - q // 3)
        return z_copy(3 if first else 4, near_z.at[at], near_z.at[at], {"plane": mid_of})

    def z_stay():
        at = z_half(keep_h)
        return pltpu.make_async_copy(z_own.at[at], near_z.at[at], load_sem.at[17])

    def z_side():
        return z_copy(6, near_z, far_z, {"core": other_c})

    @pl.when(t == Z_STEPS[0])
    def _():
        for m in range(1, n):
            for copy in attn_across(m):
                copy.wait()
        for h in range(2):
            at = pl.multiple_of(s * 2 * part + h * part, 16)
            for i in range(2):
                total = xg[pl.ds(pl.multiple_of(c * two_d + i * d + at, 16), part), :].astype(f32)
                for m in range(1, n):
                    total = total + y_in[m - 1, i, pl.ds(h * part, part), :].astype(f32)
                z_own[pl.ds(h * z_rows + i * part, part), :] = total.astype(bf16)
            total = gains_s[pl.ds(at, part), :].astype(f32)
            for m in range(1, n):
                total = total + gains_in[m - 1, pl.ds(h * part, part), :].astype(f32)
            total = total.astype(bf16)
            for r in range(part // 16):
                z_own[pl.ds(h * z_rows + 2 * part, 16), r * 128 : (r + 1) * 128] = total[
                    r * 16 : (r + 1) * 16, :
                ]

        @pl.when(ends)
        def _():
            z_to_mid().start()

    @pl.when((t == Z_STEPS[1]) & middle)
    def _():
        z_from_end().wait_recv()
        for h in range(2):
            at = pl.ds(h * z_rows, z_rows)
            other = y_side[pl.ds(two_d + h * z_rows, z_rows), :]
            z_own[at, :] = (z_own[at, :].astype(f32) + other.astype(f32)).astype(bf16)
        z_swap_sums().start()

    @pl.when((t == Z_STEPS[2]) & middle)
    def _():
        z_swap_sums().wait()
        at = z_half(keep_h)
        z_own[at, :] = (z_own[at, :].astype(f32) + z_swap[...].astype(f32)).astype(bf16)
        z_stay().start()
        z_swap_done().start()
        z_to_end(True).start()

    @pl.when((t == Z_STEPS[3]) & middle)
    def _():
        z_swap_done_in().wait_recv()
        z_stay().wait()
        z_to_end(False).start()
        z_side().start()

    @pl.when((t == Z_STEPS[4]) & ends)
    def _():
        z_to_mid().wait_send()
        z_from_mid(True).wait_recv()
        z_from_mid(False).wait_recv()
        z_side().start()

    @pl.when(t == Z_STEPS[5])
    def _():
        z_side().wait()

        @pl.when(middle)
        def _():
            z_swap_done().wait_send()
            z_to_end(True).wait_send()
            z_to_end(False).wait_send()


EARLY, AHEAD = 1, 2
DOUBLE = 9
STAGE_DELAY = (1, 2, 5, 7, 10, 12, 12)
STAGE_ORDER = (0, 1, 2, 3, 4, 5, 6)
Y_STEPS = (7, 8, 10)
HEAD_STEP = 9
Z_STEPS = (17, 19, 20, 21, 23, 24)


def layer_call(n, operands):
    tokens, eg = operands[0], operands[9]
    length, d = tokens.shape
    hb = eg.shape[2] // (2 * n)
    rows = 2 * n * length
    slots = 2 * n * CAP
    chunks = 3 * (EXPERTS + 1)
    part = d // (2 * n)
    steps = 1 + max(chunks + max(STAGE_DELAY) - DOUBLE, Z_STEPS[5] + 1)
    vmem = lambda v: pl.BlockSpec(v.shape, lambda t: (0, 0), pipeline_mode=pl.Buffered(1))
    anywhere = pl.BlockSpec(memory_space=pl.ANY)
    dma = pltpu.SemaphoreType.DMA
    shape = jax.ShapeDtypeStruct
    z_pieces = (2 * (2 * part + 16), d)
    return pl.pallas_call(
        functools.partial(layer_kernel, n),
        grid=(steps,),
        in_specs=[vmem(v) for v in operands[:4]] + [anywhere] * (len(operands) - 4),
        out_specs=[anywhere] * 11,
        out_shape=[
            shape((chunks, d, hb), bf16),
            shape((chunks, d, hb), bf16),
            shape(z_pieces, bf16),
            shape(z_pieces, bf16),
            shape((4 * d, d), bf16),
            shape((5 * length, d), bf16),
            shape((n * length, d), f32),
            shape((length, d), f32),
            shape((EXPERTS + 1, 3, n - 1, 2 * part, hb), bf16),
            shape((length, d), bf16),
            shape((length, d), bf16),
        ],
        scratch_shapes=[
            pltpu.VMEM((2 * rows, d), bf16),
            pltpu.VMEM((rows, d), f32),
            pltpu.VMEM((rows, d), f32),
            pltpu.VMEM((max(3 * slots, rows, 9 * length), d), bf16),
            pltpu.VMEM((3, d, hb), f32),
            pltpu.VMEM(((EXPERTS + 1) * d, 3 * hb), bf16),
            pltpu.VMEM((chunks, d, hb), bf16),
            pltpu.VMEM((chunks, d // 2, hb), bf16),
            pltpu.VMEM((rows, d), bf16),
            pltpu.VMEM((n - 1, 2, length, d), bf16),
            pltpu.VMEM((2, 3, d, hb), bf16),
            pltpu.VMEM((2 * n, 8, length), jnp.int32),
            pltpu.VMEM((2 * n, 8, length), f32),
            pltpu.VMEM((length, 128), f32),
            pltpu.VMEM((d, 128), bf16),
            pltpu.VMEM((slots, 1), f32),
            pltpu.VMEM((slots, 1), f32),
            pltpu.VMEM((2 * n, 8, length), f32),
            pltpu.VMEM((n, 8, length), f32),
            pltpu.VMEM((n - 1, 8, length), f32),
            pltpu.VMEM((n - 1, 8, length), f32),
            pltpu.VMEM((length, d), bf16),
            pltpu.VMEM((length, d), bf16),
            pltpu.VMEM((128, d), f32),
            pltpu.VMEM(z_pieces, bf16),
            pltpu.VMEM((2 * part + 16, d), bf16),
            dma((6, chunks)),
            dma((6, chunks)),
            dma((n - 1, chunks)),
            dma((n - 1, chunks)),
            dma((chunks,)),
            dma((8,)),
            dma((8,)),
            dma((n - 1, 3)),
            dma((n - 1, 3)),
            dma((3, n - 1)),
            dma((3, n - 1)),
            dma((n,)),
            dma((n,)),
            dma((18,)),
            pltpu.SemaphoreType.REGULAR,
            pltpu.SemaphoreType.REGULAR,
            pltpu.VMEM((d, 128), bf16),
            pltpu.VMEM((d, 128), bf16),
            pltpu.VMEM((n - 1, 2 * part, 128), bf16),
            dma((3, n - 1)),
            dma((3, n - 1)),
            dma((EXPERTS + 1, 3 * (n - 1))),
            dma((EXPERTS + 1, 3 * (n - 1))),
            dma((2, 3 * n)),
            dma((4, n - 1)),
            dma((4, n - 1)),
            dma((5,)),
            dma((5,)),
        ],
        compiler_params=pltpu.CompilerParams(
            vmem_limit_bytes=67043328, collective_id=0, has_side_effects=True
        ),
        cost_estimate=pl.CostEstimate(
            flops=30 * 10**9, bytes_accessed=200 << 20, transcendentals=0
        ),
        name="layer",
    )(*operands)


def attention_forward(tokens, small, weight, allowed, cosine, sine, outs):
    q_ref, k_ref, v_ref, att_ref, one_ref, two_ref, mid_ref, soft_ref, router_ref = outs
    length, d = tokens.shape
    pair = 2 * HD
    small_rows = jnp.transpose(small[...].astype(f32))
    gain_one, gain_two = small_rows[0:1, :], small_rows[1:2, :]
    x = tokens[...].astype(f32)
    one = (x * lax.rsqrt(jnp.mean(x * x, axis=1, keepdims=True) + EPSILON) * gain_one).astype(bf16)
    one_ref[...] = one
    lane = lax.broadcasted_iota(jnp.int32, (length, pair), 1)
    lower = lane % HD < HD // 2
    cos, sin = cosine[...], sine[...]
    for i, ref in enumerate((q_ref, k_ref, v_ref)):
        for p in range(d // pair):
            cut = slice(p * pair, (p + 1) * pair)
            value = mm(one, weight(i)[:, cut], NN)
            if i < 2:
                up = pltpu.roll(value, pair - HD // 2, 1)
                down = pltpu.roll(value, HD // 2, 1)
                value = value * cos + jnp.where(lower, -up, down) * sin
            ref[:, cut] = value.astype(bf16)
    first = lane < HD

    def heads(p, carry):
        cut = pl.ds(pl.multiple_of(p * pair, pair), pair)
        queries, keys, values = q_ref[:, cut], k_ref[:, cut], v_ref[:, cut]
        parts = []
        for side in range(2):
            mine = first if side == 0 else jnp.logical_not(first)
            chosen = jnp.where(mine, queries.astype(f32), 0.0).astype(bf16)
            scores = mm(chosen, keys, NT) * HD ** (-0.5)
            scores = jnp.where(allowed[...] > 0.0, scores, NEGATIVE)
            exponent = jnp.exp(scores - jnp.max(scores, axis=1, keepdims=True))
            soft = exponent / jnp.sum(exponent, axis=1, keepdims=True)
            h = 2 * p + side
            at = pl.ds(pl.multiple_of((h // 3) * length, length), length)
            soft_ref[at, pl.ds(pl.multiple_of((h % 3) * length, length), length)] = soft
            parts.append(mm(soft.astype(bf16), values, NN))
        att_ref[:, cut] = jnp.where(first, parts[0], parts[1]).astype(bf16)
        return carry

    lax.fori_loop(0, d // pair, heads, 0)
    middle = x + mm(att_ref[...], weight(3)[...], NN)
    mid_ref[...] = middle
    two = middle * lax.rsqrt(jnp.mean(middle * middle, axis=1, keepdims=True) + EPSILON) * gain_two
    two = two.astype(bf16)
    two_ref[...] = two
    logits = mm(two, small[...], NN)
    column = lax.broadcasted_iota(jnp.int32, logits.shape, 1)
    valid = (column >= 2) & (column < 2 + EXPERTS)
    logits = jnp.where(valid, logits, NEGATIVE)
    exponent = jnp.exp(logits - jnp.max(logits, axis=1, keepdims=True))
    exponent = jnp.where(valid, exponent, 0.0)
    router = exponent / jnp.sum(exponent, axis=1, keepdims=True)
    router_ref[...] = router
    return router


def finish_kernel(n, where_ref, own_ref, far_ref, own_z, far_z, *outs):
    step = pl.program_id(0)
    s, c = where_ref[0], where_ref[1]
    part = own_ref.shape[1] // (2 * n)
    hb = own_ref.shape[2]
    z_rows = own_z.shape[0] // 2

    def write(targets):
        for side, ref in enumerate((own_ref, far_ref)):
            for m in range(n):
                column = pl.multiple_of(((s ^ m) * 2 + (c ^ side)) * hb, 128)
                for k in range(3):
                    for h in range(2):
                        row = (h * n + m) * part
                        targets[k][0, h * part : (h + 1) * part, pl.ds(column, hb)] = ref[
                            k, row : row + part, :
                        ].astype(f32)

    @pl.when(step < EXPERTS)
    def _():
        write(outs[:3])

    @pl.when(step == EXPERTS)
    def _():
        write(outs[3:6])

    @pl.when(step == 0)
    def _():
        tail = outs[10]
        for h in range(2):
            at = slice(h * z_rows, (h + 1) * z_rows)
            mine, other = own_z[at, :].astype(f32), far_z[at, :].astype(f32)
            low = jnp.where(c == 0, mine, other)
            high = jnp.where(c == 0, other, mine)
            for i, out in enumerate(outs[6:10]):
                source = (low if i < 2 else high)[(i % 2) * part : (i % 2 + 1) * part, :]
                out[h * part : (h + 1) * part, :] = source
            for r in range(part // 16):
                row = h * part + r * 16
                tail[row : row + 16, :] = low[2 * part : 2 * part + 16, r * 128 : (r + 1) * 128]


def finish(n, where, own, far, own_z, far_z):
    hb, d = own.shape[2], own.shape[1]
    rows, hidden = d // n, hb * 2 * n
    spec = pl.BlockSpec((3, d, hb), lambda i, *_: (i, 0, 0))
    z_spec = pl.BlockSpec(own_z.shape, lambda i, *_: (0, 0))
    expert = pl.BlockSpec((1, rows, hidden), lambda i, *_: (jnp.minimum(i, EXPERTS - 1), 0, 0))
    shared = pl.BlockSpec((1, rows, hidden), lambda i, *_: (0, 0, 0))
    square = pl.BlockSpec((rows, d), lambda i, *_: (0, 0))
    tail = pl.BlockSpec((rows, 128), lambda i, *_: (0, 0))
    shape = jax.ShapeDtypeStruct
    return pl.pallas_call(
        functools.partial(finish_kernel, n),
        grid_spec=pltpu.PrefetchScalarGridSpec(
            num_scalar_prefetch=1,
            grid=(EXPERTS + 1,),
            in_specs=[spec, spec, z_spec, z_spec],
            out_specs=[expert] * 3 + [shared] * 3 + [square] * 4 + [tail],
        ),
        out_shape=[shape((EXPERTS, rows, hidden), f32)] * 3
        + [shape((1, rows, hidden), f32)] * 3
        + [shape((rows, d), f32)] * 4
        + [shape((rows, 128), f32)],
        cost_estimate=pl.CostEstimate(
            flops=0, bytes_accessed=130 * rows * hidden, transcendentals=0
        ),
        compiler_params=pltpu.CompilerParams(vmem_limit_bytes=56 << 20),
        name="finish",
    )(where, own, far, own_z, far_z)


def make_plain(n, qn):
    bits = qn.bit_length() - 1

    def place_blocks(own, blocks):
        out = jnp.zeros((n,) + blocks[0].shape, blocks[0].dtype)
        for m in range(n):
            out = lax.dynamic_update_index_in_dim(out, blocks[m], own ^ m, 0)
        return out

    def join_bit(bit, own, other, axis):
        first = jnp.where(bit == 0, own, other)
        second = jnp.where(bit == 0, other, own)
        return jnp.concatenate([first, second], axis=axis)

    def shards(
        tokens,
        cotangent,
        segments,
        padding,
        routes,
        priority,
        attn_gain,
        query_weight,
        key_weight,
        value_weight,
        output_weight,
        ffn_gain,
        router_weight,
        expert_gate,
        expert_up,
        expert_down,
        shared_gate,
        shared_up,
        shared_down,
    ):
        s = lax.axis_index("shard")
        q = lax.axis_index("plane")
        c = lax.axis_index("core")
        length, d = tokens.shape[1], tokens.shape[2]
        rows = query_weight.shape[0]
        hidden = expert_gate.shape[2]
        hb = hidden // (2 * n)
        score_scale = HD ** (-0.5)

        small = jnp.concatenate(
            [attn_gain[:, None], ffn_gain[:, None], router_weight], axis=1
        )
        small = jnp.pad(small, ((0, 0), (0, 256 - small.shape[1])))
        wide = jnp.concatenate(
            [query_weight, key_weight, value_weight, output_weight, small], axis=1
        )
        half = wide.shape[1] // 2
        mine = lax.dynamic_slice_in_dim(wide, c * half, half, 1)
        blocks = [mine] + [swap(mine, "shard", m, n) for m in range(1, n)]
        mine = place_blocks(s, blocks).reshape(d, half)
        other = swap(mine, "core", 1, 2)
        wide = join_bit(c, mine, other, 1)
        wqkv, wo = wide[:, : 3 * d], wide[:, 3 * d : 4 * d]
        gain_one = wide[:, 4 * d].astype(f32)
        gain_two = wide[:, 4 * d + 1].astype(f32)
        wr = wide[:, 4 * d + 2 : 4 * d + 2 + EXPERTS]

        def block_for(m):
            start = ((s ^ m) * 2 + c) * hb
            cut = lambda w: lax.dynamic_slice_in_dim(w, start, hb, w.ndim - 1)
            return [
                jnp.concatenate([cut(e), cut(w)[None]], axis=0)
                for e, w in (
                    (expert_gate, shared_gate),
                    (expert_up, shared_up),
                    (expert_down, shared_down),
                )
            ]

        own_blocks = block_for(0)
        sent = [block_for(m) for m in range(1, n)]
        moe_w = []
        for k in range(3):
            got = [own_blocks[k]] + [swap(sent[m - 1][k], "shard", m, n) for m in range(1, n)]
            full = jnp.zeros((EXPERTS + 1, n, rows, hb), bf16)
            for m in range(n):
                full = lax.dynamic_update_index_in_dim(full, got[m], s ^ m, 1)
            moe_w.append(full.reshape(EXPERTS + 1, d, hb))

        def plane_gather(values):
            near = jnp.stack([values] + [swap(values, "shard", m, n) for m in range(1, n)])
            return jnp.concatenate([near, swap(near, "core", 1, 2)], axis=0)

        def plane_sum(partial):
            low = partial.astype(bf16)
            pair = (partial[:n] + swap(low[n:], "core", 1, 2).astype(f32)).astype(bf16)
            total = pair[0].astype(f32)
            for m in range(1, n):
                total = total + swap(pair[m], "shard", m, n).astype(f32)
            return total

        grads_b = plane_gather(cotangent[0])

        inputs = tokens[0].astype(f32)
        factor_one = norm_factor(inputs)
        normed_one = (inputs * factor_one * gain_one).astype(bf16)
        projected = jnp.dot(normed_one, wqkv, preferred_element_type=f32)
        cosine, sine = rotary_tables(length, HD)
        heads = projected.reshape(length, 3, NH, HD)
        cos_b, sin_b = cosine[:, None, :], sine[:, None, :]
        queries = (heads[:, 0] * cos_b + rotate_half(heads[:, 0]) * sin_b).astype(bf16)
        keys_rot = (heads[:, 1] * cos_b + rotate_half(heads[:, 1]) * sin_b).astype(bf16)
        values = heads[:, 2].astype(bf16)
        allowed = attention_mask(segments[0], padding[0])
        logits = dot("qhd,khd->hqk", queries, keys_rot) * score_scale
        logits = jnp.where(allowed[None], logits, NEGATIVE)
        maxima = jnp.max(logits, axis=-1, keepdims=True)
        exponent = jnp.exp(logits - maxima)
        soft = exponent / jnp.sum(exponent, axis=-1, keepdims=True)
        probs = soft.astype(bf16)
        attended = dot("hqk,khd->qhd", probs, values).reshape(length, d).astype(bf16)
        middle = inputs + jnp.dot(attended, wo, preferred_element_type=f32)
        factor_two = norm_factor(middle)
        normed_two = (middle * factor_two * gain_two).astype(bf16)
        router = jax.nn.softmax(
            jnp.dot(normed_two, wr, preferred_element_type=f32), axis=-1
        )

        pair_expert, place, kept = pair_slots(routes[0], padding[0], priority[0])
        slot_total = EXPERTS * CAP
        slot_index = jnp.where(kept, pair_expert * CAP + place, -1).reshape(TOPK, length)
        slots = jnp.arange(slot_total, dtype=jnp.int32)
        hit = (slots[None, :, None] == slot_index[:, None, :]).any(axis=0)
        onehot = hit.astype(bf16)
        token_of = jnp.max(
            jnp.where(hit, jnp.arange(length, dtype=jnp.int32)[None, :], -1), axis=1
        )
        slot_expert = jnp.repeat(jnp.arange(EXPERTS), CAP)
        gate_of = jnp.sum(
            jnp.where(hit, jnp.repeat(router.T, CAP, axis=0), 0.0), axis=1
        )

        tokens_b = plane_gather(normed_two)
        token_of_b = plane_gather(token_of)
        gate_of_b = plane_gather(gate_of)
        group = 2 * n
        onehot_b = (
            token_of_b[:, :, None] == jnp.arange(length, dtype=jnp.int32)[None, None, :]
        ).astype(bf16)
        onehot_b = onehot_b.reshape(group, EXPERTS, CAP, length)
        gate_b = gate_of_b.reshape(group, EXPERTS, CAP, 1)

        def reduce_and_return(stack):
            k = stack.shape[0]
            piece = rows // qn
            x = stack.reshape((k, n) + (2,) * bits + (piece, hb))
            for b in range(bits):
                axis = 2 + (bits - 1 - b)
                bit = (q >> b) & 1
                keep = pick_index(x, bit, axis)
                send = pick_index(x, 1 - bit, axis).astype(bf16)
                x = keep + swap(send, "plane", 1 << b, qn).astype(f32)
            x = x.astype(bf16)
            own = pick_index(x, s, 1)
            got = [own] + [swap(pick_index(x, s ^ m, 1), "shard", m, n) for m in range(1, n)]
            x = jnp.stack(got)
            x = x[None]
            for b in reversed(range(bits)):
                bit = (q >> b) & 1
                other = swap(x, "plane", 1 << b, qn)
                lead = x.shape[0]
                pair = jnp.stack(
                    [jnp.where(bit == 0, x, other), jnp.where(bit == 0, other, x)], axis=1
                )
                x = pair.reshape((2 * lead,) + x.shape[1:])
            other = swap(x, "core", 1, 2)
            x = jnp.stack(
                [jnp.where(c == 0, x, other), jnp.where(c == 0, other, x)]
            )
            out = jnp.zeros((n,) + (2, qn, k, piece, hb), bf16)
            for m in range(n):
                out = lax.dynamic_update_index_in_dim(out, x[:, :, m], s ^ m, 0)
            return out.transpose(3, 2, 4, 0, 1, 5).reshape(k, rows, hidden).astype(f32)

        w_gate, w_up, w_down = moe_w
        tokens_f = tokens_b.reshape(group * length, d)
        grads_f = grads_b.reshape(group * length, d)
        shared_g = jnp.dot(tokens_f, w_gate[EXPERTS], preferred_element_type=f32)
        shared_u = jnp.dot(tokens_f, w_up[EXPERTS], preferred_element_type=f32)
        value, slope = silu_parts(shared_g)
        shared_hidden = (value * shared_u).astype(bf16)
        shared_q = jnp.dot(grads_f, w_down[EXPERTS], preferred_element_type=f32)
        shared_gd = (shared_q * shared_u * slope).astype(bf16)
        shared_ud = (shared_q * value).astype(bf16)
        shared_grads = jnp.stack(
            [
                dot("ld,lh->dh", tokens_f, shared_gd),
                dot("ld,lh->dh", tokens_f, shared_ud),
                dot("ld,lh->dh", grads_f, shared_hidden),
            ]
        )
        out_partial = dot("lh,dh->ld", shared_hidden, w_down[EXPERTS])
        two_partial = dot("lh,dh->ld", shared_gd, w_gate[EXPERTS]) + dot(
            "lh,dh->ld", shared_ud, w_up[EXPERTS]
        )
        out_partial = out_partial.reshape(group, length, d)
        two_partial = two_partial.reshape(group, length, d)
        shared_done = reduce_and_return(shared_grads)

        pick_parts = []
        expert_done = []
        for part in GROUPS:
            lo, hi = part[0], part[-1] + 1
            hot = onehot_b[:, lo:hi]
            x_in = jnp.einsum("bect,btd->ebcd", hot, tokens_b, preferred_element_type=bf16)
            g_in = jnp.einsum("bect,btd->ebcd", hot, grads_b, preferred_element_type=bf16)
            gate_e = jnp.swapaxes(gate_b[:, lo:hi], 0, 1)
            wg, wu, wd = w_gate[lo:hi], w_up[lo:hi], w_down[lo:hi]
            gate_act = dot("ebcd,edh->ebch", x_in, wg)
            up_act = dot("ebcd,edh->ebch", x_in, wu)
            value, slope = silu_parts(gate_act)
            hid = (value * up_act).astype(bf16)
            e_out = dot("ebch,edh->ebcd", hid, wd)
            pick_parts.append(jnp.sum(e_out * g_in.astype(f32), axis=-1))
            slot_grad = (gate_e * g_in.astype(f32)).astype(bf16)
            hid_grad = dot("ebcd,edh->ebch", slot_grad, wd)
            gate_d = (hid_grad * up_act * slope).astype(bf16)
            up_d = (hid_grad * value).astype(bf16)
            in_grad = dot("ebch,edh->ebcd", gate_d, wg) + dot("ebch,edh->ebcd", up_d, wu)
            weighted = (gate_e * e_out).astype(bf16)
            out_partial = out_partial + dot("bect,ebcd->btd", hot, weighted)
            two_partial = two_partial + dot("bect,ebcd->btd", hot, in_grad.astype(bf16))
            stack = jnp.concatenate(
                [
                    dot("ebcd,ebch->edh", x_in, gate_d),
                    dot("ebcd,ebch->edh", x_in, up_d),
                    dot("ebcd,ebch->edh", slot_grad, hid),
                ]
            )
            expert_done.append(reduce_and_return(stack))

        two_grad = plane_sum(two_partial)
        picks = jnp.concatenate(pick_parts, axis=0)
        picks = jnp.swapaxes(picks, 0, 1).reshape(group, slot_total)
        picks = picks[:n] + swap(picks[n:], "core", 1, 2)
        pick_slot = picks[0]
        for m in range(1, n):
            pick_slot = pick_slot + swap(picks[m], "shard", m, n)
        mixed = plane_sum(out_partial)
        output = (middle + mixed).astype(bf16)

        upstream = cotangent[0].astype(f32)
        pick_grad = jnp.sum(
            jnp.where(hit, pick_slot[:, None], 0.0).reshape(EXPERTS, CAP, length), axis=1
        ).T
        logit_grad = router * (pick_grad - jnp.sum(router * pick_grad, axis=1, keepdims=True))
        two_grad = two_grad + jnp.dot(logit_grad, wr.astype(f32).T, precision=highest)
        router_grad = jnp.dot(normed_two.astype(f32).T, logit_grad, precision=highest)
        middle_part, ffn_gain_grad = norm_back(middle, factor_two, gain_two, two_grad)
        middle_grad = middle_part + upstream

        branch_grad = middle_grad.astype(bf16)
        output_weight_grad = dot("ld,le->de", attended, branch_grad)
        attended_grad = (
            dot("le,de->ld", branch_grad, wo).astype(bf16).reshape(length, NH, HD)
        )
        prob_grad = dot("qhd,khd->hqk", attended_grad, values)
        row_inner = jnp.sum(soft * prob_grad, axis=-1, keepdims=True)
        score_grad = (soft * (prob_grad - row_inner)).astype(bf16)
        query_parts = dot("hqk,khd->qhd", score_grad, keys_rot) * score_scale
        key_parts = dot("hqk,qhd->khd", score_grad, queries) * score_scale
        value_parts = dot("hqk,qhd->khd", probs, attended_grad)
        query_pre = query_parts * cos_b + rotate_back(query_parts * sin_b)
        key_pre = key_parts * cos_b + rotate_back(key_parts * sin_b)
        joint_grad = jnp.concatenate(
            [v.reshape(length, d) for v in (query_pre, key_pre, value_parts)], axis=1
        ).astype(bf16)
        one_grad = dot("lf,df->ld", joint_grad, wqkv)
        joint_weight_grad = dot("ld,lf->df", normed_one, joint_grad)
        input_part, attn_gain_grad = norm_back(inputs, factor_one, gain_one, one_grad)
        input_grad = (middle_grad + input_part).astype(bf16)

        small_grad = jnp.concatenate(
            [attn_gain_grad[:, None], ffn_gain_grad[:, None], router_grad], axis=1
        )
        small_grad = jnp.pad(small_grad, ((0, 0), (0, 256 - small_grad.shape[1])))
        total = jnp.concatenate([joint_weight_grad, output_weight_grad, small_grad], axis=1)
        keep = lax.dynamic_slice_in_dim(total, c * half, half, 1)
        send = lax.dynamic_slice_in_dim(total, (1 - c) * half, half, 1).astype(bf16)
        total = keep + swap(send, "core", 1, 2).astype(f32)
        total = total.reshape(n, rows, half)
        own = pick_index(total, s)
        low = total.astype(bf16)
        for m in range(1, n):
            own = own + swap(pick_index(low, s ^ m), "shard", m, n).astype(f32)
        x = own.reshape((2,) * bits + (rows // qn, half))
        for b in range(bits):
            axis = bits - 1 - b
            bit = (q >> b) & 1
            keep = pick_index(x, bit, axis)
            send = pick_index(x, 1 - bit, axis).astype(bf16)
            x = keep + swap(send, "plane", 1 << b, qn).astype(f32)
        x = x.astype(bf16)[None]
        for b in reversed(range(bits)):
            bit = (q >> b) & 1
            other = swap(x, "plane", 1 << b, qn)
            pair = jnp.stack(
                [jnp.where(bit == 0, x, other), jnp.where(bit == 0, other, x)], axis=1
            )
            x = pair.reshape((2 * x.shape[0],) + x.shape[1:])
        x = x.reshape(rows, half)
        x = join_bit(c, x, swap(x, "core", 1, 2), 1).astype(f32)
        stacks = [[], [], []]
        for part, done in zip(GROUPS, expert_done):
            for k in range(3):
                stacks[k].append(done[k * len(part) : (k + 1) * len(part)])
        expert_grads = [jnp.concatenate(parts, axis=0) for parts in stacks]
        return (
            output[None],
            input_grad[None],
            x[:, 4 * d],
            x[:, :d],
            x[:, d : 2 * d],
            x[:, 2 * d : 3 * d],
            x[:, 3 * d : 4 * d],
            x[:, 4 * d + 1],
            x[:, 4 * d + 2 : 4 * d + 2 + EXPERTS],
            expert_grads[0],
            expert_grads[1],
            expert_grads[2],
            shared_done[0],
            shared_done[1],
            shared_done[2],
        )

    return shards


def make_fast(n, qn):
    def shards(
        tokens,
        cotangent,
        segments,
        padding,
        routes,
        priority,
        attn_gain,
        query_weight,
        key_weight,
        value_weight,
        output_weight,
        ffn_gain,
        router_weight,
        expert_gate,
        expert_up,
        expert_down,
        shared_gate,
        shared_up,
        shared_down,
    ):
        s = lax.axis_index("shard")
        c = lax.axis_index("core")
        length, d = tokens.shape[1], tokens.shape[2]
        where = jnp.stack([s, c]).astype(jnp.int32)

        pair_expert, place, kept = pair_slots(routes[0], padding[0], priority[0])
        slot_index = jnp.where(kept, pair_expert * CAP + place, -1).reshape(TOPK, length)
        slot = jnp.pad(slot_index, ((0, 8 - TOPK), (0, 0)), constant_values=-1)
        allowed = attention_mask(segments[0], padding[0])
        cosine, sine = rotary_tables(length, HD)
        cos_pair = jnp.concatenate([cosine, cosine], axis=1)
        sin_pair = jnp.concatenate([sine, sine], axis=1)
        small = jnp.concatenate([attn_gain[:, None], ffn_gain[:, None], router_weight], axis=1)
        small = jnp.pad(small, ((0, 0), (0, 128 - small.shape[1])))
        attn = jnp.stack([query_weight, key_weight, value_weight, output_weight])

        near, far, near_z, far_z, *_, output, input_grad = layer_call(
            n,
            (
                tokens[0],
                allowed.astype(f32),
                cos_pair,
                sin_pair,
                tokens[0],
                cotangent[0],
                small,
                attn,
                slot,
                expert_gate,
                expert_up,
                expert_down,
                shared_gate,
                shared_up,
                shared_down,
            ),
        )
        done = finish(n, where, near, far, near_z, far_z)
        tail = done[10]
        return (
            output[None],
            input_grad[None],
            tail[:, 0],
            *done[6:10],
            tail[:, 1],
            tail[:, 2 : 2 + EXPERTS],
            *done[:3],
            *(v[0] for v in done[3:6]),
        )

    return shards


def make_shards(n, qn):
    plain, fast = make_plain(n, qn), make_fast(n, qn)

    def shards(*arguments):
        d, hidden = arguments[0].shape[2], arguments[13].shape[2]
        fits = n == 4 and qn == 4 and d == 768 and hidden == 2048 and arguments[0].shape[1] == 256
        return (fast if fits else plain)(*arguments)

    return shards


def solution(mesh):
    n, replicas = mesh.shape["shard"], mesh.shape["replica"]
    fine = Mesh(mesh.devices.reshape(n, replicas // 2, 2), ("shard", "plane", "core"))
    every = ("shard", "plane", "core")
    in_specs = (
        P(every, None, None),
        P(every, None, None),
        P(every, None),
        P(every, None),
        P(every, None, None),
        P(every, None),
        P("shard"),
        P("shard", None),
        P("shard", None),
        P("shard", None),
        P("shard", None),
        P("shard"),
        P("shard", None),
        P(None, "shard", None),
        P(None, "shard", None),
        P(None, "shard", None),
        P("shard", None),
        P("shard", None),
        P("shard", None),
    )
    out_specs = (
        P(every, None, None),
        P(every, None, None),
        P("shard"),
        P("shard", None),
        P("shard", None),
        P("shard", None),
        P("shard", None),
        P("shard"),
        P("shard", None),
        P(None, "shard", None),
        P(None, "shard", None),
        P(None, "shard", None),
        P("shard", None),
        P("shard", None),
        P("shard", None),
    )
    return jax.shard_map(
        make_shards(n, replicas // 2),
        mesh=fine,
        in_specs=in_specs,
        out_specs=out_specs,
        check_vma=False,
    )
```

```python
import functools
import math

import jax
import jax.numpy as jnp
from jax import lax
from jax.experimental import pallas as pl
from jax.experimental.pallas import tpu as pltpu
from jax.sharding import Mesh, PartitionSpec as P

NH = 12
HD = 64
EXPERTS = 6
TOPK = 2
CAP = 96
EPSILON = 1e-06
NEGATIVE = -1e30
GROUPS = ((0, 1), (2, 3), (4, 5))

highest = lax.Precision.HIGHEST
f32 = jnp.float32
bf16 = jnp.bfloat16


def dot(spec, first, second):
    return jnp.einsum(spec, first, second, preferred_element_type=f32)


def rotate_half(values):
    half_size = values.shape[-1] // 2
    return jnp.concatenate([-values[..., half_size:], values[..., :half_size]], axis=-1)


def rotate_back(values):
    half_size = values.shape[-1] // 2
    return jnp.concatenate([values[..., half_size:], -values[..., :half_size]], axis=-1)


def rotary_tables(length, head_dim):
    positions = jnp.arange(length, dtype=f32)
    frequency = jnp.exp(
        jnp.arange(head_dim // 2, dtype=f32) * (-2.0 * math.log(10000.0) / head_dim)
    )
    angles = positions[:, None] * frequency[None, :]
    angles = jnp.concatenate([angles, angles], axis=1)
    return (jnp.cos(angles), jnp.sin(angles))


def attention_mask(segments, padding):
    places = jnp.arange(segments.shape[0])
    causal = places[None, :] <= places[:, None]
    shared_doc = segments[:, None] == segments[None, :]
    usable = (padding[None, :] == 1) | (places[None, :] == places[:, None])
    return causal & shared_doc & usable


def norm_factor(values):
    return lax.rsqrt(jnp.mean(values * values, axis=-1, keepdims=True) + EPSILON)


def norm_back(values, factor, norm_gain, gradient):
    scaled = gradient * norm_gain
    gain_grad = jnp.sum(gradient * values * factor, axis=0)
    input_part = factor * scaled - values * factor**3 * jnp.mean(
        scaled * values, axis=-1, keepdims=True
    )
    return (input_part, gain_grad)


def silu_parts(gate_act):
    sigmoid = jax.nn.sigmoid(gate_act)
    return (gate_act * sigmoid, sigmoid * (1.0 + gate_act * (1.0 - sigmoid)))


def pair_slots(routes, padding, priority):
    length = routes.shape[0]
    pair_expert = routes.T.reshape(-1)
    pair_live = jnp.tile(padding, TOPK) == 1
    pair_key = (jnp.arange(TOPK, dtype=jnp.int32)[:, None] * length + priority[None, :]).reshape(-1)
    earlier = (
        (pair_key[None, :] < pair_key[:, None])
        & (pair_expert[None, :] == pair_expert[:, None])
        & pair_live[None, :]
    )
    place = jnp.sum(earlier.astype(jnp.int32), axis=1)
    kept = pair_live & (place < CAP)
    return (pair_expert, place, kept)


def swap(values, axis, mask, size):
    return lax.ppermute(values, axis, [(i, i ^ mask) for i in range(size)])


def pick_index(values, index, axis=0):
    return lax.dynamic_index_in_dim(values, index, axis, keepdims=False)


def mm(first, second, contract):
    return lax.dot_general(
        first, second, (contract, ((), ())), preferred_element_type=f32
    )


NN = ((1,), (0,))
NT = ((1,), (1,))
TN = ((0,), (0,))


def flip(value, mask, size):
    out = 0
    for b in range(size.bit_length() - 1):
        bit = (value // (1 << b)) % 2
        out = out + (1 << b) * ((1 - bit) if (mask >> b) & 1 else bit)
    return out


MESH = pl.DeviceIdType.MESH


def layer_kernel(
    n,
    tokens,
    meta_ref,
    cos_ref,
    sin_ref,
    tok_hbm,
    cot_hbm,
    small_own,
    wq,
    wk,
    wv,
    wo,
    eg,
    eu,
    ed,
    sg,
    su,
    sd,
    near_ref,
    far_ref,
    near_z,
    far_z,
    wide_hbm,
    work_hbm,
    soft_hbm,
    mid_hbm,
    w_land,
    out_ref,
    in_grad_ref,
    xg,
    acc_y,
    acc_t,
    work,
    dw,
    own,
    land,
    swap_in,
    y_side,
    y_in,
    wbuf,
    slot_ref,
    router_ref,
    probs_ref,
    small_ref,
    allowed,
    gate_s,
    pick_s,
    pick_acc,
    pick_side,
    pick_pair,
    pick_in,
    branch_s,
    ag_s,
    small_acc,
    z_own,
    z_swap,
    ch_send,
    ch_recv,
    x_send,
    x_recv,
    stay_sem,
    z_send,
    z_recv,
    zx_send,
    zx_recv,
    y_send_sem,
    y_recv_sem,
    p_send,
    p_recv,
    load_sem,
    free_side,
    free_in,
    gains_s,
    gains_side,
    gains_in,
    a_send,
    a_recv,
    w_send,
    w_recv,
    w_load,
    t_send,
    t_recv,
    side_send,
    side_recv,
):
    t = pl.program_id(0) - 1
    group = 2 * n
    length, d = tokens.shape
    hb = dw.shape[2]
    part = d // (2 * n)
    half = n * part
    chunks = 3 * (EXPERTS + 1)
    plane_rows = group * length
    s, q, c = (lax.axis_index(a) for a in ("shard", "plane", "core"))
    middle = (q == 1) | (q == 2)
    ends = (q == 0) | (q == 3)
    keep_h, give_h = (q + 1) % 2, q % 2
    other_mid = 3 - q
    mid_of = 1 + q // 3
    end_of = (q // 2) * 3
    other_c = 1 - c
    shard_of = [None] + [flip(s, m, n) for m in range(1, n)]

    def at_chunk(u, row=0, count=d):
        start = pl.multiple_of((u // 3) * d + row, 16)
        return pl.ds(start, count), pl.ds(pl.multiple_of((u % 3) * hb, 128), hb)

    def half_rows(h):
        return pl.ds(pl.multiple_of(h * half, 16), half)

    def remote(src, dst, ssem, rsem, to):
        return pltpu.make_async_remote_copy(
            src, dst, ssem, rsem, device_id=to, device_id_type=MESH
        )

    def chunk(kind, src, dst, u, to):
        return remote(src, dst, ch_send.at[kind, u], ch_recv.at[kind, u], to)

    def to_mid(u):
        return chunk(0, own.at[at_chunk(u)], land.at[u], u, {"plane": mid_of})

    def from_end(u):
        return chunk(0, own.at[at_chunk(u)], land.at[u], u, {"plane": end_of})

    def swap_sums(u):
        src = own.at[at_chunk(u, give_h * half, half)]
        return chunk(1, src, swap_in.at[u], u, {"plane": other_mid})

    def swap_done(u):
        ref = near_ref.at[u, half_rows(keep_h)]
        return chunk(2, ref, ref, u, {"plane": other_mid})

    def swap_done_in(u):
        ref = near_ref.at[u, half_rows(give_h)]
        return chunk(2, ref, ref, u, {"plane": other_mid})

    def to_end(u, first):
        ref = near_ref.at[u, half_rows(keep_h if first else give_h)]
        return chunk(3 if first else 4, ref, ref, u, {"plane": end_of})

    def from_mid(u, first):
        ref = near_ref.at[u, half_rows((q // 3) if first else 1 - q // 3)]
        return chunk(3 if first else 4, ref, ref, u, {"plane": mid_of})

    def across(u, m):
        return remote(
            own.at[at_chunk(u, keep_h * half + m * part, part)],
            near_ref.at[u, pl.ds(pl.multiple_of(keep_h * half + m * part, 16), part)],
            x_send.at[m - 1, u],
            x_recv.at[m - 1, u],
            {"shard": shard_of[m]},
        )

    def stay(u):
        return pltpu.make_async_copy(
            own.at[at_chunk(u, keep_h * half, part)],
            near_ref.at[u, pl.ds(pl.multiple_of(keep_h * half, 16), part)],
            stay_sem.at[u],
        )

    def side(u):
        return chunk(5, near_ref.at[u], far_ref.at[u], u, {"core": other_c})

    far_rows = pl.ds(0, plane_rows)

    def y_side_copy():
        return remote(
            work.at[far_rows], y_side, y_send_sem.at[0, 0], y_recv_sem.at[0, 0], {"core": other_c}
        )

    def y_across(k, m):
        at = pl.ds((k * n + m) * length, length)
        return remote(
            y_side.at[at],
            y_in.at[m - 1, k],
            y_send_sem.at[1 + k, m - 1],
            y_recv_sem.at[1 + k, m - 1],
            {"shard": shard_of[m]},
        )

    def pick_side_copy():
        return remote(
            pick_acc.at[pl.ds(n, n)], pick_side, p_send.at[0], p_recv.at[0], {"core": other_c}
        )

    def pick_across(m):
        return remote(
            pick_pair.at[m - 1],
            pick_in.at[m - 1],
            p_send.at[m],
            p_recv.at[m],
            {"shard": shard_of[m]},
        )

    def load(i, src, dst):
        return pltpu.make_async_copy(src, dst, load_sem.at[i])

    def back_rows(i):
        return pl.ds(i * length, length)

    two_w = [length, length + d, plane_rows + length, plane_rows + length + d]

    saved_rows = pl.ds(0, 5 * length)
    soft_rows = pl.ds(n * length, n * length)
    mid_rows = pl.ds(n * length, length)

    def saved_out():
        return [
            load(2, acc_y.at[soft_rows], soft_hbm),
            load(3, acc_t.at[mid_rows], mid_hbm),
            load(4, own.at[pl.ds(0, 4 * d)], wide_hbm),
            load(5, work.at[saved_rows], work_hbm),
        ]

    def saved_in():
        copies = [
            load(6, soft_hbm, acc_y.at[soft_rows]),
            load(7, mid_hbm, acc_t.at[mid_rows]),
            load(8, work_hbm, work.at[saved_rows]),
            load(9, tok_hbm, work.at[back_rows(5)]),
        ]
        for i in range(4):
            copies.append(load(10 + i, wide_hbm.at[pl.ds(i * d, d)], xg.at[pl.ds(two_w[i], d)]))
        return copies

    def columns(m):
        owner = s if m == 0 else shard_of[m]
        return pl.ds(pl.multiple_of((owner * 2 + c) * hb, 128), hb)

    def weight_ref(e, k, m, shared):
        big, one = ((eg, sg), (eu, su), (ed, sd))[k]
        return one.at[:, columns(m)] if shared else big.at[e, :, columns(m)]

    def weight_sends(e, shared):
        return [
            remote(
                weight_ref(e, k, m, shared),
                w_land.at[e, k, m - 1],
                w_send.at[e, 3 * k + m - 1],
                w_recv.at[e, 3 * k + m - 1],
                {"shard": shard_of[m]},
            )
            for k in range(3)
            for m in range(1, n)
        ]

    def weight_loads(e, shared):
        copies = []
        for k in range(3):
            for m in range(n):
                owner = s if m == 0 else shard_of[m]
                src = weight_ref(e, k, 0, shared) if m == 0 else w_land.at[e, k, m - 1]
                dst = wbuf.at[
                    e % 2, k, pl.ds(pl.multiple_of(owner * 2 * part, 16), 2 * part)
                ]
                copies.append(pltpu.make_async_copy(src, dst, w_load.at[e % 2, n * k + m]))
        return copies

    def for_expert(e, body):
        @pl.when(e < EXPERTS)
        def _():
            body(e, False)

        @pl.when(e == EXPERTS)
        def _():
            body(e, True)

    def fetch_weights(e, shared):
        for copy in weight_sends(e, shared):
            copy.wait()
        for copy in weight_loads(e, shared):
            copy.start()

    def start_weights(e, shared):
        for copy in weight_sends(e, shared):
            copy.start()

    def finish_weights(e, shared):
        for copy in weight_loads(e, shared):
            copy.wait()

    @pl.when(t < 0)
    def _():
        barrier = pltpu.get_barrier_semaphore()
        peers = [{"core": other_c}] + [{"shard": shard_of[m]} for m in range(1, n)]
        for peer in peers:
            pl.semaphore_signal(barrier, 1, device_id=peer, device_id_type=MESH)

        @pl.when(middle)
        def _():
            for peer in ({"plane": other_mid}, {"plane": end_of}):
                pl.semaphore_signal(barrier, 1, device_id=peer, device_id_type=MESH)
            pl.semaphore_wait(barrier, len(peers) + 2)

        @pl.when(ends)
        def _():
            pl.semaphore_signal(barrier, 1, device_id={"plane": mid_of}, device_id_type=MESH)
            pl.semaphore_wait(barrier, len(peers) + 1)

        my_rows = pl.multiple_of(s * 2 * part, 16)

        def wide_at(i, row, count):
            return own.at[pl.ds(pl.multiple_of((2 * c + i) * d + row, 16), count)]

        def attn_sends(i, source):
            return [
                remote(
                    source,
                    wide_at(i, my_rows, 2 * part),
                    a_send.at[i, m - 1],
                    a_recv.at[i, m - 1],
                    {"shard": shard_of[m]},
                )
                for m in range(1, n)
            ]

        def attn_stay(i, source):
            return load(i, source, wide_at(i, my_rows, 2 * part))

        smalls = [
            remote(
                small_own,
                small_ref.at[pl.ds(my_rows, 2 * part)],
                a_send.at[2, m - 1],
                a_recv.at[2, m - 1],
                {"shard": shard_of[m]},
            )
            for m in range(1, n)
        ]
        stay_here = [
            load(14, small_own, small_ref.at[pl.ds(my_rows, 2 * part)]),
            load(15, cot_hbm, xg.at[pl.ds(plane_rows, length)]),
        ]
        for copy in smalls + stay_here:
            copy.start()
        for core, pair_of in enumerate(((wq, wk), (wv, wo))):

            @pl.when(c == core)
            def _():
                for i in range(2):
                    attn_stay(i, pair_of[i]).start()
                    for copy in attn_sends(i, pair_of[i]):
                        copy.start()

        def spread_out(i, src, place):
            return [
                remote(
                    src, place(m), t_send.at[i, m - 1], t_recv.at[i, m - 1], {"shard": shard_of[m]}
                )
                for m in range(1, n)
            ]

        def to_core(i, src, dst):
            return remote(src, dst, side_send.at[i], side_recv.at[i], {"core": other_c})

        def rows_to_core(i, base):
            return to_core(
                i, xg.at[pl.ds(base, n * length)], xg.at[pl.ds(base + n * length, n * length)]
            )

        g_copies = spread_out(
            0, cot_hbm, lambda m: xg.at[pl.ds(plane_rows + m * length, length)]
        )
        slot_copies = spread_out(1, slot_ref.at[0], lambda m: slot_ref.at[m])
        for copy in g_copies:
            copy.start()
        for e in range(EARLY):
            start_weights(e, False)
        rows_of = meta_ref[...].astype(f32)
        columns_of = jnp.transpose(
            jnp.concatenate([rows_of, jnp.zeros((120, length), f32)], axis=0)
        )
        row = lambda r: rows_of[r : r + 1, :]
        column = lambda r: columns_of[:, r : r + 1]
        above = lax.broadcasted_iota(jnp.int32, (length, length), 0)
        along = lax.broadcasted_iota(jnp.int32, (length, length), 1)
        seen = (along <= above) & (column(0) == row(0)) & ((row(1) == 1.0) | (along == above))
        allowed[...] = jnp.where(seen, 1.0, 0.0)
        live = column(1) == 1.0
        sooner = live & (column(4) < row(4))
        count = lambda hits: jnp.sum(jnp.where(hits, 1.0, 0.0), axis=0, keepdims=True)
        places = (
            count(sooner & (column(2) == row(2))),
            count(live & (column(2) == row(3))) + count(sooner & (column(3) == row(3))),
        )
        line = lax.broadcasted_iota(jnp.int32, (8, length), 0)
        table = jnp.full((8, length), -1.0, f32)
        for k in range(TOPK):
            kept = (row(1) == 1.0) & (places[k] < CAP)
            place = jnp.where(kept, row(2 + k) * CAP + places[k], -1.0)
            table = jnp.where(line == k, place, table)
        slot_ref[0] = table.astype(jnp.int32)
        for copy in stay_here:
            copy.wait()

        def gather_attn(i):
            attn_stay(i, wq).wait()
            for copy in attn_sends(i, wq):
                copy.wait()
            at = wide_at(i, 0, d)
            copy = to_core(5 * i, at, at)
            copy.start()
            return copy

        first_half = gather_attn(0)
        for copy in slot_copies:
            copy.start()
        for copy in smalls:
            copy.wait()
        first_half.wait()

        def half_way():
            gather_attn(1).wait()

        work_part = lambda i: work.at[pl.ds(i * length, length)]
        outs = tuple(work_part(i) for i in range(5)) + (
            xg.at[pl.ds(0, length)],
            acc_t.at[mid_rows],
            acc_y.at[soft_rows],
            probs_ref,
        )
        router = attention_forward(
            tokens,
            small_ref,
            lambda i: own.at[pl.ds(i * d, d)],
            allowed,
            cos_ref,
            sin_ref,
            half_way,
            outs,
        )
        router_ref[0] = jnp.transpose(router)[0:8, :]
        for copy in saved_out():
            copy.start()
        x_copies = spread_out(
            2, xg.at[pl.ds(0, length)], lambda m: xg.at[pl.ds(m * length, length)]
        )
        rt_copies = spread_out(3, router_ref.at[0], lambda m: router_ref.at[m])
        for copy in x_copies + rt_copies:
            copy.start()

        for e in range(EARLY, AHEAD):
            start_weights(e, False)
        for copy in slot_copies + g_copies:
            copy.wait()
        g_side = rows_to_core(1, plane_rows)
        slot_side = to_core(2, slot_ref.at[pl.ds(0, n)], slot_ref.at[pl.ds(n, n)])
        g_side.start()
        slot_side.start()
        for copy in saved_out():
            copy.wait()
        acc_y[...] = jnp.zeros_like(acc_y)
        acc_t[...] = jnp.zeros_like(acc_t)
        pick_acc[...] = jnp.zeros_like(pick_acc)
        fetch_weights(0, False)
        for copy in x_copies + rt_copies:
            copy.wait()
        x_side = rows_to_core(3, 0)
        rt_side = to_core(4, router_ref.at[pl.ds(0, n)], router_ref.at[pl.ds(n, n)])
        x_side.start()
        rt_side.start()
        for copy in (g_side, slot_side, x_side, rt_side):
            copy.wait()

    def branch(x, gs_rows, wg, wu, wd):
        gate_act = mm(x, wg, NN)
        up_act = mm(x, wu, NN)
        sigmoid = 1.0 / (1.0 + jnp.exp(-gate_act))
        value = gate_act * sigmoid
        slope = sigmoid * (1.0 + gate_act * (1.0 - sigmoid))
        hid = (value * up_act).astype(bf16)
        hid_grad = mm(gs_rows, wd, NN)
        gate_d = (hid_grad * up_act * slope).astype(bf16)
        up_d = (hid_grad * value).astype(bf16)
        return hid, gate_d, up_d

    slots = group * CAP
    xs_at, gs_at, sg_at = 0, slots, 2 * slots

    @pl.when((t >= 0) & (t <= EXPERTS))
    def _():
        for_expert(t + AHEAD, start_weights)
        for_expert(t, finish_weights)

    @pl.when((t >= 0) & (t < EXPERTS))
    def _():
        ids = lax.broadcasted_iota(jnp.int32, (CAP, length), 0) + t * CAP

        def slots_of(b):
            first, second = slot_ref[b, 0:1, :], slot_ref[b, 1:2, :]
            return (first == ids) | (second == ids)

        for b in range(group):
            slot = pl.ds(b * CAP, CAP)
            hit = slots_of(b)
            hot = hit.astype(f32).astype(bf16)
            row = router_ref[b, pl.ds(t + 2, 1), :]
            gate = jnp.sum(jnp.where(hit, row, 0.0), axis=1, keepdims=True)
            gate_s[slot, :] = gate
            x_rows = mm(hot, xg[pl.ds(b * length, length), :], NN)
            work[pl.ds(xs_at + b * CAP, CAP), :] = x_rows.astype(bf16)
            g_rows = mm(hot, xg[pl.ds(plane_rows + b * length, length), :], NN)
            work[pl.ds(gs_at + b * CAP, CAP), :] = g_rows.astype(bf16)
            work[pl.ds(sg_at + b * CAP, CAP), :] = (g_rows * gate).astype(bf16)
        wg, wu, wd = wbuf[t % 2, 0], wbuf[t % 2, 1], wbuf[t % 2, 2]
        x, slot_grad = work[pl.ds(xs_at, slots), :], work[pl.ds(sg_at, slots), :]
        hid, gate_d, up_d = branch(x, slot_grad, wg, wu, wd)
        dw[0] = mm(x, gate_d, TN)
        dw[1] = mm(x, up_d, TN)
        dw[2] = mm(slot_grad, hid, TN)
        e_out = mm(hid, wd, NT)
        g_rows = work[pl.ds(gs_at, slots), :].astype(f32)
        pick_s[...] = jnp.sum(e_out * g_rows, axis=1, keepdims=True)
        work[pl.ds(gs_at, slots), :] = (e_out * gate_s[...]).astype(bf16)
        work[pl.ds(xs_at, slots), :] = (mm(gate_d, wg, NT) + mm(up_d, wu, NT)).astype(bf16)
        for b in range(group):
            slot = pl.ds(b * CAP, CAP)
            seq = pl.ds(b * length, length)
            hit = slots_of(b)
            hot = hit.astype(f32).astype(bf16)
            pick_acc[b, pl.ds(t + 2, 1), :] = jnp.sum(
                jnp.where(hit, pick_s[slot, :], 0.0), axis=0, keepdims=True
            )
            acc_y[seq, :] += mm(hot, work[pl.ds(gs_at + b * CAP, CAP), :], TN)
            acc_t[seq, :] += mm(hot, work[pl.ds(xs_at + b * CAP, CAP), :], TN)

    @pl.when(t == EXPERTS)
    def _():
        dw[...] = jnp.zeros_like(dw)
        wg, wu, wd = wbuf[t % 2, 0], wbuf[t % 2, 1], wbuf[t % 2, 2]

        def rows_step(i, carry):
            at = pl.multiple_of(i * 2 * length, 2 * length)
            rows = pl.ds(at, 2 * length)
            x, g = xg[rows, :], xg[pl.ds(plane_rows + at, 2 * length), :]
            hid, gate_d, up_d = branch(x, g, wg, wu, wd)
            dw[0] += mm(x, gate_d, TN)
            dw[1] += mm(x, up_d, TN)
            dw[2] += mm(g, hid, TN)
            acc_y[rows, :] += mm(hid, wd, NT)
            acc_t[rows, :] += mm(gate_d, wg, NT) + mm(up_d, wu, NT)
            return carry

        lax.fori_loop(0, n, rows_step, 0)
        work[pl.ds(0, n * length), :] = acc_y[soft_rows, :].astype(bf16)
        work[pl.ds(n * length, n * length), :] = acc_t[soft_rows, :].astype(bf16)

    @pl.when((t >= 0) & (t <= EXPERTS))
    def _():
        for k in range(3):
            for h in range(2):
                for m in range(n):
                    owner = s if m == 0 else shard_of[m]
                    start = pl.multiple_of((owner * 2 + h) * part, 16)
                    row = pl.multiple_of(t * d + (h * n + m) * part, 16)
                    own[pl.ds(row, part), k * hb : (k + 1) * hb] = dw[
                        k, pl.ds(start, part), :
                    ].astype(bf16)

        @pl.when(ends)
        def _():
            for k in range(3):
                to_mid(3 * t + k).start()

    @pl.when(t == EXPERTS)
    def _():
        y_side_copy().start()
        pick_side_copy().start()

    def add_halves(u):
        from_end(u).wait_recv()
        for i in range(2 * n):
            rows, columns_at = at_chunk(u, i * part, part)
            own[rows, columns_at] = (
                own[rows, columns_at].astype(f32)
                + land[u, pl.ds(i * part, part), :].astype(f32)
            ).astype(bf16)
        swap_sums(u).start()

    def add_swapped(u):
        swap_sums(u).wait()
        for m in range(n):
            rows, columns_at = at_chunk(u, keep_h * half + m * part, part)
            own[rows, columns_at] = (
                own[rows, columns_at].astype(f32)
                + swap_in[u, pl.ds(m * part, part), :].astype(f32)
            ).astype(bf16)
        for m in range(1, n):
            across(u, m).start()
        stay(u).start()

    def send_done(u):
        for m in range(1, n):
            across(u, m).wait()
        stay(u).wait()
        swap_done(u).start()
        to_end(u, True).start()

    def send_second(u):
        swap_done_in(u).wait_recv()
        to_end(u, False).start()
        side(u).start()

    def end_side(u):
        to_mid(u).wait_send()
        from_mid(u, True).wait_recv()
        from_mid(u, False).wait_recv()
        side(u).start()

    def middle_last(u):
        swap_done(u).wait_send()
        to_end(u, True).wait_send()
        to_end(u, False).wait_send()
        side(u).wait()

    mine_rows = pl.ds(0, length)
    grad_rows = pl.ds((n + 1) * length, length)

    def out_copy():
        return load(14, xg.at[mine_rows], out_ref)

    def in_grad_copy():
        return load(15, work.at[back_rows(5)], in_grad_ref)

    @pl.when(t == Y_STEPS[2])
    def _():
        total = acc_y[mine_rows, :]
        for m in range(1, n):
            y_across(0, m).wait()
            total = total + y_in[m - 1, 0].astype(f32)
        xg[mine_rows, :] = (acc_t[mid_rows, :] + total).astype(bf16)
        out_copy().start()
        pl.semaphore_signal(free_side, 1, device_id={"core": other_c}, device_id_type=MESH)
        for m in range(1, n):
            pl.semaphore_signal(free_in, 1, device_id={"shard": shard_of[m]}, device_id_type=MESH)

    stages = (
        (middle, add_halves),
        (middle, add_swapped),
        (middle, send_done),
        (middle, send_second),
        (ends, end_side),
        (middle, middle_last),
        (ends, lambda u: side(u).wait()),
    )

    def chunk_step(i, carry):
        v = t + jnp.minimum(t, DOUBLE) + i
        live = (i == 0) | (t < DOUBLE)
        for k in STAGE_ORDER:
            where, body = stages[k]
            u = v - STAGE_DELAY[k]

            @pl.when(live & (u >= 0) & (u < chunks) & where)
            def _():
                body(u)

        return carry

    lax.fori_loop(0, 2, chunk_step, 0)

    @pl.when((t >= 0) & (t < EXPERTS))
    def _():
        for_expert(t + 1, fetch_weights)

    @pl.when(t == Y_STEPS[0])
    def _():
        y_side_copy().wait()
        pick_side_copy().wait()
        for copy in saved_in():
            copy.start()
        pick_acc[pl.ds(0, n)] += pick_side[...]
        for m in range(1, n):
            pick_pair[m - 1] = pick_acc[m]
        for k, acc in ((1, acc_t), (0, acc_y)):
            for m in range(n):
                seq, at = pl.ds(m * length, length), pl.ds((k * n + m) * length, length)
                total = acc[seq, :] + y_side[at, :].astype(f32)
                if m == 0:
                    acc[seq, :] = total
                else:
                    y_side[at, :] = total.astype(bf16)
            for m in range(1, n):
                y_across(k, m).start()
                if k:
                    pick_across(m).start()

    pre_at = 6 * length
    exact = lax.Precision.HIGHEST

    @pl.when(t == Y_STEPS[1])
    def _():
        for m in range(1, n):
            y_across(1, m).wait()
            pick_across(m).wait()
        for copy in saved_in():
            copy.wait()
        two = acc_t[mine_rows, :]
        picks = pick_acc[0]
        for m in range(1, n):
            two = two + y_in[m - 1, 1].astype(f32)
            picks = picks + pick_in[m - 1]
        picks = jnp.concatenate([picks, jnp.zeros((120, length), f32)], axis=0)
        picks = jnp.transpose(picks)
        router = probs_ref[...]
        logit_grad = router * (picks - jnp.sum(router * picks, axis=1, keepdims=True))
        small = small_ref[...].astype(f32)
        gain_two = jnp.transpose(small)[1:2, :]
        two = two + lax.dot_general(
            logit_grad, small, (NT, ((), ())), precision=exact, preferred_element_type=f32
        )
        router_grad = lax.dot_general(
            logit_grad,
            xg[mine_rows, :].astype(f32),
            (TN, ((), ())),
            precision=exact,
            preferred_element_type=f32,
        )
        mid = acc_t[mid_rows, :]
        factor = lax.rsqrt(jnp.mean(mid * mid, axis=1, keepdims=True) + EPSILON)
        gain_grad = jnp.sum(two * mid * factor, axis=0, keepdims=True)
        row = lax.broadcasted_iota(jnp.int32, router_grad.shape, 0)
        small_acc[...] = jnp.where(row == 1, gain_grad, router_grad)
        scaled = two * gain_two
        grad = (
            xg[pl.ds(plane_rows, length), :].astype(f32)
            + factor * scaled
            - mid * (factor * factor * factor) * jnp.mean(scaled * mid, axis=1, keepdims=True)
        )
        acc_t[grad_rows, :] = grad
        branch_s[...] = grad.astype(bf16)
        ag_s[...] = mm(branch_s[...], xg[pl.ds(two_w[3], d), :], NT).astype(bf16)

    pair = 2 * HD

    @pl.when((t >= HEAD_STEP) & (t < HEAD_STEP + 3))
    def _():
        lane = lax.broadcasted_iota(jnp.int32, (length, pair), 1)
        first = lane < HD
        lower = lane % HD < HD // 2
        cos, sin = cos_ref[...], sin_ref[...]

        def turn_back(w):
            y = w * sin
            up = pltpu.roll(y, pair - HD // 2, 1)
            down = pltpu.roll(y, HD // 2, 1)
            return w * cos + jnp.where(lower, up, -down)

        def heads(i, carry):
            p = 2 * (t - HEAD_STEP) + i
            cut = pl.ds(pl.multiple_of(p * pair, pair), pair)
            queries, keys, values = (work[back_rows(j), cut] for j in range(3))
            grads = ag_s[:, cut]
            parts = []
            for one_side in range(2):
                h = 2 * p + one_side
                rows = pl.ds(pl.multiple_of(n * length + (h // 3) * length, length), length)
                columns = pl.ds(pl.multiple_of((h % 3) * length, length), length)
                soft = acc_y[rows, columns]
                mine = first if one_side == 0 else jnp.logical_not(first)
                chosen = jnp.where(mine, grads.astype(f32), 0.0).astype(bf16)
                prob_grad = mm(chosen, values, NT)
                inner = jnp.sum(soft * prob_grad, axis=1, keepdims=True)
                score_grad = (soft * (prob_grad - inner)).astype(bf16)
                parts.append(
                    (
                        mm(score_grad, keys, NN) * HD ** (-0.5),
                        mm(score_grad, queries, TN) * HD ** (-0.5),
                        mm(soft.astype(bf16), grads, TN),
                    )
                )
            joined = [jnp.where(first, parts[0][j], parts[1][j]) for j in range(3)]
            joined = [turn_back(joined[0]), turn_back(joined[1]), joined[2]]
            for j in range(3):
                work[pl.ds(pre_at + j * length, length), cut] = joined[j].astype(bf16)
            return carry

        lax.fori_loop(0, 2, heads, 0, unroll=True)

    two_d = 2 * d
    give_rows = pl.ds(pl.multiple_of((1 - c) * two_d, 16), two_d)

    def attn_side():
        return [
            remote(
                xg.at[give_rows],
                y_side.at[pl.ds(0, two_d)],
                z_send.at[5],
                z_recv.at[5],
                {"core": other_c},
            ),
            remote(gains_s, gains_side, z_send.at[7], z_recv.at[7], {"core": other_c}),
        ]

    def attn_across(m):
        copies = []
        at = pl.multiple_of(shard_of[m] * 2 * part, 16)
        for i in range(2):
            copies.append(
                remote(
                    xg.at[pl.ds(pl.multiple_of(c * two_d + i * d + at, 16), 2 * part)],
                    y_in.at[m - 1, i, pl.ds(0, 2 * part)],
                    zx_send.at[m - 1, i],
                    zx_recv.at[m - 1, i],
                    {"shard": shard_of[m]},
                )
            )
        copies.append(
            remote(
                gains_s.at[pl.ds(at, 2 * part)],
                gains_in.at[m - 1],
                zx_send.at[m - 1, 2],
                zx_recv.at[m - 1, 2],
                {"shard": shard_of[m]},
            )
        )
        return copies

    @pl.when(t == HEAD_STEP + 3)
    def _():
        pre = [work[pl.ds(pre_at + j * length, length), :] for j in range(3)]
        one_grad = mm(pre[0], xg[pl.ds(two_w[0], d), :], NT)
        for j in (1, 2):
            one_grad = one_grad + mm(pre[j], xg[pl.ds(two_w[j], d), :], NT)
        x = work[back_rows(5), :].astype(f32)
        gain_one = jnp.transpose(small_ref[...].astype(f32))[0:1, :]
        factor = lax.rsqrt(jnp.mean(x * x, axis=1, keepdims=True) + EPSILON)
        gain_grad = jnp.sum(one_grad * x * factor, axis=0, keepdims=True)
        scaled = one_grad * gain_one
        work[back_rows(5), :] = (
            acc_t[grad_rows, :]
            + factor * scaled
            - x * (factor * factor * factor) * jnp.mean(scaled * x, axis=1, keepdims=True)
        ).astype(bf16)
        in_grad_copy().start()
        out_copy().wait()
        gains = small_acc[...]
        row = lax.broadcasted_iota(jnp.int32, gains.shape, 0)
        gains_s[...] = jnp.transpose(jnp.where(row == 0, gain_grad, gains)).astype(bf16)
        for i in range(4):
            lhs = work[back_rows(4 if i < 3 else 3), :]
            for k in range(3):
                cut = slice(k * hb, (k + 1) * hb)
                rhs = work[pl.ds(pre_at + i * length, length), cut] if i < 3 else branch_s[:, cut]
                xg[pl.ds(i * d, d), cut] = mm(lhs, rhs, TN).astype(bf16)
        pl.semaphore_wait(free_side, 1)
        for copy in attn_side():
            copy.start()

    @pl.when(t == HEAD_STEP + 4)
    def _():
        in_grad_copy().wait()
        for copy in attn_side():
            copy.wait()
        for i in range(8):
            rows = pl.ds(pl.multiple_of(c * two_d + i * (d // 4), 16), d // 4)
            other = y_side[pl.ds(i * (d // 4), d // 4), :]
            xg[rows, :] = (xg[rows, :].astype(f32) + other.astype(f32)).astype(bf16)
        gains_s[...] = (gains_s[...].astype(f32) + gains_side[...].astype(f32)).astype(bf16)
        pl.semaphore_wait(free_in, n - 1)
        for m in range(1, n):
            for copy in attn_across(m):
                copy.start()

    def z_copy(i, src, dst, to):
        return remote(src, dst, z_send.at[i], z_recv.at[i], to)

    z_rows = 2 * part + 16
    z_land = y_side.at[pl.ds(two_d, 2 * z_rows)]

    def z_half(h):
        return pl.ds(pl.multiple_of(h * z_rows, 16), z_rows)

    def z_to_mid():
        return z_copy(0, z_own, z_land, {"plane": mid_of})

    def z_from_end():
        return z_copy(0, z_own, z_land, {"plane": end_of})

    def z_swap_sums():
        return z_copy(1, z_own.at[z_half(give_h)], z_swap, {"plane": other_mid})

    def z_swap_done():
        at = z_half(keep_h)
        return z_copy(2, z_own.at[at], near_z.at[at], {"plane": other_mid})

    def z_swap_done_in():
        at = z_half(give_h)
        return z_copy(2, z_own.at[at], near_z.at[at], {"plane": other_mid})

    def z_to_end(first):
        at = z_half(keep_h if first else give_h)
        source = z_own if first else near_z
        return z_copy(3 if first else 4, source.at[at], near_z.at[at], {"plane": end_of})

    def z_from_mid(first):
        at = z_half((q // 3) if first else 1 - q // 3)
        return z_copy(3 if first else 4, near_z.at[at], near_z.at[at], {"plane": mid_of})

    def z_stay():
        at = z_half(keep_h)
        return pltpu.make_async_copy(z_own.at[at], near_z.at[at], load_sem.at[17])

    def z_side():
        return z_copy(6, near_z, far_z, {"core": other_c})

    @pl.when(t == Z_STEPS[0])
    def _():
        for m in range(1, n):
            for copy in attn_across(m):
                copy.wait()
        for h in range(2):
            at = pl.multiple_of(s * 2 * part + h * part, 16)
            for i in range(2):
                total = xg[pl.ds(pl.multiple_of(c * two_d + i * d + at, 16), part), :].astype(f32)
                for m in range(1, n):
                    total = total + y_in[m - 1, i, pl.ds(h * part, part), :].astype(f32)
                z_own[pl.ds(h * z_rows + i * part, part), :] = total.astype(bf16)
            total = gains_s[pl.ds(at, part), :].astype(f32)
            for m in range(1, n):
                total = total + gains_in[m - 1, pl.ds(h * part, part), :].astype(f32)
            total = total.astype(bf16)
            for r in range(part // 16):
                z_own[pl.ds(h * z_rows + 2 * part, 16), r * 128 : (r + 1) * 128] = total[
                    r * 16 : (r + 1) * 16, :
                ]

        @pl.when(ends)
        def _():
            z_to_mid().start()

    @pl.when((t == Z_STEPS[1]) & middle)
    def _():
        z_from_end().wait_recv()
        for h in range(2):
            at = pl.ds(h * z_rows, z_rows)
            other = y_side[pl.ds(two_d + h * z_rows, z_rows), :]
            z_own[at, :] = (z_own[at, :].astype(f32) + other.astype(f32)).astype(bf16)
        z_swap_sums().start()

    @pl.when((t == Z_STEPS[2]) & middle)
    def _():
        z_swap_sums().wait()
        at = z_half(keep_h)
        z_own[at, :] = (z_own[at, :].astype(f32) + z_swap[...].astype(f32)).astype(bf16)
        z_stay().start()
        z_swap_done().start()
        z_to_end(True).start()

    @pl.when((t == Z_STEPS[3]) & middle)
    def _():
        z_swap_done_in().wait_recv()
        z_stay().wait()
        z_to_end(False).start()
        z_side().start()

    @pl.when((t == Z_STEPS[4]) & ends)
    def _():
        z_to_mid().wait_send()
        z_from_mid(True).wait_recv()
        z_from_mid(False).wait_recv()
        z_side().start()

    @pl.when(t == Z_STEPS[5])
    def _():
        z_side().wait()

        @pl.when(middle)
        def _():
            z_swap_done().wait_send()
            z_to_end(True).wait_send()
            z_to_end(False).wait_send()


EARLY, AHEAD = 1, 2
DOUBLE = 9
STAGE_DELAY = (1, 2, 5, 7, 10, 12, 12)
STAGE_ORDER = (0, 1, 2, 3, 4, 5, 6)
Y_STEPS = (7, 8, 10)
HEAD_STEP = 9
Z_STEPS = (17, 19, 20, 21, 23, 24)


def layer_call(n, operands):
    tokens, eg = operands[0], operands[11]
    length, d = tokens.shape
    hb = eg.shape[2] // (2 * n)
    rows = 2 * n * length
    slots = 2 * n * CAP
    chunks = 3 * (EXPERTS + 1)
    part = d // (2 * n)
    steps = 1 + max(chunks + max(STAGE_DELAY) - DOUBLE, Z_STEPS[5] + 1)
    vmem = lambda v: pl.BlockSpec(v.shape, lambda t: (0, 0), pipeline_mode=pl.Buffered(1))
    anywhere = pl.BlockSpec(memory_space=pl.ANY)
    dma = pltpu.SemaphoreType.DMA
    shape = jax.ShapeDtypeStruct
    z_pieces = (2 * (2 * part + 16), d)
    return pl.pallas_call(
        functools.partial(layer_kernel, n),
        grid=(steps,),
        in_specs=[vmem(v) for v in operands[:4]] + [anywhere] * (len(operands) - 4),
        out_specs=[anywhere] * 11,
        out_shape=[
            shape((chunks, d, hb), bf16),
            shape((chunks, d, hb), bf16),
            shape(z_pieces, bf16),
            shape(z_pieces, bf16),
            shape((4 * d, d), bf16),
            shape((5 * length, d), bf16),
            shape((n * length, d), f32),
            shape((length, d), f32),
            shape((EXPERTS + 1, 3, n - 1, 2 * part, hb), bf16),
            shape((length, d), bf16),
            shape((length, d), bf16),
        ],
        scratch_shapes=[
            pltpu.VMEM((2 * rows, d), bf16),
            pltpu.VMEM((rows, d), f32),
            pltpu.VMEM((rows, d), f32),
            pltpu.VMEM((max(3 * slots, rows, 9 * length), d), bf16),
            pltpu.VMEM((3, d, hb), f32),
            pltpu.VMEM(((EXPERTS + 1) * d, 3 * hb), bf16),
            pltpu.VMEM((chunks, d, hb), bf16),
            pltpu.VMEM((chunks, d // 2, hb), bf16),
            pltpu.VMEM((rows, d), bf16),
            pltpu.VMEM((n - 1, 2, length, d), bf16),
            pltpu.VMEM((2, 3, d, hb), bf16),
            pltpu.VMEM((2 * n, 8, length), jnp.int32),
            pltpu.VMEM((2 * n, 8, length), f32),
            pltpu.VMEM((length, 128), f32),
            pltpu.VMEM((d, 128), bf16),
            pltpu.VMEM((length, length), f32),
            pltpu.VMEM((slots, 1), f32),
            pltpu.VMEM((slots, 1), f32),
            pltpu.VMEM((2 * n, 8, length), f32),
            pltpu.VMEM((n, 8, length), f32),
            pltpu.VMEM((n - 1, 8, length), f32),
            pltpu.VMEM((n - 1, 8, length), f32),
            pltpu.VMEM((length, d), bf16),
            pltpu.VMEM((length, d), bf16),
            pltpu.VMEM((128, d), f32),
            pltpu.VMEM(z_pieces, bf16),
            pltpu.VMEM((2 * part + 16, d), bf16),
            dma((6, chunks)),
            dma((6, chunks)),
            dma((n - 1, chunks)),
            dma((n - 1, chunks)),
            dma((chunks,)),
            dma((8,)),
            dma((8,)),
            dma((n - 1, 3)),
            dma((n - 1, 3)),
            dma((3, n - 1)),
            dma((3, n - 1)),
            dma((n,)),
            dma((n,)),
            dma((18,)),
            pltpu.SemaphoreType.REGULAR,
            pltpu.SemaphoreType.REGULAR,
            pltpu.VMEM((d, 128), bf16),
            pltpu.VMEM((d, 128), bf16),
            pltpu.VMEM((n - 1, 2 * part, 128), bf16),
            dma((3, n - 1)),
            dma((3, n - 1)),
            dma((EXPERTS + 1, 3 * (n - 1))),
            dma((EXPERTS + 1, 3 * (n - 1))),
            dma((2, 3 * n)),
            dma((4, n - 1)),
            dma((4, n - 1)),
            dma((6,)),
            dma((6,)),
        ],
        compiler_params=pltpu.CompilerParams(
            vmem_limit_bytes=67043328, collective_id=0, has_side_effects=True
        ),
        cost_estimate=pl.CostEstimate(
            flops=30 * 10**9, bytes_accessed=200 << 20, transcendentals=0
        ),
        name="layer",
    )(*operands)


def attention_forward(tokens, small, weight, allowed, cosine, sine, half_way, outs):
    q_ref, k_ref, v_ref, att_ref, one_ref, two_ref, mid_ref, soft_ref, router_ref = outs
    length, d = tokens.shape
    pair = 2 * HD
    small_rows = jnp.transpose(small[...].astype(f32))
    gain_one, gain_two = small_rows[0:1, :], small_rows[1:2, :]
    x = tokens[...].astype(f32)
    one = (x * lax.rsqrt(jnp.mean(x * x, axis=1, keepdims=True) + EPSILON) * gain_one).astype(bf16)
    one_ref[...] = one
    lane = lax.broadcasted_iota(jnp.int32, (length, pair), 1)
    lower = lane % HD < HD // 2
    cos, sin = cosine[...], sine[...]
    for i, ref in ((0, q_ref), (2, v_ref), (1, k_ref)):
        if i == 1:
            half_way()
        for p in range(d // (2 * pair)):
            wide = mm(one, weight(i)[:, 2 * p * pair : 2 * (p + 1) * pair], NN)
            for r in range(2):
                cut = slice((2 * p + r) * pair, (2 * p + r + 1) * pair)
                value = wide[:, r * pair : (r + 1) * pair]
                if i < 2:
                    up = pltpu.roll(value, pair - HD // 2, 1)
                    down = pltpu.roll(value, HD // 2, 1)
                    value = value * cos + jnp.where(lower, -up, down) * sin
                ref[:, cut] = value.astype(bf16)
    first = lane < HD

    def heads(p, carry):
        cut = pl.ds(pl.multiple_of(p * pair, pair), pair)
        queries, keys, values = q_ref[:, cut], k_ref[:, cut], v_ref[:, cut]
        parts = []
        for side in range(2):
            mine = first if side == 0 else jnp.logical_not(first)
            chosen = jnp.where(mine, queries.astype(f32), 0.0).astype(bf16)
            scores = mm(chosen, keys, NT) * HD ** (-0.5)
            scores = jnp.where(allowed[...] > 0.0, scores, NEGATIVE)
            exponent = jnp.exp(scores - jnp.max(scores, axis=1, keepdims=True))
            soft = exponent / jnp.sum(exponent, axis=1, keepdims=True)
            h = 2 * p + side
            at = pl.ds(pl.multiple_of((h // 3) * length, length), length)
            soft_ref[at, pl.ds(pl.multiple_of((h % 3) * length, length), length)] = soft
            parts.append(mm(soft.astype(bf16), values, NN))
        att_ref[:, cut] = jnp.where(first, parts[0], parts[1]).astype(bf16)
        return carry

    lax.fori_loop(0, d // pair, heads, 0, unroll=3)
    middle = x + mm(att_ref[...], weight(3)[...], NN)
    mid_ref[...] = middle
    two = middle * lax.rsqrt(jnp.mean(middle * middle, axis=1, keepdims=True) + EPSILON) * gain_two
    two = two.astype(bf16)
    two_ref[...] = two
    logits = mm(two, small[...], NN)
    column = lax.broadcasted_iota(jnp.int32, logits.shape, 1)
    valid = (column >= 2) & (column < 2 + EXPERTS)
    logits = jnp.where(valid, logits, NEGATIVE)
    exponent = jnp.exp(logits - jnp.max(logits, axis=1, keepdims=True))
    exponent = jnp.where(valid, exponent, 0.0)
    router = exponent / jnp.sum(exponent, axis=1, keepdims=True)
    router_ref[...] = router
    return router


def finish_kernel(n, where_ref, own_ref, far_ref, own_z, far_z, *outs):
    step = pl.program_id(0)
    s, c = where_ref[0], where_ref[1]
    part = own_ref.shape[1] // (2 * n)
    hb = own_ref.shape[2]
    z_rows = own_z.shape[0] // 2

    def write(targets):
        for side, ref in enumerate((own_ref, far_ref)):
            for m in range(n):
                column = pl.multiple_of(((s ^ m) * 2 + (c ^ side)) * hb, 128)
                for k in range(3):
                    for h in range(2):
                        row = (h * n + m) * part
                        targets[k][0, h * part : (h + 1) * part, pl.ds(column, hb)] = ref[
                            k, row : row + part, :
                        ].astype(f32)

    @pl.when(step < EXPERTS)
    def _():
        write(outs[:3])

    @pl.when(step == EXPERTS)
    def _():
        write(outs[3:6])

    @pl.when(step == 0)
    def _():
        tail = outs[10]
        for h in range(2):
            at = slice(h * z_rows, (h + 1) * z_rows)
            mine, other = own_z[at, :].astype(f32), far_z[at, :].astype(f32)
            low = jnp.where(c == 0, mine, other)
            high = jnp.where(c == 0, other, mine)
            for i, out in enumerate(outs[6:10]):
                source = (low if i < 2 else high)[(i % 2) * part : (i % 2 + 1) * part, :]
                out[h * part : (h + 1) * part, :] = source
            for r in range(part // 16):
                row = h * part + r * 16
                tail[row : row + 16, :] = low[2 * part : 2 * part + 16, r * 128 : (r + 1) * 128]


def finish(n, where, own, far, own_z, far_z):
    hb, d = own.shape[2], own.shape[1]
    rows, hidden = d // n, hb * 2 * n
    spec = pl.BlockSpec((3, d, hb), lambda i, *_: (i, 0, 0))
    z_spec = pl.BlockSpec(own_z.shape, lambda i, *_: (0, 0))
    expert = pl.BlockSpec((1, rows, hidden), lambda i, *_: (jnp.minimum(i, EXPERTS - 1), 0, 0))
    shared = pl.BlockSpec((1, rows, hidden), lambda i, *_: (0, 0, 0))
    square = pl.BlockSpec((rows, d), lambda i, *_: (0, 0))
    tail = pl.BlockSpec((rows, 128), lambda i, *_: (0, 0))
    shape = jax.ShapeDtypeStruct
    return pl.pallas_call(
        functools.partial(finish_kernel, n),
        grid_spec=pltpu.PrefetchScalarGridSpec(
            num_scalar_prefetch=1,
            grid=(EXPERTS + 1,),
            in_specs=[spec, spec, z_spec, z_spec],
            out_specs=[expert] * 3 + [shared] * 3 + [square] * 4 + [tail],
        ),
        out_shape=[shape((EXPERTS, rows, hidden), f32)] * 3
        + [shape((1, rows, hidden), f32)] * 3
        + [shape((rows, d), f32)] * 4
        + [shape((rows, 128), f32)],
        cost_estimate=pl.CostEstimate(
            flops=0, bytes_accessed=130 * rows * hidden, transcendentals=0
        ),
        compiler_params=pltpu.CompilerParams(vmem_limit_bytes=56 << 20),
        name="finish",
    )(where, own, far, own_z, far_z)


def make_plain(n, qn):
    bits = qn.bit_length() - 1

    def place_blocks(own, blocks):
        out = jnp.zeros((n,) + blocks[0].shape, blocks[0].dtype)
        for m in range(n):
            out = lax.dynamic_update_index_in_dim(out, blocks[m], own ^ m, 0)
        return out

    def join_bit(bit, own, other, axis):
        first = jnp.where(bit == 0, own, other)
        second = jnp.where(bit == 0, other, own)
        return jnp.concatenate([first, second], axis=axis)

    def shards(
        tokens,
        cotangent,
        segments,
        padding,
        routes,
        priority,
        attn_gain,
        query_weight,
        key_weight,
        value_weight,
        output_weight,
        ffn_gain,
        router_weight,
        expert_gate,
        expert_up,
        expert_down,
        shared_gate,
        shared_up,
        shared_down,
    ):
        s = lax.axis_index("shard")
        q = lax.axis_index("plane")
        c = lax.axis_index("core")
        length, d = tokens.shape[1], tokens.shape[2]
        rows = query_weight.shape[0]
        hidden = expert_gate.shape[2]
        hb = hidden // (2 * n)
        score_scale = HD ** (-0.5)

        small = jnp.concatenate(
            [attn_gain[:, None], ffn_gain[:, None], router_weight], axis=1
        )
        small = jnp.pad(small, ((0, 0), (0, 256 - small.shape[1])))
        wide = jnp.concatenate(
            [query_weight, key_weight, value_weight, output_weight, small], axis=1
        )
        half = wide.shape[1] // 2
        mine = lax.dynamic_slice_in_dim(wide, c * half, half, 1)
        blocks = [mine] + [swap(mine, "shard", m, n) for m in range(1, n)]
        mine = place_blocks(s, blocks).reshape(d, half)
        other = swap(mine, "core", 1, 2)
        wide = join_bit(c, mine, other, 1)
        wqkv, wo = wide[:, : 3 * d], wide[:, 3 * d : 4 * d]
        gain_one = wide[:, 4 * d].astype(f32)
        gain_two = wide[:, 4 * d + 1].astype(f32)
        wr = wide[:, 4 * d + 2 : 4 * d + 2 + EXPERTS]

        def block_for(m):
            start = ((s ^ m) * 2 + c) * hb
            cut = lambda w: lax.dynamic_slice_in_dim(w, start, hb, w.ndim - 1)
            return [
                jnp.concatenate([cut(e), cut(w)[None]], axis=0)
                for e, w in (
                    (expert_gate, shared_gate),
                    (expert_up, shared_up),
                    (expert_down, shared_down),
                )
            ]

        own_blocks = block_for(0)
        sent = [block_for(m) for m in range(1, n)]
        moe_w = []
        for k in range(3):
            got = [own_blocks[k]] + [swap(sent[m - 1][k], "shard", m, n) for m in range(1, n)]
            full = jnp.zeros((EXPERTS + 1, n, rows, hb), bf16)
            for m in range(n):
                full = lax.dynamic_update_index_in_dim(full, got[m], s ^ m, 1)
            moe_w.append(full.reshape(EXPERTS + 1, d, hb))

        def plane_gather(values):
            near = jnp.stack([values] + [swap(values, "shard", m, n) for m in range(1, n)])
            return jnp.concatenate([near, swap(near, "core", 1, 2)], axis=0)

        def plane_sum(partial):
            low = partial.astype(bf16)
            pair = (partial[:n] + swap(low[n:], "core", 1, 2).astype(f32)).astype(bf16)
            total = pair[0].astype(f32)
            for m in range(1, n):
                total = total + swap(pair[m], "shard", m, n).astype(f32)
            return total

        grads_b = plane_gather(cotangent[0])

        inputs = tokens[0].astype(f32)
        factor_one = norm_factor(inputs)
        normed_one = (inputs * factor_one * gain_one).astype(bf16)
        projected = jnp.dot(normed_one, wqkv, preferred_element_type=f32)
        cosine, sine = rotary_tables(length, HD)
        heads = projected.reshape(length, 3, NH, HD)
        cos_b, sin_b = cosine[:, None, :], sine[:, None, :]
        queries = (heads[:, 0] * cos_b + rotate_half(heads[:, 0]) * sin_b).astype(bf16)
        keys_rot = (heads[:, 1] * cos_b + rotate_half(heads[:, 1]) * sin_b).astype(bf16)
        values = heads[:, 2].astype(bf16)
        allowed = attention_mask(segments[0], padding[0])
        logits = dot("qhd,khd->hqk", queries, keys_rot) * score_scale
        logits = jnp.where(allowed[None], logits, NEGATIVE)
        maxima = jnp.max(logits, axis=-1, keepdims=True)
        exponent = jnp.exp(logits - maxima)
        soft = exponent / jnp.sum(exponent, axis=-1, keepdims=True)
        probs = soft.astype(bf16)
        attended = dot("hqk,khd->qhd", probs, values).reshape(length, d).astype(bf16)
        middle = inputs + jnp.dot(attended, wo, preferred_element_type=f32)
        factor_two = norm_factor(middle)
        normed_two = (middle * factor_two * gain_two).astype(bf16)
        router = jax.nn.softmax(
            jnp.dot(normed_two, wr, preferred_element_type=f32), axis=-1
        )

        pair_expert, place, kept = pair_slots(routes[0], padding[0], priority[0])
        slot_total = EXPERTS * CAP
        slot_index = jnp.where(kept, pair_expert * CAP + place, -1).reshape(TOPK, length)
        slots = jnp.arange(slot_total, dtype=jnp.int32)
        hit = (slots[None, :, None] == slot_index[:, None, :]).any(axis=0)
        onehot = hit.astype(bf16)
        token_of = jnp.max(
            jnp.where(hit, jnp.arange(length, dtype=jnp.int32)[None, :], -1), axis=1
        )
        slot_expert = jnp.repeat(jnp.arange(EXPERTS), CAP)
        gate_of = jnp.sum(
            jnp.where(hit, jnp.repeat(router.T, CAP, axis=0), 0.0), axis=1
        )

        tokens_b = plane_gather(normed_two)
        token_of_b = plane_gather(token_of)
        gate_of_b = plane_gather(gate_of)
        group = 2 * n
        onehot_b = (
            token_of_b[:, :, None] == jnp.arange(length, dtype=jnp.int32)[None, None, :]
        ).astype(bf16)
        onehot_b = onehot_b.reshape(group, EXPERTS, CAP, length)
        gate_b = gate_of_b.reshape(group, EXPERTS, CAP, 1)

        def reduce_and_return(stack):
            k = stack.shape[0]
            piece = rows // qn
            x = stack.reshape((k, n) + (2,) * bits + (piece, hb))
            for b in range(bits):
                axis = 2 + (bits - 1 - b)
                bit = (q >> b) & 1
                keep = pick_index(x, bit, axis)
                send = pick_index(x, 1 - bit, axis).astype(bf16)
                x = keep + swap(send, "plane", 1 << b, qn).astype(f32)
            x = x.astype(bf16)
            own = pick_index(x, s, 1)
            got = [own] + [swap(pick_index(x, s ^ m, 1), "shard", m, n) for m in range(1, n)]
            x = jnp.stack(got)
            x = x[None]
            for b in reversed(range(bits)):
                bit = (q >> b) & 1
                other = swap(x, "plane", 1 << b, qn)
                lead = x.shape[0]
                pair = jnp.stack(
                    [jnp.where(bit == 0, x, other), jnp.where(bit == 0, other, x)], axis=1
                )
                x = pair.reshape((2 * lead,) + x.shape[1:])
            other = swap(x, "core", 1, 2)
            x = jnp.stack(
                [jnp.where(c == 0, x, other), jnp.where(c == 0, other, x)]
            )
            out = jnp.zeros((n,) + (2, qn, k, piece, hb), bf16)
            for m in range(n):
                out = lax.dynamic_update_index_in_dim(out, x[:, :, m], s ^ m, 0)
            return out.transpose(3, 2, 4, 0, 1, 5).reshape(k, rows, hidden).astype(f32)

        w_gate, w_up, w_down = moe_w
        tokens_f = tokens_b.reshape(group * length, d)
        grads_f = grads_b.reshape(group * length, d)
        shared_g = jnp.dot(tokens_f, w_gate[EXPERTS], preferred_element_type=f32)
        shared_u = jnp.dot(tokens_f, w_up[EXPERTS], preferred_element_type=f32)
        value, slope = silu_parts(shared_g)
        shared_hidden = (value * shared_u).astype(bf16)
        shared_q = jnp.dot(grads_f, w_down[EXPERTS], preferred_element_type=f32)
        shared_gd = (shared_q * shared_u * slope).astype(bf16)
        shared_ud = (shared_q * value).astype(bf16)
        shared_grads = jnp.stack(
            [
                dot("ld,lh->dh", tokens_f, shared_gd),
                dot("ld,lh->dh", tokens_f, shared_ud),
                dot("ld,lh->dh", grads_f, shared_hidden),
            ]
        )
        out_partial = dot("lh,dh->ld", shared_hidden, w_down[EXPERTS])
        two_partial = dot("lh,dh->ld", shared_gd, w_gate[EXPERTS]) + dot(
            "lh,dh->ld", shared_ud, w_up[EXPERTS]
        )
        out_partial = out_partial.reshape(group, length, d)
        two_partial = two_partial.reshape(group, length, d)
        shared_done = reduce_and_return(shared_grads)

        pick_parts = []
        expert_done = []
        for part in GROUPS:
            lo, hi = part[0], part[-1] + 1
            hot = onehot_b[:, lo:hi]
            x_in = jnp.einsum("bect,btd->ebcd", hot, tokens_b, preferred_element_type=bf16)
            g_in = jnp.einsum("bect,btd->ebcd", hot, grads_b, preferred_element_type=bf16)
            gate_e = jnp.swapaxes(gate_b[:, lo:hi], 0, 1)
            wg, wu, wd = w_gate[lo:hi], w_up[lo:hi], w_down[lo:hi]
            gate_act = dot("ebcd,edh->ebch", x_in, wg)
            up_act = dot("ebcd,edh->ebch", x_in, wu)
            value, slope = silu_parts(gate_act)
            hid = (value * up_act).astype(bf16)
            e_out = dot("ebch,edh->ebcd", hid, wd)
            pick_parts.append(jnp.sum(e_out * g_in.astype(f32), axis=-1))
            slot_grad = (gate_e * g_in.astype(f32)).astype(bf16)
            hid_grad = dot("ebcd,edh->ebch", slot_grad, wd)
            gate_d = (hid_grad * up_act * slope).astype(bf16)
            up_d = (hid_grad * value).astype(bf16)
            in_grad = dot("ebch,edh->ebcd", gate_d, wg) + dot("ebch,edh->ebcd", up_d, wu)
            weighted = (gate_e * e_out).astype(bf16)
            out_partial = out_partial + dot("bect,ebcd->btd", hot, weighted)
            two_partial = two_partial + dot("bect,ebcd->btd", hot, in_grad.astype(bf16))
            stack = jnp.concatenate(
                [
                    dot("ebcd,ebch->edh", x_in, gate_d),
                    dot("ebcd,ebch->edh", x_in, up_d),
                    dot("ebcd,ebch->edh", slot_grad, hid),
                ]
            )
            expert_done.append(reduce_and_return(stack))

        two_grad = plane_sum(two_partial)
        picks = jnp.concatenate(pick_parts, axis=0)
        picks = jnp.swapaxes(picks, 0, 1).reshape(group, slot_total)
        picks = picks[:n] + swap(picks[n:], "core", 1, 2)
        pick_slot = picks[0]
        for m in range(1, n):
            pick_slot = pick_slot + swap(picks[m], "shard", m, n)
        mixed = plane_sum(out_partial)
        output = (middle + mixed).astype(bf16)

        upstream = cotangent[0].astype(f32)
        pick_grad = jnp.sum(
            jnp.where(hit, pick_slot[:, None], 0.0).reshape(EXPERTS, CAP, length), axis=1
        ).T
        logit_grad = router * (pick_grad - jnp.sum(router * pick_grad, axis=1, keepdims=True))
        two_grad = two_grad + jnp.dot(logit_grad, wr.astype(f32).T, precision=highest)
        router_grad = jnp.dot(normed_two.astype(f32).T, logit_grad, precision=highest)
        middle_part, ffn_gain_grad = norm_back(middle, factor_two, gain_two, two_grad)
        middle_grad = middle_part + upstream

        branch_grad = middle_grad.astype(bf16)
        output_weight_grad = dot("ld,le->de", attended, branch_grad)
        attended_grad = (
            dot("le,de->ld", branch_grad, wo).astype(bf16).reshape(length, NH, HD)
        )
        prob_grad = dot("qhd,khd->hqk", attended_grad, values)
        row_inner = jnp.sum(soft * prob_grad, axis=-1, keepdims=True)
        score_grad = (soft * (prob_grad - row_inner)).astype(bf16)
        query_parts = dot("hqk,khd->qhd", score_grad, keys_rot) * score_scale
        key_parts = dot("hqk,qhd->khd", score_grad, queries) * score_scale
        value_parts = dot("hqk,qhd->khd", probs, attended_grad)
        query_pre = query_parts * cos_b + rotate_back(query_parts * sin_b)
        key_pre = key_parts * cos_b + rotate_back(key_parts * sin_b)
        joint_grad = jnp.concatenate(
            [v.reshape(length, d) for v in (query_pre, key_pre, value_parts)], axis=1
        ).astype(bf16)
        one_grad = dot("lf,df->ld", joint_grad, wqkv)
        joint_weight_grad = dot("ld,lf->df", normed_one, joint_grad)
        input_part, attn_gain_grad = norm_back(inputs, factor_one, gain_one, one_grad)
        input_grad = (middle_grad + input_part).astype(bf16)

        small_grad = jnp.concatenate(
            [attn_gain_grad[:, None], ffn_gain_grad[:, None], router_grad], axis=1
        )
        small_grad = jnp.pad(small_grad, ((0, 0), (0, 256 - small_grad.shape[1])))
        total = jnp.concatenate([joint_weight_grad, output_weight_grad, small_grad], axis=1)
        keep = lax.dynamic_slice_in_dim(total, c * half, half, 1)
        send = lax.dynamic_slice_in_dim(total, (1 - c) * half, half, 1).astype(bf16)
        total = keep + swap(send, "core", 1, 2).astype(f32)
        total = total.reshape(n, rows, half)
        own = pick_index(total, s)
        low = total.astype(bf16)
        for m in range(1, n):
            own = own + swap(pick_index(low, s ^ m), "shard", m, n).astype(f32)
        x = own.reshape((2,) * bits + (rows // qn, half))
        for b in range(bits):
            axis = bits - 1 - b
            bit = (q >> b) & 1
            keep = pick_index(x, bit, axis)
            send = pick_index(x, 1 - bit, axis).astype(bf16)
            x = keep + swap(send, "plane", 1 << b, qn).astype(f32)
        x = x.astype(bf16)[None]
        for b in reversed(range(bits)):
            bit = (q >> b) & 1
            other = swap(x, "plane", 1 << b, qn)
            pair = jnp.stack(
                [jnp.where(bit == 0, x, other), jnp.where(bit == 0, other, x)], axis=1
            )
            x = pair.reshape((2 * x.shape[0],) + x.shape[1:])
        x = x.reshape(rows, half)
        x = join_bit(c, x, swap(x, "core", 1, 2), 1).astype(f32)
        stacks = [[], [], []]
        for part, done in zip(GROUPS, expert_done):
            for k in range(3):
                stacks[k].append(done[k * len(part) : (k + 1) * len(part)])
        expert_grads = [jnp.concatenate(parts, axis=0) for parts in stacks]
        return (
            output[None],
            input_grad[None],
            x[:, 4 * d],
            x[:, :d],
            x[:, d : 2 * d],
            x[:, 2 * d : 3 * d],
            x[:, 3 * d : 4 * d],
            x[:, 4 * d + 1],
            x[:, 4 * d + 2 : 4 * d + 2 + EXPERTS],
            expert_grads[0],
            expert_grads[1],
            expert_grads[2],
            shared_done[0],
            shared_done[1],
            shared_done[2],
        )

    return shards


def make_fast(n, qn):
    def shards(
        tokens,
        cotangent,
        segments,
        padding,
        routes,
        priority,
        attn_gain,
        query_weight,
        key_weight,
        value_weight,
        output_weight,
        ffn_gain,
        router_weight,
        expert_gate,
        expert_up,
        expert_down,
        shared_gate,
        shared_up,
        shared_down,
    ):
        s = lax.axis_index("shard")
        c = lax.axis_index("core")
        length, d = tokens.shape[1], tokens.shape[2]
        where = jnp.stack([s, c]).astype(jnp.int32)

        meta = jnp.concatenate(
            [segments, padding, routes[0].T, priority, jnp.zeros((3, length), jnp.int32)], axis=0
        )
        cosine, sine = rotary_tables(length, HD)
        cos_pair = jnp.concatenate([cosine, cosine], axis=1)
        sin_pair = jnp.concatenate([sine, sine], axis=1)
        small = jnp.concatenate([attn_gain[:, None], ffn_gain[:, None], router_weight], axis=1)
        small = jnp.pad(small, ((0, 0), (0, 128 - small.shape[1])))

        near, far, near_z, far_z, *_, output, input_grad = layer_call(
            n,
            (
                tokens[0],
                meta,
                cos_pair,
                sin_pair,
                tokens[0],
                cotangent[0],
                small,
                query_weight,
                key_weight,
                value_weight,
                output_weight,
                expert_gate,
                expert_up,
                expert_down,
                shared_gate,
                shared_up,
                shared_down,
            ),
        )
        done = finish(n, where, near, far, near_z, far_z)
        tail = done[10]
        return (
            output[None],
            input_grad[None],
            tail[:, 0],
            *done[6:10],
            tail[:, 1],
            tail[:, 2 : 2 + EXPERTS],
            *done[:3],
            *(v[0] for v in done[3:6]),
        )

    return shards


def make_shards(n, qn):
    plain, fast = make_plain(n, qn), make_fast(n, qn)

    def shards(*arguments):
        d, hidden = arguments[0].shape[2], arguments[13].shape[2]
        fits = n == 4 and qn == 4 and d == 768 and hidden == 2048 and arguments[0].shape[1] == 256
        return (fast if fits else plain)(*arguments)

    return shards


def solution(mesh):
    n, replicas = mesh.shape["shard"], mesh.shape["replica"]
    fine = Mesh(mesh.devices.reshape(n, replicas // 2, 2), ("shard", "plane", "core"))
    every = ("shard", "plane", "core")
    in_specs = (
        P(every, None, None),
        P(every, None, None),
        P(every, None),
        P(every, None),
        P(every, None, None),
        P(every, None),
        P("shard"),
        P("shard", None),
        P("shard", None),
        P("shard", None),
        P("shard", None),
        P("shard"),
        P("shard", None),
        P(None, "shard", None),
        P(None, "shard", None),
        P(None, "shard", None),
        P("shard", None),
        P("shard", None),
        P("shard", None),
    )
    out_specs = (
        P(every, None, None),
        P(every, None, None),
        P("shard"),
        P("shard", None),
        P("shard", None),
        P("shard", None),
        P("shard", None),
        P("shard"),
        P("shard", None),
        P(None, "shard", None),
        P(None, "shard", None),
        P(None, "shard", None),
        P("shard", None),
        P("shard", None),
        P("shard", None),
    )
    return jax.shard_map(
        make_shards(n, replicas // 2),
        mesh=fine,
        in_specs=in_specs,
        out_specs=out_specs,
        check_vma=False,
    )
```

```python
import functools
import math

import jax
import jax.numpy as jnp
from jax import lax
from jax.experimental import pallas as pl
from jax.experimental.pallas import tpu as pltpu
from jax.sharding import Mesh, PartitionSpec as P

NH = 12
HD = 64
EXPERTS = 6
TOPK = 2
CAP = 96
EPSILON = 1e-06
NEGATIVE = -1e30
GROUPS = ((0, 1), (2, 3), (4, 5))

highest = lax.Precision.HIGHEST
f32 = jnp.float32
bf16 = jnp.bfloat16


def dot(spec, first, second):
    return jnp.einsum(spec, first, second, preferred_element_type=f32)


def rotate_half(values):
    half_size = values.shape[-1] // 2
    return jnp.concatenate([-values[..., half_size:], values[..., :half_size]], axis=-1)


def rotate_back(values):
    half_size = values.shape[-1] // 2
    return jnp.concatenate([values[..., half_size:], -values[..., :half_size]], axis=-1)


def rotary_tables(length, head_dim):
    positions = jnp.arange(length, dtype=f32)
    frequency = jnp.exp(
        jnp.arange(head_dim // 2, dtype=f32) * (-2.0 * math.log(10000.0) / head_dim)
    )
    angles = positions[:, None] * frequency[None, :]
    angles = jnp.concatenate([angles, angles], axis=1)
    return (jnp.cos(angles), jnp.sin(angles))


def attention_mask(segments, padding):
    places = jnp.arange(segments.shape[0])
    causal = places[None, :] <= places[:, None]
    shared_doc = segments[:, None] == segments[None, :]
    usable = (padding[None, :] == 1) | (places[None, :] == places[:, None])
    return causal & shared_doc & usable


def norm_factor(values):
    return lax.rsqrt(jnp.mean(values * values, axis=-1, keepdims=True) + EPSILON)


def norm_back(values, factor, norm_gain, gradient):
    scaled = gradient * norm_gain
    gain_grad = jnp.sum(gradient * values * factor, axis=0)
    input_part = factor * scaled - values * factor**3 * jnp.mean(
        scaled * values, axis=-1, keepdims=True
    )
    return (input_part, gain_grad)


def silu_parts(gate_act):
    sigmoid = jax.nn.sigmoid(gate_act)
    return (gate_act * sigmoid, sigmoid * (1.0 + gate_act * (1.0 - sigmoid)))


def pair_slots(routes, padding, priority):
    length = routes.shape[0]
    pair_expert = routes.T.reshape(-1)
    pair_live = jnp.tile(padding, TOPK) == 1
    pair_key = (jnp.arange(TOPK, dtype=jnp.int32)[:, None] * length + priority[None, :]).reshape(-1)
    earlier = (
        (pair_key[None, :] < pair_key[:, None])
        & (pair_expert[None, :] == pair_expert[:, None])
        & pair_live[None, :]
    )
    place = jnp.sum(earlier.astype(jnp.int32), axis=1)
    kept = pair_live & (place < CAP)
    return (pair_expert, place, kept)


def swap(values, axis, mask, size):
    return lax.ppermute(values, axis, [(i, i ^ mask) for i in range(size)])


def pick_index(values, index, axis=0):
    return lax.dynamic_index_in_dim(values, index, axis, keepdims=False)


def mm(first, second, contract):
    return lax.dot_general(
        first, second, (contract, ((), ())), preferred_element_type=f32
    )


NN = ((1,), (0,))
NT = ((1,), (1,))
TN = ((0,), (0,))


def flip(value, mask, size):
    out = 0
    for b in range(size.bit_length() - 1):
        bit = (value // (1 << b)) % 2
        out = out + (1 << b) * ((1 - bit) if (mask >> b) & 1 else bit)
    return out


MESH = pl.DeviceIdType.MESH


def layer_kernel(
    n,
    tokens,
    meta_ref,
    cos_ref,
    sin_ref,
    tok_hbm,
    cot_hbm,
    small_own,
    wq,
    wk,
    wv,
    wo,
    eg,
    eu,
    ed,
    sg,
    su,
    sd,
    near_ref,
    far_ref,
    near_z,
    far_z,
    wide_hbm,
    work_hbm,
    soft_hbm,
    mid_hbm,
    w_land,
    out_ref,
    in_grad_ref,
    xg,
    acc_y,
    acc_t,
    work,
    dw,
    own,
    land,
    swap_in,
    y_side,
    y_in,
    wbuf,
    slot_ref,
    router_ref,
    probs_ref,
    small_ref,
    allowed,
    gate_s,
    pick_s,
    pick_acc,
    pick_side,
    pick_pair,
    pick_in,
    branch_s,
    ag_s,
    small_acc,
    z_own,
    z_swap,
    ch_send,
    ch_recv,
    x_send,
    x_recv,
    stay_sem,
    z_send,
    z_recv,
    zx_send,
    zx_recv,
    y_send_sem,
    y_recv_sem,
    p_send,
    p_recv,
    load_sem,
    free_side,
    free_in,
    gains_s,
    gains_side,
    gains_in,
    a_send,
    a_recv,
    w_send,
    w_recv,
    w_load,
    t_send,
    t_recv,
    side_send,
    side_recv,
):
    t = pl.program_id(0) - 1
    group = 2 * n
    length, d = tokens.shape
    hb = dw.shape[2]
    part = d // (2 * n)
    half = n * part
    chunks = 3 * (EXPERTS + 1)
    plane_rows = group * length
    s, q, c = (lax.axis_index(a) for a in ("shard", "plane", "core"))
    middle = (q == 1) | (q == 2)
    ends = (q == 0) | (q == 3)
    keep_h, give_h = (q + 1) % 2, q % 2
    other_mid = 3 - q
    mid_of = 1 + q // 3
    end_of = (q // 2) * 3
    other_c = 1 - c
    shard_of = [None] + [flip(s, m, n) for m in range(1, n)]

    def at_chunk(u, row=0, count=d):
        start = pl.multiple_of((u // 3) * d + row, 16)
        return pl.ds(start, count), pl.ds(pl.multiple_of((u % 3) * hb, 128), hb)

    def half_rows(h):
        return pl.ds(pl.multiple_of(h * half, 16), half)

    def remote(src, dst, ssem, rsem, to):
        return pltpu.make_async_remote_copy(
            src, dst, ssem, rsem, device_id=to, device_id_type=MESH
        )

    def chunk(kind, src, dst, u, to):
        return remote(src, dst, ch_send.at[kind, u], ch_recv.at[kind, u], to)

    def to_mid(u):
        return chunk(0, own.at[at_chunk(u)], land.at[u], u, {"plane": mid_of})

    def from_end(u):
        return chunk(0, own.at[at_chunk(u)], land.at[u], u, {"plane": end_of})

    def swap_sums(u):
        src = own.at[at_chunk(u, give_h * half, half)]
        return chunk(1, src, swap_in.at[u], u, {"plane": other_mid})

    def swap_done(u):
        ref = near_ref.at[u, half_rows(keep_h)]
        return chunk(2, ref, ref, u, {"plane": other_mid})

    def swap_done_in(u):
        ref = near_ref.at[u, half_rows(give_h)]
        return chunk(2, ref, ref, u, {"plane": other_mid})

    def to_end(u, first):
        ref = near_ref.at[u, half_rows(keep_h if first else give_h)]
        return chunk(3 if first else 4, ref, ref, u, {"plane": end_of})

    def from_mid(u, first):
        ref = near_ref.at[u, half_rows((q // 3) if first else 1 - q // 3)]
        return chunk(3 if first else 4, ref, ref, u, {"plane": mid_of})

    def across(u, m):
        return remote(
            own.at[at_chunk(u, keep_h * half + m * part, part)],
            near_ref.at[u, pl.ds(pl.multiple_of(keep_h * half + m * part, 16), part)],
            x_send.at[m - 1, u],
            x_recv.at[m - 1, u],
            {"shard": shard_of[m]},
        )

    def stay(u):
        return pltpu.make_async_copy(
            own.at[at_chunk(u, keep_h * half, part)],
            near_ref.at[u, pl.ds(pl.multiple_of(keep_h * half, 16), part)],
            stay_sem.at[u],
        )

    def side(u):
        return chunk(5, near_ref.at[u], far_ref.at[u], u, {"core": other_c})

    far_rows = pl.ds(0, plane_rows)

    def y_side_copy():
        return remote(
            work.at[far_rows], y_side, y_send_sem.at[0, 0], y_recv_sem.at[0, 0], {"core": other_c}
        )

    def y_across(k, m):
        at = pl.ds((k * n + m) * length, length)
        return remote(
            y_side.at[at],
            y_in.at[m - 1, k],
            y_send_sem.at[1 + k, m - 1],
            y_recv_sem.at[1 + k, m - 1],
            {"shard": shard_of[m]},
        )

    def pick_side_copy():
        return remote(
            pick_acc.at[pl.ds(n, n)], pick_side, p_send.at[0], p_recv.at[0], {"core": other_c}
        )

    def pick_across(m):
        return remote(
            pick_pair.at[m - 1],
            pick_in.at[m - 1],
            p_send.at[m],
            p_recv.at[m],
            {"shard": shard_of[m]},
        )

    def load(i, src, dst):
        return pltpu.make_async_copy(src, dst, load_sem.at[i])

    def back_rows(i):
        return pl.ds(i * length, length)

    two_w = [length, length + d, plane_rows + length, plane_rows + length + d]

    saved_rows = pl.ds(0, 5 * length)
    soft_rows = pl.ds(n * length, n * length)
    mid_rows = pl.ds(n * length, length)

    def saved_out():
        return [
            load(2, acc_y.at[soft_rows], soft_hbm),
            load(3, acc_t.at[mid_rows], mid_hbm),
            load(4, own.at[pl.ds(0, 4 * d)], wide_hbm),
            load(5, work.at[saved_rows], work_hbm),
        ]

    def saved_in():
        copies = [
            load(6, soft_hbm, acc_y.at[soft_rows]),
            load(7, mid_hbm, acc_t.at[mid_rows]),
            load(8, work_hbm, work.at[saved_rows]),
            load(9, tok_hbm, work.at[back_rows(5)]),
        ]
        for i in range(4):
            copies.append(load(10 + i, wide_hbm.at[pl.ds(i * d, d)], xg.at[pl.ds(two_w[i], d)]))
        return copies

    def columns(m):
        owner = s if m == 0 else shard_of[m]
        return pl.ds(pl.multiple_of((owner * 2 + c) * hb, 128), hb)

    def weight_ref(e, k, m, shared):
        big, one = ((eg, sg), (eu, su), (ed, sd))[k]
        return one.at[:, columns(m)] if shared else big.at[e, :, columns(m)]

    def weight_sends(e, shared):
        return [
            remote(
                weight_ref(e, k, m, shared),
                w_land.at[e, k, m - 1],
                w_send.at[e, 3 * k + m - 1],
                w_recv.at[e, 3 * k + m - 1],
                {"shard": shard_of[m]},
            )
            for k in range(3)
            for m in range(1, n)
        ]

    def weight_loads(e, shared):
        copies = []
        for k in range(3):
            for m in range(n):
                owner = s if m == 0 else shard_of[m]
                src = weight_ref(e, k, 0, shared) if m == 0 else w_land.at[e, k, m - 1]
                dst = wbuf.at[
                    e % 2, k, pl.ds(pl.multiple_of(owner * 2 * part, 16), 2 * part)
                ]
                copies.append(pltpu.make_async_copy(src, dst, w_load.at[e % 2, n * k + m]))
        return copies

    def for_expert(e, body):
        @pl.when(e < EXPERTS)
        def _():
            body(e, False)

        @pl.when(e == EXPERTS)
        def _():
            body(e, True)

    def fetch_weights(e, shared):
        for copy in weight_sends(e, shared):
            copy.wait()
        for copy in weight_loads(e, shared):
            copy.start()

    def start_weights(e, shared):
        for copy in weight_sends(e, shared):
            copy.start()

    def finish_weights(e, shared):
        for copy in weight_loads(e, shared):
            copy.wait()

    @pl.when(t < 0)
    def _():
        barrier = pltpu.get_barrier_semaphore()
        peers = [{"core": other_c}] + [{"shard": shard_of[m]} for m in range(1, n)]
        for peer in peers:
            pl.semaphore_signal(barrier, 1, device_id=peer, device_id_type=MESH)

        @pl.when(middle)
        def _():
            for peer in ({"plane": other_mid}, {"plane": end_of}):
                pl.semaphore_signal(barrier, 1, device_id=peer, device_id_type=MESH)
            pl.semaphore_wait(barrier, len(peers) + 2)

        @pl.when(ends)
        def _():
            pl.semaphore_signal(barrier, 1, device_id={"plane": mid_of}, device_id_type=MESH)
            pl.semaphore_wait(barrier, len(peers) + 1)

        my_rows = pl.multiple_of(s * 2 * part, 16)

        def wide_at(i, row, count):
            return own.at[pl.ds(pl.multiple_of((2 * c + i) * d + row, 16), count)]

        def attn_sends(i, source):
            return [
                remote(
                    source,
                    wide_at(i, my_rows, 2 * part),
                    a_send.at[i, m - 1],
                    a_recv.at[i, m - 1],
                    {"shard": shard_of[m]},
                )
                for m in range(1, n)
            ]

        def attn_stay(i, source):
            return load(i, source, wide_at(i, my_rows, 2 * part))

        smalls = [
            remote(
                small_own,
                small_ref.at[pl.ds(my_rows, 2 * part)],
                a_send.at[2, m - 1],
                a_recv.at[2, m - 1],
                {"shard": shard_of[m]},
            )
            for m in range(1, n)
        ]
        stay_here = [
            load(14, small_own, small_ref.at[pl.ds(my_rows, 2 * part)]),
            load(15, cot_hbm, xg.at[pl.ds(plane_rows, length)]),
        ]
        for copy in smalls + stay_here:
            copy.start()
        for core, pair_of in enumerate(((wq, wk), (wv, wo))):

            @pl.when(c == core)
            def _():
                for i in range(2):
                    attn_stay(i, pair_of[i]).start()
                    for copy in attn_sends(i, pair_of[i]):
                        copy.start()

        def spread_out(i, src, place):
            return [
                remote(
                    src, place(m), t_send.at[i, m - 1], t_recv.at[i, m - 1], {"shard": shard_of[m]}
                )
                for m in range(1, n)
            ]

        def to_core(i, src, dst):
            return remote(src, dst, side_send.at[i], side_recv.at[i], {"core": other_c})

        def rows_to_core(i, base):
            return to_core(
                i, xg.at[pl.ds(base, n * length)], xg.at[pl.ds(base + n * length, n * length)]
            )

        g_copies = spread_out(
            0, cot_hbm, lambda m: xg.at[pl.ds(plane_rows + m * length, length)]
        )
        slot_copies = spread_out(1, slot_ref.at[0], lambda m: slot_ref.at[m])
        for copy in g_copies:
            copy.start()
        for e in range(EARLY):
            start_weights(e, False)
        rows_of = meta_ref[...].astype(f32)
        columns_of = jnp.transpose(
            jnp.concatenate([rows_of, jnp.zeros((120, length), f32)], axis=0)
        )
        row = lambda r: rows_of[r : r + 1, :]
        column = lambda r: columns_of[:, r : r + 1]
        above = lax.broadcasted_iota(jnp.int32, (length, length), 0)
        along = lax.broadcasted_iota(jnp.int32, (length, length), 1)
        seen = (along <= above) & (column(0) == row(0)) & ((row(1) == 1.0) | (along == above))
        allowed[...] = jnp.where(seen, 1.0, 0.0)
        live = column(1) == 1.0
        sooner = live & (column(4) < row(4))
        count = lambda hits: jnp.sum(jnp.where(hits, 1.0, 0.0), axis=0, keepdims=True)
        places = (
            count(sooner & (column(2) == row(2))),
            count(live & (column(2) == row(3))) + count(sooner & (column(3) == row(3))),
        )
        line = lax.broadcasted_iota(jnp.int32, (8, length), 0)
        table = jnp.full((8, length), -1.0, f32)
        for k in range(TOPK):
            kept = (row(1) == 1.0) & (places[k] < CAP)
            place = jnp.where(kept, row(2 + k) * CAP + places[k], -1.0)
            table = jnp.where(line == k, place, table)
        slot_ref[0] = table.astype(jnp.int32)
        for copy in stay_here:
            copy.wait()

        def gather_attn(i):
            attn_stay(i, wq).wait()
            for copy in attn_sends(i, wq):
                copy.wait()
            at = wide_at(i, 0, d)
            copy = to_core(5 * i, at, at)
            copy.start()
            return copy

        first_half = gather_attn(0)
        for copy in slot_copies:
            copy.start()
        for copy in smalls:
            copy.wait()
        first_half.wait()

        def half_way():
            gather_attn(1).wait()

        work_part = lambda i: work.at[pl.ds(i * length, length)]
        outs = tuple(work_part(i) for i in range(5)) + (
            xg.at[pl.ds(0, length)],
            acc_t.at[mid_rows],
            acc_y.at[soft_rows],
            probs_ref,
        )
        router = attention_forward(
            tokens,
            small_ref,
            lambda i: own.at[pl.ds(i * d, d)],
            allowed,
            cos_ref,
            sin_ref,
            half_way,
            outs,
        )
        router_ref[0] = jnp.transpose(router)[0:8, :]
        for copy in saved_out():
            copy.start()
        x_copies = spread_out(
            2, xg.at[pl.ds(0, length)], lambda m: xg.at[pl.ds(m * length, length)]
        )
        rt_copies = spread_out(3, router_ref.at[0], lambda m: router_ref.at[m])
        for copy in x_copies + rt_copies:
            copy.start()

        for e in range(EARLY, AHEAD):
            start_weights(e, False)
        for copy in slot_copies + g_copies:
            copy.wait()
        g_side = rows_to_core(1, plane_rows)
        slot_side = to_core(2, slot_ref.at[pl.ds(0, n)], slot_ref.at[pl.ds(n, n)])
        g_side.start()
        slot_side.start()
        for copy in saved_out():
            copy.wait()
        acc_y[...] = jnp.zeros_like(acc_y)
        acc_t[...] = jnp.zeros_like(acc_t)
        pick_acc[...] = jnp.zeros_like(pick_acc)
        fetch_weights(0, False)
        for copy in x_copies + rt_copies:
            copy.wait()
        x_side = rows_to_core(3, 0)
        rt_side = to_core(4, router_ref.at[pl.ds(0, n)], router_ref.at[pl.ds(n, n)])
        x_side.start()
        rt_side.start()
        for copy in (g_side, slot_side, x_side, rt_side):
            copy.wait()

    def branch(x, gs_rows, wg, wu, wd):
        gate_act = mm(x, wg, NN)
        up_act = mm(x, wu, NN)
        sigmoid = 1.0 / (1.0 + jnp.exp(-gate_act))
        value = gate_act * sigmoid
        slope = sigmoid * (1.0 + gate_act * (1.0 - sigmoid))
        hid = (value * up_act).astype(bf16)
        hid_grad = mm(gs_rows, wd, NN)
        gate_d = (hid_grad * up_act * slope).astype(bf16)
        up_d = (hid_grad * value).astype(bf16)
        return hid, gate_d, up_d

    slots = group * CAP
    xs_at, gs_at, sg_at = 0, slots, 2 * slots

    @pl.when((t >= 0) & (t <= EXPERTS))
    def _():
        for_expert(t + AHEAD, start_weights)
        for_expert(t, finish_weights)

    @pl.when((t >= 0) & (t < EXPERTS))
    def _():
        ids = lax.broadcasted_iota(jnp.int32, (CAP, length), 0) + t * CAP

        def slots_of(b):
            first, second = slot_ref[b, 0:1, :], slot_ref[b, 1:2, :]
            return (first == ids) | (second == ids)

        for b in range(group):
            slot = pl.ds(b * CAP, CAP)
            hit = slots_of(b)
            hot = hit.astype(f32).astype(bf16)
            row = router_ref[b, pl.ds(t + 2, 1), :]
            gate = jnp.sum(jnp.where(hit, row, 0.0), axis=1, keepdims=True)
            gate_s[slot, :] = gate
            x_rows = mm(hot, xg[pl.ds(b * length, length), :], NN)
            work[pl.ds(xs_at + b * CAP, CAP), :] = x_rows.astype(bf16)
            g_rows = mm(hot, xg[pl.ds(plane_rows + b * length, length), :], NN)
            work[pl.ds(gs_at + b * CAP, CAP), :] = g_rows.astype(bf16)
            work[pl.ds(sg_at + b * CAP, CAP), :] = (g_rows * gate).astype(bf16)
        wg, wu, wd = wbuf[t % 2, 0], wbuf[t % 2, 1], wbuf[t % 2, 2]
        x, slot_grad = work[pl.ds(xs_at, slots), :], work[pl.ds(sg_at, slots), :]
        hid, gate_d, up_d = branch(x, slot_grad, wg, wu, wd)
        dw[0] = mm(x, gate_d, TN)
        dw[1] = mm(x, up_d, TN)
        dw[2] = mm(slot_grad, hid, TN)
        e_out = mm(hid, wd, NT)
        g_rows = work[pl.ds(gs_at, slots), :].astype(f32)
        pick_s[...] = jnp.sum(e_out * g_rows, axis=1, keepdims=True)
        work[pl.ds(gs_at, slots), :] = (e_out * gate_s[...]).astype(bf16)
        work[pl.ds(xs_at, slots), :] = (mm(gate_d, wg, NT) + mm(up_d, wu, NT)).astype(bf16)
        for b in range(group):
            slot = pl.ds(b * CAP, CAP)
            seq = pl.ds(b * length, length)
            hit = slots_of(b)
            hot = hit.astype(f32).astype(bf16)
            pick_acc[b, pl.ds(t + 2, 1), :] = jnp.sum(
                jnp.where(hit, pick_s[slot, :], 0.0), axis=0, keepdims=True
            )
            acc_y[seq, :] += mm(hot, work[pl.ds(gs_at + b * CAP, CAP), :], TN)
            acc_t[seq, :] += mm(hot, work[pl.ds(xs_at + b * CAP, CAP), :], TN)

    @pl.when(t == EXPERTS)
    def _():
        dw[...] = jnp.zeros_like(dw)
        wg, wu, wd = wbuf[t % 2, 0], wbuf[t % 2, 1], wbuf[t % 2, 2]

        def rows_step(i, carry):
            at = pl.multiple_of(i * 2 * length, 2 * length)
            rows = pl.ds(at, 2 * length)
            x, g = xg[rows, :], xg[pl.ds(plane_rows + at, 2 * length), :]
            hid, gate_d, up_d = branch(x, g, wg, wu, wd)
            dw[0] += mm(x, gate_d, TN)
            dw[1] += mm(x, up_d, TN)
            dw[2] += mm(g, hid, TN)
            acc_y[rows, :] += mm(hid, wd, NT)
            acc_t[rows, :] += mm(gate_d, wg, NT) + mm(up_d, wu, NT)
            return carry

        lax.fori_loop(0, n, rows_step, 0)
        work[pl.ds(0, n * length), :] = acc_y[soft_rows, :].astype(bf16)
        work[pl.ds(n * length, n * length), :] = acc_t[soft_rows, :].astype(bf16)

    @pl.when((t >= 0) & (t <= EXPERTS))
    def _():
        for k in range(3):
            for h in range(2):
                for m in range(n):
                    owner = s if m == 0 else shard_of[m]
                    start = pl.multiple_of((owner * 2 + h) * part, 16)
                    row = pl.multiple_of(t * d + (h * n + m) * part, 16)
                    own[pl.ds(row, part), k * hb : (k + 1) * hb] = dw[
                        k, pl.ds(start, part), :
                    ].astype(bf16)

        @pl.when(ends)
        def _():
            for k in range(3):
                to_mid(3 * t + k).start()

    @pl.when(t == EXPERTS)
    def _():
        y_side_copy().start()
        pick_side_copy().start()

    def add_halves(u):
        from_end(u).wait_recv()
        for i in range(2 * n):
            rows, columns_at = at_chunk(u, i * part, part)
            own[rows, columns_at] = (
                own[rows, columns_at].astype(f32)
                + land[u, pl.ds(i * part, part), :].astype(f32)
            ).astype(bf16)
        swap_sums(u).start()

    def add_swapped(u):
        swap_sums(u).wait()
        for m in range(n):
            rows, columns_at = at_chunk(u, keep_h * half + m * part, part)
            own[rows, columns_at] = (
                own[rows, columns_at].astype(f32)
                + swap_in[u, pl.ds(m * part, part), :].astype(f32)
            ).astype(bf16)
        for m in range(1, n):
            across(u, m).start()
        stay(u).start()

    def send_done(u):
        for m in range(1, n):
            across(u, m).wait()
        stay(u).wait()
        swap_done(u).start()
        to_end(u, True).start()

    def send_second(u):
        swap_done_in(u).wait_recv()
        to_end(u, False).start()
        side(u).start()

    def end_side(u):
        to_mid(u).wait_send()
        from_mid(u, True).wait_recv()
        from_mid(u, False).wait_recv()
        side(u).start()

    def middle_last(u):
        swap_done(u).wait_send()
        to_end(u, True).wait_send()
        to_end(u, False).wait_send()
        side(u).wait()

    mine_rows = pl.ds(0, length)
    grad_rows = pl.ds((n + 1) * length, length)

    def out_copy():
        return load(14, xg.at[mine_rows], out_ref)

    def in_grad_copy():
        return load(15, work.at[back_rows(5)], in_grad_ref)

    @pl.when(t == Y_STEPS[2])
    def _():
        total = acc_y[mine_rows, :]
        for m in range(1, n):
            y_across(0, m).wait()
            total = total + y_in[m - 1, 0].astype(f32)
        xg[mine_rows, :] = (acc_t[mid_rows, :] + total).astype(bf16)
        out_copy().start()
        pl.semaphore_signal(free_side, 1, device_id={"core": other_c}, device_id_type=MESH)
        for m in range(1, n):
            pl.semaphore_signal(free_in, 1, device_id={"shard": shard_of[m]}, device_id_type=MESH)

    stages = (
        (middle, add_halves),
        (middle, add_swapped),
        (middle, send_done),
        (middle, send_second),
        (ends, end_side),
        (middle, middle_last),
        (ends, lambda u: side(u).wait()),
    )

    def chunk_step(i, carry):
        v = t + jnp.minimum(t, DOUBLE) + i
        live = (i == 0) | (t < DOUBLE)
        for k in STAGE_ORDER:
            where, body = stages[k]
            u = v - STAGE_DELAY[k]

            @pl.when(live & (u >= 0) & (u < chunks) & where)
            def _():
                body(u)

        return carry

    lax.fori_loop(0, 2, chunk_step, 0)

    @pl.when((t >= 0) & (t < EXPERTS))
    def _():
        for_expert(t + 1, fetch_weights)

    @pl.when(t == Y_STEPS[0])
    def _():
        y_side_copy().wait()
        pick_side_copy().wait()
        for copy in saved_in():
            copy.start()
        pick_acc[pl.ds(0, n)] += pick_side[...]
        for m in range(1, n):
            pick_pair[m - 1] = pick_acc[m]
        for k, acc in ((1, acc_t), (0, acc_y)):
            for m in range(n):
                seq, at = pl.ds(m * length, length), pl.ds((k * n + m) * length, length)
                total = acc[seq, :] + y_side[at, :].astype(f32)
                if m == 0:
                    acc[seq, :] = total
                else:
                    y_side[at, :] = total.astype(bf16)
            for m in range(1, n):
                y_across(k, m).start()
                if k:
                    pick_across(m).start()

    pre_at = 6 * length
    exact = lax.Precision.HIGHEST

    @pl.when(t == Y_STEPS[1])
    def _():
        for m in range(1, n):
            y_across(1, m).wait()
            pick_across(m).wait()
        for copy in saved_in():
            copy.wait()
        two = acc_t[mine_rows, :]
        picks = pick_acc[0]
        for m in range(1, n):
            two = two + y_in[m - 1, 1].astype(f32)
            picks = picks + pick_in[m - 1]
        picks = jnp.concatenate([picks, jnp.zeros((120, length), f32)], axis=0)
        picks = jnp.transpose(picks)
        router = probs_ref[...]
        logit_grad = router * (picks - jnp.sum(router * picks, axis=1, keepdims=True))
        small = small_ref[...].astype(f32)
        gain_two = jnp.transpose(small)[1:2, :]
        two = two + lax.dot_general(
            logit_grad, small, (NT, ((), ())), precision=exact, preferred_element_type=f32
        )
        router_grad = lax.dot_general(
            logit_grad,
            xg[mine_rows, :].astype(f32),
            (TN, ((), ())),
            precision=exact,
            preferred_element_type=f32,
        )
        mid = acc_t[mid_rows, :]
        factor = lax.rsqrt(jnp.mean(mid * mid, axis=1, keepdims=True) + EPSILON)
        gain_grad = jnp.sum(two * mid * factor, axis=0, keepdims=True)
        row = lax.broadcasted_iota(jnp.int32, router_grad.shape, 0)
        small_acc[...] = jnp.where(row == 1, gain_grad, router_grad)
        scaled = two * gain_two
        grad = (
            xg[pl.ds(plane_rows, length), :].astype(f32)
            + factor * scaled
            - mid * (factor * factor * factor) * jnp.mean(scaled * mid, axis=1, keepdims=True)
        )
        acc_t[grad_rows, :] = grad
        branch_s[...] = grad.astype(bf16)
        ag_s[...] = mm(branch_s[...], xg[pl.ds(two_w[3], d), :], NT).astype(bf16)

    pair = 2 * HD

    @pl.when((t >= HEAD_STEP) & (t < HEAD_STEP + 3))
    def _():
        lane = lax.broadcasted_iota(jnp.int32, (length, pair), 1)
        first = lane < HD
        lower = lane % HD < HD // 2
        cos, sin = cos_ref[...], sin_ref[...]

        def turn_back(w):
            y = w * sin
            up = pltpu.roll(y, pair - HD // 2, 1)
            down = pltpu.roll(y, HD // 2, 1)
            return w * cos + jnp.where(lower, up, -down)

        def heads(i, carry):
            p = 2 * (t - HEAD_STEP) + i
            cut = pl.ds(pl.multiple_of(p * pair, pair), pair)
            queries, keys, values = (work[back_rows(j), cut] for j in range(3))
            grads = ag_s[:, cut]
            parts = []
            for one_side in range(2):
                h = 2 * p + one_side
                rows = pl.ds(pl.multiple_of(n * length + (h // 3) * length, length), length)
                columns = pl.ds(pl.multiple_of((h % 3) * length, length), length)
                soft = acc_y[rows, columns]
                mine = first if one_side == 0 else jnp.logical_not(first)
                chosen = jnp.where(mine, grads.astype(f32), 0.0).astype(bf16)
                prob_grad = mm(chosen, values, NT)
                inner = jnp.sum(soft * prob_grad, axis=1, keepdims=True)
                score_grad = (soft * (prob_grad - inner)).astype(bf16)
                parts.append(
                    (
                        mm(score_grad, keys, NN) * HD ** (-0.5),
                        mm(score_grad, queries, TN) * HD ** (-0.5),
                        mm(soft.astype(bf16), grads, TN),
                    )
                )
            joined = [jnp.where(first, parts[0][j], parts[1][j]) for j in range(3)]
            joined = [turn_back(joined[0]), turn_back(joined[1]), joined[2]]
            for j in range(3):
                work[pl.ds(pre_at + j * length, length), cut] = joined[j].astype(bf16)
            return carry

        lax.fori_loop(0, 2, heads, 0, unroll=True)

    two_d = 2 * d
    give_rows = pl.ds(pl.multiple_of((1 - c) * two_d, 16), two_d)

    def attn_side():
        return [
            remote(
                xg.at[give_rows],
                y_side.at[pl.ds(0, two_d)],
                z_send.at[5],
                z_recv.at[5],
                {"core": other_c},
            ),
            remote(gains_s, gains_side, z_send.at[7], z_recv.at[7], {"core": other_c}),
        ]

    def attn_across(m):
        copies = []
        at = pl.multiple_of(shard_of[m] * 2 * part, 16)
        for i in range(2):
            copies.append(
                remote(
                    xg.at[pl.ds(pl.multiple_of(c * two_d + i * d + at, 16), 2 * part)],
                    y_in.at[m - 1, i, pl.ds(0, 2 * part)],
                    zx_send.at[m - 1, i],
                    zx_recv.at[m - 1, i],
                    {"shard": shard_of[m]},
                )
            )
        copies.append(
            remote(
                gains_s.at[pl.ds(at, 2 * part)],
                gains_in.at[m - 1],
                zx_send.at[m - 1, 2],
                zx_recv.at[m - 1, 2],
                {"shard": shard_of[m]},
            )
        )
        return copies

    @pl.when(t == HEAD_STEP + 3)
    def _():
        pre = [work[pl.ds(pre_at + j * length, length), :] for j in range(3)]
        one_grad = mm(pre[0], xg[pl.ds(two_w[0], d), :], NT)
        for j in (1, 2):
            one_grad = one_grad + mm(pre[j], xg[pl.ds(two_w[j], d), :], NT)
        x = work[back_rows(5), :].astype(f32)
        gain_one = jnp.transpose(small_ref[...].astype(f32))[0:1, :]
        factor = lax.rsqrt(jnp.mean(x * x, axis=1, keepdims=True) + EPSILON)
        gain_grad = jnp.sum(one_grad * x * factor, axis=0, keepdims=True)
        scaled = one_grad * gain_one
        work[back_rows(5), :] = (
            acc_t[grad_rows, :]
            + factor * scaled
            - x * (factor * factor * factor) * jnp.mean(scaled * x, axis=1, keepdims=True)
        ).astype(bf16)
        in_grad_copy().start()
        out_copy().wait()
        gains = small_acc[...]
        row = lax.broadcasted_iota(jnp.int32, gains.shape, 0)
        gains_s[...] = jnp.transpose(jnp.where(row == 0, gain_grad, gains)).astype(bf16)
        for i in range(4):
            lhs = work[back_rows(4 if i < 3 else 3), :]
            for k in range(3):
                cut = slice(k * hb, (k + 1) * hb)
                rhs = work[pl.ds(pre_at + i * length, length), cut] if i < 3 else branch_s[:, cut]
                xg[pl.ds(i * d, d), cut] = mm(lhs, rhs, TN).astype(bf16)
        pl.semaphore_wait(free_side, 1)
        for copy in attn_side():
            copy.start()

    @pl.when(t == HEAD_STEP + 4)
    def _():
        in_grad_copy().wait()
        for copy in attn_side():
            copy.wait()
        for i in range(8):
            rows = pl.ds(pl.multiple_of(c * two_d + i * (d // 4), 16), d // 4)
            other = y_side[pl.ds(i * (d // 4), d // 4), :]
            xg[rows, :] = (xg[rows, :].astype(f32) + other.astype(f32)).astype(bf16)
        gains_s[...] = (gains_s[...].astype(f32) + gains_side[...].astype(f32)).astype(bf16)
        pl.semaphore_wait(free_in, n - 1)
        for m in range(1, n):
            for copy in attn_across(m):
                copy.start()

    def z_copy(i, src, dst, to):
        return remote(src, dst, z_send.at[i], z_recv.at[i], to)

    z_rows = 2 * part + 16
    z_land = y_side.at[pl.ds(two_d, 2 * z_rows)]

    def z_half(h):
        return pl.ds(pl.multiple_of(h * z_rows, 16), z_rows)

    def z_to_mid():
        return z_copy(0, z_own, z_land, {"plane": mid_of})

    def z_from_end():
        return z_copy(0, z_own, z_land, {"plane": end_of})

    def z_swap_sums():
        return z_copy(1, z_own.at[z_half(give_h)], z_swap, {"plane": other_mid})

    def z_swap_done():
        at = z_half(keep_h)
        return z_copy(2, z_own.at[at], near_z.at[at], {"plane": other_mid})

    def z_swap_done_in():
        at = z_half(give_h)
        return z_copy(2, z_own.at[at], near_z.at[at], {"plane": other_mid})

    def z_to_end(first):
        at = z_half(keep_h if first else give_h)
        source = z_own if first else near_z
        return z_copy(3 if first else 4, source.at[at], near_z.at[at], {"plane": end_of})

    def z_from_mid(first):
        at = z_half((q // 3) if first else 1 - q // 3)
        return z_copy(3 if first else 4, near_z.at[at], near_z.at[at], {"plane": mid_of})

    def z_stay():
        at = z_half(keep_h)
        return pltpu.make_async_copy(z_own.at[at], near_z.at[at], load_sem.at[17])

    def z_side():
        return z_copy(6, near_z, far_z, {"core": other_c})

    @pl.when(t == Z_STEPS[0])
    def _():
        for m in range(1, n):
            for copy in attn_across(m):
                copy.wait()
        for h in range(2):
            at = pl.multiple_of(s * 2 * part + h * part, 16)
            for i in range(2):
                total = xg[pl.ds(pl.multiple_of(c * two_d + i * d + at, 16), part), :].astype(f32)
                for m in range(1, n):
                    total = total + y_in[m - 1, i, pl.ds(h * part, part), :].astype(f32)
                z_own[pl.ds(h * z_rows + i * part, part), :] = total.astype(bf16)
            total = gains_s[pl.ds(at, part), :].astype(f32)
            for m in range(1, n):
                total = total + gains_in[m - 1, pl.ds(h * part, part), :].astype(f32)
            total = total.astype(bf16)
            for r in range(part // 16):
                z_own[pl.ds(h * z_rows + 2 * part, 16), r * 128 : (r + 1) * 128] = total[
                    r * 16 : (r + 1) * 16, :
                ]

        @pl.when(ends)
        def _():
            z_to_mid().start()

    @pl.when((t == Z_STEPS[1]) & middle)
    def _():
        z_from_end().wait_recv()
        for h in range(2):
            at = pl.ds(h * z_rows, z_rows)
            other = y_side[pl.ds(two_d + h * z_rows, z_rows), :]
            z_own[at, :] = (z_own[at, :].astype(f32) + other.astype(f32)).astype(bf16)
        z_swap_sums().start()

    @pl.when((t == Z_STEPS[2]) & middle)
    def _():
        z_swap_sums().wait()
        at = z_half(keep_h)
        z_own[at, :] = (z_own[at, :].astype(f32) + z_swap[...].astype(f32)).astype(bf16)
        z_stay().start()
        z_swap_done().start()
        z_to_end(True).start()

    @pl.when((t == Z_STEPS[3]) & middle)
    def _():
        z_swap_done_in().wait_recv()
        z_stay().wait()
        z_to_end(False).start()
        z_side().start()

    @pl.when((t == Z_STEPS[4]) & ends)
    def _():
        z_to_mid().wait_send()
        z_from_mid(True).wait_recv()
        z_from_mid(False).wait_recv()
        z_side().start()

    @pl.when(t == Z_STEPS[5])
    def _():
        z_side().wait()

        @pl.when(middle)
        def _():
            z_swap_done().wait_send()
            z_to_end(True).wait_send()
            z_to_end(False).wait_send()


EARLY, AHEAD = 1, 2
DOUBLE = 9
STAGE_DELAY = (2, 3, 7, 9, 14, 15, 15)
STAGE_ORDER = (0, 3, 5, 6, 2, 4, 1)
Y_STEPS = (7, 9, 11)
HEAD_STEP = 10
Z_STEPS = (18, 19, 20, 23, 26, 28)


def layer_call(n, operands):
    tokens, eg = operands[0], operands[11]
    length, d = tokens.shape
    hb = eg.shape[2] // (2 * n)
    rows = 2 * n * length
    slots = 2 * n * CAP
    chunks = 3 * (EXPERTS + 1)
    part = d // (2 * n)
    steps = 1 + max(chunks + max(STAGE_DELAY) - DOUBLE, Z_STEPS[5] + 1)
    vmem = lambda v: pl.BlockSpec(v.shape, lambda t: (0, 0), pipeline_mode=pl.Buffered(1))
    anywhere = pl.BlockSpec(memory_space=pl.ANY)
    dma = pltpu.SemaphoreType.DMA
    shape = jax.ShapeDtypeStruct
    z_pieces = (2 * (2 * part + 16), d)
    return pl.pallas_call(
        functools.partial(layer_kernel, n),
        grid=(steps,),
        in_specs=[vmem(v) for v in operands[:4]] + [anywhere] * (len(operands) - 4),
        out_specs=[anywhere] * 11,
        out_shape=[
            shape((chunks, d, hb), bf16),
            shape((chunks, d, hb), bf16),
            shape(z_pieces, bf16),
            shape(z_pieces, bf16),
            shape((4 * d, d), bf16),
            shape((5 * length, d), bf16),
            shape((n * length, d), f32),
            shape((length, d), f32),
            shape((EXPERTS + 1, 3, n - 1, 2 * part, hb), bf16),
            shape((length, d), bf16),
            shape((length, d), bf16),
        ],
        scratch_shapes=[
            pltpu.VMEM((2 * rows, d), bf16),
            pltpu.VMEM((rows, d), f32),
            pltpu.VMEM((rows, d), f32),
            pltpu.VMEM((max(3 * slots, rows, 9 * length), d), bf16),
            pltpu.VMEM((3, d, hb), f32),
            pltpu.VMEM(((EXPERTS + 1) * d, 3 * hb), bf16),
            pltpu.VMEM((chunks, d, hb), bf16),
            pltpu.VMEM((chunks, d // 2, hb), bf16),
            pltpu.VMEM((rows, d), bf16),
            pltpu.VMEM((n - 1, 2, length, d), bf16),
            pltpu.VMEM((2, 3, d, hb), bf16),
            pltpu.VMEM((2 * n, 8, length), jnp.int32),
            pltpu.VMEM((2 * n, 8, length), f32),
            pltpu.VMEM((length, 128), f32),
            pltpu.VMEM((d, 128), bf16),
            pltpu.VMEM((length, length), f32),
            pltpu.VMEM((slots, 1), f32),
            pltpu.VMEM((slots, 1), f32),
            pltpu.VMEM((2 * n, 8, length), f32),
            pltpu.VMEM((n, 8, length), f32),
            pltpu.VMEM((n - 1, 8, length), f32),
            pltpu.VMEM((n - 1, 8, length), f32),
            pltpu.VMEM((length, d), bf16),
            pltpu.VMEM((length, d), bf16),
            pltpu.VMEM((128, d), f32),
            pltpu.VMEM(z_pieces, bf16),
            pltpu.VMEM((2 * part + 16, d), bf16),
            dma((6, chunks)),
            dma((6, chunks)),
            dma((n - 1, chunks)),
            dma((n - 1, chunks)),
            dma((chunks,)),
            dma((8,)),
            dma((8,)),
            dma((n - 1, 3)),
            dma((n - 1, 3)),
            dma((3, n - 1)),
            dma((3, n - 1)),
            dma((n,)),
            dma((n,)),
            dma((18,)),
            pltpu.SemaphoreType.REGULAR,
            pltpu.SemaphoreType.REGULAR,
            pltpu.VMEM((d, 128), bf16),
            pltpu.VMEM((d, 128), bf16),
            pltpu.VMEM((n - 1, 2 * part, 128), bf16),
            dma((3, n - 1)),
            dma((3, n - 1)),
            dma((EXPERTS + 1, 3 * (n - 1))),
            dma((EXPERTS + 1, 3 * (n - 1))),
            dma((2, 3 * n)),
            dma((4, n - 1)),
            dma((4, n - 1)),
            dma((6,)),
            dma((6,)),
        ],
        compiler_params=pltpu.CompilerParams(
            vmem_limit_bytes=67043328, collective_id=0, has_side_effects=True
        ),
        cost_estimate=pl.CostEstimate(
            flops=30 * 10**9, bytes_accessed=200 << 20, transcendentals=0
        ),
        name="layer",
    )(*operands)


def attention_forward(tokens, small, weight, allowed, cosine, sine, half_way, outs):
    q_ref, k_ref, v_ref, att_ref, one_ref, two_ref, mid_ref, soft_ref, router_ref = outs
    length, d = tokens.shape
    pair = 2 * HD
    small_rows = jnp.transpose(small[...].astype(f32))
    gain_one, gain_two = small_rows[0:1, :], small_rows[1:2, :]
    x = tokens[...].astype(f32)
    one = (x * lax.rsqrt(jnp.mean(x * x, axis=1, keepdims=True) + EPSILON) * gain_one).astype(bf16)
    one_ref[...] = one
    lane = lax.broadcasted_iota(jnp.int32, (length, pair), 1)
    lower = lane % HD < HD // 2
    cos, sin = cosine[...], sine[...]
    for i, ref in ((0, q_ref), (2, v_ref), (1, k_ref)):
        if i == 1:
            half_way()
        for p in range(d // (2 * pair)):
            wide = mm(one, weight(i)[:, 2 * p * pair : 2 * (p + 1) * pair], NN)
            for r in range(2):
                cut = slice((2 * p + r) * pair, (2 * p + r + 1) * pair)
                value = wide[:, r * pair : (r + 1) * pair]
                if i < 2:
                    up = pltpu.roll(value, pair - HD // 2, 1)
                    down = pltpu.roll(value, HD // 2, 1)
                    value = value * cos + jnp.where(lower, -up, down) * sin
                ref[:, cut] = value.astype(bf16)
    first = lane < HD

    def heads(p, carry):
        cut = pl.ds(pl.multiple_of(p * pair, pair), pair)
        queries, keys, values = q_ref[:, cut], k_ref[:, cut], v_ref[:, cut]
        parts = []
        for side in range(2):
            mine = first if side == 0 else jnp.logical_not(first)
            chosen = jnp.where(mine, queries.astype(f32), 0.0).astype(bf16)
            scores = mm(chosen, keys, NT) * HD ** (-0.5)
            scores = jnp.where(allowed[...] > 0.0, scores, NEGATIVE)
            exponent = jnp.exp(scores - jnp.max(scores, axis=1, keepdims=True))
            soft = exponent / jnp.sum(exponent, axis=1, keepdims=True)
            h = 2 * p + side
            at = pl.ds(pl.multiple_of((h // 3) * length, length), length)
            soft_ref[at, pl.ds(pl.multiple_of((h % 3) * length, length), length)] = soft
            parts.append(mm(soft.astype(bf16), values, NN))
        att_ref[:, cut] = jnp.where(first, parts[0], parts[1]).astype(bf16)
        return carry

    lax.fori_loop(0, d // pair, heads, 0, unroll=3)
    middle = x + mm(att_ref[...], weight(3)[...], NN)
    mid_ref[...] = middle
    two = middle * lax.rsqrt(jnp.mean(middle * middle, axis=1, keepdims=True) + EPSILON) * gain_two
    two = two.astype(bf16)
    two_ref[...] = two
    logits = mm(two, small[...], NN)
    column = lax.broadcasted_iota(jnp.int32, logits.shape, 1)
    valid = (column >= 2) & (column < 2 + EXPERTS)
    logits = jnp.where(valid, logits, NEGATIVE)
    exponent = jnp.exp(logits - jnp.max(logits, axis=1, keepdims=True))
    exponent = jnp.where(valid, exponent, 0.0)
    router = exponent / jnp.sum(exponent, axis=1, keepdims=True)
    router_ref[...] = router
    return router


def finish_kernel(n, where_ref, own_ref, far_ref, own_z, far_z, *outs):
    step = pl.program_id(0)
    s, c = where_ref[0], where_ref[1]
    part = own_ref.shape[1] // (2 * n)
    hb = own_ref.shape[2]
    z_rows = own_z.shape[0] // 2

    def write(targets):
        for side, ref in enumerate((own_ref, far_ref)):
            for m in range(n):
                column = pl.multiple_of(((s ^ m) * 2 + (c ^ side)) * hb, 128)
                for k in range(3):
                    for h in range(2):
                        row = (h * n + m) * part
                        targets[k][0, h * part : (h + 1) * part, pl.ds(column, hb)] = ref[
                            k, row : row + part, :
                        ].astype(f32)

    @pl.when(step < EXPERTS)
    def _():
        write(outs[:3])

    @pl.when(step == EXPERTS)
    def _():
        write(outs[3:6])

    @pl.when(step == 0)
    def _():
        tail = outs[10]
        for h in range(2):
            at = slice(h * z_rows, (h + 1) * z_rows)
            mine, other = own_z[at, :].astype(f32), far_z[at, :].astype(f32)
            low = jnp.where(c == 0, mine, other)
            high = jnp.where(c == 0, other, mine)
            for i, out in enumerate(outs[6:10]):
                source = (low if i < 2 else high)[(i % 2) * part : (i % 2 + 1) * part, :]
                out[h * part : (h + 1) * part, :] = source
            for r in range(part // 16):
                row = h * part + r * 16
                tail[row : row + 16, :] = low[2 * part : 2 * part + 16, r * 128 : (r + 1) * 128]


def finish(n, where, own, far, own_z, far_z):
    hb, d = own.shape[2], own.shape[1]
    rows, hidden = d // n, hb * 2 * n
    spec = pl.BlockSpec((3, d, hb), lambda i, *_: (i, 0, 0))
    z_spec = pl.BlockSpec(own_z.shape, lambda i, *_: (0, 0))
    expert = pl.BlockSpec((1, rows, hidden), lambda i, *_: (jnp.minimum(i, EXPERTS - 1), 0, 0))
    shared = pl.BlockSpec((1, rows, hidden), lambda i, *_: (0, 0, 0))
    square = pl.BlockSpec((rows, d), lambda i, *_: (0, 0))
    tail = pl.BlockSpec((rows, 128), lambda i, *_: (0, 0))
    shape = jax.ShapeDtypeStruct
    return pl.pallas_call(
        functools.partial(finish_kernel, n),
        grid_spec=pltpu.PrefetchScalarGridSpec(
            num_scalar_prefetch=1,
            grid=(EXPERTS + 1,),
            in_specs=[spec, spec, z_spec, z_spec],
            out_specs=[expert] * 3 + [shared] * 3 + [square] * 4 + [tail],
        ),
        out_shape=[shape((EXPERTS, rows, hidden), f32)] * 3
        + [shape((1, rows, hidden), f32)] * 3
        + [shape((rows, d), f32)] * 4
        + [shape((rows, 128), f32)],
        cost_estimate=pl.CostEstimate(
            flops=0, bytes_accessed=130 * rows * hidden, transcendentals=0
        ),
        compiler_params=pltpu.CompilerParams(vmem_limit_bytes=56 << 20),
        name="finish",
    )(where, own, far, own_z, far_z)


def make_plain(n, qn):
    bits = qn.bit_length() - 1

    def place_blocks(own, blocks):
        out = jnp.zeros((n,) + blocks[0].shape, blocks[0].dtype)
        for m in range(n):
            out = lax.dynamic_update_index_in_dim(out, blocks[m], own ^ m, 0)
        return out

    def join_bit(bit, own, other, axis):
        first = jnp.where(bit == 0, own, other)
        second = jnp.where(bit == 0, other, own)
        return jnp.concatenate([first, second], axis=axis)

    def shards(
        tokens,
        cotangent,
        segments,
        padding,
        routes,
        priority,
        attn_gain,
        query_weight,
        key_weight,
        value_weight,
        output_weight,
        ffn_gain,
        router_weight,
        expert_gate,
        expert_up,
        expert_down,
        shared_gate,
        shared_up,
        shared_down,
    ):
        s = lax.axis_index("shard")
        q = lax.axis_index("plane")
        c = lax.axis_index("core")
        length, d = tokens.shape[1], tokens.shape[2]
        rows = query_weight.shape[0]
        hidden = expert_gate.shape[2]
        hb = hidden // (2 * n)
        score_scale = HD ** (-0.5)

        small = jnp.concatenate(
            [attn_gain[:, None], ffn_gain[:, None], router_weight], axis=1
        )
        small = jnp.pad(small, ((0, 0), (0, 256 - small.shape[1])))
        wide = jnp.concatenate(
            [query_weight, key_weight, value_weight, output_weight, small], axis=1
        )
        half = wide.shape[1] // 2
        mine = lax.dynamic_slice_in_dim(wide, c * half, half, 1)
        blocks = [mine] + [swap(mine, "shard", m, n) for m in range(1, n)]
        mine = place_blocks(s, blocks).reshape(d, half)
        other = swap(mine, "core", 1, 2)
        wide = join_bit(c, mine, other, 1)
        wqkv, wo = wide[:, : 3 * d], wide[:, 3 * d : 4 * d]
        gain_one = wide[:, 4 * d].astype(f32)
        gain_two = wide[:, 4 * d + 1].astype(f32)
        wr = wide[:, 4 * d + 2 : 4 * d + 2 + EXPERTS]

        def block_for(m):
            start = ((s ^ m) * 2 + c) * hb
            cut = lambda w: lax.dynamic_slice_in_dim(w, start, hb, w.ndim - 1)
            return [
                jnp.concatenate([cut(e), cut(w)[None]], axis=0)
                for e, w in (
                    (expert_gate, shared_gate),
                    (expert_up, shared_up),
                    (expert_down, shared_down),
                )
            ]

        own_blocks = block_for(0)
        sent = [block_for(m) for m in range(1, n)]
        moe_w = []
        for k in range(3):
            got = [own_blocks[k]] + [swap(sent[m - 1][k], "shard", m, n) for m in range(1, n)]
            full = jnp.zeros((EXPERTS + 1, n, rows, hb), bf16)
            for m in range(n):
                full = lax.dynamic_update_index_in_dim(full, got[m], s ^ m, 1)
            moe_w.append(full.reshape(EXPERTS + 1, d, hb))

        def plane_gather(values):
            near = jnp.stack([values] + [swap(values, "shard", m, n) for m in range(1, n)])
            return jnp.concatenate([near, swap(near, "core", 1, 2)], axis=0)

        def plane_sum(partial):
            low = partial.astype(bf16)
            pair = (partial[:n] + swap(low[n:], "core", 1, 2).astype(f32)).astype(bf16)
            total = pair[0].astype(f32)
            for m in range(1, n):
                total = total + swap(pair[m], "shard", m, n).astype(f32)
            return total

        grads_b = plane_gather(cotangent[0])

        inputs = tokens[0].astype(f32)
        factor_one = norm_factor(inputs)
        normed_one = (inputs * factor_one * gain_one).astype(bf16)
        projected = jnp.dot(normed_one, wqkv, preferred_element_type=f32)
        cosine, sine = rotary_tables(length, HD)
        heads = projected.reshape(length, 3, NH, HD)
        cos_b, sin_b = cosine[:, None, :], sine[:, None, :]
        queries = (heads[:, 0] * cos_b + rotate_half(heads[:, 0]) * sin_b).astype(bf16)
        keys_rot = (heads[:, 1] * cos_b + rotate_half(heads[:, 1]) * sin_b).astype(bf16)
        values = heads[:, 2].astype(bf16)
        allowed = attention_mask(segments[0], padding[0])
        logits = dot("qhd,khd->hqk", queries, keys_rot) * score_scale
        logits = jnp.where(allowed[None], logits, NEGATIVE)
        maxima = jnp.max(logits, axis=-1, keepdims=True)
        exponent = jnp.exp(logits - maxima)
        soft = exponent / jnp.sum(exponent, axis=-1, keepdims=True)
        probs = soft.astype(bf16)
        attended = dot("hqk,khd->qhd", probs, values).reshape(length, d).astype(bf16)
        middle = inputs + jnp.dot(attended, wo, preferred_element_type=f32)
        factor_two = norm_factor(middle)
        normed_two = (middle * factor_two * gain_two).astype(bf16)
        router = jax.nn.softmax(
            jnp.dot(normed_two, wr, preferred_element_type=f32), axis=-1
        )

        pair_expert, place, kept = pair_slots(routes[0], padding[0], priority[0])
        slot_total = EXPERTS * CAP
        slot_index = jnp.where(kept, pair_expert * CAP + place, -1).reshape(TOPK, length)
        slots = jnp.arange(slot_total, dtype=jnp.int32)
        hit = (slots[None, :, None] == slot_index[:, None, :]).any(axis=0)
        onehot = hit.astype(bf16)
        token_of = jnp.max(
            jnp.where(hit, jnp.arange(length, dtype=jnp.int32)[None, :], -1), axis=1
        )
        slot_expert = jnp.repeat(jnp.arange(EXPERTS), CAP)
        gate_of = jnp.sum(
            jnp.where(hit, jnp.repeat(router.T, CAP, axis=0), 0.0), axis=1
        )

        tokens_b = plane_gather(normed_two)
        token_of_b = plane_gather(token_of)
        gate_of_b = plane_gather(gate_of)
        group = 2 * n
        onehot_b = (
            token_of_b[:, :, None] == jnp.arange(length, dtype=jnp.int32)[None, None, :]
        ).astype(bf16)
        onehot_b = onehot_b.reshape(group, EXPERTS, CAP, length)
        gate_b = gate_of_b.reshape(group, EXPERTS, CAP, 1)

        def reduce_and_return(stack):
            k = stack.shape[0]
            piece = rows // qn
            x = stack.reshape((k, n) + (2,) * bits + (piece, hb))
            for b in range(bits):
                axis = 2 + (bits - 1 - b)
                bit = (q >> b) & 1
                keep = pick_index(x, bit, axis)
                send = pick_index(x, 1 - bit, axis).astype(bf16)
                x = keep + swap(send, "plane", 1 << b, qn).astype(f32)
            x = x.astype(bf16)
            own = pick_index(x, s, 1)
            got = [own] + [swap(pick_index(x, s ^ m, 1), "shard", m, n) for m in range(1, n)]
            x = jnp.stack(got)
            x = x[None]
            for b in reversed(range(bits)):
                bit = (q >> b) & 1
                other = swap(x, "plane", 1 << b, qn)
                lead = x.shape[0]
                pair = jnp.stack(
                    [jnp.where(bit == 0, x, other), jnp.where(bit == 0, other, x)], axis=1
                )
                x = pair.reshape((2 * lead,) + x.shape[1:])
            other = swap(x, "core", 1, 2)
            x = jnp.stack(
                [jnp.where(c == 0, x, other), jnp.where(c == 0, other, x)]
            )
            out = jnp.zeros((n,) + (2, qn, k, piece, hb), bf16)
            for m in range(n):
                out = lax.dynamic_update_index_in_dim(out, x[:, :, m], s ^ m, 0)
            return out.transpose(3, 2, 4, 0, 1, 5).reshape(k, rows, hidden).astype(f32)

        w_gate, w_up, w_down = moe_w
        tokens_f = tokens_b.reshape(group * length, d)
        grads_f = grads_b.reshape(group * length, d)
        shared_g = jnp.dot(tokens_f, w_gate[EXPERTS], preferred_element_type=f32)
        shared_u = jnp.dot(tokens_f, w_up[EXPERTS], preferred_element_type=f32)
        value, slope = silu_parts(shared_g)
        shared_hidden = (value * shared_u).astype(bf16)
        shared_q = jnp.dot(grads_f, w_down[EXPERTS], preferred_element_type=f32)
        shared_gd = (shared_q * shared_u * slope).astype(bf16)
        shared_ud = (shared_q * value).astype(bf16)
        shared_grads = jnp.stack(
            [
                dot("ld,lh->dh", tokens_f, shared_gd),
                dot("ld,lh->dh", tokens_f, shared_ud),
                dot("ld,lh->dh", grads_f, shared_hidden),
            ]
        )
        out_partial = dot("lh,dh->ld", shared_hidden, w_down[EXPERTS])
        two_partial = dot("lh,dh->ld", shared_gd, w_gate[EXPERTS]) + dot(
            "lh,dh->ld", shared_ud, w_up[EXPERTS]
        )
        out_partial = out_partial.reshape(group, length, d)
        two_partial = two_partial.reshape(group, length, d)
        shared_done = reduce_and_return(shared_grads)

        pick_parts = []
        expert_done = []
        for part in GROUPS:
            lo, hi = part[0], part[-1] + 1
            hot = onehot_b[:, lo:hi]
            x_in = jnp.einsum("bect,btd->ebcd", hot, tokens_b, preferred_element_type=bf16)
            g_in = jnp.einsum("bect,btd->ebcd", hot, grads_b, preferred_element_type=bf16)
            gate_e = jnp.swapaxes(gate_b[:, lo:hi], 0, 1)
            wg, wu, wd = w_gate[lo:hi], w_up[lo:hi], w_down[lo:hi]
            gate_act = dot("ebcd,edh->ebch", x_in, wg)
            up_act = dot("ebcd,edh->ebch", x_in, wu)
            value, slope = silu_parts(gate_act)
            hid = (value * up_act).astype(bf16)
            e_out = dot("ebch,edh->ebcd", hid, wd)
            pick_parts.append(jnp.sum(e_out * g_in.astype(f32), axis=-1))
            slot_grad = (gate_e * g_in.astype(f32)).astype(bf16)
            hid_grad = dot("ebcd,edh->ebch", slot_grad, wd)
            gate_d = (hid_grad * up_act * slope).astype(bf16)
            up_d = (hid_grad * value).astype(bf16)
            in_grad = dot("ebch,edh->ebcd", gate_d, wg) + dot("ebch,edh->ebcd", up_d, wu)
            weighted = (gate_e * e_out).astype(bf16)
            out_partial = out_partial + dot("bect,ebcd->btd", hot, weighted)
            two_partial = two_partial + dot("bect,ebcd->btd", hot, in_grad.astype(bf16))
            stack = jnp.concatenate(
                [
                    dot("ebcd,ebch->edh", x_in, gate_d),
                    dot("ebcd,ebch->edh", x_in, up_d),
                    dot("ebcd,ebch->edh", slot_grad, hid),
                ]
            )
            expert_done.append(reduce_and_return(stack))

        two_grad = plane_sum(two_partial)
        picks = jnp.concatenate(pick_parts, axis=0)
        picks = jnp.swapaxes(picks, 0, 1).reshape(group, slot_total)
        picks = picks[:n] + swap(picks[n:], "core", 1, 2)
        pick_slot = picks[0]
        for m in range(1, n):
            pick_slot = pick_slot + swap(picks[m], "shard", m, n)
        mixed = plane_sum(out_partial)
        output = (middle + mixed).astype(bf16)

        upstream = cotangent[0].astype(f32)
        pick_grad = jnp.sum(
            jnp.where(hit, pick_slot[:, None], 0.0).reshape(EXPERTS, CAP, length), axis=1
        ).T
        logit_grad = router * (pick_grad - jnp.sum(router * pick_grad, axis=1, keepdims=True))
        two_grad = two_grad + jnp.dot(logit_grad, wr.astype(f32).T, precision=highest)
        router_grad = jnp.dot(normed_two.astype(f32).T, logit_grad, precision=highest)
        middle_part, ffn_gain_grad = norm_back(middle, factor_two, gain_two, two_grad)
        middle_grad = middle_part + upstream

        branch_grad = middle_grad.astype(bf16)
        output_weight_grad = dot("ld,le->de", attended, branch_grad)
        attended_grad = (
            dot("le,de->ld", branch_grad, wo).astype(bf16).reshape(length, NH, HD)
        )
        prob_grad = dot("qhd,khd->hqk", attended_grad, values)
        row_inner = jnp.sum(soft * prob_grad, axis=-1, keepdims=True)
        score_grad = (soft * (prob_grad - row_inner)).astype(bf16)
        query_parts = dot("hqk,khd->qhd", score_grad, keys_rot) * score_scale
        key_parts = dot("hqk,qhd->khd", score_grad, queries) * score_scale
        value_parts = dot("hqk,qhd->khd", probs, attended_grad)
        query_pre = query_parts * cos_b + rotate_back(query_parts * sin_b)
        key_pre = key_parts * cos_b + rotate_back(key_parts * sin_b)
        joint_grad = jnp.concatenate(
            [v.reshape(length, d) for v in (query_pre, key_pre, value_parts)], axis=1
        ).astype(bf16)
        one_grad = dot("lf,df->ld", joint_grad, wqkv)
        joint_weight_grad = dot("ld,lf->df", normed_one, joint_grad)
        input_part, attn_gain_grad = norm_back(inputs, factor_one, gain_one, one_grad)
        input_grad = (middle_grad + input_part).astype(bf16)

        small_grad = jnp.concatenate(
            [attn_gain_grad[:, None], ffn_gain_grad[:, None], router_grad], axis=1
        )
        small_grad = jnp.pad(small_grad, ((0, 0), (0, 256 - small_grad.shape[1])))
        total = jnp.concatenate([joint_weight_grad, output_weight_grad, small_grad], axis=1)
        keep = lax.dynamic_slice_in_dim(total, c * half, half, 1)
        send = lax.dynamic_slice_in_dim(total, (1 - c) * half, half, 1).astype(bf16)
        total = keep + swap(send, "core", 1, 2).astype(f32)
        total = total.reshape(n, rows, half)
        own = pick_index(total, s)
        low = total.astype(bf16)
        for m in range(1, n):
            own = own + swap(pick_index(low, s ^ m), "shard", m, n).astype(f32)
        x = own.reshape((2,) * bits + (rows // qn, half))
        for b in range(bits):
            axis = bits - 1 - b
            bit = (q >> b) & 1
            keep = pick_index(x, bit, axis)
            send = pick_index(x, 1 - bit, axis).astype(bf16)
            x = keep + swap(send, "plane", 1 << b, qn).astype(f32)
        x = x.astype(bf16)[None]
        for b in reversed(range(bits)):
            bit = (q >> b) & 1
            other = swap(x, "plane", 1 << b, qn)
            pair = jnp.stack(
                [jnp.where(bit == 0, x, other), jnp.where(bit == 0, other, x)], axis=1
            )
            x = pair.reshape((2 * x.shape[0],) + x.shape[1:])
        x = x.reshape(rows, half)
        x = join_bit(c, x, swap(x, "core", 1, 2), 1).astype(f32)
        stacks = [[], [], []]
        for part, done in zip(GROUPS, expert_done):
            for k in range(3):
                stacks[k].append(done[k * len(part) : (k + 1) * len(part)])
        expert_grads = [jnp.concatenate(parts, axis=0) for parts in stacks]
        return (
            output[None],
            input_grad[None],
            x[:, 4 * d],
            x[:, :d],
            x[:, d : 2 * d],
            x[:, 2 * d : 3 * d],
            x[:, 3 * d : 4 * d],
            x[:, 4 * d + 1],
            x[:, 4 * d + 2 : 4 * d + 2 + EXPERTS],
            expert_grads[0],
            expert_grads[1],
            expert_grads[2],
            shared_done[0],
            shared_done[1],
            shared_done[2],
        )

    return shards


def make_fast(n, qn):
    def shards(
        tokens,
        cotangent,
        segments,
        padding,
        routes,
        priority,
        attn_gain,
        query_weight,
        key_weight,
        value_weight,
        output_weight,
        ffn_gain,
        router_weight,
        expert_gate,
        expert_up,
        expert_down,
        shared_gate,
        shared_up,
        shared_down,
    ):
        s = lax.axis_index("shard")
        c = lax.axis_index("core")
        length, d = tokens.shape[1], tokens.shape[2]
        where = jnp.stack([s, c]).astype(jnp.int32)

        meta = jnp.concatenate(
            [segments, padding, routes[0].T, priority, jnp.zeros((3, length), jnp.int32)], axis=0
        )
        cosine, sine = rotary_tables(length, HD)
        cos_pair = jnp.concatenate([cosine, cosine], axis=1)
        sin_pair = jnp.concatenate([sine, sine], axis=1)
        small = jnp.concatenate([attn_gain[:, None], ffn_gain[:, None], router_weight], axis=1)
        small = jnp.pad(small, ((0, 0), (0, 128 - small.shape[1])))

        near, far, near_z, far_z, *_, output, input_grad = layer_call(
            n,
            (
                tokens[0],
                meta,
                cos_pair,
                sin_pair,
                tokens[0],
                cotangent[0],
                small,
                query_weight,
                key_weight,
                value_weight,
                output_weight,
                expert_gate,
                expert_up,
                expert_down,
                shared_gate,
                shared_up,
                shared_down,
            ),
        )
        done = finish(n, where, near, far, near_z, far_z)
        tail = done[10]
        return (
            output[None],
            input_grad[None],
            tail[:, 0],
            *done[6:10],
            tail[:, 1],
            tail[:, 2 : 2 + EXPERTS],
            *done[:3],
            *(v[0] for v in done[3:6]),
        )

    return shards


def make_shards(n, qn):
    plain, fast = make_plain(n, qn), make_fast(n, qn)

    def shards(*arguments):
        d, hidden = arguments[0].shape[2], arguments[13].shape[2]
        fits = n == 4 and qn == 4 and d == 768 and hidden == 2048 and arguments[0].shape[1] == 256
        return (fast if fits else plain)(*arguments)

    return shards


def solution(mesh):
    n, replicas = mesh.shape["shard"], mesh.shape["replica"]
    fine = Mesh(mesh.devices.reshape(n, replicas // 2, 2), ("shard", "plane", "core"))
    every = ("shard", "plane", "core")
    in_specs = (
        P(every, None, None),
        P(every, None, None),
        P(every, None),
        P(every, None),
        P(every, None, None),
        P(every, None),
        P("shard"),
        P("shard", None),
        P("shard", None),
        P("shard", None),
        P("shard", None),
        P("shard"),
        P("shard", None),
        P(None, "shard", None),
        P(None, "shard", None),
        P(None, "shard", None),
        P("shard", None),
        P("shard", None),
        P("shard", None),
    )
    out_specs = (
        P(every, None, None),
        P(every, None, None),
        P("shard"),
        P("shard", None),
        P("shard", None),
        P("shard", None),
        P("shard", None),
        P("shard"),
        P("shard", None),
        P(None, "shard", None),
        P(None, "shard", None),
        P(None, "shard", None),
        P("shard", None),
        P("shard", None),
        P("shard", None),
    )
    return jax.shard_map(
        make_shards(n, replicas // 2),
        mesh=fine,
        in_specs=in_specs,
        out_specs=out_specs,
        check_vma=False,
    )
```

```python
import functools
import math

import jax
import jax.numpy as jnp
from jax import lax
from jax.experimental import pallas as pl
from jax.experimental.pallas import tpu as pltpu
from jax.sharding import Mesh, PartitionSpec as P

NH = 12
HD = 64
EXPERTS = 6
TOPK = 2
CAP = 96
EPSILON = 1e-06
NEGATIVE = -1e30
GROUPS = ((0, 1), (2, 3), (4, 5))

highest = lax.Precision.HIGHEST
f32 = jnp.float32
bf16 = jnp.bfloat16


def dot(spec, first, second):
    return jnp.einsum(spec, first, second, preferred_element_type=f32)


def rotate_half(values):
    half_size = values.shape[-1] // 2
    return jnp.concatenate([-values[..., half_size:], values[..., :half_size]], axis=-1)


def rotate_back(values):
    half_size = values.shape[-1] // 2
    return jnp.concatenate([values[..., half_size:], -values[..., :half_size]], axis=-1)


def rotary_tables(length, head_dim):
    positions = jnp.arange(length, dtype=f32)
    frequency = jnp.exp(
        jnp.arange(head_dim // 2, dtype=f32) * (-2.0 * math.log(10000.0) / head_dim)
    )
    angles = positions[:, None] * frequency[None, :]
    angles = jnp.concatenate([angles, angles], axis=1)
    return (jnp.cos(angles), jnp.sin(angles))


def attention_mask(segments, padding):
    places = jnp.arange(segments.shape[0])
    causal = places[None, :] <= places[:, None]
    shared_doc = segments[:, None] == segments[None, :]
    usable = (padding[None, :] == 1) | (places[None, :] == places[:, None])
    return causal & shared_doc & usable


def norm_factor(values):
    return lax.rsqrt(jnp.mean(values * values, axis=-1, keepdims=True) + EPSILON)


def norm_back(values, factor, norm_gain, gradient):
    scaled = gradient * norm_gain
    gain_grad = jnp.sum(gradient * values * factor, axis=0)
    input_part = factor * scaled - values * factor**3 * jnp.mean(
        scaled * values, axis=-1, keepdims=True
    )
    return (input_part, gain_grad)


def silu_parts(gate_act):
    sigmoid = jax.nn.sigmoid(gate_act)
    return (gate_act * sigmoid, sigmoid * (1.0 + gate_act * (1.0 - sigmoid)))


def pair_slots(routes, padding, priority):
    length = routes.shape[0]
    pair_expert = routes.T.reshape(-1)
    pair_live = jnp.tile(padding, TOPK) == 1
    pair_key = (jnp.arange(TOPK, dtype=jnp.int32)[:, None] * length + priority[None, :]).reshape(-1)
    earlier = (
        (pair_key[None, :] < pair_key[:, None])
        & (pair_expert[None, :] == pair_expert[:, None])
        & pair_live[None, :]
    )
    place = jnp.sum(earlier.astype(jnp.int32), axis=1)
    kept = pair_live & (place < CAP)
    return (pair_expert, place, kept)


def swap(values, axis, mask, size):
    return lax.ppermute(values, axis, [(i, i ^ mask) for i in range(size)])


def pick_index(values, index, axis=0):
    return lax.dynamic_index_in_dim(values, index, axis, keepdims=False)


def mm(first, second, contract):
    return lax.dot_general(
        first, second, (contract, ((), ())), preferred_element_type=f32
    )


NN = ((1,), (0,))
NT = ((1,), (1,))
TN = ((0,), (0,))


def flip(value, mask, size):
    out = 0
    for b in range(size.bit_length() - 1):
        bit = (value // (1 << b)) % 2
        out = out + (1 << b) * ((1 - bit) if (mask >> b) & 1 else bit)
    return out


MESH = pl.DeviceIdType.MESH


def layer_kernel(
    n,
    tokens,
    meta_ref,
    cos_ref,
    sin_ref,
    tok_hbm,
    cot_hbm,
    small_own,
    wq,
    wk,
    wv,
    wo,
    eg,
    eu,
    ed,
    sg,
    su,
    sd,
    near_ref,
    far_ref,
    near_z,
    far_z,
    wide_hbm,
    work_hbm,
    soft_hbm,
    mid_hbm,
    w_land,
    out_ref,
    in_grad_ref,
    xg,
    acc_y,
    acc_t,
    work,
    dw,
    own,
    land,
    swap_in,
    y_side,
    y_in,
    wbuf,
    slot_ref,
    router_ref,
    probs_ref,
    small_ref,
    allowed,
    gate_s,
    pick_s,
    pick_acc,
    pick_side,
    pick_pair,
    pick_in,
    branch_s,
    ag_s,
    small_acc,
    z_own,
    z_swap,
    ch_send,
    ch_recv,
    x_send,
    x_recv,
    stay_sem,
    z_send,
    z_recv,
    zx_send,
    zx_recv,
    y_send_sem,
    y_recv_sem,
    p_send,
    p_recv,
    load_sem,
    free_side,
    free_in,
    gains_s,
    gains_side,
    gains_in,
    a_send,
    a_recv,
    w_send,
    w_recv,
    w_load,
    t_send,
    t_recv,
    side_send,
    side_recv,
):
    t = pl.program_id(0) - 1
    group = 2 * n
    length, d = tokens.shape
    hb = dw.shape[2]
    part = d // (2 * n)
    half = n * part
    chunks = 3 * (EXPERTS + 1)
    plane_rows = group * length
    s, q, c = (lax.axis_index(a) for a in ("shard", "plane", "core"))
    middle = (q == 1) | (q == 2)
    ends = (q == 0) | (q == 3)
    keep_h, give_h = (q + 1) % 2, q % 2
    other_mid = 3 - q
    mid_of = 1 + q // 3
    end_of = (q // 2) * 3
    other_c = 1 - c
    shard_of = [None] + [flip(s, m, n) for m in range(1, n)]

    def at_chunk(u, row=0, count=d):
        start = pl.multiple_of((u // 3) * d + row, 16)
        return pl.ds(start, count), pl.ds(pl.multiple_of((u % 3) * hb, 128), hb)

    def half_rows(h):
        return pl.ds(pl.multiple_of(h * half, 16), half)

    def remote(src, dst, ssem, rsem, to):
        return pltpu.make_async_remote_copy(
            src, dst, ssem, rsem, device_id=to, device_id_type=MESH
        )

    def chunk(kind, src, dst, u, to):
        return remote(src, dst, ch_send.at[kind, u], ch_recv.at[kind, u], to)

    def to_mid(u):
        return chunk(0, own.at[at_chunk(u)], land.at[u], u, {"plane": mid_of})

    def from_end(u):
        return chunk(0, own.at[at_chunk(u)], land.at[u], u, {"plane": end_of})

    def swap_sums(u):
        src = own.at[at_chunk(u, give_h * half, half)]
        return chunk(1, src, swap_in.at[u], u, {"plane": other_mid})

    def swap_done(u):
        ref = near_ref.at[u, half_rows(keep_h)]
        return chunk(2, ref, ref, u, {"plane": other_mid})

    def swap_done_in(u):
        ref = near_ref.at[u, half_rows(give_h)]
        return chunk(2, ref, ref, u, {"plane": other_mid})

    def to_end(u, first):
        ref = near_ref.at[u, half_rows(keep_h if first else give_h)]
        return chunk(3 if first else 4, ref, ref, u, {"plane": end_of})

    def from_mid(u, first):
        ref = near_ref.at[u, half_rows((q // 3) if first else 1 - q // 3)]
        return chunk(3 if first else 4, ref, ref, u, {"plane": mid_of})

    def across(u, m):
        return remote(
            own.at[at_chunk(u, keep_h * half + m * part, part)],
            near_ref.at[u, pl.ds(pl.multiple_of(keep_h * half + m * part, 16), part)],
            x_send.at[m - 1, u],
            x_recv.at[m - 1, u],
            {"shard": shard_of[m]},
        )

    def stay(u):
        return pltpu.make_async_copy(
            own.at[at_chunk(u, keep_h * half, part)],
            near_ref.at[u, pl.ds(pl.multiple_of(keep_h * half, 16), part)],
            stay_sem.at[u],
        )

    def side(u):
        return chunk(5, near_ref.at[u], far_ref.at[u], u, {"core": other_c})

    far_rows = pl.ds(0, plane_rows)

    def y_side_copy():
        return remote(
            work.at[far_rows], y_side, y_send_sem.at[0, 0], y_recv_sem.at[0, 0], {"core": other_c}
        )

    def y_across(k, m):
        at = pl.ds((k * n + m) * length, length)
        return remote(
            y_side.at[at],
            y_in.at[m - 1, k],
            y_send_sem.at[1 + k, m - 1],
            y_recv_sem.at[1 + k, m - 1],
            {"shard": shard_of[m]},
        )

    def pick_side_copy():
        return remote(
            pick_acc.at[pl.ds(n, n)], pick_side, p_send.at[0], p_recv.at[0], {"core": other_c}
        )

    def pick_across(m):
        return remote(
            pick_pair.at[m - 1],
            pick_in.at[m - 1],
            p_send.at[m],
            p_recv.at[m],
            {"shard": shard_of[m]},
        )

    def load(i, src, dst):
        return pltpu.make_async_copy(src, dst, load_sem.at[i])

    def back_rows(i):
        return pl.ds(i * length, length)

    two_w = [length, length + d, plane_rows + length, plane_rows + length + d]

    saved_rows = pl.ds(0, 5 * length)
    soft_rows = pl.ds(n * length, n * length)
    mid_rows = pl.ds(n * length, length)

    def saved_out():
        return [
            load(2, acc_y.at[soft_rows], soft_hbm),
            load(3, acc_t.at[mid_rows], mid_hbm),
            load(4, own.at[pl.ds(0, 4 * d)], wide_hbm),
            load(5, work.at[saved_rows], work_hbm),
        ]

    def saved_in():
        copies = [
            load(6, soft_hbm, acc_y.at[soft_rows]),
            load(7, mid_hbm, acc_t.at[mid_rows]),
            load(8, work_hbm, work.at[saved_rows]),
            load(9, tok_hbm, work.at[back_rows(5)]),
        ]
        for i in range(4):
            copies.append(load(10 + i, wide_hbm.at[pl.ds(i * d, d)], xg.at[pl.ds(two_w[i], d)]))
        return copies

    def columns(m):
        owner = s if m == 0 else shard_of[m]
        return pl.ds(pl.multiple_of((owner * 2 + c) * hb, 128), hb)

    def weight_ref(e, k, m, shared):
        big, one = ((eg, sg), (eu, su), (ed, sd))[k]
        return one.at[:, columns(m)] if shared else big.at[e, :, columns(m)]

    def weight_sends(e, shared):
        return [
            remote(
                weight_ref(e, k, m, shared),
                w_land.at[e, k, m - 1],
                w_send.at[e, 3 * k + m - 1],
                w_recv.at[e, 3 * k + m - 1],
                {"shard": shard_of[m]},
            )
            for k in range(3)
            for m in range(1, n)
        ]

    def weight_loads(e, shared):
        copies = []
        for k in range(3):
            for m in range(n):
                owner = s if m == 0 else shard_of[m]
                src = weight_ref(e, k, 0, shared) if m == 0 else w_land.at[e, k, m - 1]
                dst = wbuf.at[
                    e % 2, k, pl.ds(pl.multiple_of(owner * 2 * part, 16), 2 * part)
                ]
                copies.append(pltpu.make_async_copy(src, dst, w_load.at[e % 2, n * k + m]))
        return copies

    def for_expert(e, body):
        @pl.when(e < EXPERTS)
        def _():
            body(e, False)

        @pl.when(e == EXPERTS)
        def _():
            body(e, True)

    def fetch_weights(e, shared):
        for copy in weight_sends(e, shared):
            copy.wait()
        for copy in weight_loads(e, shared):
            copy.start()

    def start_weights(e, shared):
        for copy in weight_sends(e, shared):
            copy.start()

    def finish_weights(e, shared):
        for copy in weight_loads(e, shared):
            copy.wait()

    @pl.when(t < 0)
    def _():
        barrier = pltpu.get_barrier_semaphore()
        peers = [{"core": other_c}] + [{"shard": shard_of[m]} for m in range(1, n)]
        for peer in peers:
            pl.semaphore_signal(barrier, 1, device_id=peer, device_id_type=MESH)

        @pl.when(middle)
        def _():
            for peer in ({"plane": other_mid}, {"plane": end_of}):
                pl.semaphore_signal(barrier, 1, device_id=peer, device_id_type=MESH)
            pl.semaphore_wait(barrier, len(peers) + 2)

        @pl.when(ends)
        def _():
            pl.semaphore_signal(barrier, 1, device_id={"plane": mid_of}, device_id_type=MESH)
            pl.semaphore_wait(barrier, len(peers) + 1)

        my_rows = pl.multiple_of(s * 2 * part, 16)

        def wide_at(i, row, count):
            return own.at[pl.ds(pl.multiple_of((2 * c + i) * d + row, 16), count)]

        def attn_sends(i, source):
            return [
                remote(
                    source,
                    wide_at(i, my_rows, 2 * part),
                    a_send.at[i, m - 1],
                    a_recv.at[i, m - 1],
                    {"shard": shard_of[m]},
                )
                for m in range(1, n)
            ]

        def attn_stay(i, source):
            return load(i, source, wide_at(i, my_rows, 2 * part))

        smalls = [
            remote(
                small_own,
                small_ref.at[pl.ds(my_rows, 2 * part)],
                a_send.at[2, m - 1],
                a_recv.at[2, m - 1],
                {"shard": shard_of[m]},
            )
            for m in range(1, n)
        ]
        stay_here = [
            load(14, small_own, small_ref.at[pl.ds(my_rows, 2 * part)]),
            load(15, cot_hbm, xg.at[pl.ds(plane_rows, length)]),
        ]
        for copy in smalls + stay_here:
            copy.start()
        for core, pair_of in enumerate(((wq, wk), (wv, wo))):

            @pl.when(c == core)
            def _():
                for i in range(2):
                    attn_stay(i, pair_of[i]).start()
                    for copy in attn_sends(i, pair_of[i]):
                        copy.start()

        def spread_out(i, src, place):
            return [
                remote(
                    src, place(m), t_send.at[i, m - 1], t_recv.at[i, m - 1], {"shard": shard_of[m]}
                )
                for m in range(1, n)
            ]

        def to_core(i, src, dst):
            return remote(src, dst, side_send.at[i], side_recv.at[i], {"core": other_c})

        def rows_to_core(i, base):
            return to_core(
                i, xg.at[pl.ds(base, n * length)], xg.at[pl.ds(base + n * length, n * length)]
            )

        g_copies = spread_out(
            0, cot_hbm, lambda m: xg.at[pl.ds(plane_rows + m * length, length)]
        )
        slot_copies = spread_out(1, slot_ref.at[0], lambda m: slot_ref.at[m])
        for copy in g_copies:
            copy.start()
        for e in range(EARLY):
            start_weights(e, False)
        rows_of = meta_ref[...].astype(f32)
        columns_of = jnp.transpose(
            jnp.concatenate([rows_of, jnp.zeros((120, length), f32)], axis=0)
        )
        row = lambda r: rows_of[r : r + 1, :]
        column = lambda r: columns_of[:, r : r + 1]
        above = lax.broadcasted_iota(jnp.int32, (length, length), 0)
        along = lax.broadcasted_iota(jnp.int32, (length, length), 1)
        seen = (along <= above) & (column(0) == row(0)) & ((row(1) == 1.0) | (along == above))
        allowed[...] = jnp.where(seen, 1.0, 0.0)
        live = column(1) == 1.0
        sooner = live & (column(4) < row(4))
        count = lambda hits: jnp.sum(jnp.where(hits, 1.0, 0.0), axis=0, keepdims=True)
        places = (
            count(sooner & (column(2) == row(2))),
            count(live & (column(2) == row(3))) + count(sooner & (column(3) == row(3))),
        )
        line = lax.broadcasted_iota(jnp.int32, (8, length), 0)
        table = jnp.full((8, length), -1.0, f32)
        for k in range(TOPK):
            kept = (row(1) == 1.0) & (places[k] < CAP)
            place = jnp.where(kept, row(2 + k) * CAP + places[k], -1.0)
            table = jnp.where(line == k, place, table)
        slot_ref[0] = table.astype(jnp.int32)
        for copy in stay_here:
            copy.wait()

        def gather_attn(i):
            attn_stay(i, wq).wait()
            for copy in attn_sends(i, wq):
                copy.wait()
            at = wide_at(i, 0, d)
            copy = to_core(5 * i, at, at)
            copy.start()
            return copy

        first_half = gather_attn(0)
        for copy in slot_copies:
            copy.start()
        for copy in smalls:
            copy.wait()
        first_half.wait()

        def half_way():
            gather_attn(1).wait()

        work_part = lambda i: work.at[pl.ds(i * length, length)]
        outs = tuple(work_part(i) for i in range(5)) + (
            xg.at[pl.ds(0, length)],
            acc_t.at[mid_rows],
            acc_y.at[soft_rows],
            probs_ref,
        )
        router = attention_forward(
            tokens,
            small_ref,
            lambda i: own.at[pl.ds(i * d, d)],
            allowed,
            cos_ref,
            sin_ref,
            half_way,
            outs,
        )
        router_ref[0] = jnp.transpose(router)[0:8, :]
        for copy in saved_out():
            copy.start()
        x_copies = spread_out(
            2, xg.at[pl.ds(0, length)], lambda m: xg.at[pl.ds(m * length, length)]
        )
        rt_copies = spread_out(3, router_ref.at[0], lambda m: router_ref.at[m])
        for copy in x_copies + rt_copies:
            copy.start()

        for e in range(EARLY, AHEAD):
            start_weights(e, False)
        for copy in slot_copies + g_copies:
            copy.wait()
        g_side = rows_to_core(1, plane_rows)
        slot_side = to_core(2, slot_ref.at[pl.ds(0, n)], slot_ref.at[pl.ds(n, n)])
        g_side.start()
        slot_side.start()
        for copy in saved_out():
            copy.wait()
        acc_y[...] = jnp.zeros_like(acc_y)
        acc_t[...] = jnp.zeros_like(acc_t)
        pick_acc[...] = jnp.zeros_like(pick_acc)
        fetch_weights(0, False)
        for copy in x_copies + rt_copies:
            copy.wait()
        x_side = rows_to_core(3, 0)
        rt_side = to_core(4, router_ref.at[pl.ds(0, n)], router_ref.at[pl.ds(n, n)])
        x_side.start()
        rt_side.start()
        for copy in (g_side, slot_side, x_side, rt_side):
            copy.wait()

    def branch(x, gs_rows, wg, wu, wd):
        gate_act = mm(x, wg, NN)
        up_act = mm(x, wu, NN)
        sigmoid = 1.0 / (1.0 + jnp.exp(-gate_act))
        value = gate_act * sigmoid
        slope = sigmoid * (1.0 + gate_act * (1.0 - sigmoid))
        hid = (value * up_act).astype(bf16)
        hid_grad = mm(gs_rows, wd, NN)
        gate_d = (hid_grad * up_act * slope).astype(bf16)
        up_d = (hid_grad * value).astype(bf16)
        return hid, gate_d, up_d

    slots = group * CAP
    xs_at, gs_at, sg_at = 0, slots, 2 * slots

    @pl.when((t >= 0) & (t <= EXPERTS))
    def _():
        for_expert(t + AHEAD, start_weights)
        for_expert(t, finish_weights)

    @pl.when((t >= 0) & (t < EXPERTS))
    def _():
        ids = lax.broadcasted_iota(jnp.int32, (CAP, length), 0) + t * CAP

        def slots_of(b):
            first, second = slot_ref[b, 0:1, :], slot_ref[b, 1:2, :]
            return (first == ids) | (second == ids)

        for b in range(group):
            slot = pl.ds(b * CAP, CAP)
            hit = slots_of(b)
            hot = hit.astype(f32).astype(bf16)
            row = router_ref[b, pl.ds(t + 2, 1), :]
            gate = jnp.sum(jnp.where(hit, row, 0.0), axis=1, keepdims=True)
            gate_s[slot, :] = gate
            x_rows = mm(hot, xg[pl.ds(b * length, length), :], NN)
            work[pl.ds(xs_at + b * CAP, CAP), :] = x_rows.astype(bf16)
            g_rows = mm(hot, xg[pl.ds(plane_rows + b * length, length), :], NN)
            work[pl.ds(gs_at + b * CAP, CAP), :] = g_rows.astype(bf16)
            work[pl.ds(sg_at + b * CAP, CAP), :] = (g_rows * gate).astype(bf16)
        wg, wu, wd = wbuf[t % 2, 0], wbuf[t % 2, 1], wbuf[t % 2, 2]
        x, slot_grad = work[pl.ds(xs_at, slots), :], work[pl.ds(sg_at, slots), :]
        hid, gate_d, up_d = branch(x, slot_grad, wg, wu, wd)
        dw[0] = mm(x, gate_d, TN)
        dw[1] = mm(x, up_d, TN)
        dw[2] = mm(slot_grad, hid, TN)
        e_out = mm(hid, wd, NT)
        g_rows = work[pl.ds(gs_at, slots), :].astype(f32)
        pick_s[...] = jnp.sum(e_out * g_rows, axis=1, keepdims=True)
        work[pl.ds(gs_at, slots), :] = (e_out * gate_s[...]).astype(bf16)
        work[pl.ds(xs_at, slots), :] = (mm(gate_d, wg, NT) + mm(up_d, wu, NT)).astype(bf16)
        for b in range(group):
            slot = pl.ds(b * CAP, CAP)
            seq = pl.ds(b * length, length)
            hit = slots_of(b)
            hot = hit.astype(f32).astype(bf16)
            pick_acc[b, pl.ds(t + 2, 1), :] = jnp.sum(
                jnp.where(hit, pick_s[slot, :], 0.0), axis=0, keepdims=True
            )
            acc_y[seq, :] += mm(hot, work[pl.ds(gs_at + b * CAP, CAP), :], TN)
            acc_t[seq, :] += mm(hot, work[pl.ds(xs_at + b * CAP, CAP), :], TN)

    @pl.when(t == EXPERTS)
    def _():
        dw[...] = jnp.zeros_like(dw)
        wg, wu, wd = wbuf[t % 2, 0], wbuf[t % 2, 1], wbuf[t % 2, 2]

        def rows_step(i, carry):
            at = pl.multiple_of(i * 2 * length, 2 * length)
            rows = pl.ds(at, 2 * length)
            x, g = xg[rows, :], xg[pl.ds(plane_rows + at, 2 * length), :]
            hid, gate_d, up_d = branch(x, g, wg, wu, wd)
            dw[0] += mm(x, gate_d, TN)
            dw[1] += mm(x, up_d, TN)
            dw[2] += mm(g, hid, TN)
            acc_y[rows, :] += mm(hid, wd, NT)
            acc_t[rows, :] += mm(gate_d, wg, NT) + mm(up_d, wu, NT)
            return carry

        lax.fori_loop(0, n, rows_step, 0)
        work[pl.ds(0, n * length), :] = acc_y[soft_rows, :].astype(bf16)
        work[pl.ds(n * length, n * length), :] = acc_t[soft_rows, :].astype(bf16)

    @pl.when((t >= 0) & (t <= EXPERTS))
    def _():
        for k in range(3):
            for h in range(2):
                for m in range(n):
                    owner = s if m == 0 else shard_of[m]
                    start = pl.multiple_of((owner * 2 + h) * part, 16)
                    row = pl.multiple_of(t * d + (h * n + m) * part, 16)
                    own[pl.ds(row, part), k * hb : (k + 1) * hb] = dw[
                        k, pl.ds(start, part), :
                    ].astype(bf16)

        @pl.when(ends)
        def _():
            for k in range(3):
                to_mid(3 * t + k).start()

    @pl.when(t == EXPERTS)
    def _():
        y_side_copy().start()
        pick_side_copy().start()

    def add_halves(u):
        from_end(u).wait_recv()
        for i in range(2 * n):
            rows, columns_at = at_chunk(u, i * part, part)
            own[rows, columns_at] = (
                own[rows, columns_at].astype(f32)
                + land[u, pl.ds(i * part, part), :].astype(f32)
            ).astype(bf16)
        swap_sums(u).start()

    def add_swapped(u):
        swap_sums(u).wait()
        for m in range(n):
            rows, columns_at = at_chunk(u, keep_h * half + m * part, part)
            own[rows, columns_at] = (
                own[rows, columns_at].astype(f32)
                + swap_in[u, pl.ds(m * part, part), :].astype(f32)
            ).astype(bf16)
        for m in range(1, n):
            across(u, m).start()
        stay(u).start()

    def send_done(u):
        for m in range(1, n):
            across(u, m).wait()
        stay(u).wait()
        swap_done(u).start()
        to_end(u, True).start()

    def send_second(u):
        swap_done_in(u).wait_recv()
        to_end(u, False).start()
        side(u).start()

    def end_side(u):
        to_mid(u).wait_send()
        from_mid(u, True).wait_recv()
        from_mid(u, False).wait_recv()
        side(u).start()

    def middle_last(u):
        swap_done(u).wait_send()
        to_end(u, True).wait_send()
        to_end(u, False).wait_send()
        side(u).wait()

    mine_rows = pl.ds(0, length)
    grad_rows = pl.ds((n + 1) * length, length)

    def out_copy():
        return load(14, xg.at[mine_rows], out_ref)

    def in_grad_copy():
        return load(15, work.at[back_rows(5)], in_grad_ref)

    @pl.when(t == Y_STEPS[2])
    def _():
        total = acc_y[mine_rows, :]
        for m in range(1, n):
            y_across(0, m).wait()
            total = total + y_in[m - 1, 0].astype(f32)
        xg[mine_rows, :] = (acc_t[mid_rows, :] + total).astype(bf16)
        out_copy().start()
        pl.semaphore_signal(free_side, 1, device_id={"core": other_c}, device_id_type=MESH)
        for m in range(1, n):
            pl.semaphore_signal(free_in, 1, device_id={"shard": shard_of[m]}, device_id_type=MESH)

    stages = (
        (middle, add_halves),
        (middle, add_swapped),
        (middle, send_done),
        (middle, send_second),
        (ends, end_side),
        (middle, middle_last),
        (ends, lambda u: side(u).wait()),
    )

    def chunk_step(i, carry):
        v = t + jnp.minimum(t, DOUBLE) + i
        live = (i == 0) | (t < DOUBLE)
        for k in STAGE_ORDER:
            where, body = stages[k]
            u = v - STAGE_DELAY[k]

            @pl.when(live & (u >= 0) & (u < chunks) & where)
            def _():
                body(u)

        return carry

    lax.fori_loop(0, 2, chunk_step, 0)

    @pl.when((t >= 0) & (t < EXPERTS))
    def _():
        for_expert(t + 1, fetch_weights)

    @pl.when(t == Y_STEPS[0])
    def _():
        y_side_copy().wait()
        pick_side_copy().wait()
        for copy in saved_in():
            copy.start()
        pick_acc[pl.ds(0, n)] += pick_side[...]
        for m in range(1, n):
            pick_pair[m - 1] = pick_acc[m]
        for k, acc in ((1, acc_t), (0, acc_y)):
            for m in range(n):
                seq, at = pl.ds(m * length, length), pl.ds((k * n + m) * length, length)
                total = acc[seq, :] + y_side[at, :].astype(f32)
                if m == 0:
                    acc[seq, :] = total
                else:
                    y_side[at, :] = total.astype(bf16)
            for m in range(1, n):
                y_across(k, m).start()
                if k:
                    pick_across(m).start()

    pre_at = 6 * length
    exact = lax.Precision.HIGHEST

    @pl.when(t == Y_STEPS[1])
    def _():
        for m in range(1, n):
            y_across(1, m).wait()
            pick_across(m).wait()
        for copy in saved_in():
            copy.wait()
        two = acc_t[mine_rows, :]
        picks = pick_acc[0]
        for m in range(1, n):
            two = two + y_in[m - 1, 1].astype(f32)
            picks = picks + pick_in[m - 1]
        picks = jnp.concatenate([picks, jnp.zeros((120, length), f32)], axis=0)
        picks = jnp.transpose(picks)
        router = probs_ref[...]
        logit_grad = router * (picks - jnp.sum(router * picks, axis=1, keepdims=True))
        small = small_ref[...].astype(f32)
        gain_two = jnp.transpose(small)[1:2, :]
        two = two + lax.dot_general(
            logit_grad, small, (NT, ((), ())), precision=exact, preferred_element_type=f32
        )
        router_grad = lax.dot_general(
            logit_grad,
            xg[mine_rows, :].astype(f32),
            (TN, ((), ())),
            precision=exact,
            preferred_element_type=f32,
        )
        mid = acc_t[mid_rows, :]
        factor = lax.rsqrt(jnp.mean(mid * mid, axis=1, keepdims=True) + EPSILON)
        gain_grad = jnp.sum(two * mid * factor, axis=0, keepdims=True)
        row = lax.broadcasted_iota(jnp.int32, router_grad.shape, 0)
        small_acc[...] = jnp.where(row == 1, gain_grad, router_grad)
        scaled = two * gain_two
        grad = (
            xg[pl.ds(plane_rows, length), :].astype(f32)
            + factor * scaled
            - mid * (factor * factor * factor) * jnp.mean(scaled * mid, axis=1, keepdims=True)
        )
        acc_t[grad_rows, :] = grad
        branch_s[...] = grad.astype(bf16)
        ag_s[...] = mm(branch_s[...], xg[pl.ds(two_w[3], d), :], NT).astype(bf16)

    pair = 2 * HD

    @pl.when((t >= HEAD_STEP) & (t < HEAD_STEP + 3))
    def _():
        lane = lax.broadcasted_iota(jnp.int32, (length, pair), 1)
        first = lane < HD
        lower = lane % HD < HD // 2
        cos, sin = cos_ref[...], sin_ref[...]

        def turn_back(w):
            y = w * sin
            up = pltpu.roll(y, pair - HD // 2, 1)
            down = pltpu.roll(y, HD // 2, 1)
            return w * cos + jnp.where(lower, up, -down)

        def heads(i, carry):
            p = 2 * (t - HEAD_STEP) + i
            cut = pl.ds(pl.multiple_of(p * pair, pair), pair)
            queries, keys, values = (work[back_rows(j), cut] for j in range(3))
            grads = ag_s[:, cut]
            parts = []
            for one_side in range(2):
                h = 2 * p + one_side
                rows = pl.ds(pl.multiple_of(n * length + (h // 3) * length, length), length)
                columns = pl.ds(pl.multiple_of((h % 3) * length, length), length)
                soft = acc_y[rows, columns]
                mine = first if one_side == 0 else jnp.logical_not(first)
                chosen = jnp.where(mine, grads.astype(f32), 0.0).astype(bf16)
                prob_grad = mm(chosen, values, NT)
                inner = jnp.sum(soft * prob_grad, axis=1, keepdims=True)
                score_grad = (soft * (prob_grad - inner)).astype(bf16)
                parts.append(
                    (
                        mm(score_grad, keys, NN) * HD ** (-0.5),
                        mm(score_grad, queries, TN) * HD ** (-0.5),
                        mm(soft.astype(bf16), grads, TN),
                    )
                )
            joined = [jnp.where(first, parts[0][j], parts[1][j]) for j in range(3)]
            joined = [turn_back(joined[0]), turn_back(joined[1]), joined[2]]
            for j in range(3):
                work[pl.ds(pre_at + j * length, length), cut] = joined[j].astype(bf16)
            return carry

        lax.fori_loop(0, 2, heads, 0, unroll=True)

    two_d = 2 * d
    give_rows = pl.ds(pl.multiple_of((1 - c) * two_d, 16), two_d)

    def attn_side():
        return [
            remote(
                xg.at[give_rows],
                y_side.at[pl.ds(0, two_d)],
                z_send.at[5],
                z_recv.at[5],
                {"core": other_c},
            ),
            remote(gains_s, gains_side, z_send.at[7], z_recv.at[7], {"core": other_c}),
        ]

    def attn_across(m):
        copies = []
        at = pl.multiple_of(shard_of[m] * 2 * part, 16)
        for i in range(2):
            copies.append(
                remote(
                    xg.at[pl.ds(pl.multiple_of(c * two_d + i * d + at, 16), 2 * part)],
                    y_in.at[m - 1, i, pl.ds(0, 2 * part)],
                    zx_send.at[m - 1, i],
                    zx_recv.at[m - 1, i],
                    {"shard": shard_of[m]},
                )
            )
        copies.append(
            remote(
                gains_s.at[pl.ds(at, 2 * part)],
                gains_in.at[m - 1],
                zx_send.at[m - 1, 2],
                zx_recv.at[m - 1, 2],
                {"shard": shard_of[m]},
            )
        )
        return copies

    @pl.when(t == HEAD_STEP + 3)
    def _():
        pre = [work[pl.ds(pre_at + j * length, length), :] for j in range(3)]
        one_grad = mm(pre[0], xg[pl.ds(two_w[0], d), :], NT)
        for j in (1, 2):
            one_grad = one_grad + mm(pre[j], xg[pl.ds(two_w[j], d), :], NT)
        x = work[back_rows(5), :].astype(f32)
        gain_one = jnp.transpose(small_ref[...].astype(f32))[0:1, :]
        factor = lax.rsqrt(jnp.mean(x * x, axis=1, keepdims=True) + EPSILON)
        gain_grad = jnp.sum(one_grad * x * factor, axis=0, keepdims=True)
        scaled = one_grad * gain_one
        work[back_rows(5), :] = (
            acc_t[grad_rows, :]
            + factor * scaled
            - x * (factor * factor * factor) * jnp.mean(scaled * x, axis=1, keepdims=True)
        ).astype(bf16)
        in_grad_copy().start()
        out_copy().wait()
        gains = small_acc[...]
        row = lax.broadcasted_iota(jnp.int32, gains.shape, 0)
        gains_s[...] = jnp.transpose(jnp.where(row == 0, gain_grad, gains)).astype(bf16)
        for i in range(4):
            lhs = work[back_rows(4 if i < 3 else 3), :]
            for k in range(3):
                cut = slice(k * hb, (k + 1) * hb)
                rhs = work[pl.ds(pre_at + i * length, length), cut] if i < 3 else branch_s[:, cut]
                xg[pl.ds(i * d, d), cut] = mm(lhs, rhs, TN).astype(bf16)
        pl.semaphore_wait(free_side, 1)
        for copy in attn_side():
            copy.start()

    @pl.when(t == HEAD_STEP + 4)
    def _():
        in_grad_copy().wait()
        for copy in attn_side():
            copy.wait()
        for i in range(8):
            rows = pl.ds(pl.multiple_of(c * two_d + i * (d // 4), 16), d // 4)
            other = y_side[pl.ds(i * (d // 4), d // 4), :]
            xg[rows, :] = (xg[rows, :].astype(f32) + other.astype(f32)).astype(bf16)
        gains_s[...] = (gains_s[...].astype(f32) + gains_side[...].astype(f32)).astype(bf16)
        pl.semaphore_wait(free_in, n - 1)
        for m in range(1, n):
            for copy in attn_across(m):
                copy.start()

    def z_copy(i, src, dst, to):
        return remote(src, dst, z_send.at[i], z_recv.at[i], to)

    z_rows = 2 * part + 16
    z_land = y_side.at[pl.ds(two_d, 2 * z_rows)]

    def z_half(h):
        return pl.ds(pl.multiple_of(h * z_rows, 16), z_rows)

    def z_to_mid():
        return z_copy(0, z_own, z_land, {"plane": mid_of})

    def z_from_end():
        return z_copy(0, z_own, z_land, {"plane": end_of})

    def z_swap_sums():
        return z_copy(1, z_own.at[z_half(give_h)], z_swap, {"plane": other_mid})

    def z_swap_done():
        at = z_half(keep_h)
        return z_copy(2, z_own.at[at], near_z.at[at], {"plane": other_mid})

    def z_swap_done_in():
        at = z_half(give_h)
        return z_copy(2, z_own.at[at], near_z.at[at], {"plane": other_mid})

    def z_to_end(first):
        at = z_half(keep_h if first else give_h)
        source = z_own if first else near_z
        return z_copy(3 if first else 4, source.at[at], near_z.at[at], {"plane": end_of})

    def z_from_mid(first):
        at = z_half((q // 3) if first else 1 - q // 3)
        return z_copy(3 if first else 4, near_z.at[at], near_z.at[at], {"plane": mid_of})

    def z_stay():
        at = z_half(keep_h)
        return pltpu.make_async_copy(z_own.at[at], near_z.at[at], load_sem.at[17])

    def z_side():
        return z_copy(6, near_z, far_z, {"core": other_c})

    @pl.when(t == Z_STEPS[0])
    def _():
        for m in range(1, n):
            for copy in attn_across(m):
                copy.wait()
        for h in range(2):
            at = pl.multiple_of(s * 2 * part + h * part, 16)
            for i in range(2):
                total = xg[pl.ds(pl.multiple_of(c * two_d + i * d + at, 16), part), :].astype(f32)
                for m in range(1, n):
                    total = total + y_in[m - 1, i, pl.ds(h * part, part), :].astype(f32)
                z_own[pl.ds(h * z_rows + i * part, part), :] = total.astype(bf16)
            total = gains_s[pl.ds(at, part), :].astype(f32)
            for m in range(1, n):
                total = total + gains_in[m - 1, pl.ds(h * part, part), :].astype(f32)
            total = total.astype(bf16)
            for r in range(part // 16):
                z_own[pl.ds(h * z_rows + 2 * part, 16), r * 128 : (r + 1) * 128] = total[
                    r * 16 : (r + 1) * 16, :
                ]

        @pl.when(ends)
        def _():
            z_to_mid().start()

    @pl.when((t == Z_STEPS[1]) & middle)
    def _():
        z_from_end().wait_recv()
        for h in range(2):
            at = pl.ds(h * z_rows, z_rows)
            other = y_side[pl.ds(two_d + h * z_rows, z_rows), :]
            z_own[at, :] = (z_own[at, :].astype(f32) + other.astype(f32)).astype(bf16)
        z_swap_sums().start()

    @pl.when((t == Z_STEPS[2]) & middle)
    def _():
        z_swap_sums().wait()
        at = z_half(keep_h)
        z_own[at, :] = (z_own[at, :].astype(f32) + z_swap[...].astype(f32)).astype(bf16)
        z_stay().start()
        z_swap_done().start()
        z_to_end(True).start()

    @pl.when((t == Z_STEPS[3]) & middle)
    def _():
        z_swap_done_in().wait_recv()
        z_stay().wait()
        z_to_end(False).start()
        z_side().start()

    @pl.when((t == Z_STEPS[4]) & ends)
    def _():
        z_to_mid().wait_send()
        z_from_mid(True).wait_recv()
        z_from_mid(False).wait_recv()
        z_side().start()

    @pl.when(t == Z_STEPS[5])
    def _():
        z_side().wait()

        @pl.when(middle)
        def _():
            z_swap_done().wait_send()
            z_to_end(True).wait_send()
            z_to_end(False).wait_send()


EARLY, AHEAD = 1, 2
DOUBLE = 9
STAGE_DELAY = (1, 2, 4, 6, 8, 10, 10)
STAGE_ORDER = (0, 1, 2, 3, 4, 5, 6)
Y_STEPS = (7, 8, 10)
HEAD_STEP = 9
Z_STEPS = (17, 19, 20, 21, 22, 23)


def layer_call(n, operands):
    tokens, eg = operands[0], operands[11]
    length, d = tokens.shape
    hb = eg.shape[2] // (2 * n)
    rows = 2 * n * length
    slots = 2 * n * CAP
    chunks = 3 * (EXPERTS + 1)
    part = d // (2 * n)
    steps = 1 + max(chunks + max(STAGE_DELAY) - DOUBLE, Z_STEPS[5] + 1)
    vmem = lambda v: pl.BlockSpec(v.shape, lambda t: (0, 0), pipeline_mode=pl.Buffered(1))
    anywhere = pl.BlockSpec(memory_space=pl.ANY)
    dma = pltpu.SemaphoreType.DMA
    shape = jax.ShapeDtypeStruct
    z_pieces = (2 * (2 * part + 16), d)
    return pl.pallas_call(
        functools.partial(layer_kernel, n),
        grid=(steps,),
        in_specs=[vmem(v) for v in operands[:4]] + [anywhere] * (len(operands) - 4),
        out_specs=[anywhere] * 11,
        out_shape=[
            shape((chunks, d, hb), bf16),
            shape((chunks, d, hb), bf16),
            shape(z_pieces, bf16),
            shape(z_pieces, bf16),
            shape((4 * d, d), bf16),
            shape((5 * length, d), bf16),
            shape((n * length, d), f32),
            shape((length, d), f32),
            shape((EXPERTS + 1, 3, n - 1, 2 * part, hb), bf16),
            shape((length, d), bf16),
            shape((length, d), bf16),
        ],
        scratch_shapes=[
            pltpu.VMEM((2 * rows, d), bf16),
            pltpu.VMEM((rows, d), f32),
            pltpu.VMEM((rows, d), f32),
            pltpu.VMEM((max(3 * slots, rows, 9 * length), d), bf16),
            pltpu.VMEM((3, d, hb), f32),
            pltpu.VMEM(((EXPERTS + 1) * d, 3 * hb), bf16),
            pltpu.VMEM((chunks, d, hb), bf16),
            pltpu.VMEM((chunks, d // 2, hb), bf16),
            pltpu.VMEM((rows, d), bf16),
            pltpu.VMEM((n - 1, 2, length, d), bf16),
            pltpu.VMEM((2, 3, d, hb), bf16),
            pltpu.VMEM((2 * n, 8, length), jnp.int32),
            pltpu.VMEM((2 * n, 8, length), f32),
            pltpu.VMEM((length, 128), f32),
            pltpu.VMEM((d, 128), bf16),
            pltpu.VMEM((length, length), f32),
            pltpu.VMEM((slots, 1), f32),
            pltpu.VMEM((slots, 1), f32),
            pltpu.VMEM((2 * n, 8, length), f32),
            pltpu.VMEM((n, 8, length), f32),
            pltpu.VMEM((n - 1, 8, length), f32),
            pltpu.VMEM((n - 1, 8, length), f32),
            pltpu.VMEM((length, d), bf16),
            pltpu.VMEM((length, d), bf16),
            pltpu.VMEM((128, d), f32),
            pltpu.VMEM(z_pieces, bf16),
            pltpu.VMEM((2 * part + 16, d), bf16),
            dma((6, chunks)),
            dma((6, chunks)),
            dma((n - 1, chunks)),
            dma((n - 1, chunks)),
            dma((chunks,)),
            dma((8,)),
            dma((8,)),
            dma((n - 1, 3)),
            dma((n - 1, 3)),
            dma((3, n - 1)),
            dma((3, n - 1)),
            dma((n,)),
            dma((n,)),
            dma((18,)),
            pltpu.SemaphoreType.REGULAR,
            pltpu.SemaphoreType.REGULAR,
            pltpu.VMEM((d, 128), bf16),
            pltpu.VMEM((d, 128), bf16),
            pltpu.VMEM((n - 1, 2 * part, 128), bf16),
            dma((3, n - 1)),
            dma((3, n - 1)),
            dma((EXPERTS + 1, 3 * (n - 1))),
            dma((EXPERTS + 1, 3 * (n - 1))),
            dma((2, 3 * n)),
            dma((4, n - 1)),
            dma((4, n - 1)),
            dma((6,)),
            dma((6,)),
        ],
        compiler_params=pltpu.CompilerParams(
            vmem_limit_bytes=67043328, collective_id=0, has_side_effects=True
        ),
        cost_estimate=pl.CostEstimate(
            flops=30 * 10**9, bytes_accessed=200 << 20, transcendentals=0
        ),
        name="layer",
    )(*operands)


def attention_forward(tokens, small, weight, allowed, cosine, sine, half_way, outs):
    q_ref, k_ref, v_ref, att_ref, one_ref, two_ref, mid_ref, soft_ref, router_ref = outs
    length, d = tokens.shape
    pair = 2 * HD
    small_rows = jnp.transpose(small[...].astype(f32))
    gain_one, gain_two = small_rows[0:1, :], small_rows[1:2, :]
    x = tokens[...].astype(f32)
    one = (x * lax.rsqrt(jnp.mean(x * x, axis=1, keepdims=True) + EPSILON) * gain_one).astype(bf16)
    one_ref[...] = one
    lane = lax.broadcasted_iota(jnp.int32, (length, pair), 1)
    lower = lane % HD < HD // 2
    cos, sin = cosine[...], sine[...]
    for i, ref in ((0, q_ref), (2, v_ref), (1, k_ref)):
        if i == 1:
            half_way()
        for p in range(d // (2 * pair)):
            wide = mm(one, weight(i)[:, 2 * p * pair : 2 * (p + 1) * pair], NN)
            for r in range(2):
                cut = slice((2 * p + r) * pair, (2 * p + r + 1) * pair)
                value = wide[:, r * pair : (r + 1) * pair]
                if i < 2:
                    up = pltpu.roll(value, pair - HD // 2, 1)
                    down = pltpu.roll(value, HD // 2, 1)
                    value = value * cos + jnp.where(lower, -up, down) * sin
                ref[:, cut] = value.astype(bf16)
    first = lane < HD

    def heads(p, carry):
        cut = pl.ds(pl.multiple_of(p * pair, pair), pair)
        queries, keys, values = q_ref[:, cut], k_ref[:, cut], v_ref[:, cut]
        parts = []
        for side in range(2):
            mine = first if side == 0 else jnp.logical_not(first)
            chosen = jnp.where(mine, queries.astype(f32), 0.0).astype(bf16)
            scores = mm(chosen, keys, NT) * HD ** (-0.5)
            scores = jnp.where(allowed[...] > 0.0, scores, NEGATIVE)
            exponent = jnp.exp(scores - jnp.max(scores, axis=1, keepdims=True))
            soft = exponent / jnp.sum(exponent, axis=1, keepdims=True)
            h = 2 * p + side
            at = pl.ds(pl.multiple_of((h // 3) * length, length), length)
            soft_ref[at, pl.ds(pl.multiple_of((h % 3) * length, length), length)] = soft
            parts.append(mm(soft.astype(bf16), values, NN))
        att_ref[:, cut] = jnp.where(first, parts[0], parts[1]).astype(bf16)
        return carry

    lax.fori_loop(0, d // pair, heads, 0, unroll=3)
    middle = x + mm(att_ref[...], weight(3)[...], NN)
    mid_ref[...] = middle
    two = middle * lax.rsqrt(jnp.mean(middle * middle, axis=1, keepdims=True) + EPSILON) * gain_two
    two = two.astype(bf16)
    two_ref[...] = two
    logits = mm(two, small[...], NN)
    column = lax.broadcasted_iota(jnp.int32, logits.shape, 1)
    valid = (column >= 2) & (column < 2 + EXPERTS)
    logits = jnp.where(valid, logits, NEGATIVE)
    exponent = jnp.exp(logits - jnp.max(logits, axis=1, keepdims=True))
    exponent = jnp.where(valid, exponent, 0.0)
    router = exponent / jnp.sum(exponent, axis=1, keepdims=True)
    router_ref[...] = router
    return router


def finish_kernel(n, where_ref, own_ref, far_ref, own_z, far_z, *outs):
    step = pl.program_id(0)
    s, c = where_ref[0], where_ref[1]
    part = own_ref.shape[1] // (2 * n)
    hb = own_ref.shape[2]
    z_rows = own_z.shape[0] // 2

    def write(targets):
        for side, ref in enumerate((own_ref, far_ref)):
            for m in range(n):
                column = pl.multiple_of(((s ^ m) * 2 + (c ^ side)) * hb, 128)
                for k in range(3):
                    for h in range(2):
                        row = (h * n + m) * part
                        targets[k][0, h * part : (h + 1) * part, pl.ds(column, hb)] = ref[
                            k, row : row + part, :
                        ].astype(f32)

    @pl.when(step < EXPERTS)
    def _():
        write(outs[:3])

    @pl.when(step == EXPERTS)
    def _():
        write(outs[3:6])

    @pl.when(step == 0)
    def _():
        tail = outs[10]
        for h in range(2):
            at = slice(h * z_rows, (h + 1) * z_rows)
            mine, other = own_z[at, :].astype(f32), far_z[at, :].astype(f32)
            low = jnp.where(c == 0, mine, other)
            high = jnp.where(c == 0, other, mine)
            for i, out in enumerate(outs[6:10]):
                source = (low if i < 2 else high)[(i % 2) * part : (i % 2 + 1) * part, :]
                out[h * part : (h + 1) * part, :] = source
            for r in range(part // 16):
                row = h * part + r * 16
                tail[row : row + 16, :] = low[2 * part : 2 * part + 16, r * 128 : (r + 1) * 128]


def finish(n, where, own, far, own_z, far_z):
    hb, d = own.shape[2], own.shape[1]
    rows, hidden = d // n, hb * 2 * n
    spec = pl.BlockSpec((3, d, hb), lambda i, *_: (i, 0, 0))
    z_spec = pl.BlockSpec(own_z.shape, lambda i, *_: (0, 0))
    expert = pl.BlockSpec((1, rows, hidden), lambda i, *_: (jnp.minimum(i, EXPERTS - 1), 0, 0))
    shared = pl.BlockSpec((1, rows, hidden), lambda i, *_: (0, 0, 0))
    square = pl.BlockSpec((rows, d), lambda i, *_: (0, 0))
    tail = pl.BlockSpec((rows, 128), lambda i, *_: (0, 0))
    shape = jax.ShapeDtypeStruct
    return pl.pallas_call(
        functools.partial(finish_kernel, n),
        grid_spec=pltpu.PrefetchScalarGridSpec(
            num_scalar_prefetch=1,
            grid=(EXPERTS + 1,),
            in_specs=[spec, spec, z_spec, z_spec],
            out_specs=[expert] * 3 + [shared] * 3 + [square] * 4 + [tail],
        ),
        out_shape=[shape((EXPERTS, rows, hidden), f32)] * 3
        + [shape((1, rows, hidden), f32)] * 3
        + [shape((rows, d), f32)] * 4
        + [shape((rows, 128), f32)],
        cost_estimate=pl.CostEstimate(
            flops=0, bytes_accessed=130 * rows * hidden, transcendentals=0
        ),
        compiler_params=pltpu.CompilerParams(vmem_limit_bytes=56 << 20),
        name="finish",
    )(where, own, far, own_z, far_z)


def make_plain(n, qn):
    bits = qn.bit_length() - 1

    def place_blocks(own, blocks):
        out = jnp.zeros((n,) + blocks[0].shape, blocks[0].dtype)
        for m in range(n):
            out = lax.dynamic_update_index_in_dim(out, blocks[m], own ^ m, 0)
        return out

    def join_bit(bit, own, other, axis):
        first = jnp.where(bit == 0, own, other)
        second = jnp.where(bit == 0, other, own)
        return jnp.concatenate([first, second], axis=axis)

    def shards(
        tokens,
        cotangent,
        segments,
        padding,
        routes,
        priority,
        attn_gain,
        query_weight,
        key_weight,
        value_weight,
        output_weight,
        ffn_gain,
        router_weight,
        expert_gate,
        expert_up,
        expert_down,
        shared_gate,
        shared_up,
        shared_down,
    ):
        s = lax.axis_index("shard")
        q = lax.axis_index("plane")
        c = lax.axis_index("core")
        length, d = tokens.shape[1], tokens.shape[2]
        rows = query_weight.shape[0]
        hidden = expert_gate.shape[2]
        hb = hidden // (2 * n)
        score_scale = HD ** (-0.5)

        small = jnp.concatenate(
            [attn_gain[:, None], ffn_gain[:, None], router_weight], axis=1
        )
        small = jnp.pad(small, ((0, 0), (0, 256 - small.shape[1])))
        wide = jnp.concatenate(
            [query_weight, key_weight, value_weight, output_weight, small], axis=1
        )
        half = wide.shape[1] // 2
        mine = lax.dynamic_slice_in_dim(wide, c * half, half, 1)
        blocks = [mine] + [swap(mine, "shard", m, n) for m in range(1, n)]
        mine = place_blocks(s, blocks).reshape(d, half)
        other = swap(mine, "core", 1, 2)
        wide = join_bit(c, mine, other, 1)
        wqkv, wo = wide[:, : 3 * d], wide[:, 3 * d : 4 * d]
        gain_one = wide[:, 4 * d].astype(f32)
        gain_two = wide[:, 4 * d + 1].astype(f32)
        wr = wide[:, 4 * d + 2 : 4 * d + 2 + EXPERTS]

        def block_for(m):
            start = ((s ^ m) * 2 + c) * hb
            cut = lambda w: lax.dynamic_slice_in_dim(w, start, hb, w.ndim - 1)
            return [
                jnp.concatenate([cut(e), cut(w)[None]], axis=0)
                for e, w in (
                    (expert_gate, shared_gate),
                    (expert_up, shared_up),
                    (expert_down, shared_down),
                )
            ]

        own_blocks = block_for(0)
        sent = [block_for(m) for m in range(1, n)]
        moe_w = []
        for k in range(3):
            got = [own_blocks[k]] + [swap(sent[m - 1][k], "shard", m, n) for m in range(1, n)]
            full = jnp.zeros((EXPERTS + 1, n, rows, hb), bf16)
            for m in range(n):
                full = lax.dynamic_update_index_in_dim(full, got[m], s ^ m, 1)
            moe_w.append(full.reshape(EXPERTS + 1, d, hb))

        def plane_gather(values):
            near = jnp.stack([values] + [swap(values, "shard", m, n) for m in range(1, n)])
            return jnp.concatenate([near, swap(near, "core", 1, 2)], axis=0)

        def plane_sum(partial):
            low = partial.astype(bf16)
            pair = (partial[:n] + swap(low[n:], "core", 1, 2).astype(f32)).astype(bf16)
            total = pair[0].astype(f32)
            for m in range(1, n):
                total = total + swap(pair[m], "shard", m, n).astype(f32)
            return total

        grads_b = plane_gather(cotangent[0])

        inputs = tokens[0].astype(f32)
        factor_one = norm_factor(inputs)
        normed_one = (inputs * factor_one * gain_one).astype(bf16)
        projected = jnp.dot(normed_one, wqkv, preferred_element_type=f32)
        cosine, sine = rotary_tables(length, HD)
        heads = projected.reshape(length, 3, NH, HD)
        cos_b, sin_b = cosine[:, None, :], sine[:, None, :]
        queries = (heads[:, 0] * cos_b + rotate_half(heads[:, 0]) * sin_b).astype(bf16)
        keys_rot = (heads[:, 1] * cos_b + rotate_half(heads[:, 1]) * sin_b).astype(bf16)
        values = heads[:, 2].astype(bf16)
        allowed = attention_mask(segments[0], padding[0])
        logits = dot("qhd,khd->hqk", queries, keys_rot) * score_scale
        logits = jnp.where(allowed[None], logits, NEGATIVE)
        maxima = jnp.max(logits, axis=-1, keepdims=True)
        exponent = jnp.exp(logits - maxima)
        soft = exponent / jnp.sum(exponent, axis=-1, keepdims=True)
        probs = soft.astype(bf16)
        attended = dot("hqk,khd->qhd", probs, values).reshape(length, d).astype(bf16)
        middle = inputs + jnp.dot(attended, wo, preferred_element_type=f32)
        factor_two = norm_factor(middle)
        normed_two = (middle * factor_two * gain_two).astype(bf16)
        router = jax.nn.softmax(
            jnp.dot(normed_two, wr, preferred_element_type=f32), axis=-1
        )

        pair_expert, place, kept = pair_slots(routes[0], padding[0], priority[0])
        slot_total = EXPERTS * CAP
        slot_index = jnp.where(kept, pair_expert * CAP + place, -1).reshape(TOPK, length)
        slots = jnp.arange(slot_total, dtype=jnp.int32)
        hit = (slots[None, :, None] == slot_index[:, None, :]).any(axis=0)
        onehot = hit.astype(bf16)
        token_of = jnp.max(
            jnp.where(hit, jnp.arange(length, dtype=jnp.int32)[None, :], -1), axis=1
        )
        slot_expert = jnp.repeat(jnp.arange(EXPERTS), CAP)
        gate_of = jnp.sum(
            jnp.where(hit, jnp.repeat(router.T, CAP, axis=0), 0.0), axis=1
        )

        tokens_b = plane_gather(normed_two)
        token_of_b = plane_gather(token_of)
        gate_of_b = plane_gather(gate_of)
        group = 2 * n
        onehot_b = (
            token_of_b[:, :, None] == jnp.arange(length, dtype=jnp.int32)[None, None, :]
        ).astype(bf16)
        onehot_b = onehot_b.reshape(group, EXPERTS, CAP, length)
        gate_b = gate_of_b.reshape(group, EXPERTS, CAP, 1)

        def reduce_and_return(stack):
            k = stack.shape[0]
            piece = rows // qn
            x = stack.reshape((k, n) + (2,) * bits + (piece, hb))
            for b in range(bits):
                axis = 2 + (bits - 1 - b)
                bit = (q >> b) & 1
                keep = pick_index(x, bit, axis)
                send = pick_index(x, 1 - bit, axis).astype(bf16)
                x = keep + swap(send, "plane", 1 << b, qn).astype(f32)
            x = x.astype(bf16)
            own = pick_index(x, s, 1)
            got = [own] + [swap(pick_index(x, s ^ m, 1), "shard", m, n) for m in range(1, n)]
            x = jnp.stack(got)
            x = x[None]
            for b in reversed(range(bits)):
                bit = (q >> b) & 1
                other = swap(x, "plane", 1 << b, qn)
                lead = x.shape[0]
                pair = jnp.stack(
                    [jnp.where(bit == 0, x, other), jnp.where(bit == 0, other, x)], axis=1
                )
                x = pair.reshape((2 * lead,) + x.shape[1:])
            other = swap(x, "core", 1, 2)
            x = jnp.stack(
                [jnp.where(c == 0, x, other), jnp.where(c == 0, other, x)]
            )
            out = jnp.zeros((n,) + (2, qn, k, piece, hb), bf16)
            for m in range(n):
                out = lax.dynamic_update_index_in_dim(out, x[:, :, m], s ^ m, 0)
            return out.transpose(3, 2, 4, 0, 1, 5).reshape(k, rows, hidden).astype(f32)

        w_gate, w_up, w_down = moe_w
        tokens_f = tokens_b.reshape(group * length, d)
        grads_f = grads_b.reshape(group * length, d)
        shared_g = jnp.dot(tokens_f, w_gate[EXPERTS], preferred_element_type=f32)
        shared_u = jnp.dot(tokens_f, w_up[EXPERTS], preferred_element_type=f32)
        value, slope = silu_parts(shared_g)
        shared_hidden = (value * shared_u).astype(bf16)
        shared_q = jnp.dot(grads_f, w_down[EXPERTS], preferred_element_type=f32)
        shared_gd = (shared_q * shared_u * slope).astype(bf16)
        shared_ud = (shared_q * value).astype(bf16)
        shared_grads = jnp.stack(
            [
                dot("ld,lh->dh", tokens_f, shared_gd),
                dot("ld,lh->dh", tokens_f, shared_ud),
                dot("ld,lh->dh", grads_f, shared_hidden),
            ]
        )
        out_partial = dot("lh,dh->ld", shared_hidden, w_down[EXPERTS])
        two_partial = dot("lh,dh->ld", shared_gd, w_gate[EXPERTS]) + dot(
            "lh,dh->ld", shared_ud, w_up[EXPERTS]
        )
        out_partial = out_partial.reshape(group, length, d)
        two_partial = two_partial.reshape(group, length, d)
        shared_done = reduce_and_return(shared_grads)

        pick_parts = []
        expert_done = []
        for part in GROUPS:
            lo, hi = part[0], part[-1] + 1
            hot = onehot_b[:, lo:hi]
            x_in = jnp.einsum("bect,btd->ebcd", hot, tokens_b, preferred_element_type=bf16)
            g_in = jnp.einsum("bect,btd->ebcd", hot, grads_b, preferred_element_type=bf16)
            gate_e = jnp.swapaxes(gate_b[:, lo:hi], 0, 1)
            wg, wu, wd = w_gate[lo:hi], w_up[lo:hi], w_down[lo:hi]
            gate_act = dot("ebcd,edh->ebch", x_in, wg)
            up_act = dot("ebcd,edh->ebch", x_in, wu)
            value, slope = silu_parts(gate_act)
            hid = (value * up_act).astype(bf16)
            e_out = dot("ebch,edh->ebcd", hid, wd)
            pick_parts.append(jnp.sum(e_out * g_in.astype(f32), axis=-1))
            slot_grad = (gate_e * g_in.astype(f32)).astype(bf16)
            hid_grad = dot("ebcd,edh->ebch", slot_grad, wd)
            gate_d = (hid_grad * up_act * slope).astype(bf16)
            up_d = (hid_grad * value).astype(bf16)
            in_grad = dot("ebch,edh->ebcd", gate_d, wg) + dot("ebch,edh->ebcd", up_d, wu)
            weighted = (gate_e * e_out).astype(bf16)
            out_partial = out_partial + dot("bect,ebcd->btd", hot, weighted)
            two_partial = two_partial + dot("bect,ebcd->btd", hot, in_grad.astype(bf16))
            stack = jnp.concatenate(
                [
                    dot("ebcd,ebch->edh", x_in, gate_d),
                    dot("ebcd,ebch->edh", x_in, up_d),
                    dot("ebcd,ebch->edh", slot_grad, hid),
                ]
            )
            expert_done.append(reduce_and_return(stack))

        two_grad = plane_sum(two_partial)
        picks = jnp.concatenate(pick_parts, axis=0)
        picks = jnp.swapaxes(picks, 0, 1).reshape(group, slot_total)
        picks = picks[:n] + swap(picks[n:], "core", 1, 2)
        pick_slot = picks[0]
        for m in range(1, n):
            pick_slot = pick_slot + swap(picks[m], "shard", m, n)
        mixed = plane_sum(out_partial)
        output = (middle + mixed).astype(bf16)

        upstream = cotangent[0].astype(f32)
        pick_grad = jnp.sum(
            jnp.where(hit, pick_slot[:, None], 0.0).reshape(EXPERTS, CAP, length), axis=1
        ).T
        logit_grad = router * (pick_grad - jnp.sum(router * pick_grad, axis=1, keepdims=True))
        two_grad = two_grad + jnp.dot(logit_grad, wr.astype(f32).T, precision=highest)
        router_grad = jnp.dot(normed_two.astype(f32).T, logit_grad, precision=highest)
        middle_part, ffn_gain_grad = norm_back(middle, factor_two, gain_two, two_grad)
        middle_grad = middle_part + upstream

        branch_grad = middle_grad.astype(bf16)
        output_weight_grad = dot("ld,le->de", attended, branch_grad)
        attended_grad = (
            dot("le,de->ld", branch_grad, wo).astype(bf16).reshape(length, NH, HD)
        )
        prob_grad = dot("qhd,khd->hqk", attended_grad, values)
        row_inner = jnp.sum(soft * prob_grad, axis=-1, keepdims=True)
        score_grad = (soft * (prob_grad - row_inner)).astype(bf16)
        query_parts = dot("hqk,khd->qhd", score_grad, keys_rot) * score_scale
        key_parts = dot("hqk,qhd->khd", score_grad, queries) * score_scale
        value_parts = dot("hqk,qhd->khd", probs, attended_grad)
        query_pre = query_parts * cos_b + rotate_back(query_parts * sin_b)
        key_pre = key_parts * cos_b + rotate_back(key_parts * sin_b)
        joint_grad = jnp.concatenate(
            [v.reshape(length, d) for v in (query_pre, key_pre, value_parts)], axis=1
        ).astype(bf16)
        one_grad = dot("lf,df->ld", joint_grad, wqkv)
        joint_weight_grad = dot("ld,lf->df", normed_one, joint_grad)
        input_part, attn_gain_grad = norm_back(inputs, factor_one, gain_one, one_grad)
        input_grad = (middle_grad + input_part).astype(bf16)

        small_grad = jnp.concatenate(
            [attn_gain_grad[:, None], ffn_gain_grad[:, None], router_grad], axis=1
        )
        small_grad = jnp.pad(small_grad, ((0, 0), (0, 256 - small_grad.shape[1])))
        total = jnp.concatenate([joint_weight_grad, output_weight_grad, small_grad], axis=1)
        keep = lax.dynamic_slice_in_dim(total, c * half, half, 1)
        send = lax.dynamic_slice_in_dim(total, (1 - c) * half, half, 1).astype(bf16)
        total = keep + swap(send, "core", 1, 2).astype(f32)
        total = total.reshape(n, rows, half)
        own = pick_index(total, s)
        low = total.astype(bf16)
        for m in range(1, n):
            own = own + swap(pick_index(low, s ^ m), "shard", m, n).astype(f32)
        x = own.reshape((2,) * bits + (rows // qn, half))
        for b in range(bits):
            axis = bits - 1 - b
            bit = (q >> b) & 1
            keep = pick_index(x, bit, axis)
            send = pick_index(x, 1 - bit, axis).astype(bf16)
            x = keep + swap(send, "plane", 1 << b, qn).astype(f32)
        x = x.astype(bf16)[None]
        for b in reversed(range(bits)):
            bit = (q >> b) & 1
            other = swap(x, "plane", 1 << b, qn)
            pair = jnp.stack(
                [jnp.where(bit == 0, x, other), jnp.where(bit == 0, other, x)], axis=1
            )
            x = pair.reshape((2 * x.shape[0],) + x.shape[1:])
        x = x.reshape(rows, half)
        x = join_bit(c, x, swap(x, "core", 1, 2), 1).astype(f32)
        stacks = [[], [], []]
        for part, done in zip(GROUPS, expert_done):
            for k in range(3):
                stacks[k].append(done[k * len(part) : (k + 1) * len(part)])
        expert_grads = [jnp.concatenate(parts, axis=0) for parts in stacks]
        return (
            output[None],
            input_grad[None],
            x[:, 4 * d],
            x[:, :d],
            x[:, d : 2 * d],
            x[:, 2 * d : 3 * d],
            x[:, 3 * d : 4 * d],
            x[:, 4 * d + 1],
            x[:, 4 * d + 2 : 4 * d + 2 + EXPERTS],
            expert_grads[0],
            expert_grads[1],
            expert_grads[2],
            shared_done[0],
            shared_done[1],
            shared_done[2],
        )

    return shards


def make_fast(n, qn):
    def shards(
        tokens,
        cotangent,
        segments,
        padding,
        routes,
        priority,
        attn_gain,
        query_weight,
        key_weight,
        value_weight,
        output_weight,
        ffn_gain,
        router_weight,
        expert_gate,
        expert_up,
        expert_down,
        shared_gate,
        shared_up,
        shared_down,
    ):
        s = lax.axis_index("shard")
        c = lax.axis_index("core")
        length, d = tokens.shape[1], tokens.shape[2]
        where = jnp.stack([s, c]).astype(jnp.int32)

        meta = jnp.concatenate(
            [segments, padding, routes[0].T, priority, jnp.zeros((3, length), jnp.int32)], axis=0
        )
        cosine, sine = rotary_tables(length, HD)
        cos_pair = jnp.concatenate([cosine, cosine], axis=1)
        sin_pair = jnp.concatenate([sine, sine], axis=1)
        small = jnp.concatenate([attn_gain[:, None], ffn_gain[:, None], router_weight], axis=1)
        small = jnp.pad(small, ((0, 0), (0, 128 - small.shape[1])))

        near, far, near_z, far_z, *_, output, input_grad = layer_call(
            n,
            (
                tokens[0],
                meta,
                cos_pair,
                sin_pair,
                tokens[0],
                cotangent[0],
                small,
                query_weight,
                key_weight,
                value_weight,
                output_weight,
                expert_gate,
                expert_up,
                expert_down,
                shared_gate,
                shared_up,
                shared_down,
            ),
        )
        done = finish(n, where, near, far, near_z, far_z)
        tail = done[10]
        return (
            output[None],
            input_grad[None],
            tail[:, 0],
            *done[6:10],
            tail[:, 1],
            tail[:, 2 : 2 + EXPERTS],
            *done[:3],
            *(v[0] for v in done[3:6]),
        )

    return shards


def make_shards(n, qn):
    plain, fast = make_plain(n, qn), make_fast(n, qn)

    def shards(*arguments):
        d, hidden = arguments[0].shape[2], arguments[13].shape[2]
        fits = n == 4 and qn == 4 and d == 768 and hidden == 2048 and arguments[0].shape[1] == 256
        return (fast if fits else plain)(*arguments)

    return shards


def solution(mesh):
    n, replicas = mesh.shape["shard"], mesh.shape["replica"]
    fine = Mesh(mesh.devices.reshape(n, replicas // 2, 2), ("shard", "plane", "core"))
    every = ("shard", "plane", "core")
    in_specs = (
        P(every, None, None),
        P(every, None, None),
        P(every, None),
        P(every, None),
        P(every, None, None),
        P(every, None),
        P("shard"),
        P("shard", None),
        P("shard", None),
        P("shard", None),
        P("shard", None),
        P("shard"),
        P("shard", None),
        P(None, "shard", None),
        P(None, "shard", None),
        P(None, "shard", None),
        P("shard", None),
        P("shard", None),
        P("shard", None),
    )
    out_specs = (
        P(every, None, None),
        P(every, None, None),
        P("shard"),
        P("shard", None),
        P("shard", None),
        P("shard", None),
        P("shard", None),
        P("shard"),
        P("shard", None),
        P(None, "shard", None),
        P(None, "shard", None),
        P(None, "shard", None),
        P("shard", None),
        P("shard", None),
        P("shard", None),
    )
    return jax.shard_map(
        make_shards(n, replicas // 2),
        mesh=fine,
        in_specs=in_specs,
        out_specs=out_specs,
        check_vma=False,
    )
```
